32 devices in a mesh: data: 32 (over z, y, x, core).
Axes of the slice: x: 2, y: 2, z: 4, core: 2. Of those that a mesh axis runs over, the one named last changes fastest.
Arguments:
- feat_a: bfloat16 [16384, 2048], P('data')
- feat_b: bfloat16 [16384, 2048], P('data')
- w_in: bfloat16 [2048, 2048], replicated
- w_mid: bfloat16 [2048, 2048], replicated
- w_out: bfloat16 [2048, 2048], replicated
- t_in: bfloat16 [2048, 2048], replicated
- t_mid: bfloat16 [2048, 2048], replicated
- t_out: bfloat16 [2048, 2048], replicated
- gain_1: float32 [2048], replicated
- bias_1: float32 [2048], replicated
- gain_2: float32 [2048], replicated
- bias_2: float32 [2048], replicated
- off_weight: float32 [], replicated
Outputs:
- output 1: float32 [], replicated
- output 2: float32 [16384, 2048], P('data')
- output 3: float32 [2048, 2048], replicated
- output 4: float32 [2048, 2048], replicated
- output 5: float32 [2048, 2048], replicated
- output 6: float32 [2048], replicated
- output 7: float32 [2048], replicated
- output 8: float32 [2048], replicated
- output 9: float32 [2048], replicated
All inputs are finite; a program needn't handle non-finite values.
Results may differ from the reference program's by a relative error of at most 0.00413.
Values are sent between devices in bfloat16 or wider.
A program may use at most 1 GiB of HBM per device.

```python
import jax
import jax.numpy as jnp
from jax import lax

FEAT_DIM = 2048
PROJ_DIM = 2048
ROWS_DEV = 512
SHARDS = 32
ROWS = ROWS_DEV * SHARDS
NORM_EPS = 1e-5


def setup_inputs(seed: int = 0) -> dict:
    key_list = jax.random.split(jax.random.key(seed), 16)
    row_shape = (SHARDS, ROWS_DEV, FEAT_DIM)
    base_draw = jax.random.normal(key_list[0], row_shape, jnp.float32)
    view_noise = jax.random.normal(key_list[1], row_shape, jnp.float32)
    shard_shift = 0.5 * jax.random.normal(key_list[2], (SHARDS, 1, FEAT_DIM), jnp.float32)
    shard_scale = jax.random.uniform(key_list[3], (SHARDS, 1, FEAT_DIM), jnp.float32, 0.6, 1.4)
    feat_a = (base_draw * shard_scale + shard_shift).reshape(ROWS, FEAT_DIM)
    feat_b = ((0.8 * base_draw + 0.6 * view_noise) * shard_scale + shard_shift).reshape(ROWS, FEAT_DIM)
    in_scale = FEAT_DIM ** -0.5
    hid_scale = PROJ_DIM ** -0.5
    in_shape = (FEAT_DIM, PROJ_DIM)
    hid_shape = (PROJ_DIM, PROJ_DIM)
    w_in = in_scale * jax.random.normal(key_list[4], in_shape, jnp.float32)
    w_mid = hid_scale * jax.random.normal(key_list[5], hid_shape, jnp.float32)
    w_out = hid_scale * jax.random.normal(key_list[6], hid_shape, jnp.float32)
    t_in = 0.8 * w_in + 0.6 * in_scale * jax.random.normal(key_list[7], in_shape, jnp.float32)
    t_mid = 0.8 * w_mid + 0.6 * hid_scale * jax.random.normal(key_list[8], hid_shape, jnp.float32)
    t_out = 0.8 * w_out + 0.6 * hid_scale * jax.random.normal(key_list[9], hid_shape, jnp.float32)
    gain_1 = jax.random.uniform(key_list[10], (PROJ_DIM,), jnp.float32, 0.5, 1.5)
    bias_1 = 0.3 * jax.random.normal(key_list[11], (PROJ_DIM,), jnp.float32)
    gain_2 = jax.random.uniform(key_list[12], (PROJ_DIM,), jnp.float32, 0.5, 1.5)
    bias_2 = 0.3 * jax.random.normal(key_list[13], (PROJ_DIM,), jnp.float32)
    off_weight = (ROWS / PROJ_DIM) * jax.random.uniform(key_list[14], (), jnp.float32, 0.1, 0.3)
    return {
        "feat_a": feat_a.astype(jnp.bfloat16),
        "feat_b": feat_b.astype(jnp.bfloat16),
        "w_in": w_in.astype(jnp.bfloat16),
        "w_mid": w_mid.astype(jnp.bfloat16),
        "w_out": w_out.astype(jnp.bfloat16),
        "t_in": t_in.astype(jnp.bfloat16),
        "t_mid": t_mid.astype(jnp.bfloat16),
        "t_out": t_out.astype(jnp.bfloat16),
        "gain_1": gain_1,
        "bias_1": bias_1,
        "gain_2": gain_2,
        "bias_2": bias_2,
        "off_weight": off_weight,
    }


def batch_norm(pre_norm):
    mean_u = jnp.mean(pre_norm, axis=0)
    centered = pre_norm - mean_u
    inv_std = lax.rsqrt(jnp.mean(centered * centered, axis=0) + NORM_EPS)
    return centered * inv_std, inv_std


def hidden_layer(layer_in, weight, gain_vec, bias_vec):
    normed, inv_std = batch_norm(jnp.dot(layer_in, weight, preferred_element_type=jnp.float32))
    pre_act = normed * gain_vec + bias_vec
    return jnp.maximum(pre_act, 0.0).astype(jnp.bfloat16), normed, inv_std, pre_act > 0.0


def norm_back(grad_n, normed, inv_std):
    mean_g = jnp.mean(grad_n, axis=0)
    mean_gn = jnp.mean(grad_n * normed, axis=0)
    return (grad_n - mean_g - normed * mean_gn) * inv_std


def reference(feat_a, feat_b, w_in, w_mid, w_out, t_in, t_mid, t_out, gain_1, bias_1, gain_2, bias_2, off_weight):
    row_count = feat_a.shape[0]
    act_1, normed_1, inv_1, mask_1 = hidden_layer(feat_a, w_in, gain_1, bias_1)
    act_2, normed_2, inv_2, mask_2 = hidden_layer(act_1, w_mid, gain_2, bias_2)
    zh_a, inv_z = batch_norm(jnp.dot(act_2, w_out, preferred_element_type=jnp.float32))
    teach_1 = hidden_layer(feat_b, t_in, gain_1, bias_1)[0]
    teach_2 = hidden_layer(teach_1, t_mid, gain_2, bias_2)[0]
    zh_b = batch_norm(jnp.dot(teach_2, t_out, preferred_element_type=jnp.float32))[0]
    emb_a = zh_a.astype(jnp.bfloat16)
    emb_b = zh_b.astype(jnp.bfloat16)
    corr_mat = jnp.dot(emb_a.T, emb_b, preferred_element_type=jnp.float32) / row_count
    proj_width = corr_mat.shape[0]
    on_diag = jnp.arange(proj_width)[:, None] == jnp.arange(proj_width)[None, :]
    loss_value = jnp.sum(jnp.square(1.0 - jnp.diagonal(corr_mat))) + off_weight * jnp.sum(jnp.square(jnp.where(on_diag, 0.0, corr_mat)))
    grad_c = jnp.where(on_diag, -2.0 * (1.0 - corr_mat), 2.0 * off_weight * corr_mat).astype(jnp.bfloat16)
    grad_emb = jnp.dot(emb_b, grad_c.T, preferred_element_type=jnp.float32) / row_count
    grad_z = norm_back(grad_emb, zh_a, inv_z).astype(jnp.bfloat16)
    grad_w_out = jnp.dot(act_2.T, grad_z, preferred_element_type=jnp.float32)
    grad_pre_2 = jnp.where(mask_2, jnp.dot(grad_z, w_out.T, preferred_element_type=jnp.float32), 0.0)
    grad_gain_2 = jnp.sum(grad_pre_2 * normed_2, axis=0)
    grad_bias_2 = jnp.sum(grad_pre_2, axis=0)
    grad_u_2 = norm_back(grad_pre_2 * gain_2, normed_2, inv_2).astype(jnp.bfloat16)
    grad_w_mid = jnp.dot(act_1.T, grad_u_2, preferred_element_type=jnp.float32)
    grad_pre_1 = jnp.where(mask_1, jnp.dot(grad_u_2, w_mid.T, preferred_element_type=jnp.float32), 0.0)
    grad_gain_1 = jnp.sum(grad_pre_1 * normed_1, axis=0)
    grad_bias_1 = jnp.sum(grad_pre_1, axis=0)
    grad_u_1 = norm_back(grad_pre_1 * gain_1, normed_1, inv_1).astype(jnp.bfloat16)
    grad_w_in = jnp.dot(feat_a.T, grad_u_1, preferred_element_type=jnp.float32)
    return (loss_value, grad_emb, grad_w_in, grad_w_mid, grad_w_out, grad_gain_1, grad_bias_1, grad_gain_2, grad_bias_2)
```

```python
import functools

import jax
import jax.numpy as jnp
from jax import lax
from jax.experimental import pallas as pl
from jax.experimental.pallas import tpu as pltpu
from jax.sharding import PartitionSpec as P

NORM_EPS = 1e-5
DATA_AXIS = "data"
MESH = pl.DeviceIdType.MESH
VMEM_BYTES = 62 * 1024 * 1024
LANES = 128
PLANE = 8
DEPTH = 4
CORE, AXIS_X, AXIS_Y, AXIS_Z0, AXIS_Z1 = 1, 2, 4, 8, 16


def contract_rows(left_op, right_op):
    return lax.dot_general(left_op, right_op, (((0,), (0,)), ((), ())), preferred_element_type=jnp.float32)


def contract_cols(left_op, right_op):
    return lax.dot_general(left_op, right_op, (((1,), (1,)), ((), ())), preferred_element_type=jnp.float32)


def signal_all(sem, peers):
    for peer in peers:
        pl.semaphore_signal(sem, inc=1, device_id=(peer,), device_id_type=MESH)


def small_sum_kernel(x_ref, o_ref, plane_buf, depth_buf, own_buf, s1, r1, s2, r2, s3, r3):
    me = lax.axis_index(DATA_AXIS)
    pos, plane = me % PLANE, me // PLANE
    mates = [(pos + d) % PLANE for d in range(1, PLANE)]
    levels = [(plane + d) % DEPTH for d in range(1, DEPTH)]
    peers = [plane * PLANE + m for m in mates] + [lv * PLANE + pos for lv in levels]
    barrier = pltpu.get_barrier_semaphore()
    signal_all(barrier, peers)
    pl.semaphore_wait(barrier, len(peers))

    def plane_copy(src, dst, send, recv, mate):
        return pltpu.make_async_remote_copy(src, dst, send, recv, device_id=(plane * PLANE + mate,), device_id_type=MESH)

    out1 = [plane_copy(x_ref.at[m], plane_buf.at[pos], s1.at[m], r1.at[pos], m) for m in mates]
    for c in out1:
        c.start()
    plane_buf[pos] = x_ref[pos]
    for m in mates:
        plane_copy(x_ref.at[m], plane_buf.at[m], s1.at[m], r1.at[m], m).wait_recv()
    total = plane_buf[0]
    for i in range(1, PLANE):
        total = total + plane_buf[i]
    own_buf[0] = total
    depth_buf[plane] = total

    def depth_copy(slot, level):
        return pltpu.make_async_remote_copy(
            own_buf.at[0], depth_buf.at[slot], s2.at[level], r2.at[slot], device_id=(level * PLANE + pos,), device_id_type=MESH
        )

    out2 = [depth_copy(plane, lv) for lv in levels]
    for c in out2:
        c.start()
    for lv in levels:
        depth_copy(lv, lv).wait_recv()
    total = depth_buf[0]
    for i in range(1, DEPTH):
        total = total + depth_buf[i]
    own_buf[1] = total
    o_ref[pos] = total
    out3 = [plane_copy(own_buf.at[1], o_ref.at[pos], s3.at[m], r3.at[pos], m) for m in mates]
    for c in out3:
        c.start()
    for m in mates:
        plane_copy(own_buf.at[1], o_ref.at[m], s3.at[m], r3.at[m], m).wait_recv()
    for c in out1 + out2 + out3:
        c.wait_send()


def small_sum(rows):
    count, width = rows.shape
    tile = (PLANE, PLANE, LANES)
    size = PLANE * PLANE * LANES
    flat = jnp.pad(rows.reshape(-1), (0, size - count * width)).reshape(tile)
    total = pl.pallas_call(
        small_sum_kernel,
        name="small_sum",
        out_shape=jax.ShapeDtypeStruct(tile, jnp.float32),
        in_specs=[pl.BlockSpec(memory_space=pltpu.VMEM)],
        out_specs=pl.BlockSpec(memory_space=pltpu.VMEM),
        scratch_shapes=[
            pltpu.VMEM(tile, jnp.float32),
            pltpu.VMEM((DEPTH, PLANE, LANES), jnp.float32),
            pltpu.VMEM((2, PLANE, LANES), jnp.float32),
        ]
        + [pltpu.SemaphoreType.DMA((n,)) for n in (PLANE, PLANE, DEPTH, DEPTH, PLANE, PLANE)],
        compiler_params=pltpu.CompilerParams(collective_id=0, has_side_effects=True),
    )(flat)
    return total.reshape(-1)[: count * width].reshape(count, width)


LAGS = (0, 1, 3, 5, 6, 7, 8, 9, 11, 13)
ORDER = (0, 1, 5, 4, 6, 3, 7, 2, 8, 9)


def large_sum_kernel(mats, chunks, z_first, finish, *refs):
    ins, refs = refs[:mats], refs[mats:]
    extra, refs = refs[: finish.inputs], refs[finish.inputs :]
    outs, refs = refs[:mats], refs[mats:]
    extra_out, refs = refs[: finish.outputs], refs[finish.outputs :]
    acc, half, rx, ry, rz, rl, gathered, load_sem, store_sem, send, recv = refs
    if not finish.narrow:
        gathered = half
    chunk_rows = ins[0].shape[0] // chunks
    half_rows = chunk_rows // 2
    me = lax.axis_index(DATA_AXIS)
    core, bx, by, bz0, bz1 = me % 2, (me // 2) % 2, (me // 4) % 2, (me // 8) % 2, (me // 16) % 2

    barrier = pltpu.get_barrier_semaphore()
    mates = [me + s * (1 - 2 * b) for s, b in ((1, core), (2, bx), (4, by), (8, bz0), (16, bz1))]
    signal_all(barrier, mates)
    pl.semaphore_wait(barrier, len(mates))

    xy = ((2 + 2 * core, core * by + (1 - core) * bx), (4 - 2 * core, core * bx + (1 - core) * by))
    zz = ((8, bz0), (16, bz1))

    def steps_of(k):
        part = k % chunks
        zf = 0
        for z in z_first:
            same = part - z
            zf = zf + (1 - lax.min(same * same, 1))
        pairs = []
        for a, b in zip(xy + zz, zz + xy):
            stride = zf * b[0] + (1 - zf) * a[0]
            bit = zf * b[1] + (1 - zf) * a[1]
            pairs.append((me + stride * (1 - 2 * bit), bit))
        return pairs

    def offsets(pairs):
        offs, size = [0], half_rows
        for _, bit in pairs[:3]:
            size = size // 2
            offs.append(offs[-1] + bit * size)
        return offs

    def rows(off, size):
        return pl.ds(pl.multiple_of(off, size), size)

    def remote(src, dst, stage, k, mate):
        return pltpu.make_async_remote_copy(src, dst, send.at[stage, k], recv.at[stage, k], device_id=(mate,), device_id_type=MESH)

    def mat_row(k, side):
        return pl.multiple_of((k % chunks) * chunk_rows + side * half_rows, half_rows)

    other_core = mates[0]

    def first_copy(w, k):
        return remote(ins[w].at[pl.ds(mat_row(k, 1 - core), half_rows)], half.at[k], 0, k, other_core)

    def load_copy(w, k):
        return pltpu.make_async_copy(ins[w].at[pl.ds(mat_row(k, core), half_rows)], acc.at[k], load_sem.at[k])

    def last_copy(w, k, side):
        return remote(gathered.at[k], outs[w].at[pl.ds(mat_row(k, side), half_rows)], 8, k, other_core)

    def store_copy(w, k):
        return pltpu.make_async_copy(gathered.at[k], outs[w].at[pl.ds(mat_row(k, core), half_rows)], store_sem.at[k])

    landing = (rx, ry, rz, rl)

    def reduce_copy(i, k, pairs, offs):
        size = half_rows >> (i + 1)
        if i == 3:
            size = half_rows >> 3
            off = offs[3]
        else:
            off = offs[i] + (1 - pairs[i][1]) * size
        return remote(acc.at[k, rows(off, size)], landing[i].at[k], 1 + i, k, pairs[i][0])

    def gather_copy(i, k, pairs, offs):
        size = half_rows >> (i + 1)
        block = gathered.at[k, rows(offs[i + 1], size)]
        return remote(block, block, 7 - i, k, pairs[i][0])

    def add_rows(dst, k, off, size, buf):
        step = min(size, 16)

        def body(i, carry):
            at = pl.ds(pl.multiple_of(off + i * step, step), step)
            dst[k, at] = acc[k, at] + buf[k, pl.ds(pl.multiple_of(i * step, step), step)]
            return carry

        lax.fori_loop(0, size // step, body, 0)

    def for_mat(k, what):
        for w in range(mats):
            pl.when(k // chunks == w)(functools.partial(what, w))

    def stage(i, k):
        pairs = steps_of(k)
        offs = offsets(pairs)
        if i == 0:

            def begin(w):
                first_copy(w, k).start()
                load_copy(w, k).start()

            for_mat(k, begin)
        elif i == 1:

            def arrive(w):
                load_copy(w, k).wait()
                first_copy(w, k).wait_recv()

            for_mat(k, arrive)
            add_rows(acc, k, 0, half_rows, half)
            reduce_copy(0, k, pairs, offs).start()
        elif i < 5:
            reduce_copy(i - 2, k, pairs, offs).wait_recv()
            add_rows(acc, k, offs[i - 1], half_rows >> (i - 1), landing[i - 2])
            reduce_copy(i - 1, k, pairs, offs).start()
        elif i == 5:
            reduce_copy(3, k, pairs, offs).wait_recv()
            if finish.narrow:
                row = mat_row(k, core) + offs[3]
                finish.apply(extra, extra_out, acc, rl, gathered, k, offs[3], half_rows >> 3, row)
            else:
                add_rows(gathered, k, offs[3], half_rows >> 3, rl)
            gather_copy(2, k, pairs, offs).start()
        elif i < 8:
            gather_copy(8 - i, k, pairs, offs).wait_recv()
            gather_copy(7 - i, k, pairs, offs).start()
        elif i == 8:
            gather_copy(0, k, pairs, offs).wait_recv()

            def emit(w):
                last_copy(w, k, core).start()
                store_copy(w, k).start()

            for_mat(k, emit)
        else:

            def close(w):
                last_copy(w, k, 1 - core).wait_recv()
                store_copy(w, k).wait()
                last_copy(w, k, core).wait_send()
                first_copy(w, k).wait_send()

            for_mat(k, close)
            for n in range(4):
                reduce_copy(n, k, pairs, offs).wait_send()
            for n in range(3):
                gather_copy(n, k, pairs, offs).wait_send()

    if finish.narrow:
        finish.begin(extra_out)
    count = mats * chunks

    def slot(t, carry):
        for i in ORDER:
            k = t - LAGS[i]

            @pl.when((k >= 0) & (k < count))
            def _():
                stage(i, k)

        return carry

    lax.fori_loop(0, count + LAGS[-1], slot, 0)


class PlainFinish:
    narrow = False
    inputs = 0
    outputs = 0
    out_dtype = jnp.float32


class CorrFinish:
    narrow = True
    inputs = 1
    outputs = 1
    out_dtype = jnp.bfloat16

    def __init__(self, row_count):
        self.row_count = row_count

    def begin(self, extra_out):
        extra_out[0][...] = jnp.zeros_like(extra_out[0])

    def apply(self, extra, extra_out, acc, rl, gathered, k, off, size, row):
        width = acc.shape[-1]
        at = pl.ds(pl.multiple_of(off, size), size)
        corr = (acc[k, at] + rl[k]) / self.row_count
        diag = (row + lax.broadcasted_iota(jnp.int32, (size, width), 0)) == lax.broadcasted_iota(jnp.int32, (size, width), 1)
        off_weight = extra[0][0]
        miss = 1.0 - corr
        terms = jnp.where(diag, miss * miss, off_weight * (corr * corr))
        extra_out[0][...] += jnp.sum(terms, axis=0, keepdims=True)
        gathered[k, at] = jnp.where(diag, -2.0 * miss, 2.0 * off_weight * corr).astype(jnp.bfloat16)


def large_sum(arrays, chunks, z_first, finish, extra, collective_id):
    mats = len(arrays)
    n_rows, width = arrays[0].shape
    half_rows = n_rows // chunks // 2
    count = mats * chunks
    any_spec = pl.BlockSpec(memory_space=pl.ANY)
    out_shape = [jax.ShapeDtypeStruct((n_rows, width), finish.out_dtype) for _ in arrays]
    out_specs = [any_spec] * mats
    if finish.outputs:
        out_shape.append(jax.ShapeDtypeStruct((1, width), jnp.float32))
        out_specs.append(pl.BlockSpec(memory_space=pltpu.VMEM))

    def buf(rows, dtype=jnp.float32):
        return pltpu.VMEM((count, rows, width), dtype)

    narrow_buf = buf(half_rows, finish.out_dtype) if finish.narrow else pltpu.VMEM((8, LANES), jnp.float32)
    return pl.pallas_call(
        functools.partial(large_sum_kernel, mats, chunks, z_first, finish),
        name="large_sum",
        out_shape=out_shape,
        in_specs=[any_spec] * mats + [pl.BlockSpec(memory_space=pltpu.SMEM)] * len(extra),
        out_specs=out_specs,
        scratch_shapes=[
            buf(half_rows),
            buf(half_rows),
            buf(half_rows // 2),
            buf(half_rows // 4),
            buf(half_rows // 8),
            buf(half_rows // 8),
            narrow_buf,
            pltpu.SemaphoreType.DMA((count,)),
            pltpu.SemaphoreType.DMA((count,)),
            pltpu.SemaphoreType.DMA((9, count)),
            pltpu.SemaphoreType.DMA((9, count)),
        ],
        compiler_params=pltpu.CompilerParams(collective_id=collective_id, has_side_effects=True, vmem_limit_bytes=VMEM_BYTES),
    )(*arrays, *extra)


def solution(mesh):
    shards = mesh.shape[DATA_AXIS]
    row_part = P(DATA_AXIS, None)
    replicated = P()

    def local_step(feat_a, feat_b, w_in, w_mid, w_out, t_in, t_mid, t_out, gain_1, bias_1, gain_2, bias_2, off_weight):
        row_count = feat_a.shape[0] * shards

        def norm_pair(pre_a, pre_b):
            stat_sums = jnp.stack([jnp.sum(pre_a, axis=0), jnp.sum(pre_a * pre_a, axis=0), jnp.sum(pre_b, axis=0), jnp.sum(pre_b * pre_b, axis=0)])
            stat_means = small_sum(stat_sums) / row_count
            inv_a = lax.rsqrt(stat_means[1] - stat_means[0] * stat_means[0] + NORM_EPS)
            inv_b = lax.rsqrt(stat_means[3] - stat_means[2] * stat_means[2] + NORM_EPS)
            return (pre_a - stat_means[0]) * inv_a, inv_a, (pre_b - stat_means[2]) * inv_b

        def hidden_pair(in_a, in_b, weight_a, weight_b, gain_vec, bias_vec):
            normed_a, inv_a, normed_b = norm_pair(jnp.dot(in_a, weight_a, preferred_element_type=jnp.float32), jnp.dot(in_b, weight_b, preferred_element_type=jnp.float32))
            pre_act = normed_a * gain_vec + bias_vec
            act_a = jnp.maximum(pre_act, 0.0).astype(jnp.bfloat16)
            act_b = jnp.maximum(normed_b * gain_vec + bias_vec, 0.0).astype(jnp.bfloat16)
            return act_a, act_b, normed_a, inv_a, pre_act > 0.0

        def affine_back(grad_pre, normed, inv_std, gain_vec):
            stat_sums = small_sum(jnp.stack([jnp.sum(grad_pre * normed, axis=0), jnp.sum(grad_pre, axis=0)]))
            grad_u = (grad_pre - stat_sums[1] / row_count - normed * (stat_sums[0] / row_count)) * (gain_vec * inv_std)
            return grad_u.astype(jnp.bfloat16), stat_sums[0], stat_sums[1]

        act_1, teach_1, normed_1, inv_1, mask_1 = hidden_pair(feat_a, feat_b, w_in, t_in, gain_1, bias_1)
        act_2, teach_2, normed_2, inv_2, mask_2 = hidden_pair(act_1, teach_1, w_mid, t_mid, gain_2, bias_2)
        zh_a, inv_z, zh_b = norm_pair(jnp.dot(act_2, w_out, preferred_element_type=jnp.float32), jnp.dot(teach_2, t_out, preferred_element_type=jnp.float32))
        emb_a = zh_a.astype(jnp.bfloat16)
        emb_b = zh_b.astype(jnp.bfloat16)
        corr_part = contract_rows(emb_a, emb_b)
        grad_c, loss_cols = large_sum([corr_part], 8, (3, 7), CorrFinish(row_count), [off_weight.reshape(1)], 1)
        grad_emb = contract_cols(emb_b, grad_c) / row_count
        loss_row = jnp.sum(loss_cols, axis=0)
        stat_sums = small_sum(jnp.stack([jnp.sum(grad_emb, axis=0), jnp.sum(grad_emb * zh_a, axis=0), loss_row]))
        loss_value = jnp.sum(stat_sums[2]) * 0.5
        grad_z = ((grad_emb - stat_sums[0] / row_count - zh_a * (stat_sums[1] / row_count)) * inv_z).astype(jnp.bfloat16)
        grad_w_out = lax.psum(contract_rows(act_2, grad_z), DATA_AXIS)
        grad_pre_2 = jnp.where(mask_2, contract_cols(grad_z, w_out), 0.0)
        grad_u_2, grad_gain_2, grad_bias_2 = affine_back(grad_pre_2, normed_2, inv_2, gain_2)
        part_mid = contract_rows(act_1, grad_u_2)
        grad_pre_1 = jnp.where(mask_1, contract_cols(grad_u_2, w_mid), 0.0)
        grad_u_1, grad_gain_1, grad_bias_1 = affine_back(grad_pre_1, normed_1, inv_1, gain_1)
        part_in = contract_rows(feat_a, grad_u_1)
        grad_w_mid, grad_w_in = large_sum([part_mid, part_in], 8, (3, 7), PlainFinish, [], 2)
        return (loss_value, grad_emb, grad_w_in, grad_w_mid, grad_w_out, grad_gain_1, grad_bias_1, grad_gain_2, grad_bias_2)

    return jax.shard_map(local_step, mesh=mesh, in_specs=(row_part, row_part) + (replicated,) * 11, out_specs=(replicated, row_part) + (replicated,) * 7, check_vma=False)
```

```python
import functools

import jax
import jax.numpy as jnp
from jax import lax
from jax.experimental import pallas as pl
from jax.experimental.pallas import tpu as pltpu
from jax.sharding import PartitionSpec as P

NORM_EPS = 1e-5
DATA_AXIS = "data"
MESH = pl.DeviceIdType.MESH
VMEM_BYTES = 62 * 1024 * 1024
LANES = 128
PLANE = 8
DEPTH = 4
CORE, AXIS_X, AXIS_Y, AXIS_Z0, AXIS_Z1 = 1, 2, 4, 8, 16


def contract_rows(left_op, right_op):
    return lax.dot_general(left_op, right_op, (((0,), (0,)), ((), ())), preferred_element_type=jnp.float32)


def contract_cols(left_op, right_op):
    return lax.dot_general(left_op, right_op, (((1,), (1,)), ((), ())), preferred_element_type=jnp.float32)


def signal_all(sem, peers):
    for peer in peers:
        pl.semaphore_signal(sem, inc=1, device_id=(peer,), device_id_type=MESH)


def small_sum_kernel(x_ref, o_ref, plane_buf, depth_buf, own_buf, s1, r1, s2, r2, s3, r3):
    me = lax.axis_index(DATA_AXIS)
    pos, plane = me % PLANE, me // PLANE
    mates = [(pos + d) % PLANE for d in range(1, PLANE)]
    levels = [(plane + d) % DEPTH for d in range(1, DEPTH)]
    peers = [plane * PLANE + m for m in mates] + [lv * PLANE + pos for lv in levels]
    barrier = pltpu.get_barrier_semaphore()
    signal_all(barrier, peers)
    pl.semaphore_wait(barrier, len(peers))

    def plane_copy(src, dst, send, recv, mate):
        return pltpu.make_async_remote_copy(src, dst, send, recv, device_id=(plane * PLANE + mate,), device_id_type=MESH)

    out1 = [plane_copy(x_ref.at[m], plane_buf.at[pos], s1.at[m], r1.at[pos], m) for m in mates]
    for c in out1:
        c.start()
    plane_buf[pos] = x_ref[pos]
    for m in mates:
        plane_copy(x_ref.at[m], plane_buf.at[m], s1.at[m], r1.at[m], m).wait_recv()
    total = plane_buf[0]
    for i in range(1, PLANE):
        total = total + plane_buf[i]
    own_buf[0] = total
    depth_buf[plane] = total

    def depth_copy(slot, level):
        return pltpu.make_async_remote_copy(
            own_buf.at[0], depth_buf.at[slot], s2.at[level], r2.at[slot], device_id=(level * PLANE + pos,), device_id_type=MESH
        )

    out2 = [depth_copy(plane, lv) for lv in levels]
    for c in out2:
        c.start()
    for lv in levels:
        depth_copy(lv, lv).wait_recv()
    total = depth_buf[0]
    for i in range(1, DEPTH):
        total = total + depth_buf[i]
    own_buf[1] = total
    o_ref[pos] = total
    out3 = [plane_copy(own_buf.at[1], o_ref.at[pos], s3.at[m], r3.at[pos], m) for m in mates]
    for c in out3:
        c.start()
    for m in mates:
        plane_copy(own_buf.at[1], o_ref.at[m], s3.at[m], r3.at[m], m).wait_recv()
    for c in out1 + out2 + out3:
        c.wait_send()


def small_sum(rows):
    count, width = rows.shape
    tile = (PLANE, PLANE, LANES)
    size = PLANE * PLANE * LANES
    flat = jnp.pad(rows.reshape(-1), (0, size - count * width)).reshape(tile)
    total = pl.pallas_call(
        small_sum_kernel,
        name="small_sum",
        out_shape=jax.ShapeDtypeStruct(tile, jnp.float32),
        in_specs=[pl.BlockSpec(memory_space=pltpu.VMEM)],
        out_specs=pl.BlockSpec(memory_space=pltpu.VMEM),
        scratch_shapes=[
            pltpu.VMEM(tile, jnp.float32),
            pltpu.VMEM((DEPTH, PLANE, LANES), jnp.float32),
            pltpu.VMEM((2, PLANE, LANES), jnp.float32),
        ]
        + [pltpu.SemaphoreType.DMA((n,)) for n in (PLANE, PLANE, DEPTH, DEPTH, PLANE, PLANE)],
        compiler_params=pltpu.CompilerParams(collective_id=0, has_side_effects=True),
    )(flat)
    return total.reshape(-1)[: count * width].reshape(count, width)


LAGS = (0, 1, 3, 5, 6, 7, 8, 9, 11, 13)
ORDER = (0, 1, 5, 4, 6, 3, 7, 2, 8, 9)


def large_sum_kernel(mats, chunks, z_first, finish, *refs):
    ins, refs = refs[:mats], refs[mats:]
    extra, refs = refs[: finish.inputs], refs[finish.inputs :]
    outs, refs = refs[:mats], refs[mats:]
    extra_out, refs = refs[: finish.outputs], refs[finish.outputs :]
    acc, half, rx, ry, rz, rl, gathered, load_sem, store_sem, send, recv = refs
    if not finish.narrow:
        gathered = half
    chunk_rows = ins[0].shape[0] // chunks
    half_rows = chunk_rows // 2
    me = lax.axis_index(DATA_AXIS)
    core, bx, by, bz0, bz1 = me % 2, (me // 2) % 2, (me // 4) % 2, (me // 8) % 2, (me // 16) % 2

    barrier = pltpu.get_barrier_semaphore()
    mates = [me + s * (1 - 2 * b) for s, b in ((1, core), (2, bx), (4, by), (8, bz0), (16, bz1))]
    signal_all(barrier, mates)
    pl.semaphore_wait(barrier, len(mates))

    xy = ((2 + 2 * core, core * by + (1 - core) * bx), (4 - 2 * core, core * bx + (1 - core) * by))
    zz = ((8, bz0), (16, bz1))

    def steps_of(k):
        part = k % chunks
        zf = 0
        for z in z_first:
            same = part - z
            zf = zf + (1 - lax.min(same * same, 1))
        pairs = []
        for a, b in zip(xy + zz, zz + xy):
            stride = zf * b[0] + (1 - zf) * a[0]
            bit = zf * b[1] + (1 - zf) * a[1]
            pairs.append((me + stride * (1 - 2 * bit), bit))
        return pairs

    def offsets(pairs):
        offs, size = [0], half_rows
        for _, bit in pairs[:3]:
            size = size // 2
            offs.append(offs[-1] + bit * size)
        return offs

    def rows(off, size):
        return pl.ds(pl.multiple_of(off, size), size)

    def remote(src, dst, stage, k, mate):
        return pltpu.make_async_remote_copy(src, dst, send.at[stage, k], recv.at[stage, k], device_id=(mate,), device_id_type=MESH)

    def mat_row(k, side):
        return pl.multiple_of((k % chunks) * chunk_rows + side * half_rows, half_rows)

    other_core = mates[0]

    def first_copy(w, k):
        return remote(ins[w].at[pl.ds(mat_row(k, 1 - core), half_rows)], half.at[k], 0, k, other_core)

    def load_copy(w, k):
        return pltpu.make_async_copy(ins[w].at[pl.ds(mat_row(k, core), half_rows)], acc.at[k], load_sem.at[k])

    def last_copy(w, k, side):
        return remote(gathered.at[k], outs[w].at[pl.ds(mat_row(k, side), half_rows)], 8, k, other_core)

    def store_copy(w, k):
        return pltpu.make_async_copy(gathered.at[k], outs[w].at[pl.ds(mat_row(k, core), half_rows)], store_sem.at[k])

    landing = (rx, ry, rz, rl)

    def reduce_copy(i, k, pairs, offs):
        size = half_rows >> (i + 1)
        if i == 3:
            size = half_rows >> 3
            off = offs[3]
        else:
            off = offs[i] + (1 - pairs[i][1]) * size
        return remote(acc.at[k, rows(off, size)], landing[i].at[k], 1 + i, k, pairs[i][0])

    def gather_copy(i, k, pairs, offs):
        size = half_rows >> (i + 1)
        block = gathered.at[k, rows(offs[i + 1], size)]
        return remote(block, block, 7 - i, k, pairs[i][0])

    def add_rows(dst, k, off, size, buf):
        step = min(size, 16)

        def body(i, carry):
            at = pl.ds(pl.multiple_of(off + i * step, step), step)
            dst[k, at] = acc[k, at] + buf[k, pl.ds(pl.multiple_of(i * step, step), step)]
            return carry

        lax.fori_loop(0, size // step, body, 0)

    def for_mat(k, what):
        for w in range(mats):
            pl.when(k // chunks == w)(functools.partial(what, w))

    def stage(i, k):
        pairs = steps_of(k)
        offs = offsets(pairs)
        if i == 0:

            def begin(w):
                first_copy(w, k).start()
                load_copy(w, k).start()

            for_mat(k, begin)
        elif i == 1:

            def arrive(w):
                load_copy(w, k).wait()
                first_copy(w, k).wait_recv()

            for_mat(k, arrive)
            add_rows(acc, k, 0, half_rows, half)
            reduce_copy(0, k, pairs, offs).start()
        elif i < 5:
            reduce_copy(i - 2, k, pairs, offs).wait_recv()
            add_rows(acc, k, offs[i - 1], half_rows >> (i - 1), landing[i - 2])
            reduce_copy(i - 1, k, pairs, offs).start()
        elif i == 5:
            reduce_copy(3, k, pairs, offs).wait_recv()
            if finish.narrow:
                row = mat_row(k, core) + offs[3]
                finish.apply(extra, extra_out, acc, rl, gathered, k, offs[3], half_rows >> 3, row)
            else:
                add_rows(gathered, k, offs[3], half_rows >> 3, rl)
            gather_copy(2, k, pairs, offs).start()
        elif i < 8:
            gather_copy(8 - i, k, pairs, offs).wait_recv()
            gather_copy(7 - i, k, pairs, offs).start()
        elif i == 8:
            gather_copy(0, k, pairs, offs).wait_recv()

            def emit(w):
                last_copy(w, k, core).start()
                store_copy(w, k).start()

            for_mat(k, emit)
        else:

            def close(w):
                last_copy(w, k, 1 - core).wait_recv()
                store_copy(w, k).wait()
                last_copy(w, k, core).wait_send()
                first_copy(w, k).wait_send()

            for_mat(k, close)
            for n in range(4):
                reduce_copy(n, k, pairs, offs).wait_send()
            for n in range(3):
                gather_copy(n, k, pairs, offs).wait_send()

    if finish.narrow:
        finish.begin(extra_out)
    count = mats * chunks

    def slot(t, carry):
        for i in ORDER:
            k = t - LAGS[i]

            @pl.when((k >= 0) & (k < count))
            def _():
                stage(i, k)

        return carry

    lax.fori_loop(0, count + LAGS[-1], slot, 0)


class PlainFinish:
    narrow = False
    inputs = 0
    outputs = 0
    out_dtype = jnp.float32


class CorrFinish:
    narrow = True
    inputs = 1
    outputs = 1
    out_dtype = jnp.bfloat16

    def __init__(self, row_count):
        self.row_count = row_count

    def begin(self, extra_out):
        extra_out[0][...] = jnp.zeros_like(extra_out[0])

    def apply(self, extra, extra_out, acc, rl, gathered, k, off, size, row):
        width = acc.shape[-1]
        at = pl.ds(pl.multiple_of(off, size), size)
        corr = (acc[k, at] + rl[k]) / self.row_count
        diag = (row + lax.broadcasted_iota(jnp.int32, (size, width), 0)) == lax.broadcasted_iota(jnp.int32, (size, width), 1)
        off_weight = extra[0][0]
        miss = 1.0 - corr
        terms = jnp.where(diag, miss * miss, off_weight * (corr * corr))
        extra_out[0][...] += jnp.sum(terms, axis=0, keepdims=True)
        gathered[k, at] = jnp.where(diag, -2.0 * miss, 2.0 * off_weight * corr).astype(jnp.bfloat16)


def large_sum(arrays, chunks, z_first, finish, extra, collective_id):
    mats = len(arrays)
    n_rows, width = arrays[0].shape
    half_rows = n_rows // chunks // 2
    count = mats * chunks
    any_spec = pl.BlockSpec(memory_space=pl.ANY)
    out_shape = [jax.ShapeDtypeStruct((n_rows, width), finish.out_dtype) for _ in arrays]
    out_specs = [any_spec] * mats
    if finish.outputs:
        out_shape.append(jax.ShapeDtypeStruct((1, width), jnp.float32))
        out_specs.append(pl.BlockSpec(memory_space=pltpu.VMEM))

    def buf(rows, dtype=jnp.float32):
        return pltpu.VMEM((count, rows, width), dtype)

    narrow_buf = buf(half_rows, finish.out_dtype) if finish.narrow else pltpu.VMEM((8, LANES), jnp.float32)
    return pl.pallas_call(
        functools.partial(large_sum_kernel, mats, chunks, z_first, finish),
        name="large_sum",
        out_shape=out_shape,
        in_specs=[any_spec] * mats + [pl.BlockSpec(memory_space=pltpu.SMEM)] * len(extra),
        out_specs=out_specs,
        scratch_shapes=[
            buf(half_rows),
            buf(half_rows),
            buf(half_rows // 2),
            buf(half_rows // 4),
            buf(half_rows // 8),
            buf(half_rows // 8),
            narrow_buf,
            pltpu.SemaphoreType.DMA((count,)),
            pltpu.SemaphoreType.DMA((count,)),
            pltpu.SemaphoreType.DMA((9, count)),
            pltpu.SemaphoreType.DMA((9, count)),
        ],
        compiler_params=pltpu.CompilerParams(collective_id=collective_id, has_side_effects=True, vmem_limit_bytes=VMEM_BYTES),
    )(*arrays, *extra)


PARTS = 8
MATS = 3
SLOTS = 12
TILE = 256
BACK_LAGS = (0, 1, 3, 5, 6, 7, 8, 9, 11, 13)
Z_FIRST = (3, 7)


def back_kernel(dz_hbm, xt2, xt1, xt0, w_out, w_mid, u2, u1, vec, out2, out1, out0, sums, *scratch):
    (dy_own, dy_peer, xt_own, xt_peer, w_buf, u_buf, dpre, payload, plane_buf, depth_buf, own_buf) = scratch[:11]
    (acc, gathered, rx, ry, rz, rl) = scratch[11:17]
    (in_sem, tile_sem, peer_send, peer_recv, s1, r1, s2, r2, s3, r3, store_sem, send, recv) = scratch[17:]
    rows_dev, width = dz_hbm.shape
    tiles = width // TILE
    row_count = rows_dev * 4 * PLANE
    part_rows = width // 2 // PARTS
    count = MATS * PARTS
    xts, outs, weights, pres = (xt2, xt1, xt0), (out2, out1, out0), (w_out, w_mid), (u2, u1)

    me = lax.axis_index(DATA_AXIS)
    pos, plane = me % PLANE, me // PLANE
    core, bx, by, bz0, bz1 = me % 2, (me // 2) % 2, (me // 4) % 2, (me // 8) % 2, (me // 16) % 2
    other_core = me + 1 - 2 * core
    mates = [(pos + d) % PLANE for d in range(1, PLANE)]
    levels = [(plane + d) % DEPTH for d in range(1, DEPTH)]
    peers = [plane * PLANE + m for m in mates] + [lv * PLANE + pos for lv in levels]

    def rows(off, size):
        return pl.ds(pl.multiple_of(off, size), size)

    def cols(i, size=TILE):
        return pl.ds(pl.multiple_of(i * size, size), size)

    barrier = pltpu.get_barrier_semaphore()
    signal_all(barrier, peers)

    half = width // 2

    def own_xt(w):
        return pltpu.make_async_copy(xts[w].at[rows(core * half, half)], xt_own.at[w], in_sem.at[w])

    dz_load = pltpu.make_async_copy(dz_hbm, dy_own.at[0], in_sem.at[MATS])

    def peer_xt(w):
        return pltpu.make_async_remote_copy(
            xts[w].at[rows((1 - core) * half, half)], xt_peer.at[w], peer_send.at[w], peer_recv.at[w], device_id=(other_core,), device_id_type=MESH
        )

    def peer_dy(w):
        src = dz_hbm if w == 0 else dy_own.at[w % 2]
        return pltpu.make_async_remote_copy(
            src, dy_peer.at[w % 2], peer_send.at[MATS + w], peer_recv.at[MATS + w], device_id=(other_core,), device_id_type=MESH
        )

    def w_tile(layer, i):
        return pltpu.make_async_copy(weights[layer].at[cols(i)], w_buf.at[i % 2], tile_sem.at[0, i % 2])

    def u_tile(layer, i):
        return pltpu.make_async_copy(pres[layer].at[:, cols(i)], u_buf.at[i % 2], tile_sem.at[1, i % 2])

    dz_load.start()
    w_tile(0, 0).start()
    u_tile(0, 0).start()
    for w in range(MATS):
        own_xt(w).start()
    pl.semaphore_wait(barrier, len(peers))
    peer_dy(0).start()
    for w in range(MATS):
        peer_xt(w).start()
    dz_load.wait()

    def vec_row(layer, which, i):
        return vec[layer * 4 + which : layer * 4 + which + 1, cols(i)]

    BLOCK = 64

    def row_loop(body, carry):
        return lax.fori_loop(0, rows_dev // BLOCK, lambda r, c: body(rows(r * BLOCK, BLOCK), c), carry)

    def chain(layer):
        def tile(i, carry):
            w_tile(layer, i).wait()
            u_tile(layer, i).wait()

            @pl.when(i + 1 < tiles)
            def _():
                w_tile(layer, i + 1).start()
                u_tile(layer, i + 1).start()

            dpre[:, cols(i)] = contract_cols(dy_own[layer], w_buf[i % 2])
            gain, bias, mean, inv = (vec_row(layer, j, i) for j in range(4))

            def block(at, sums2):
                n = (u_buf[i % 2, at] - mean) * inv
                g = jnp.where(n * gain + bias > 0.0, dpre[at, cols(i)], 0.0)
                dpre[at, cols(i)] = g
                gn = g * n
                return tuple(
                    s + jnp.sum(v.reshape(BLOCK // 8, 8, TILE), axis=0) for s, v in zip(sums2, (gn, g))
                )

            zero = jnp.zeros((8, TILE), jnp.float32)
            sn, sg = row_loop(block, (zero, zero))
            payload[layer, i, 0:1] = jnp.sum(sn, axis=0, keepdims=True)
            payload[layer, i, 1:2] = jnp.sum(sg, axis=0, keepdims=True)
            return carry

        lax.fori_loop(0, tiles, tile, 0)

    def du(layer):
        u_tile(layer, 0).start()

        def tile(i, carry):
            u_tile(layer, i).wait()

            @pl.when(i + 1 < tiles)
            def _():
                u_tile(layer, i + 1).start()

            gain, mean, inv = vec_row(layer, 0, i), vec_row(layer, 2, i), vec_row(layer, 3, i)
            mean_gn = sums[layer, i, 0:1] / row_count
            mean_g = sums[layer, i, 1:2] / row_count
            scale = gain * inv

            def block(at, c):
                n = (u_buf[i % 2, at] - mean) * inv
                dy_own[1 - layer, at, cols(i)] = ((dpre[at, cols(i)] - mean_g - n * mean_gn) * scale).astype(jnp.bfloat16)
                return c

            row_loop(block, 0)
            return carry

        lax.fori_loop(0, tiles, tile, 0)

    def plane_copy(src, dst, send_sem, recv_sem, mate):
        return pltpu.make_async_remote_copy(src, dst, send_sem, recv_sem, device_id=(plane * PLANE + mate,), device_id_type=MESH)

    def first(layer, m, slot):
        return plane_copy(payload.at[layer, m], plane_buf.at[layer, slot], s1.at[layer, m], r1.at[layer, slot], m)

    def second(layer, lv, slot):
        return pltpu.make_async_remote_copy(
            own_buf.at[layer, 0], depth_buf.at[layer, slot], s2.at[layer, lv], r2.at[layer, slot], device_id=(lv * PLANE + pos,), device_id_type=MESH
        )

    def third(layer, m, slot):
        return plane_copy(own_buf.at[layer, 1], sums.at[layer, slot], s3.at[layer, m], r3.at[layer, slot], m)

    def small_begin(layer):
        for m in mates:
            first(layer, m, pos).start()
        plane_buf[layer, pos] = payload[layer, pos]

    def small_middle(layer):
        for m in mates:
            first(layer, m, m).wait_recv()
        total = plane_buf[layer, 0]
        for i in range(1, PLANE):
            total = total + plane_buf[layer, i]
        own_buf[layer, 0] = total
        depth_buf[layer, plane] = total
        for lv in levels:
            second(layer, lv, plane).start()

    def small_last(layer):
        for lv in levels:
            second(layer, lv, lv).wait_recv()
        total = depth_buf[layer, 0]
        for i in range(1, DEPTH):
            total = total + depth_buf[layer, i]
        own_buf[layer, 1] = total
        sums[layer, pos] = total
        for m in mates:
            third(layer, m, pos).start()

    def small_end(layer):
        for m in mates:
            third(layer, m, m).wait_recv()
            first(layer, m, pos).wait_send()
            third(layer, m, pos).wait_send()
        for lv in levels:
            second(layer, lv, plane).wait_send()

    xy = ((2 + 2 * core, core * by + (1 - core) * bx), (4 - 2 * core, core * bx + (1 - core) * by))
    zz = ((8, bz0), (16, bz1))

    def steps_of(k):
        part = k % PARTS
        zf = 0
        for z in Z_FIRST:
            same = part - z
            zf = zf + (1 - lax.min(same * same, 1))
        pairs = []
        for a, b in zip(xy + zz, zz + xy):
            stride = zf * b[0] + (1 - zf) * a[0]
            bit = zf * b[1] + (1 - zf) * a[1]
            pairs.append((me + stride * (1 - 2 * bit), bit))
        offs, size = [0], part_rows
        for _, bit in pairs[:3]:
            size = size // 2
            offs.append(offs[-1] + bit * size)
        return pairs, offs

    landing = (rx, ry, rz, rl)

    def remote(src, dst, stage, k, mate):
        return pltpu.make_async_remote_copy(src, dst, send.at[stage, k], recv.at[stage, k], device_id=(mate,), device_id_type=MESH)

    def reduce_copy(i, k, pairs, offs):
        size = part_rows >> (i + 1)
        if i == 3:
            size = part_rows >> 3
            off = offs[3]
        else:
            off = offs[i] + (1 - pairs[i][1]) * size
        return remote(acc.at[k % SLOTS, rows(off, size)], landing[i].at[k % SLOTS], i, k, pairs[i][0])

    def gather_copy(i, k, pairs, offs):
        block = gathered.at[k % SLOTS, rows(offs[i + 1], part_rows >> (i + 1))]
        return remote(block, block, 6 - i, k, pairs[i][0])

    def out_rows(k, side):
        return pl.ds(pl.multiple_of(side * half + (k % PARTS) * part_rows, part_rows), part_rows)

    def last_copy(w, k, side):
        return remote(gathered.at[k % SLOTS], outs[w].at[out_rows(k, side)], 7, k, other_core)

    def store_copy(w, k):
        return pltpu.make_async_copy(gathered.at[k % SLOTS], outs[w].at[out_rows(k, core)], store_sem.at[k])

    def add_rows(dst, k, off, size, buf):
        step = min(size, 16)
        j = k % SLOTS

        def body(i, carry):
            at = rows(off + i * step, step)
            dst[j, at] = acc[j, at] + buf[j, rows(i * step, step)]
            return carry

        lax.fori_loop(0, size // step, body, 0)

    def for_mat(k, what):
        for w in range(MATS):
            pl.when(k // PARTS == w)(functools.partial(what, w))

    def form(k):
        w, j = k // PARTS, k % SLOTS
        at = rows((k % PARTS) * part_rows, part_rows)
        step = min(512, width)

        def col(c, carry):
            cs = cols(c, step)
            acc[j, :, cs] = jnp.dot(xt_own[w, at], dy_own[w % 2, :, cs], preferred_element_type=jnp.float32) + jnp.dot(
                xt_peer[w, at], dy_peer[w % 2, :, cs], preferred_element_type=jnp.float32
            )
            return carry

        lax.fori_loop(0, width // step, col, 0)

    def stage(i, k):
        pairs, offs = steps_of(k)
        if i == 0:

            @pl.when(k == 2 * PARTS)
            def _():
                peer_dy(2).wait_recv()

            form(k)
        elif i == 1:
            reduce_copy(0, k, pairs, offs).start()
        elif i < 5:
            reduce_copy(i - 2, k, pairs, offs).wait_recv()
            add_rows(acc, k, offs[i - 1], part_rows >> (i - 1), landing[i - 2])
            reduce_copy(i - 1, k, pairs, offs).start()
        elif i == 5:
            reduce_copy(3, k, pairs, offs).wait_recv()
            add_rows(gathered, k, offs[3], part_rows >> 3, rl)
            gather_copy(2, k, pairs, offs).start()
        elif i < 8:
            gather_copy(8 - i, k, pairs, offs).wait_recv()
            gather_copy(7 - i, k, pairs, offs).start()
            if i == 6:
                for n in range(4):
                    reduce_copy(n, k, pairs, offs).wait_send()
        elif i == 8:
            gather_copy(0, k, pairs, offs).wait_recv()

            def emit(w):
                last_copy(w, k, core).start()
                store_copy(w, k).start()

            for_mat(k, emit)
        else:

            def close(w):
                last_copy(w, k, 1 - core).wait_recv()
                store_copy(w, k).wait()
                last_copy(w, k, core).wait_send()

            for_mat(k, close)
            for n in range(3):
                gather_copy(n, k, pairs, offs).wait_send()

    def chunk_loop(first_k, last_k, i):
        def body(k, carry):
            stage(i, k)
            return carry

        lax.fori_loop(first_k, last_k, body, 0)

    ready = {0: SLOTS, 1: 2}

    def slot(t, carry):
        for i in ORDER:
            k = t - BACK_LAGS[i]

            @pl.when((k >= ready.get(i, 0)) & (k < count))
            def _():
                stage(i, k)

        return carry

    chain(0)
    w_tile(1, 0).start()
    small_begin(0)
    for w in range(MATS):
        own_xt(w).wait()
        peer_xt(w).wait_recv()
    peer_dy(0).wait_recv()
    chunk_loop(0, PARTS // 2, 0)
    small_middle(0)
    chunk_loop(PARTS // 2, PARTS, 0)
    small_last(0)
    chunk_loop(0, 2, 1)
    small_end(0)
    du(0)
    peer_dy(1).start()
    u_tile(1, 0).start()
    chain(1)
    small_begin(1)
    peer_dy(1).wait_recv()
    chunk_loop(PARTS, PARTS + 2, 0)
    small_middle(1)
    chunk_loop(PARTS + 2, SLOTS, 0)
    small_last(1)
    slot(3, 0)
    small_end(1)
    peer_dy(0).wait_send()
    du(1)
    peer_dy(2).start()
    lax.fori_loop(4, count + BACK_LAGS[-1], slot, 0)
    for w in range(MATS):
        peer_xt(w).wait_send()
    peer_dy(1).wait_send()
    peer_dy(2).wait_send()


def backward(grad_z, xt2, xt1, xt0, w_out, w_mid, u2, u1, vec):
    rows_dev, width = grad_z.shape
    tiles = width // TILE
    part_rows = width // 2 // PARTS
    count = MATS * PARTS
    any_spec = pl.BlockSpec(memory_space=pl.ANY)
    vmem_spec = pl.BlockSpec(memory_space=pltpu.VMEM)
    mat = jax.ShapeDtypeStruct((width, width), jnp.float32)

    def slots(n):
        return pltpu.VMEM((SLOTS, n, width), jnp.float32)

    dma = pltpu.SemaphoreType.DMA
    return pl.pallas_call(
        back_kernel,
        name="backward",
        out_shape=[mat, mat, mat, jax.ShapeDtypeStruct((2, tiles, 2, TILE), jnp.float32)],
        in_specs=[any_spec] * 8 + [vmem_spec],
        out_specs=[any_spec] * 3 + [vmem_spec],
        scratch_shapes=[
            pltpu.VMEM((2, rows_dev, width), jnp.bfloat16),
            pltpu.VMEM((2, rows_dev, width), jnp.bfloat16),
            pltpu.VMEM((MATS, width // 2, rows_dev), jnp.bfloat16),
            pltpu.VMEM((MATS, width // 2, rows_dev), jnp.bfloat16),
            pltpu.VMEM((2, TILE, width), jnp.bfloat16),
            pltpu.VMEM((2, rows_dev, TILE), jnp.float32),
            pltpu.VMEM((rows_dev, width), jnp.float32),
            pltpu.VMEM((2, tiles, 2, TILE), jnp.float32),
            pltpu.VMEM((2, PLANE, 2, TILE), jnp.float32),
            pltpu.VMEM((2, DEPTH, 2, TILE), jnp.float32),
            pltpu.VMEM((2, 2, 2, TILE), jnp.float32),
            slots(part_rows),
            slots(part_rows),
            slots(part_rows // 2),
            slots(part_rows // 4),
            slots(part_rows // 8),
            slots(part_rows // 8),
            dma((MATS + 1,)),
            dma((2, 2)),
            dma((2 * MATS,)),
            dma((2 * MATS,)),
            dma((2, PLANE)),
            dma((2, PLANE)),
            dma((2, DEPTH)),
            dma((2, DEPTH)),
            dma((2, PLANE)),
            dma((2, PLANE)),
            dma((count,)),
            dma((8, count)),
            dma((8, count)),
        ],
        compiler_params=pltpu.CompilerParams(collective_id=2, has_side_effects=True, vmem_limit_bytes=VMEM_BYTES),
    )(grad_z, xt2, xt1, xt0, w_out, w_mid, u2, u1, vec)


def solution(mesh):
    shards = mesh.shape[DATA_AXIS]
    row_part = P(DATA_AXIS, None)
    replicated = P()

    def local_step(feat_a, feat_b, w_in, w_mid, w_out, t_in, t_mid, t_out, gain_1, bias_1, gain_2, bias_2, off_weight):
        row_count = feat_a.shape[0] * shards

        def norm_pair(pre_a, pre_b):
            stat_sums = jnp.stack([jnp.sum(pre_a, axis=0), jnp.sum(pre_a * pre_a, axis=0), jnp.sum(pre_b, axis=0), jnp.sum(pre_b * pre_b, axis=0)])
            stat_means = small_sum(stat_sums) / row_count
            inv_a = lax.rsqrt(stat_means[1] - stat_means[0] * stat_means[0] + NORM_EPS)
            inv_b = lax.rsqrt(stat_means[3] - stat_means[2] * stat_means[2] + NORM_EPS)
            return (pre_a - stat_means[0]) * inv_a, (pre_b - stat_means[2]) * inv_b, stat_means[0], inv_a

        def hidden_pair(in_a, in_b, weight_a, weight_b, gain_vec, bias_vec):
            pre_a = jnp.dot(in_a, weight_a, preferred_element_type=jnp.float32)
            normed_a, normed_b, mean_a, inv_a = norm_pair(pre_a, jnp.dot(in_b, weight_b, preferred_element_type=jnp.float32))
            act_a = jnp.maximum(normed_a * gain_vec + bias_vec, 0.0).astype(jnp.bfloat16)
            act_b = jnp.maximum(normed_b * gain_vec + bias_vec, 0.0).astype(jnp.bfloat16)
            return act_a, act_b, pre_a, [gain_vec, bias_vec, mean_a, inv_a]

        act_1, teach_1, pre_1, vec_1 = hidden_pair(feat_a, feat_b, w_in, t_in, gain_1, bias_1)
        act_2, teach_2, pre_2, vec_2 = hidden_pair(act_1, teach_1, w_mid, t_mid, gain_2, bias_2)
        pre_z = jnp.dot(act_2, w_out, preferred_element_type=jnp.float32)
        zh_a, zh_b, _, inv_z = norm_pair(pre_z, jnp.dot(teach_2, t_out, preferred_element_type=jnp.float32))
        emb_a = zh_a.astype(jnp.bfloat16)
        emb_b = zh_b.astype(jnp.bfloat16)
        corr_part = contract_rows(emb_a, emb_b)
        grad_c, loss_cols = large_sum([corr_part], 8, (3, 7), CorrFinish(row_count), [off_weight.reshape(1)], 1)
        grad_emb = contract_cols(emb_b, grad_c) / row_count
        loss_row = jnp.sum(loss_cols, axis=0)
        stat_sums = small_sum(jnp.stack([jnp.sum(grad_emb, axis=0), jnp.sum(grad_emb * zh_a, axis=0), loss_row]))
        loss_value = jnp.sum(stat_sums[2]) * 0.5
        grad_z = ((grad_emb - stat_sums[0] / row_count - zh_a * (stat_sums[1] / row_count)) * inv_z).astype(jnp.bfloat16)
        grad_w_out, grad_w_mid, grad_w_in, sums = backward(
            grad_z, act_2.T, act_1.T, feat_a.T, w_out, w_mid, pre_2, pre_1, jnp.stack(vec_2 + vec_1)
        )
        sums = jnp.transpose(sums, (0, 2, 1, 3)).reshape(2, 2, -1)
        return (loss_value, grad_emb, grad_w_in, grad_w_mid, grad_w_out, sums[1, 0], sums[1, 1], sums[0, 0], sums[0, 1])

    return jax.shard_map(local_step, mesh=mesh, in_specs=(row_part, row_part) + (replicated,) * 11, out_specs=(replicated, row_part) + (replicated,) * 7, check_vma=False)
```

```python
import functools

import jax
import jax.numpy as jnp
from jax import lax
from jax.experimental import pallas as pl
from jax.experimental.pallas import tpu as pltpu
from jax.sharding import PartitionSpec as P

NORM_EPS = 1e-5
DATA_AXIS = "data"
MESH = pl.DeviceIdType.MESH
VMEM_BYTES = 62 * 1024 * 1024
BACK_VMEM = 67_043_328
LANES = 128
PLANE = 8
DEPTH = 4
CORE, AXIS_X, AXIS_Y, AXIS_Z0, AXIS_Z1 = 1, 2, 4, 8, 16


def contract_rows(left_op, right_op):
    return lax.dot_general(left_op, right_op, (((0,), (0,)), ((), ())), preferred_element_type=jnp.float32)


def contract_cols(left_op, right_op):
    return lax.dot_general(left_op, right_op, (((1,), (1,)), ((), ())), preferred_element_type=jnp.float32)


def signal_all(sem, peers):
    for peer in peers:
        pl.semaphore_signal(sem, inc=1, device_id=(peer,), device_id_type=MESH)


def small_sum_kernel(x_ref, o_ref, plane_buf, depth_buf, own_buf, s1, r1, s2, r2, s3, r3):
    me = lax.axis_index(DATA_AXIS)
    pos, plane = me % PLANE, me // PLANE
    mates = [(pos + d) % PLANE for d in range(1, PLANE)]
    levels = [(plane + d) % DEPTH for d in range(1, DEPTH)]
    peers = [plane * PLANE + m for m in mates] + [lv * PLANE + pos for lv in levels]
    barrier = pltpu.get_barrier_semaphore()
    signal_all(barrier, peers)
    pl.semaphore_wait(barrier, len(peers))

    def plane_copy(src, dst, send, recv, mate):
        return pltpu.make_async_remote_copy(src, dst, send, recv, device_id=(plane * PLANE + mate,), device_id_type=MESH)

    out1 = [plane_copy(x_ref.at[m], plane_buf.at[pos], s1.at[m], r1.at[pos], m) for m in mates]
    for c in out1:
        c.start()
    plane_buf[pos] = x_ref[pos]
    for m in mates:
        plane_copy(x_ref.at[m], plane_buf.at[m], s1.at[m], r1.at[m], m).wait_recv()
    total = plane_buf[0]
    for i in range(1, PLANE):
        total = total + plane_buf[i]
    own_buf[0] = total
    depth_buf[plane] = total

    def depth_copy(slot, level):
        return pltpu.make_async_remote_copy(
            own_buf.at[0], depth_buf.at[slot], s2.at[level], r2.at[slot], device_id=(level * PLANE + pos,), device_id_type=MESH
        )

    out2 = [depth_copy(plane, lv) for lv in levels]
    for c in out2:
        c.start()
    for lv in levels:
        depth_copy(lv, lv).wait_recv()
    total = depth_buf[0]
    for i in range(1, DEPTH):
        total = total + depth_buf[i]
    own_buf[1] = total
    o_ref[pos] = total
    out3 = [plane_copy(own_buf.at[1], o_ref.at[pos], s3.at[m], r3.at[pos], m) for m in mates]
    for c in out3:
        c.start()
    for m in mates:
        plane_copy(own_buf.at[1], o_ref.at[m], s3.at[m], r3.at[m], m).wait_recv()
    for c in out1 + out2 + out3:
        c.wait_send()


def small_sum(rows):
    count, width = rows.shape
    tile = (PLANE, PLANE, LANES)
    size = PLANE * PLANE * LANES
    flat = jnp.pad(rows.reshape(-1), (0, size - count * width)).reshape(tile)
    total = pl.pallas_call(
        small_sum_kernel,
        name="small_sum",
        out_shape=jax.ShapeDtypeStruct(tile, jnp.float32),
        in_specs=[pl.BlockSpec(memory_space=pltpu.VMEM)],
        out_specs=pl.BlockSpec(memory_space=pltpu.VMEM),
        scratch_shapes=[
            pltpu.VMEM(tile, jnp.float32),
            pltpu.VMEM((DEPTH, PLANE, LANES), jnp.float32),
            pltpu.VMEM((2, PLANE, LANES), jnp.float32),
        ]
        + [pltpu.SemaphoreType.DMA((n,)) for n in (PLANE, PLANE, DEPTH, DEPTH, PLANE, PLANE)],
        compiler_params=pltpu.CompilerParams(collective_id=0, has_side_effects=True),
    )(flat)
    return total.reshape(-1)[: count * width].reshape(count, width)


LAGS = (0, 1, 3, 5, 6, 7, 8, 9, 11, 13)
ORDER = (0, 1, 5, 4, 6, 3, 7, 2, 8, 9)


def large_sum_kernel(mats, chunks, z_first, finish, *refs):
    ins, refs = refs[:mats], refs[mats:]
    extra, refs = refs[: finish.inputs], refs[finish.inputs :]
    outs, refs = refs[:mats], refs[mats:]
    extra_out, refs = refs[: finish.outputs], refs[finish.outputs :]
    acc, half, rx, ry, rz, rl, gathered, load_sem, store_sem, send, recv = refs
    if not finish.narrow:
        gathered = half
    chunk_rows = ins[0].shape[0] // chunks
    half_rows = chunk_rows // 2
    me = lax.axis_index(DATA_AXIS)
    core, bx, by, bz0, bz1 = me % 2, (me // 2) % 2, (me // 4) % 2, (me // 8) % 2, (me // 16) % 2

    barrier = pltpu.get_barrier_semaphore()
    mates = [me + s * (1 - 2 * b) for s, b in ((1, core), (2, bx), (4, by), (8, bz0), (16, bz1))]
    signal_all(barrier, mates)
    pl.semaphore_wait(barrier, len(mates))

    xy = ((2 + 2 * core, core * by + (1 - core) * bx), (4 - 2 * core, core * bx + (1 - core) * by))
    zz = ((8, bz0), (16, bz1))

    def steps_of(k):
        part = k % chunks
        zf = 0
        for z in z_first:
            same = part - z
            zf = zf + (1 - lax.min(same * same, 1))
        pairs = []
        for a, b in zip(xy + zz, zz + xy):
            stride = zf * b[0] + (1 - zf) * a[0]
            bit = zf * b[1] + (1 - zf) * a[1]
            pairs.append((me + stride * (1 - 2 * bit), bit))
        return pairs

    def offsets(pairs):
        offs, size = [0], half_rows
        for _, bit in pairs[:3]:
            size = size // 2
            offs.append(offs[-1] + bit * size)
        return offs

    def rows(off, size):
        return pl.ds(pl.multiple_of(off, size), size)

    def remote(src, dst, stage, k, mate):
        return pltpu.make_async_remote_copy(src, dst, send.at[stage, k], recv.at[stage, k], device_id=(mate,), device_id_type=MESH)

    def mat_row(k, side):
        return pl.multiple_of((k % chunks) * chunk_rows + side * half_rows, half_rows)

    other_core = mates[0]

    def first_copy(w, k):
        return remote(ins[w].at[pl.ds(mat_row(k, 1 - core), half_rows)], half.at[k], 0, k, other_core)

    def load_copy(w, k):
        return pltpu.make_async_copy(ins[w].at[pl.ds(mat_row(k, core), half_rows)], acc.at[k], load_sem.at[k])

    def last_copy(w, k, side):
        return remote(gathered.at[k], outs[w].at[pl.ds(mat_row(k, side), half_rows)], 8, k, other_core)

    def store_copy(w, k):
        return pltpu.make_async_copy(gathered.at[k], outs[w].at[pl.ds(mat_row(k, core), half_rows)], store_sem.at[k])

    landing = (rx, ry, rz, rl)

    def reduce_copy(i, k, pairs, offs):
        size = half_rows >> (i + 1)
        if i == 3:
            size = half_rows >> 3
            off = offs[3]
        else:
            off = offs[i] + (1 - pairs[i][1]) * size
        return remote(acc.at[k, rows(off, size)], landing[i].at[k], 1 + i, k, pairs[i][0])

    def gather_copy(i, k, pairs, offs):
        size = half_rows >> (i + 1)
        block = gathered.at[k, rows(offs[i + 1], size)]
        return remote(block, block, 7 - i, k, pairs[i][0])

    def add_rows(dst, k, off, size, buf):
        step = min(size, 16)

        def body(i, carry):
            at = pl.ds(pl.multiple_of(off + i * step, step), step)
            dst[k, at] = acc[k, at] + buf[k, pl.ds(pl.multiple_of(i * step, step), step)]
            return carry

        lax.fori_loop(0, size // step, body, 0)

    def for_mat(k, what):
        for w in range(mats):
            pl.when(k // chunks == w)(functools.partial(what, w))

    def stage(i, k):
        pairs = steps_of(k)
        offs = offsets(pairs)
        if i == 0:

            def begin(w):
                first_copy(w, k).start()
                load_copy(w, k).start()

            for_mat(k, begin)
        elif i == 1:

            def arrive(w):
                load_copy(w, k).wait()
                first_copy(w, k).wait_recv()

            for_mat(k, arrive)
            add_rows(acc, k, 0, half_rows, half)
            reduce_copy(0, k, pairs, offs).start()
        elif i < 5:
            reduce_copy(i - 2, k, pairs, offs).wait_recv()
            add_rows(acc, k, offs[i - 1], half_rows >> (i - 1), landing[i - 2])
            reduce_copy(i - 1, k, pairs, offs).start()
        elif i == 5:
            reduce_copy(3, k, pairs, offs).wait_recv()
            if finish.narrow:
                row = mat_row(k, core) + offs[3]
                finish.apply(extra, extra_out, acc, rl, gathered, k, offs[3], half_rows >> 3, row)
            else:
                add_rows(gathered, k, offs[3], half_rows >> 3, rl)
            gather_copy(2, k, pairs, offs).start()
        elif i < 8:
            gather_copy(8 - i, k, pairs, offs).wait_recv()
            gather_copy(7 - i, k, pairs, offs).start()
        elif i == 8:
            gather_copy(0, k, pairs, offs).wait_recv()

            def emit(w):
                last_copy(w, k, core).start()
                store_copy(w, k).start()

            for_mat(k, emit)
        else:

            def close(w):
                last_copy(w, k, 1 - core).wait_recv()
                store_copy(w, k).wait()
                last_copy(w, k, core).wait_send()
                first_copy(w, k).wait_send()

            for_mat(k, close)
            for n in range(4):
                reduce_copy(n, k, pairs, offs).wait_send()
            for n in range(3):
                gather_copy(n, k, pairs, offs).wait_send()

    if finish.narrow:
        finish.begin(extra_out)
    count = mats * chunks

    def slot(t, carry):
        for i in ORDER:
            k = t - LAGS[i]

            @pl.when((k >= 0) & (k < count))
            def _():
                stage(i, k)

        return carry

    lax.fori_loop(0, count + LAGS[-1], slot, 0)


class PlainFinish:
    narrow = False
    inputs = 0
    outputs = 0
    out_dtype = jnp.float32


class CorrFinish:
    narrow = True
    inputs = 1
    outputs = 1
    out_dtype = jnp.bfloat16

    def __init__(self, row_count):
        self.row_count = row_count

    def begin(self, extra_out):
        extra_out[0][...] = jnp.zeros_like(extra_out[0])

    def apply(self, extra, extra_out, acc, rl, gathered, k, off, size, row):
        width = acc.shape[-1]
        at = pl.ds(pl.multiple_of(off, size), size)
        corr = (acc[k, at] + rl[k]) / self.row_count
        diag = (row + lax.broadcasted_iota(jnp.int32, (size, width), 0)) == lax.broadcasted_iota(jnp.int32, (size, width), 1)
        off_weight = extra[0][0]
        miss = 1.0 - corr
        terms = jnp.where(diag, miss * miss, off_weight * (corr * corr))
        extra_out[0][...] += jnp.sum(terms, axis=0, keepdims=True)
        gathered[k, at] = jnp.where(diag, -2.0 * miss, 2.0 * off_weight * corr).astype(jnp.bfloat16)


def large_sum(arrays, chunks, z_first, finish, extra, collective_id):
    mats = len(arrays)
    n_rows, width = arrays[0].shape
    half_rows = n_rows // chunks // 2
    count = mats * chunks
    any_spec = pl.BlockSpec(memory_space=pl.ANY)
    out_shape = [jax.ShapeDtypeStruct((n_rows, width), finish.out_dtype) for _ in arrays]
    out_specs = [any_spec] * mats
    if finish.outputs:
        out_shape.append(jax.ShapeDtypeStruct((1, width), jnp.float32))
        out_specs.append(pl.BlockSpec(memory_space=pltpu.VMEM))

    def buf(rows, dtype=jnp.float32):
        return pltpu.VMEM((count, rows, width), dtype)

    narrow_buf = buf(half_rows, finish.out_dtype) if finish.narrow else pltpu.VMEM((8, LANES), jnp.float32)
    return pl.pallas_call(
        functools.partial(large_sum_kernel, mats, chunks, z_first, finish),
        name="large_sum",
        out_shape=out_shape,
        in_specs=[any_spec] * mats + [pl.BlockSpec(memory_space=pltpu.SMEM)] * len(extra),
        out_specs=out_specs,
        scratch_shapes=[
            buf(half_rows),
            buf(half_rows),
            buf(half_rows // 2),
            buf(half_rows // 4),
            buf(half_rows // 8),
            buf(half_rows // 8),
            narrow_buf,
            pltpu.SemaphoreType.DMA((count,)),
            pltpu.SemaphoreType.DMA((count,)),
            pltpu.SemaphoreType.DMA((9, count)),
            pltpu.SemaphoreType.DMA((9, count)),
        ],
        compiler_params=pltpu.CompilerParams(collective_id=collective_id, has_side_effects=True, vmem_limit_bytes=VMEM_BYTES),
    )(*arrays, *extra)


PARTS = 8
MATS = 3
SLOTS = 12
TILE = 256
WIDE = 512
BACK_LAGS = (0, 0, 2, 4, 5, 6, 7, 8, 10, 12)
Z_FIRST = (2, 7, 12, 17, 21)
LAYER_SLOTS = 6


def back_kernel(dz_hbm, x2, x1, x0, w_out, w_mid, u2, u1, vec, out2, out1, out0, sums, *scratch):
    (dy, xs, w_buf, u_buf, dpre, payload, plane_buf, depth_buf, own_buf) = scratch[:9]
    (acc, gathered, rx, ry, rz, rl) = scratch[9:15]
    (in_sem, tile_sem, peer_send, peer_recv, s1, r1, s2, r2, s3, r3, store_sem, send, recv) = scratch[15:]
    rows_dev, width = dz_hbm.shape
    wide = w_buf.shape[1]
    tiles = width // wide
    per_slot = tiles // 2
    row_count = rows_dev * 4 * PLANE
    half = width // 2
    part_rows = half // PARTS
    count = MATS * PARTS
    mats_in, outs, weights, pres = (x2, x1, x0), (out2, out1, out0), (w_out, w_mid), (u2, u1)

    me = lax.axis_index(DATA_AXIS)
    pos, plane = me % PLANE, me // PLANE
    core, bx, by, bz0, bz1 = me % 2, (me // 2) % 2, (me // 4) % 2, (me // 8) % 2, (me // 16) % 2
    other_core = me + 1 - 2 * core
    mates = [(pos + d) % PLANE for d in range(1, PLANE)]
    levels = [(plane + d) % DEPTH for d in range(1, DEPTH)]
    peers = [plane * PLANE + m for m in mates] + [lv * PLANE + pos for lv in levels]

    def rows(off, size):
        return pl.ds(pl.multiple_of(off, size), size)

    mine = rows(core * rows_dev, rows_dev)

    def pick(index, choices, what):
        for i, c in enumerate(choices):
            pl.when(index == i)(functools.partial(what, c))

    barrier = pltpu.get_barrier_semaphore()
    signal_all(barrier, peers)

    def own_x(w):
        return pltpu.make_async_copy(mats_in[w].at[:, rows(core * half, half)], xs.at[w, mine], in_sem.at[w])

    def peer_x(w):
        return pltpu.make_async_remote_copy(
            mats_in[w].at[:, rows((1 - core) * half, half)], xs.at[w, mine], peer_send.at[w], peer_recv.at[w], device_id=(other_core,), device_id_type=MESH
        )

    def peer_dy(w):
        block = dy.at[w % 2, mine]
        return pltpu.make_async_remote_copy(block, block, peer_send.at[MATS + w], peer_recv.at[MATS + w], device_id=(other_core,), device_id_type=MESH)

    def x_arrive(w):
        block = xs.at[w, mine]
        pltpu.make_async_copy(block, block, in_sem.at[w]).wait()
        pltpu.make_async_remote_copy(block, block, peer_send.at[w], peer_recv.at[w], device_id=(other_core,), device_id_type=MESH).wait_recv()

    def w_tile(ref, i):
        return pltpu.make_async_copy(ref.at[rows(i * wide, wide)], w_buf.at[i % 2], tile_sem.at[0, i % 2])

    def u_tile(ref, i):
        return pltpu.make_async_copy(ref.at[:, rows(i * wide, wide)], u_buf.at[i % 2], tile_sem.at[1, i % 2])

    def start_w(layer, i):
        pick(layer, weights, lambda ref: w_tile(ref, i).start())

    def start_u(layer, i):
        pick(layer, pres, lambda ref: u_tile(ref, i).start())

    dz_load = pltpu.make_async_copy(dz_hbm, dy.at[0, mine], in_sem.at[MATS])
    dz_load.start()
    for w in range(MATS):
        own_x(w).start()
    w_tile(weights[0], 0).start()
    u_tile(pres[0], 0).start()
    pl.semaphore_wait(barrier, len(peers))
    peer_x(0).start()
    dz_load.wait()
    peer_dy(0).start()
    for w in range(1, MATS):
        peer_x(w).start()

    BLOCK = 32

    def row_loop(body, carry):
        return lax.fori_loop(0, rows_dev // BLOCK, lambda r, c: body(r, c), carry)

    def chain_tile(layer, i):
        w_tile(w_out, i).wait()
        u_tile(u2, i).wait()

        @pl.when(i + 1 < tiles)
        def _():
            start_w(layer, i + 1)
            start_u(layer, i + 1)

        at_cols = rows(i * wide, wide)
        dpre[:, at_cols] = contract_cols(dy[layer, mine], w_buf[i % 2])
        gain, bias, mean, inv = (vec[layer * 4 + j, :, at_cols] for j in range(4))

        def block(r, sums2):
            at = rows(r * BLOCK, BLOCK)
            n = (u_buf[i % 2, at] - mean) * inv
            g = jnp.where(n * gain + bias > 0.0, dpre[at, at_cols], 0.0)
            dpre[at, at_cols] = g
            gn = g * n
            return tuple(s + jnp.sum(v.reshape(BLOCK // 8, 8, wide), axis=0) for s, v in zip(sums2, (gn, g)))

        zero = jnp.zeros((8, wide), jnp.float32)
        for row, total in enumerate(row_loop(block, (zero, zero))):
            total = jnp.sum(total, axis=0, keepdims=True)
            for c in range(wide // TILE):
                payload[layer, i * (wide // TILE) + c, row : row + 1] = total[:, c * TILE : (c + 1) * TILE]

    def du(layer):
        start_u(layer, 0)

        def tile(i, carry):
            u_tile(u2, i).wait()

            @pl.when(i + 1 < tiles)
            def _():
                start_u(layer, i + 1)

            at_cols = rows(i * wide, wide)
            gain, mean, inv = (vec[layer * 4 + j, :, at_cols] for j in (0, 2, 3))
            total = jnp.concatenate([sums[layer, i * (wide // TILE) + c] for c in range(wide // TILE)], axis=1)
            mean_gn = total[0:1] / row_count
            mean_g = total[1:2] / row_count
            scale = gain * inv

            def block(r, c):
                at = rows(r * BLOCK, BLOCK)
                n = (u_buf[i % 2, at] - mean) * inv
                value = (dpre[at, at_cols] - mean_g - n * mean_gn) * scale
                dy[1 - layer, rows(core * rows_dev + r * BLOCK, BLOCK), at_cols] = value.astype(jnp.bfloat16)
                return c

            row_loop(block, 0)
            return carry

        lax.fori_loop(0, tiles, tile, 0)

    def plane_copy(src, dst, send_sem, recv_sem, mate):
        return pltpu.make_async_remote_copy(src, dst, send_sem, recv_sem, device_id=(plane * PLANE + mate,), device_id_type=MESH)

    def first(layer, m, slot):
        return plane_copy(payload.at[layer, m], plane_buf.at[layer, slot], s1.at[layer, m], r1.at[layer, slot], m)

    def second(layer, lv, slot):
        return pltpu.make_async_remote_copy(
            own_buf.at[layer, 0], depth_buf.at[layer, slot], s2.at[layer, lv], r2.at[layer, slot], device_id=(lv * PLANE + pos,), device_id_type=MESH
        )

    def third(layer, m, slot):
        return plane_copy(own_buf.at[layer, 1], sums.at[layer, slot], s3.at[layer, m], r3.at[layer, slot], m)

    def small_begin(layer):
        for m in mates:
            first(layer, m, pos).start()
        plane_buf[layer, pos] = payload[layer, pos]

    def small_middle(layer):
        for m in mates:
            first(layer, m, m).wait_recv()
        total = plane_buf[layer, 0]
        for i in range(1, PLANE):
            total = total + plane_buf[layer, i]
        own_buf[layer, 0] = total
        depth_buf[layer, plane] = total
        for lv in levels:
            second(layer, lv, plane).start()

    def small_last(layer):
        for lv in levels:
            second(layer, lv, lv).wait_recv()
        total = depth_buf[layer, 0]
        for i in range(1, DEPTH):
            total = total + depth_buf[layer, i]
        own_buf[layer, 1] = total
        sums[layer, pos] = total
        for m in mates:
            third(layer, m, pos).start()

    def small_end(layer):
        for m in mates:
            third(layer, m, m).wait_recv()
            first(layer, m, pos).wait_send()
            third(layer, m, pos).wait_send()
        for lv in levels:
            second(layer, lv, plane).wait_send()

    xy = ((2 + 2 * core, core * by + (1 - core) * bx), (4 - 2 * core, core * bx + (1 - core) * by))
    zz = ((8, bz0), (16, bz1))

    def steps_of(k):
        zf = 0
        for z in Z_FIRST:
            same = k - z
            zf = zf + (1 - lax.min(same * same, 1))
        pairs = []
        for a, b in zip(xy + zz, zz + xy):
            stride = zf * b[0] + (1 - zf) * a[0]
            bit = zf * b[1] + (1 - zf) * a[1]
            pairs.append((me + stride * (1 - 2 * bit), bit))
        offs, size = [0], part_rows
        for _, bit in pairs[:3]:
            size = size // 2
            offs.append(offs[-1] + bit * size)
        return pairs, offs

    landing = (rx, ry, rz, rl)

    def remote(src, dst, stage, k, mate):
        return pltpu.make_async_remote_copy(src, dst, send.at[stage, k], recv.at[stage, k], device_id=(mate,), device_id_type=MESH)

    def reduce_copy(i, k, pairs, offs):
        size = part_rows >> (i + 1)
        if i == 3:
            size = part_rows >> 3
            off = offs[3]
        else:
            off = offs[i] + (1 - pairs[i][1]) * size
        return remote(acc.at[k % SLOTS, rows(off, size)], landing[i].at[k % SLOTS], i, k, pairs[i][0])

    def gather_copy(i, k, pairs, offs):
        block = gathered.at[k % SLOTS, rows(offs[i + 1], part_rows >> (i + 1))]
        return remote(block, block, 6 - i, k, pairs[i][0])

    def out_rows(k, side):
        return pl.ds(pl.multiple_of(side * half + (k % PARTS) * part_rows, part_rows), part_rows)

    def last_copy(out, k, side):
        return remote(gathered.at[k % SLOTS], out.at[out_rows(k, side)], 7, k, other_core)

    def store_copy(out, k):
        return pltpu.make_async_copy(gathered.at[k % SLOTS], out.at[out_rows(k, core)], store_sem.at[k])

    def add_rows(dst, k, off, size, buf):
        step = min(size, 16)
        j = k % SLOTS

        def body(i, carry):
            at = rows(off + i * step, step)
            dst[j, at] = acc[j, at] + buf[j, rows(i * step, step)]
            return carry

        lax.fori_loop(0, size // step, body, 0)

    def form(k):
        w, j = k // PARTS, k % SLOTS

        @pl.when(k % PARTS == 0)
        def _():
            x_arrive(w)
            peer_dy(w).wait_recv()

        at = rows((k % PARTS) * part_rows, 2 * part_rows)
        step = min(1024, width)

        def col(c, carry):
            cs = rows(c * step, step)
            acc[pl.ds(j, 2), :, cs] = contract_rows(xs[w, :, at], dy[w % 2, :, cs]).reshape(2, part_rows, step)
            return carry

        lax.fori_loop(0, width // step, col, 0)

    def stage(i, k):
        pairs, offs = steps_of(k)
        if i == 0:
            pl.when(k % 2 == 0)(lambda: form(k))
        elif i == 1:
            reduce_copy(0, k, pairs, offs).start()
        elif i < 5:
            reduce_copy(i - 2, k, pairs, offs).wait_recv()
            add_rows(acc, k, offs[i - 1], part_rows >> (i - 1), landing[i - 2])
            reduce_copy(i - 1, k, pairs, offs).start()
        elif i == 5:
            reduce_copy(3, k, pairs, offs).wait_recv()
            add_rows(gathered, k, offs[3], part_rows >> 3, rl)
            gather_copy(2, k, pairs, offs).start()
        elif i < 8:
            gather_copy(8 - i, k, pairs, offs).wait_recv()
            gather_copy(7 - i, k, pairs, offs).start()
            if i == 6:
                for n in range(4):
                    reduce_copy(n, k, pairs, offs).wait_send()
        elif i == 8:
            gather_copy(0, k, pairs, offs).wait_recv()

            def emit(out):
                last_copy(out, k, core).start()
                store_copy(out, k).start()

            pick(k // PARTS, outs, emit)
        else:

            def close(out):
                last_copy(out, k, 1 - core).wait_recv()
                store_copy(out, k).wait()
                last_copy(out, k, core).wait_send()

            pick(k // PARTS, outs, close)
            for n in range(3):
                gather_copy(n, k, pairs, offs).wait_send()

    def layer_work(t):
        layer = t // LAYER_SLOTS
        at = t - LAYER_SLOTS * layer

        @pl.when(at < 2)
        def _():
            def body(i, carry):
                chain_tile(layer, i)
                return carry

            lax.fori_loop(at * per_slot, at * per_slot + per_slot, body, 0)

        pl.when(at == 2)(lambda: small_begin(layer))
        pl.when(at == 3)(lambda: small_middle(layer))
        pl.when(at == 4)(lambda: small_last(layer))

        @pl.when(at == 5)
        def _():
            small_end(layer)
            pl.when(layer == 1)(lambda: peer_dy(0).wait_send())
            du(layer)
            peer_dy(layer + 1).start()

            @pl.when(layer == 0)
            def _():
                w_tile(weights[1], 0).start()
                u_tile(pres[1], 0).start()

    def slot(t, carry):
        for i in ORDER:
            k = t - BACK_LAGS[i]

            @pl.when((k >= 0) & (k < count))
            def _():
                stage(i, k)

            if i == 1:
                pl.when(t < 2 * LAYER_SLOTS)(lambda: layer_work(t))
        return carry

    lax.fori_loop(0, count + BACK_LAGS[-1], slot, 0)
    for w in range(MATS):
        peer_x(w).wait_send()
    peer_dy(1).wait_send()
    peer_dy(2).wait_send()


def backward(grad_z, x2, x1, x0, w_out, w_mid, u2, u1, vec):
    rows_dev, width = grad_z.shape
    tiles = width // TILE
    part_rows = width // 2 // PARTS
    count = MATS * PARTS
    any_spec = pl.BlockSpec(memory_space=pl.ANY)
    vmem_spec = pl.BlockSpec(memory_space=pltpu.VMEM)
    mat = jax.ShapeDtypeStruct((width, width), jnp.float32)

    def slots(n):
        return pltpu.VMEM((SLOTS, n, width), jnp.float32)

    dma = pltpu.SemaphoreType.DMA
    return pl.pallas_call(
        back_kernel,
        name="backward",
        out_shape=[mat, mat, mat, jax.ShapeDtypeStruct((2, tiles, 2, TILE), jnp.float32)],
        in_specs=[any_spec] * 8 + [vmem_spec],
        out_specs=[any_spec] * 3 + [vmem_spec],
        scratch_shapes=[
            pltpu.VMEM((2, 2 * rows_dev, width), jnp.bfloat16),
            pltpu.VMEM((MATS, 2 * rows_dev, width // 2), jnp.bfloat16),
            pltpu.VMEM((2, WIDE, width), jnp.bfloat16),
            pltpu.VMEM((2, rows_dev, WIDE), jnp.float32),
            pltpu.VMEM((rows_dev, width), jnp.float32),
            pltpu.VMEM((2, tiles, 2, TILE), jnp.float32),
            pltpu.VMEM((2, PLANE, 2, TILE), jnp.float32),
            pltpu.VMEM((2, DEPTH, 2, TILE), jnp.float32),
            pltpu.VMEM((2, 2, 2, TILE), jnp.float32),
            slots(part_rows),
            slots(part_rows),
            slots(part_rows // 2),
            slots(part_rows // 4),
            slots(part_rows // 8),
            slots(part_rows // 8),
            dma((MATS + 1,)),
            dma((2, 2)),
            dma((2 * MATS,)),
            dma((2 * MATS,)),
            dma((2, PLANE)),
            dma((2, PLANE)),
            dma((2, DEPTH)),
            dma((2, DEPTH)),
            dma((2, PLANE)),
            dma((2, PLANE)),
            dma((count,)),
            dma((8, count)),
            dma((8, count)),
        ],
        compiler_params=pltpu.CompilerParams(collective_id=2, has_side_effects=True, vmem_limit_bytes=BACK_VMEM),
    )(grad_z, x2, x1, x0, w_out, w_mid, u2, u1, vec)


def solution(mesh):
    shards = mesh.shape[DATA_AXIS]
    row_part = P(DATA_AXIS, None)
    replicated = P()

    def local_step(feat_a, feat_b, w_in, w_mid, w_out, t_in, t_mid, t_out, gain_1, bias_1, gain_2, bias_2, off_weight):
        row_count = feat_a.shape[0] * shards

        def norm_pair(pre_a, pre_b):
            stat_sums = jnp.stack([jnp.sum(pre_a, axis=0), jnp.sum(pre_a * pre_a, axis=0), jnp.sum(pre_b, axis=0), jnp.sum(pre_b * pre_b, axis=0)])
            stat_means = small_sum(stat_sums) / row_count
            inv_a = lax.rsqrt(stat_means[1] - stat_means[0] * stat_means[0] + NORM_EPS)
            inv_b = lax.rsqrt(stat_means[3] - stat_means[2] * stat_means[2] + NORM_EPS)
            return (pre_a - stat_means[0]) * inv_a, (pre_b - stat_means[2]) * inv_b, stat_means[0], inv_a

        def hidden_pair(in_a, in_b, weight_a, weight_b, gain_vec, bias_vec):
            pre_a = jnp.dot(in_a, weight_a, preferred_element_type=jnp.float32)
            normed_a, normed_b, mean_a, inv_a = norm_pair(pre_a, jnp.dot(in_b, weight_b, preferred_element_type=jnp.float32))
            act_a = jnp.maximum(normed_a * gain_vec + bias_vec, 0.0).astype(jnp.bfloat16)
            act_b = jnp.maximum(normed_b * gain_vec + bias_vec, 0.0).astype(jnp.bfloat16)
            return act_a, act_b, pre_a, [gain_vec, bias_vec, mean_a, inv_a]

        act_1, teach_1, pre_1, vec_1 = hidden_pair(feat_a, feat_b, w_in, t_in, gain_1, bias_1)
        act_2, teach_2, pre_2, vec_2 = hidden_pair(act_1, teach_1, w_mid, t_mid, gain_2, bias_2)
        pre_z = jnp.dot(act_2, w_out, preferred_element_type=jnp.float32)
        zh_a, zh_b, _, inv_z = norm_pair(pre_z, jnp.dot(teach_2, t_out, preferred_element_type=jnp.float32))
        emb_a = zh_a.astype(jnp.bfloat16)
        emb_b = zh_b.astype(jnp.bfloat16)
        corr_part = contract_rows(emb_a, emb_b)
        grad_c, loss_cols = large_sum([corr_part], 8, (3, 7), CorrFinish(row_count), [off_weight.reshape(1)], 1)
        grad_emb = contract_cols(emb_b, grad_c) / row_count
        loss_row = jnp.sum(loss_cols, axis=0)
        stat_sums = small_sum(jnp.stack([jnp.sum(grad_emb, axis=0), jnp.sum(grad_emb * zh_a, axis=0), loss_row]))
        loss_value = jnp.sum(stat_sums[2]) * 0.5
        grad_z = ((grad_emb - stat_sums[0] / row_count - zh_a * (stat_sums[1] / row_count)) * inv_z).astype(jnp.bfloat16)
        grad_w_out, grad_w_mid, grad_w_in, sums = backward(
            grad_z, act_2, act_1, feat_a, w_out, w_mid, pre_2, pre_1, jnp.stack(vec_2 + vec_1)[:, None, :]
        )
        sums = jnp.transpose(sums, (0, 2, 1, 3)).reshape(2, 2, -1)
        return (loss_value, grad_emb, grad_w_in, grad_w_mid, grad_w_out, sums[1, 0], sums[1, 1], sums[0, 0], sums[0, 1])

    return jax.shard_map(local_step, mesh=mesh, in_specs=(row_part, row_part) + (replicated,) * 11, out_specs=(replicated, row_part) + (replicated,) * 7, check_vma=False)
```

```python
import functools

import jax
import jax.numpy as jnp
from jax import lax
from jax.experimental import pallas as pl
from jax.experimental.pallas import tpu as pltpu
from jax.sharding import PartitionSpec as P

NORM_EPS = 1e-5
DATA_AXIS = "data"
MESH = pl.DeviceIdType.MESH
VMEM_BYTES = 67_043_328
PLANE = 8
DEPTH = 4
TILE = 256
WIDE = 512
BLOCK = 32
SUM_ROWS = 4
PARTS = 8
MATS = 3
SLOTS = 12
JOBS = 6
W_BUFS = 3
LAYER_SLOTS = 6
LAGS = (0, 0, 2, 4, 5, 6, 7, 8, 10, 12)
ORDER = (0, 1, 5, 4, 6, 3, 7, 2, 8, 9)
FRONT_Z_FIRST = (2, 6)
BACK_Z_FIRST = (2, 6, 10, 14, 18, 22)


def contract_rows(left_op, right_op):
    return lax.dot_general(left_op, right_op, (((0,), (0,)), ((), ())), preferred_element_type=jnp.float32)


def contract_cols(left_op, right_op):
    return lax.dot_general(left_op, right_op, (((1,), (1,)), ((), ())), preferred_element_type=jnp.float32)


def rows(off, size):
    return pl.ds(pl.multiple_of(off, size), size)


def pick(index, choices, what):
    for i, c in enumerate(choices):
        pl.when(index == i)(functools.partial(what, c))


def loop(lo, hi, body):
    def step(i, carry):
        body(i)
        return carry

    lax.fori_loop(lo, hi, step, 0)


def remote_copy(src, dst, send, recv, mate):
    return pltpu.make_async_remote_copy(src, dst, send, recv, device_id=(mate,), device_id_type=MESH)


class Place:
    def __init__(self):
        me = lax.axis_index(DATA_AXIS)
        self.me = me
        self.pos, self.plane = me % PLANE, me // PLANE
        self.core, self.bx, self.by, self.bz0, self.bz1 = me % 2, (me // 2) % 2, (me // 4) % 2, (me // 8) % 2, (me // 16) % 2
        self.other_core = me + 1 - 2 * self.core
        self.mates = [(self.pos + d) % PLANE for d in range(1, PLANE)]
        self.levels = [(self.plane + d) % DEPTH for d in range(1, DEPTH)]

    def peers(self):
        return [self.plane * PLANE + m for m in self.mates] + [lv * PLANE + self.pos for lv in self.levels]

    def arrive(self):
        sem = pltpu.get_barrier_semaphore()
        for peer in self.peers():
            pl.semaphore_signal(sem, inc=1, device_id=(peer,), device_id_type=MESH)

    def all_here(self):
        pl.semaphore_wait(pltpu.get_barrier_semaphore(), PLANE + DEPTH - 2)


class SmallSum:
    def __init__(self, place, payload, total, plane_buf, depth_buf, own_buf, sems):
        self.p, self.payload, self.total = place, payload, total
        self.plane_buf, self.depth_buf, self.own_buf, self.sems = plane_buf, depth_buf, own_buf, sems

    def first(self, j, m, slot):
        s, r = self.sems[0], self.sems[1]
        return remote_copy(self.payload.at[j, m], self.plane_buf.at[j, slot], s.at[j, m], r.at[j, slot], self.p.plane * PLANE + m)

    def second(self, j, lv, slot):
        s, r = self.sems[2], self.sems[3]
        return remote_copy(self.own_buf.at[j, 0], self.depth_buf.at[j, slot], s.at[j, lv], r.at[j, slot], lv * PLANE + self.p.pos)

    def third(self, j, m, slot):
        s, r = self.sems[4], self.sems[5]
        return remote_copy(self.own_buf.at[j, 1], self.total.at[j, slot], s.at[j, m], r.at[j, slot], self.p.plane * PLANE + m)

    def begin(self, j):
        for m in self.p.mates:
            self.first(j, m, self.p.pos).start()
        self.plane_buf[j, self.p.pos] = self.payload[j, self.p.pos]

    def middle(self, j):
        for m in self.p.mates:
            self.first(j, m, m).wait_recv()
        total = self.plane_buf[j, 0]
        for i in range(1, PLANE):
            total = total + self.plane_buf[j, i]
        self.own_buf[j, 0] = total
        self.depth_buf[j, self.p.plane] = total
        for lv in self.p.levels:
            self.second(j, lv, self.p.plane).start()

    def last(self, j):
        for lv in self.p.levels:
            self.second(j, lv, lv).wait_recv()
        total = self.depth_buf[j, 0]
        for i in range(1, DEPTH):
            total = total + self.depth_buf[j, i]
        self.own_buf[j, 1] = total
        self.total[j, self.p.pos] = total
        for m in self.p.mates:
            self.third(j, m, self.p.pos).start()

    def end(self, j):
        for m in self.p.mates:
            self.third(j, m, m).wait_recv()
            self.first(j, m, self.p.pos).wait_send()
            self.third(j, m, self.p.pos).wait_send()
        for lv in self.p.levels:
            self.second(j, lv, self.p.plane).wait_send()


def small_scratch(count):
    def buf(*lead):
        return pltpu.VMEM((count, *lead, SUM_ROWS, TILE), jnp.float32)

    bufs = [buf(PLANE), buf(PLANE), buf(PLANE), buf(DEPTH), buf(2)]
    return bufs + [pltpu.SemaphoreType.DMA((count, n)) for n in (PLANE, PLANE, DEPTH, DEPTH, PLANE, PLANE)]


SMALL_REFS = 11


def small_sum(place, refs):
    payload, total, plane_buf, depth_buf, own_buf = refs[:5]
    return SmallSum(place, payload, total, plane_buf, depth_buf, own_buf, refs[5:])


class ChunkSum:
    def __init__(self, place, z_first, slots, acc, gathered, landing, send, recv, finish):
        self.p, self.z_first, self.slots = place, z_first, slots
        self.acc, self.gathered, self.landing, self.send, self.recv, self.finish = acc, gathered, landing, send, recv, finish
        self.size = acc.shape[1]
        core, bx, by = place.core, place.bx, place.by
        self.xy = ((2 + 2 * core, core * by + (1 - core) * bx), (4 - 2 * core, core * bx + (1 - core) * by))
        self.zz = ((8, place.bz0), (16, place.bz1))
        self.is_mid = place.bz0 + place.bz1 - 2 * place.bz0 * place.bz1
        self.z_mate = place.me + 8 * (1 - 2 * place.bz0)
        self.mid_mate = place.me + 8 * (1 - 2 * place.bz1)

    def steps(self, k):
        zf = 0
        for z in self.z_first:
            same = k - z
            zf = zf + (1 - lax.min(same * same, 1))
        pairs = []
        for a, b in zip(self.xy + self.zz, self.zz + self.xy):
            stride = zf * b[0] + (1 - zf) * a[0]
            bit = zf * b[1] + (1 - zf) * a[1]
            pairs.append((self.p.me + stride * (1 - 2 * bit), bit))
        offs, size = [0], self.size
        for _, bit in pairs[:3]:
            size = size // 2
            offs.append(offs[-1] + bit * size)
        return zf, pairs, offs

    def copy(self, src, dst, stage, k, mate):
        return remote_copy(src, dst, self.send.at[stage, k], self.recv.at[stage, k], mate)

    def down(self, stage, k, off, size, mate):
        j = k % self.slots
        return self.copy(self.acc.at[j, rows(off, size)], self.landing[stage].at[j, pl.ds(0, size)], stage, k, mate)

    def up(self, stage, k, off, size, mate):
        block = self.gathered.at[k % self.slots, rows(off, size)]
        return self.copy(block, block, stage, k, mate)

    def add(self, k, off, size, buf):
        step = min(size, 16)
        j = k % self.slots

        def body(i):
            at = rows(off + i * step, step)
            self.acc[j, at] = self.acc[j, at] + buf[j, rows(i * step, step)]

        loop(0, size // step, body)

    def close(self, k, off, size):
        step = min(size, 16)

        def body(i):
            self.finish(k, off + i * step, step, self.landing[3], i * step)

        loop(0, size // step, body)

    def stage(self, i, k):
        zf, pairs, offs = self.steps(k)
        s2, s4, s8 = self.size // 2, self.size // 4, self.size // 8
        l1, l2, l3, l4 = self.landing
        keep = self.is_mid
        z_first = zf == 1
        mid = (zf == 0) & (keep == 1)
        end = (zf == 0) & (keep == 0)

        half_copy = lambda: self.down(0, k, offs[0] + (1 - pairs[0][1]) * s2, s2, pairs[0][0])
        quarter_copy = lambda: self.down(1, k, offs[1] + (1 - pairs[1][1]) * s4, s4, pairs[1][0])
        eighth_copy = lambda: self.down(2, k, offs[2] + (1 - pairs[2][1]) * s8, s8, pairs[2][0])
        whole_copy = lambda: self.down(3, k, offs[3], s8, pairs[3][0])
        inward = lambda: self.down(2, k, offs[2], s4, self.z_mate)
        across = lambda: self.down(3, k, offs[2], s4, self.mid_mate)
        back8 = lambda: self.up(4, k, offs[3], s8, pairs[2][0])
        outward = lambda: self.up(4, k, offs[2], s4, self.z_mate)
        back4 = lambda: self.up(5, k, offs[2], s4, pairs[1][0])
        back2 = lambda: self.up(6, k, offs[1], s2, pairs[0][0])

        if i == 1:
            half_copy().start()
        elif i == 2:
            half_copy().wait_recv()
            self.add(k, offs[1], s2, l1)
            quarter_copy().start()
        elif i == 3:
            quarter_copy().wait_recv()
            self.add(k, offs[2], s4, l2)
            pl.when(z_first)(lambda: eighth_copy().start())
            pl.when(end)(lambda: inward().start())
        elif i == 4:

            @pl.when(z_first)
            def _():
                eighth_copy().wait_recv()
                self.add(k, offs[3], s8, l3)
                whole_copy().start()

            @pl.when(mid)
            def _():
                inward().wait_recv()
                self.add(k, offs[2], s4, l3)
                across().start()

        elif i == 5:

            @pl.when(z_first)
            def _():
                whole_copy().wait_recv()
                self.close(k, offs[3], s8)
                back8().start()

            @pl.when(mid)
            def _():
                across().wait_recv()
                self.close(k, offs[2], s4)
                outward().start()

        elif i == 6:
            pl.when(z_first)(lambda: back8().wait_recv())
            pl.when(end)(lambda: outward().wait_recv())
            back4().start()
            half_copy().wait_send()
            quarter_copy().wait_send()

            @pl.when(z_first)
            def _():
                eighth_copy().wait_send()
                whole_copy().wait_send()

            pl.when(end)(lambda: inward().wait_send())
            pl.when(mid)(lambda: across().wait_send())
        elif i == 7:
            back4().wait_recv()
            back2().start()
        elif i == 8:
            back2().wait_recv()
        else:
            pl.when(z_first)(lambda: back8().wait_send())
            pl.when(mid)(lambda: outward().wait_send())
            back4().wait_send()
            back2().wait_send()


def run_slots(count, stage, between):
    def slot(t):
        for i in ORDER:
            k = t - LAGS[i]

            @pl.when((k >= 0) & (k < count))
            def _():
                stage(i, k)

            if i == 1:
                between(t)

    loop(0, count + LAGS[-1], slot)


def chunk_scratch(slots, part_rows, width, count, dtype):
    def buf(n, kind=jnp.float32):
        return pltpu.VMEM((slots, n, width), kind)

    dma = pltpu.SemaphoreType.DMA
    return [buf(part_rows), buf(part_rows, dtype), buf(part_rows // 2), buf(part_rows // 4), buf(part_rows // 4), buf(part_rows // 4)] + [
        dma((8, count)),
        dma((8, count)),
    ]


CHUNK_REFS = 8


def fold(value):
    return jnp.sum(value.reshape(value.shape[0] // 8, 8, value.shape[1]), axis=0)


def front_kernel(feat_a, feat_b, w_in, t_in, w_mid, t_mid, w_out, t_out, affine, off_weight, pre1, pre2, act1, act2, dz, grad_emb, vec, loss, *scratch):
    (x_buf, u_buf, w_buf, stats, ea, eb, g_peer) = scratch[:7]
    (x_sem, w_sem, keep_sem, ge_sem, e_send, e_recv) = scratch[7:13]
    small_refs = scratch[13 : 13 + SMALL_REFS]
    acc, gathered, l1, l2, l3, l4, send, recv = scratch[13 + SMALL_REFS :]
    rows_dev, width = feat_a.shape
    wide = w_buf.shape[2]
    tiles = width // wide
    half = width // 2
    part_rows = half // PARTS
    row_count = rows_dev * DEPTH * PLANE
    weights, feats = (w_in, t_in, w_mid, t_mid, w_out, t_out), (feat_a, feat_b)
    place = Place()
    core = place.core
    mine = rows(core * rows_dev, rows_dev)
    place.arrive()
    small = small_sum(place, small_refs)
    payload, total = small.payload, small.total

    def feat(v):
        return pltpu.make_async_copy(feats[v], x_buf.at[v], x_sem.at[v])

    def w_tile(ref, g):
        return pltpu.make_async_copy(ref.at[:, rows((g % tiles) * wide, wide)], w_buf.at[g % W_BUFS], w_sem.at[g % W_BUFS])

    def start_w(g):
        pick(g // tiles, weights, lambda ref: w_tile(ref, g).start())

    feat(0).start()
    w_tile(weights[0], 0).start()
    feat(1).start()
    for g in range(1, W_BUFS - 1):
        start_w(g)
    feat(0).wait()
    payload[...] = jnp.zeros_like(payload)

    def keep_pre(ref):
        return pltpu.make_async_copy(u_buf.at[0], ref, keep_sem.at[0])

    def keep_act(ref):
        return pltpu.make_async_copy(x_buf.at[0], ref, keep_sem.at[1])

    def row_loop(body, carry):
        return lax.fori_loop(0, rows_dev // BLOCK, lambda r, c: body(rows(r * BLOCK, BLOCK), c), carry)

    def put_sums(j, i, row, value):
        value = jnp.sum(value, axis=0, keepdims=True)
        for c in range(value.shape[1] // TILE):
            payload[j, i + c, row : row + 1] = value[:, c * TILE : (c + 1) * TILE]

    def product(g):
        job, i = g // tiles, g % tiles
        view = job % 2
        w_tile(w_in, g).wait()
        pl.when(g + W_BUFS - 1 < JOBS * tiles)(lambda: start_w(g + W_BUFS - 1))
        at_cols = rows(i * wide, wide)
        u_buf[view, :, at_cols] = jnp.dot(x_buf[view], w_buf[g % W_BUFS], preferred_element_type=jnp.float32)

        def block(at, sums):
            u = u_buf[view, at, at_cols]
            return sums[0] + fold(u), sums[1] + fold(u * u)

        zero = jnp.zeros((8, wide), jnp.float32)
        for row, value in enumerate(row_loop(block, (zero, zero))):
            put_sums(job, i * (wide // TILE), row, value)

    def begin(job):
        small.begin(job)

        @pl.when(job % 2 == 0)
        def _():
            pick(job // 2, (pre1, pre2), lambda ref: keep_pre(ref).start())

    def norm(job):
        layer, view = job // 2, job % 2
        small.end(job)
        for c in range(PLANE):
            at = slice(c * TILE, (c + 1) * TILE)
            means = total[job, c] / row_count
            stats[job, 0, :, at] = means[0:1]
            stats[job, 1, :, at] = lax.rsqrt(means[1:2] - means[0:1] * means[0:1] + NORM_EPS)

        @pl.when((view == 0) & (layer == 1))
        def _():
            keep_act(act1).wait()

        @pl.when((view == 0) & (layer == 2))
        def _():
            keep_act(act2).wait()

        def hidden(i):
            at_cols = rows(i * wide, wide)
            mean, inv = stats[job, 0, :, at_cols], stats[job, 1, :, at_cols]
            gain, bias = affine[layer * 2, :, at_cols], affine[layer * 2 + 1, :, at_cols]

            def block(at, c):
                n = (u_buf[view, at, at_cols] - mean) * inv
                x_buf[view, at, at_cols] = jnp.maximum(n * gain + bias, 0.0).astype(jnp.bfloat16)
                return c

            row_loop(block, 0)

        def student(i):
            at_cols = rows(i * wide, wide)
            mean, inv = stats[job, 0, :, at_cols], stats[job, 1, :, at_cols]

            def block(at, c):
                n = (u_buf[0, at, at_cols] - mean) * inv
                u_buf[0, at, at_cols] = n
                x_buf[0, at, at_cols] = n.astype(jnp.bfloat16)
                return c

            row_loop(block, 0)

        def student_own(i):
            def block(r, c):
                ea[rows(core * rows_dev + r * BLOCK, BLOCK), rows(i * wide, wide)] = x_buf[0, rows(r * BLOCK, BLOCK), rows(core * half + i * wide, wide)]
                return c

            lax.fori_loop(0, rows_dev // BLOCK, block, 0)

        def teacher(i):
            at_cols = rows(i * wide, wide)
            mean, inv = stats[job, 0, :, at_cols], stats[job, 1, :, at_cols]

            def block(r, c):
                n = (u_buf[1, rows(r * BLOCK, BLOCK), at_cols] - mean) * inv
                eb[rows(core * rows_dev + r * BLOCK, BLOCK), at_cols] = n.astype(jnp.bfloat16)
                return c

            lax.fori_loop(0, rows_dev // BLOCK, block, 0)

        @pl.when(layer < 2)
        def _():
            loop(0, tiles, hidden)

            @pl.when(view == 0)
            def _():
                pick(layer, (act1, act2), lambda ref: keep_act(ref).start())
                keep_pre(pre1).wait()

        @pl.when((layer == 2) & (view == 0))
        def _():
            loop(0, tiles, student)
            ea_copy().start()
            loop(0, tiles // 2, student_own)

        @pl.when((layer == 2) & (view == 1))
        def _():
            loop(0, tiles, teacher)
            eb_copy().start()

    ea_copy = lambda: remote_copy(x_buf.at[0, :, rows((1 - core) * half, half)], ea.at[mine], e_send.at[0], e_recv.at[0], place.other_core)
    eb_copy = lambda: remote_copy(eb.at[mine], eb.at[mine], e_send.at[1], e_recv.at[1], place.other_core)

    def step(g):
        job, i = g // tiles, g % tiles
        view = job % 2
        pl.when(g == tiles)(lambda: feat(1).wait())
        product(g)
        pl.when(g == tiles - 1)(lambda: place.all_here())

        @pl.when((view == 0) & (i == 0) & (job > 0))
        def _():
            small.last(job - 1)

        @pl.when((view == 1) & (i == tiles // 2 - 1))
        def _():
            small.middle(job - 1)

        @pl.when(i == tiles - 1)
        def _():
            begin(job)

            @pl.when(view == 1)
            def _():
                small.last(job - 1)
                small.middle(job)

            pl.when(job > 0)(lambda: norm(job - 1))

    loop(0, JOBS * tiles, step)
    small.last(JOBS - 1)
    norm(JOBS - 1)
    for j, source in enumerate((affine.at[2], affine.at[3], stats.at[2, 0], stats.at[2, 1], affine.at[0], affine.at[1], stats.at[0, 0], stats.at[0, 1])):
        vec[j] = source[...]

    loss[...] = jnp.zeros_like(loss)

    def finish(k, off, size, buf, buf_off):
        at = rows(off, size)
        corr = (acc[k, at] + buf[k, rows(buf_off, size)]) / row_count
        row = core * half + k * part_rows + off
        diag = (row + lax.broadcasted_iota(jnp.int32, (size, width), 0)) == lax.broadcasted_iota(jnp.int32, (size, width), 1)
        weight = off_weight[0]
        miss = 1.0 - corr
        loss[...] += jnp.sum(jnp.where(diag, miss * miss, weight * (corr * corr)), axis=0, keepdims=True)
        gathered[k, at] = jnp.where(diag, -2.0 * miss, 2.0 * weight * corr).astype(jnp.bfloat16)

    chunks = ChunkSum(place, FRONT_Z_FIRST, PARTS, acc, gathered, (l1, l2, l3, l4), send, recv, finish)

    def form(k):
        @pl.when(k == 0)
        def _():
            ea_copy().wait_recv()
            eb_copy().wait_recv()

        at = rows(k * part_rows, 2 * part_rows)
        size = min(1024, width)

        def col(c):
            cs = rows(c * size, size)
            acc[pl.ds(k, 2), :, cs] = contract_rows(ea[:, at], eb[:, cs]).reshape(2, part_rows, size)

        loop(0, width // size, col)

    def swap(k):
        return chunks.copy(gathered.at[k], g_peer.at[k], 7, k, place.other_core)

    def ge_cols(k, side):
        return rows(side * half + k * part_rows, 2 * part_rows)

    def ge_copy(k, side):
        at = ge_cols(k, side)
        return pltpu.make_async_copy(u_buf.at[1, :, at], grad_emb.at[:, at], ge_sem.at[k // 2, side])

    def embed(k, side, g_rows):
        at_cols = ge_cols(k, side)
        grad = contract_cols(eb[mine], g_rows.reshape(2 * part_rows, width)) / row_count
        u_buf[1, :, at_cols] = grad
        ge_copy(k, side).start()

        def block(at, sums):
            g = u_buf[1, at, at_cols]
            return sums[0] + fold(g * u_buf[0, at, at_cols]), sums[1] + fold(g)

        zero = jnp.zeros((8, 2 * part_rows), jnp.float32)
        for row, value in enumerate(row_loop(block, (zero, zero))):
            payload[JOBS, (side * half + k * part_rows) // TILE, row : row + 1] = jnp.sum(value, axis=0, keepdims=True)

    def stage(i, k):
        if i == 0:
            pl.when(k % 2 == 0)(lambda: form(k))
            return
        chunks.stage(i, k)
        if i == 8:
            swap(k).start()

            @pl.when(k % 2 == 1)
            def _():
                embed(k - 1, core, gathered[pl.ds(k - 1, 2)])

        if i == 9:
            swap(k).wait_recv()
            swap(k).wait_send()

            @pl.when(k % 2 == 1)
            def _():
                embed(k - 1, 1 - core, g_peer[pl.ds(k - 1, 2)])

    run_slots(PARTS, stage, lambda t: None)
    for c in range(PLANE):
        payload[JOBS, c, 2:3] = loss[:, c * TILE : (c + 1) * TILE]
    small.begin(JOBS)
    ea_copy().wait_send()
    eb_copy().wait_send()
    small.middle(JOBS)
    for k in range(0, PARTS, 2):
        for side in range(2):
            ge_copy(k, side).wait()
    small.last(JOBS)
    small.end(JOBS)

    def dz_tile(i):
        at_cols = rows(i * wide, wide)
        sums = jnp.concatenate([total[JOBS, i * (wide // TILE) + c] for c in range(wide // TILE)], axis=1) / row_count
        mean_gn, mean_g = sums[0:1], sums[1:2]
        inv = stats[JOBS - 2, 1, :, at_cols]

        def block(at, c):
            value = (u_buf[1, at, at_cols] - mean_g - u_buf[0, at, at_cols] * mean_gn) * inv
            x_buf[0, at, at_cols] = value.astype(jnp.bfloat16)
            return c

        row_loop(block, 0)

    loop(0, tiles, dz_tile)
    keep_act(dz).start()
    for c in range(PLANE):
        loss[:, c * TILE : (c + 1) * TILE] = total[JOBS, c, 2:3]
    keep_act(dz).wait()


def front(feat_a, feat_b, weights, affine, off_weight):
    rows_dev, width = feat_a.shape
    half = width // 2
    part_rows = half // PARTS
    any_spec = pl.BlockSpec(memory_space=pl.ANY)
    vmem_spec = pl.BlockSpec(memory_space=pltpu.VMEM)
    wide_f32 = jax.ShapeDtypeStruct((rows_dev, width), jnp.float32)
    wide_bf16 = jax.ShapeDtypeStruct((rows_dev, width), jnp.bfloat16)
    dma = pltpu.SemaphoreType.DMA
    return pl.pallas_call(
        front_kernel,
        name="front",
        out_shape=[wide_f32, wide_f32, wide_bf16, wide_bf16, wide_bf16, wide_f32]
        + [jax.ShapeDtypeStruct((8, 1, width), jnp.float32), jax.ShapeDtypeStruct((1, width), jnp.float32)],
        in_specs=[any_spec] * 8 + [vmem_spec, pl.BlockSpec(memory_space=pltpu.SMEM)],
        out_specs=[any_spec] * 6 + [vmem_spec] * 2,
        scratch_shapes=[
            pltpu.VMEM((2, rows_dev, width), jnp.bfloat16),
            pltpu.VMEM((2, rows_dev, width), jnp.float32),
            pltpu.VMEM((W_BUFS, width, WIDE), jnp.bfloat16),
            pltpu.VMEM((JOBS, 2, 1, width), jnp.float32),
            pltpu.VMEM((2 * rows_dev, half), jnp.bfloat16),
            pltpu.VMEM((2 * rows_dev, width), jnp.bfloat16),
            pltpu.VMEM((PARTS, part_rows, width), jnp.bfloat16),
            dma((2,)),
            dma((W_BUFS,)),
            dma((2,)),
            dma((PARTS // 2, 2)),
            dma((2,)),
            dma((2,)),
        ]
        + small_scratch(JOBS + 1)
        + chunk_scratch(PARTS, part_rows, width, PARTS, jnp.bfloat16),
        compiler_params=pltpu.CompilerParams(collective_id=0, has_side_effects=True, vmem_limit_bytes=VMEM_BYTES),
    )(feat_a, feat_b, *weights, affine, off_weight)


def back_kernel(dz_hbm, x2, x1, x0, w_out, w_mid, u2, u1, vec, out2, out1, out0, sums_out, *scratch):
    (dy, xs, w_buf, u_buf, dpre) = scratch[:5]
    (in_sem, tile_sem, peer_send, peer_recv, store_sem) = scratch[5:10]
    small_refs = scratch[10 : 10 + SMALL_REFS]
    acc, gathered, l1, l2, l3, l4, send, recv = scratch[10 + SMALL_REFS :]
    rows_dev, width = dz_hbm.shape
    wide = w_buf.shape[1]
    tiles = width // wide
    per_slot = tiles // 2
    row_count = rows_dev * DEPTH * PLANE
    half = width // 2
    part_rows = half // PARTS
    count = MATS * PARTS
    mats_in, outs, weights, pres = (x2, x1, x0), (out2, out1, out0), (w_out, w_mid), (u2, u1)
    place = Place()
    core, other_core = place.core, place.other_core
    mine = rows(core * rows_dev, rows_dev)
    place.arrive()
    small = small_sum(place, small_refs)
    payload, sums = small.payload, small.total

    def own_x(w):
        return pltpu.make_async_copy(mats_in[w].at[:, rows(core * half, half)], xs.at[w % 2, mine], in_sem.at[w])

    def peer_x(w):
        return remote_copy(mats_in[w].at[:, rows((1 - core) * half, half)], xs.at[w % 2, mine], peer_send.at[w], peer_recv.at[w], other_core)

    def peer_dy(w):
        block = dy.at[w % 2, mine]
        return remote_copy(block, block, peer_send.at[MATS + w], peer_recv.at[MATS + w], other_core)

    def x_arrive(w):
        block = xs.at[w % 2, mine]
        pltpu.make_async_copy(block, block, in_sem.at[w]).wait()
        remote_copy(block, block, peer_send.at[w], peer_recv.at[w], other_core).wait_recv()

    def w_tile(ref, i):
        return pltpu.make_async_copy(ref.at[rows(i * wide, wide)], w_buf.at[i % 2], tile_sem.at[0, i % 2])

    def u_tile(ref, i):
        return pltpu.make_async_copy(ref.at[:, rows(i * wide, wide)], u_buf.at[i % 2], tile_sem.at[1, i % 2])

    def start_w(layer, i):
        pick(layer, weights, lambda ref: w_tile(ref, i).start())

    def start_u(layer, i):
        pick(layer, pres, lambda ref: u_tile(ref, i).start())

    dz_load = pltpu.make_async_copy(dz_hbm, dy.at[0, mine], in_sem.at[MATS])
    dz_load.start()
    for w in range(2):
        own_x(w).start()
    w_tile(weights[0], 0).start()
    u_tile(pres[0], 0).start()
    payload[...] = jnp.zeros_like(payload)
    place.all_here()
    peer_x(0).start()
    dz_load.wait()
    peer_dy(0).start()
    peer_x(1).start()

    def row_loop(body, carry):
        return lax.fori_loop(0, rows_dev // BLOCK, body, carry)

    def chain_tile(layer, i):
        w_tile(w_out, i).wait()
        u_tile(u2, i).wait()

        @pl.when(i + 1 < tiles)
        def _():
            start_w(layer, i + 1)
            start_u(layer, i + 1)

        at_cols = rows(i * wide, wide)
        dpre[:, at_cols] = contract_cols(dy[layer, mine], w_buf[i % 2])
        gain, bias, mean, inv = (vec[layer * 4 + j, :, at_cols] for j in range(4))

        def block(r, carry):
            at = rows(r * BLOCK, BLOCK)
            n = (u_buf[i % 2, at] - mean) * inv
            g = jnp.where(n * gain + bias > 0.0, dpre[at, at_cols], 0.0)
            dpre[at, at_cols] = g
            return carry[0] + fold(g * n), carry[1] + fold(g)

        zero = jnp.zeros((8, wide), jnp.float32)
        for row, value in enumerate(row_loop(block, (zero, zero))):
            value = jnp.sum(value, axis=0, keepdims=True)
            for c in range(wide // TILE):
                payload[layer, i * (wide // TILE) + c, row : row + 1] = value[:, c * TILE : (c + 1) * TILE]

    def du(layer):
        start_u(layer, 0)

        def tile(i):
            u_tile(u2, i).wait()
            pl.when(i + 1 < tiles)(lambda: start_u(layer, i + 1))
            at_cols = rows(i * wide, wide)
            gain, mean, inv = (vec[layer * 4 + j, :, at_cols] for j in (0, 2, 3))
            means = jnp.concatenate([sums[layer, i * (wide // TILE) + c] for c in range(wide // TILE)], axis=1) / row_count
            mean_gn, mean_g = means[0:1], means[1:2]
            scale = gain * inv

            def block(r, c):
                at = rows(r * BLOCK, BLOCK)
                n = (u_buf[i % 2, at] - mean) * inv
                value = (dpre[at, at_cols] - mean_g - n * mean_gn) * scale
                dy[1 - layer, rows(core * rows_dev + r * BLOCK, BLOCK), at_cols] = value.astype(jnp.bfloat16)
                return c

            row_loop(block, 0)

        loop(0, tiles, tile)

    def finish(k, off, size, buf, buf_off):
        j = k % SLOTS
        gathered[j, rows(off, size)] = acc[j, rows(off, size)] + buf[j, rows(buf_off, size)]

    chunks = ChunkSum(place, BACK_Z_FIRST, SLOTS, acc, gathered, (l1, l2, l3, l4), send, recv, finish)

    def form(k):
        w, j = k // PARTS, k % SLOTS

        @pl.when(k % PARTS == 0)
        def _():
            x_arrive(w)
            peer_dy(w).wait_recv()

        at = rows((k % PARTS) * part_rows, 2 * part_rows)
        size = min(1024, width)

        def col(c):
            cs = rows(c * size, size)
            acc[pl.ds(j, 2), :, cs] = contract_rows(xs[w % 2, :, at], dy[w % 2, :, cs]).reshape(2, part_rows, size)

        loop(0, width // size, col)

    def out_rows(k, side):
        return pl.ds(pl.multiple_of(side * half + (k % PARTS) * part_rows, part_rows), part_rows)

    def last_copy(out, k, side):
        return chunks.copy(gathered.at[k % SLOTS], out.at[out_rows(k, side)], 7, k, other_core)

    def store_copy(out, k):
        return pltpu.make_async_copy(gathered.at[k % SLOTS], out.at[out_rows(k, core)], store_sem.at[k])

    def stage(i, k):
        if i == 0:
            pl.when(k % 2 == 0)(lambda: form(k))
            return
        chunks.stage(i, k)
        if i == 8:

            def emit(out):
                last_copy(out, k, core).start()
                store_copy(out, k).start()

            pick(k // PARTS, outs, emit)
        if i == 9:

            def close(out):
                last_copy(out, k, 1 - core).wait_recv()
                store_copy(out, k).wait()
                last_copy(out, k, core).wait_send()

            pick(k // PARTS, outs, close)

    def layer_work(t):
        layer = t // LAYER_SLOTS
        at = t - LAYER_SLOTS * layer
        pl.when(at < 2)(lambda: loop(at * per_slot, at * per_slot + per_slot, lambda i: chain_tile(layer, i)))
        pl.when(at == 2)(lambda: small.begin(layer))
        pl.when(at == 3)(lambda: small.middle(layer))
        pl.when(at == 4)(lambda: small.last(layer))

        @pl.when(at == 5)
        def _():
            small.end(layer)
            pl.when(layer == 1)(lambda: peer_dy(0).wait_send())
            du(layer)
            peer_dy(layer + 1).start()

            @pl.when(layer == 0)
            def _():
                w_tile(weights[1], 0).start()
                u_tile(pres[1], 0).start()

            @pl.when(layer == 1)
            def _():
                peer_x(0).wait_send()
                own_x(2).start()
                peer_x(2).start()

    run_slots(count, stage, lambda t: pl.when(t < 2 * LAYER_SLOTS)(lambda: layer_work(t)))
    for w in (1, 2):
        peer_x(w).wait_send()
        peer_dy(w).wait_send()
    sums_out[...] = sums[...]


def backward(grad_z, x2, x1, x0, w_out, w_mid, u2, u1, vec):
    rows_dev, width = grad_z.shape
    part_rows = width // 2 // PARTS
    count = MATS * PARTS
    any_spec = pl.BlockSpec(memory_space=pl.ANY)
    vmem_spec = pl.BlockSpec(memory_space=pltpu.VMEM)
    mat = jax.ShapeDtypeStruct((width, width), jnp.float32)
    dma = pltpu.SemaphoreType.DMA
    return pl.pallas_call(
        back_kernel,
        name="backward",
        out_shape=[mat, mat, mat, jax.ShapeDtypeStruct((2, PLANE, SUM_ROWS, TILE), jnp.float32)],
        in_specs=[any_spec] * 8 + [vmem_spec],
        out_specs=[any_spec] * 3 + [vmem_spec],
        scratch_shapes=[
            pltpu.VMEM((2, 2 * rows_dev, width), jnp.bfloat16),
            pltpu.VMEM((2, 2 * rows_dev, width // 2), jnp.bfloat16),
            pltpu.VMEM((2, WIDE, width), jnp.bfloat16),
            pltpu.VMEM((2, rows_dev, WIDE), jnp.float32),
            pltpu.VMEM((rows_dev, width), jnp.float32),
            dma((MATS + 1,)),
            dma((2, 2)),
            dma((2 * MATS,)),
            dma((2 * MATS,)),
            dma((count,)),
        ]
        + small_scratch(2)
        + chunk_scratch(SLOTS, part_rows, width, count, jnp.float32),
        compiler_params=pltpu.CompilerParams(collective_id=1, has_side_effects=True, vmem_limit_bytes=VMEM_BYTES),
    )(grad_z, x2, x1, x0, w_out, w_mid, u2, u1, vec)


def solution(mesh):
    row_part = P(DATA_AXIS, None)
    replicated = P()

    def local_step(feat_a, feat_b, w_in, w_mid, w_out, t_in, t_mid, t_out, gain_1, bias_1, gain_2, bias_2, off_weight):
        affine = jnp.stack([gain_1, bias_1, gain_2, bias_2])[:, None, :]
        pre_1, pre_2, act_1, act_2, grad_z, grad_emb, vec, loss_cols = front(
            feat_a, feat_b, (w_in, t_in, w_mid, t_mid, w_out, t_out), affine, off_weight.reshape(1)
        )
        loss_value = jnp.sum(loss_cols) * 0.5
        grad_w_out, grad_w_mid, grad_w_in, sums = backward(grad_z, act_2, act_1, feat_a, w_out, w_mid, pre_2, pre_1, vec)
        sums = jnp.transpose(sums[:, :, :2], (0, 2, 1, 3)).reshape(2, 2, -1)
        return (loss_value, grad_emb, grad_w_in, grad_w_mid, grad_w_out, sums[1, 0], sums[1, 1], sums[0, 0], sums[0, 1])

    return jax.shard_map(local_step, mesh=mesh, in_specs=(row_part, row_part) + (replicated,) * 11, out_specs=(replicated, row_part) + (replicated,) * 7, check_vma=False)
```

```python
import functools

import jax
import jax.numpy as jnp
from jax import lax
from jax.experimental import pallas as pl
from jax.experimental.pallas import tpu as pltpu
from jax.sharding import PartitionSpec as P

NORM_EPS = 1e-5
DATA_AXIS = "data"
MESH = pl.DeviceIdType.MESH
VMEM_BYTES = 67_043_328
PLANE = 8
DEPTH = 4
TILE = 256
WIDE = 512
BLOCK = 128
SUM_ROWS = 4
PARTS = 16
GROUP = 4
MATS = 3
SLOTS = 16
JOBS = 6
W_BUFS = 3
LAYER_SLOTS = 8
LAGS = (0, 0, 2, 4, 5, 6, 7, 8, 10, 12)
ORDER = (0, 1, 5, 4, 6, 3, 7, 2, 8, 9)
Z_FIRST_EVERY, Z_FIRST_AT = 4, 2


def contract_rows(left_op, right_op):
    return lax.dot_general(left_op, right_op, (((0,), (0,)), ((), ())), preferred_element_type=jnp.float32)


def contract_cols(left_op, right_op):
    return lax.dot_general(left_op, right_op, (((1,), (1,)), ((), ())), preferred_element_type=jnp.float32)


def rows(off, size):
    return pl.ds(pl.multiple_of(off, size), size)


def pick(index, choices, what):
    for i, c in enumerate(choices):
        pl.when(index == i)(functools.partial(what, c))


def loop(lo, hi, body):
    def step(i, carry):
        body(i)
        return carry

    lax.fori_loop(lo, hi, step, 0)


def remote_copy(src, dst, send, recv, mate):
    return pltpu.make_async_remote_copy(src, dst, send, recv, device_id=(mate,), device_id_type=MESH)


class Place:
    def __init__(self):
        me = lax.axis_index(DATA_AXIS)
        self.me = me
        self.pos, self.plane = me % PLANE, me // PLANE
        self.core, self.bx, self.by, self.bz0, self.bz1 = me % 2, (me // 2) % 2, (me // 4) % 2, (me // 8) % 2, (me // 16) % 2
        self.other_core = me + 1 - 2 * self.core
        self.mates = [(self.pos + d) % PLANE for d in range(1, PLANE)]
        self.levels = [(self.plane + d) % DEPTH for d in range(1, DEPTH)]

    def peers(self):
        return [self.plane * PLANE + m for m in self.mates] + [lv * PLANE + self.pos for lv in self.levels]

    def arrive(self):
        sem = pltpu.get_barrier_semaphore()
        for peer in self.peers():
            pl.semaphore_signal(sem, inc=1, device_id=(peer,), device_id_type=MESH)

    def all_here(self):
        pl.semaphore_wait(pltpu.get_barrier_semaphore(), PLANE + DEPTH - 2)


class SmallSum:
    def __init__(self, place, payload, total, plane_buf, depth_buf, own_buf, sems):
        self.p, self.payload, self.total = place, payload, total
        self.plane_buf, self.depth_buf, self.own_buf, self.sems = plane_buf, depth_buf, own_buf, sems

    def first(self, j, m, slot):
        s, r = self.sems[0], self.sems[1]
        return remote_copy(self.payload.at[j, m], self.plane_buf.at[j, slot], s.at[j, m], r.at[j, slot], self.p.plane * PLANE + m)

    def second(self, j, lv, slot):
        s, r = self.sems[2], self.sems[3]
        return remote_copy(self.own_buf.at[j, 0], self.depth_buf.at[j, slot], s.at[j, lv], r.at[j, slot], lv * PLANE + self.p.pos)

    def third(self, j, m, slot):
        s, r = self.sems[4], self.sems[5]
        return remote_copy(self.own_buf.at[j, 1], self.total.at[j, slot], s.at[j, m], r.at[j, slot], self.p.plane * PLANE + m)

    def begin(self, j):
        for m in self.p.mates:
            self.first(j, m, self.p.pos).start()
        self.plane_buf[j, self.p.pos] = self.payload[j, self.p.pos]

    def middle(self, j):
        for m in self.p.mates:
            self.first(j, m, m).wait_recv()
        total = self.plane_buf[j, 0]
        for i in range(1, PLANE):
            total = total + self.plane_buf[j, i]
        self.own_buf[j, 0] = total
        self.depth_buf[j, self.p.plane] = total
        for lv in self.p.levels:
            self.second(j, lv, self.p.plane).start()

    def last(self, j):
        for lv in self.p.levels:
            self.second(j, lv, lv).wait_recv()
        total = self.depth_buf[j, 0]
        for i in range(1, DEPTH):
            total = total + self.depth_buf[j, i]
        self.own_buf[j, 1] = total
        self.total[j, self.p.pos] = total
        for m in self.p.mates:
            self.third(j, m, self.p.pos).start()

    def end(self, j):
        for m in self.p.mates:
            self.third(j, m, m).wait_recv()
            self.first(j, m, self.p.pos).wait_send()
            self.third(j, m, self.p.pos).wait_send()
        for lv in self.p.levels:
            self.second(j, lv, self.p.plane).wait_send()


def small_scratch(count):
    def buf(*lead):
        return pltpu.VMEM((count, *lead, SUM_ROWS, TILE), jnp.float32)

    bufs = [buf(PLANE), buf(PLANE), buf(PLANE), buf(DEPTH), buf(2)]
    return bufs + [pltpu.SemaphoreType.DMA((count, n)) for n in (PLANE, PLANE, DEPTH, DEPTH, PLANE, PLANE)]


SMALL_REFS = 11


def small_sum(place, refs):
    payload, total, plane_buf, depth_buf, own_buf = refs[:5]
    return SmallSum(place, payload, total, plane_buf, depth_buf, own_buf, refs[5:])


class ChunkSum:
    def __init__(self, place, slots, acc, gathered, landing, send, recv, finish):
        self.p, self.slots = place, slots
        self.acc, self.gathered, self.landing, self.send, self.recv, self.finish = acc, gathered, landing, send, recv, finish
        self.size = acc.shape[1]
        core, bx, by = place.core, place.bx, place.by
        self.xy = ((2 + 2 * core, core * by + (1 - core) * bx), (4 - 2 * core, core * bx + (1 - core) * by))
        self.zz = ((8, place.bz0), (16, place.bz1))
        self.is_mid = place.bz0 + place.bz1 - 2 * place.bz0 * place.bz1
        self.z_mate = place.me + 8 * (1 - 2 * place.bz0)
        self.mid_mate = place.me + 8 * (1 - 2 * place.bz1)

    def z_first(self, k):
        off = k % Z_FIRST_EVERY - Z_FIRST_AT
        return 1 - lax.min(off * off, 1)

    def steps(self, k):
        zf = self.z_first(k)
        pairs = []
        for a, b in zip(self.xy + self.zz, self.zz + self.xy):
            stride = zf * b[0] + (1 - zf) * a[0]
            bit = zf * b[1] + (1 - zf) * a[1]
            pairs.append((self.p.me + stride * (1 - 2 * bit), bit))
        s2, s4 = self.size // 2, self.size // 4
        offs = (0, pairs[0][1] * s2, pairs[0][1] * s2 + pairs[1][1] * s4)
        return zf, pairs, offs

    def copy(self, src, dst, stage, k, mate):
        return remote_copy(src, dst, self.send.at[stage, k], self.recv.at[stage, k], mate)

    def down(self, stage, k, off, size, mate):
        j = k % self.slots
        return self.copy(self.acc.at[j, rows(off, size)], self.landing[stage].at[j], stage, k, mate)

    def up(self, stage, k, off, size, mate):
        block = self.gathered.at[k % self.slots, rows(off, size)]
        return self.copy(block, block, stage, k, mate)

    def add(self, k, off, size, buf):
        step = min(size, 16)
        j = k % self.slots

        def body(i):
            at = rows(off + i * step, step)
            self.acc[j, at] = self.acc[j, at] + buf[j, rows(i * step, step)]

        loop(0, size // step, body)

    def stage(self, i, k):
        zf, pairs, offs = self.steps(k)
        s2, s4 = self.size // 2, self.size // 4
        l1, l2, l3, l4 = self.landing
        z_first = zf == 1
        mid = (zf == 0) & (self.is_mid == 1)
        end = (zf == 0) & (self.is_mid == 0)

        half_copy = lambda: self.down(0, k, offs[0] + (1 - pairs[0][1]) * s2, s2, pairs[0][0])
        quarter_copy = lambda: self.down(1, k, offs[1] + (1 - pairs[1][1]) * s4, s4, pairs[1][0])
        inward = lambda: self.down(2, k, offs[2], s4, zf * pairs[2][0] + (1 - zf) * self.z_mate)
        across = lambda: self.down(3, k, offs[2], s4, zf * pairs[3][0] + (1 - zf) * self.mid_mate)
        outward = lambda: self.up(4, k, offs[2], s4, self.z_mate)
        back4 = lambda: self.up(5, k, offs[2], s4, pairs[1][0])
        back2 = lambda: self.up(6, k, offs[1], s2, pairs[0][0])

        if i == 1:
            half_copy().start()
        elif i == 2:
            half_copy().wait_recv()
            self.add(k, offs[1], s2, l1)
            quarter_copy().start()
        elif i == 3:
            quarter_copy().wait_recv()
            self.add(k, offs[2], s4, l2)
            pl.when(z_first | end)(lambda: inward().start())
        elif i == 4:

            @pl.when(z_first | mid)
            def _():
                inward().wait_recv()
                pl.when(z_first)(lambda: inward().wait_send())
                self.add(k, offs[2], s4, l3)
                across().start()

        elif i == 5:

            @pl.when(z_first | mid)
            def _():
                across().wait_recv()
                self.finish(k, offs[2], s4, l4)
                pl.when(mid)(lambda: outward().start())

        elif i == 6:
            pl.when(end)(lambda: outward().wait_recv())
            back4().start()
            half_copy().wait_send()
            quarter_copy().wait_send()
            pl.when(end)(lambda: inward().wait_send())
            pl.when(z_first | mid)(lambda: across().wait_send())
        elif i == 7:
            back4().wait_recv()
            back2().start()
        elif i == 8:
            back2().wait_recv()
        else:
            pl.when(mid)(lambda: outward().wait_send())
            back4().wait_send()
            back2().wait_send()


def run_slots(count, stage, between):
    def slot(t):
        for i in ORDER:
            k = t - LAGS[i]

            @pl.when((k >= 0) & (k < count))
            def _():
                stage(i, k)

            if i == 1:
                between(t)

    loop(0, count + LAGS[-1], slot)


def chunk_scratch(slots, part_rows, width, count, dtype):
    def buf(n, kind=jnp.float32):
        return pltpu.VMEM((slots, n, width), kind)

    dma = pltpu.SemaphoreType.DMA
    return [buf(part_rows), buf(part_rows, dtype), buf(part_rows // 2), buf(part_rows // 4), buf(part_rows // 4), buf(part_rows // 4)] + [
        dma((8, count)),
        dma((8, count)),
    ]


CHUNK_REFS = 8


def fold(value):
    return jnp.sum(value.reshape(value.shape[0] // 8, 8, value.shape[1]), axis=0)


def front_kernel(feat_a, feat_b, w_in, t_in, w_mid, t_mid, w_out, t_out, gain1, bias1, gain2, bias2, off_weight, pre1, pre2, act1, act2, dz, grad_emb, vec, *scratch):
    (x_buf, u_buf, w_buf, stats, affine, loss, ea, eb, g_peer) = scratch[:9]
    (x_sem, w_sem, keep_sem, ge_sem, e_send, e_recv) = scratch[9:15]
    small_refs = scratch[15 : 15 + SMALL_REFS]
    acc, gathered, l1, l2, l3, l4, send, recv = scratch[15 + SMALL_REFS :]
    rows_dev, width = feat_a.shape
    wide = w_buf.shape[2]
    tiles = width // wide
    half = width // 2
    part_rows = half // PARTS
    row_count = rows_dev * DEPTH * PLANE
    weights, feats = (w_in, t_in, w_mid, t_mid, w_out, t_out), (feat_a, feat_b)
    place = Place()
    core = place.core
    mine = rows(core * rows_dev, rows_dev)
    place.arrive()
    small = small_sum(place, small_refs)
    payload, total = small.payload, small.total

    def feat(v):
        return pltpu.make_async_copy(feats[v], x_buf.at[v], x_sem.at[v])

    def w_tile(ref, g):
        return pltpu.make_async_copy(ref.at[:, rows((g % tiles) * wide, wide)], w_buf.at[g % W_BUFS], w_sem.at[g % W_BUFS])

    def start_w(g):
        pick(g // tiles, weights, lambda ref: w_tile(ref, g).start())

    feat(0).start()
    w_tile(weights[0], 0).start()
    feat(1).start()
    for g in range(1, W_BUFS - 1):
        start_w(g)
    for j, ref in enumerate((gain1, bias1, gain2, bias2)):
        affine[j] = ref[...]
    feat(0).wait()
    payload[...] = jnp.zeros_like(payload)

    def keep_pre(ref):
        return pltpu.make_async_copy(u_buf.at[0], ref, keep_sem.at[0])

    def keep_act(ref):
        return pltpu.make_async_copy(x_buf.at[0], ref, keep_sem.at[1])

    def row_loop(body, carry):
        return lax.fori_loop(0, rows_dev // BLOCK, lambda r, c: body(rows(r * BLOCK, BLOCK), c), carry)

    def put_sums(j, i, row, value):
        value = jnp.sum(value, axis=0, keepdims=True)
        for c in range(value.shape[1] // TILE):
            payload[j, i + c, row : row + 1] = value[:, c * TILE : (c + 1) * TILE]

    def product(g):
        job, i = g // tiles, g % tiles
        view = job % 2
        w_tile(w_in, g).wait()
        pl.when(g + W_BUFS - 1 < JOBS * tiles)(lambda: start_w(g + W_BUFS - 1))
        at_cols = rows(i * wide, wide)
        u_buf[view, :, at_cols] = jnp.dot(x_buf[view], w_buf[g % W_BUFS], preferred_element_type=jnp.float32)

        def block(at, sums):
            u = u_buf[view, at, at_cols]
            return sums[0] + fold(u), sums[1] + fold(u * u)

        zero = jnp.zeros((8, wide), jnp.float32)
        for row, value in enumerate(row_loop(block, (zero, zero))):
            put_sums(job, i * (wide // TILE), row, value)

    def begin(job):
        small.begin(job)

        @pl.when(job % 2 == 0)
        def _():
            pick(job // 2, (pre1, pre2), lambda ref: keep_pre(ref).start())

    def norm(job):
        layer, view = job // 2, job % 2
        small.end(job)
        for c in range(PLANE):
            at = slice(c * TILE, (c + 1) * TILE)
            means = total[job, c] / row_count
            stats[job, 0, :, at] = means[0:1]
            stats[job, 1, :, at] = lax.rsqrt(means[1:2] - means[0:1] * means[0:1] + NORM_EPS)

        @pl.when((view == 0) & (layer == 1))
        def _():
            keep_act(act1).wait()

        @pl.when((view == 0) & (layer == 2))
        def _():
            keep_act(act2).wait()

        def hidden(i):
            at_cols = rows(i * wide, wide)
            mean, inv = stats[job, 0, :, at_cols], stats[job, 1, :, at_cols]
            gain, bias = affine[layer * 2, :, at_cols], affine[layer * 2 + 1, :, at_cols]

            def block(at, c):
                n = (u_buf[view, at, at_cols] - mean) * inv
                x_buf[view, at, at_cols] = jnp.maximum(n * gain + bias, 0.0).astype(jnp.bfloat16)
                return c

            row_loop(block, 0)

        def student(i):
            at_cols = rows(i * wide, wide)
            mean, inv = stats[job, 0, :, at_cols], stats[job, 1, :, at_cols]

            def block(at, c):
                n = (u_buf[0, at, at_cols] - mean) * inv
                u_buf[0, at, at_cols] = n
                x_buf[0, at, at_cols] = n.astype(jnp.bfloat16)
                return c

            row_loop(block, 0)

        def student_own(i):
            def block(r, c):
                ea[rows(core * rows_dev + r * BLOCK, BLOCK), rows(i * wide, wide)] = x_buf[0, rows(r * BLOCK, BLOCK), rows(core * half + i * wide, wide)]
                return c

            lax.fori_loop(0, rows_dev // BLOCK, block, 0)

        def teacher(i):
            at_cols = rows(i * wide, wide)
            mean, inv = stats[job, 0, :, at_cols], stats[job, 1, :, at_cols]

            def block(r, c):
                n = (u_buf[1, rows(r * BLOCK, BLOCK), at_cols] - mean) * inv
                eb[rows(core * rows_dev + r * BLOCK, BLOCK), at_cols] = n.astype(jnp.bfloat16)
                return c

            lax.fori_loop(0, rows_dev // BLOCK, block, 0)

        @pl.when(layer < 2)
        def _():
            loop(0, tiles, hidden)

            @pl.when(view == 0)
            def _():
                pick(layer, (act1, act2), lambda ref: keep_act(ref).start())
                keep_pre(pre1).wait()

        @pl.when((layer == 2) & (view == 0))
        def _():
            loop(0, tiles, student)
            ea_copy().start()
            loop(0, tiles // 2, student_own)

        @pl.when((layer == 2) & (view == 1))
        def _():
            loop(0, tiles, teacher)
            eb_copy().start()

    ea_copy = lambda: remote_copy(x_buf.at[0, :, rows((1 - core) * half, half)], ea.at[mine], e_send.at[0], e_recv.at[0], place.other_core)
    eb_copy = lambda: remote_copy(eb.at[mine], eb.at[mine], e_send.at[1], e_recv.at[1], place.other_core)

    def step(g):
        job, i = g // tiles, g % tiles
        view = job % 2
        pl.when(g == tiles)(lambda: feat(1).wait())
        product(g)
        pl.when(g == tiles - 1)(lambda: place.all_here())

        @pl.when((view == 0) & (i == 0) & (job > 0))
        def _():
            small.last(job - 1)

        @pl.when((view == 1) & (i == tiles // 2 - 1))
        def _():
            small.middle(job - 1)

        @pl.when(i == tiles - 1)
        def _():
            begin(job)

            @pl.when(view == 1)
            def _():
                small.last(job - 1)
                small.middle(job)

            pl.when(job > 0)(lambda: norm(job - 1))

    loop(0, JOBS * tiles, step)
    small.last(JOBS - 1)
    norm(JOBS - 1)
    for j, source in enumerate((affine.at[2], affine.at[3], stats.at[2, 0], stats.at[2, 1], affine.at[0], affine.at[1], stats.at[0, 0], stats.at[0, 1])):
        vec[j] = source[...]

    loss[...] = jnp.zeros_like(loss)

    def finish(k, off, size, buf):
        share = 0.5 - 0.25 * chunks.z_first(k).astype(jnp.float32)
        at = rows(off, size)
        corr = (acc[k, at] + buf[k]) / row_count
        row = core * half + k * part_rows + off
        diag = (row + lax.broadcasted_iota(jnp.int32, (size, width), 0)) == lax.broadcasted_iota(jnp.int32, (size, width), 1)
        weight = off_weight[0]
        miss = 1.0 - corr
        loss[...] += share * jnp.sum(jnp.where(diag, miss * miss, weight * (corr * corr)), axis=0, keepdims=True)
        gathered[k, at] = jnp.where(diag, -2.0 * miss, 2.0 * weight * corr).astype(jnp.bfloat16)

    chunks = ChunkSum(place, PARTS, acc, gathered, (l1, l2, l3, l4), send, recv, finish)

    def form(k):
        @pl.when(k == 0)
        def _():
            ea_copy().wait_recv()
            eb_copy().wait_recv()

        at = rows(k * part_rows, GROUP * part_rows)
        size = min(1024, width)

        def col(c):
            cs = rows(c * size, size)
            acc[pl.ds(k, GROUP), :, cs] = contract_rows(ea[:, at], eb[:, cs]).reshape(GROUP, part_rows, size)

        loop(0, width // size, col)

    def swap(k):
        return chunks.copy(gathered.at[k], g_peer.at[k], 7, k, place.other_core)

    def ge_cols(k, side):
        return rows(side * half + k * part_rows, GROUP * part_rows)

    def ge_copy(k, side):
        at = ge_cols(k, side)
        return pltpu.make_async_copy(u_buf.at[1, :, at], grad_emb.at[:, at], ge_sem.at[k // GROUP, side])

    def embed(k, side, g_rows):
        at_cols = ge_cols(k, side)
        grad = contract_cols(eb[mine], g_rows.reshape(GROUP * part_rows, width)) / row_count
        u_buf[1, :, at_cols] = grad
        ge_copy(k, side).start()

        def block(at, sums):
            g = u_buf[1, at, at_cols]
            return sums[0] + fold(g * u_buf[0, at, at_cols]), sums[1] + fold(g)

        zero = jnp.zeros((8, GROUP * part_rows), jnp.float32)
        for row, value in enumerate(row_loop(block, (zero, zero))):
            payload[JOBS, (side * half + k * part_rows) // TILE, row : row + 1] = jnp.sum(value, axis=0, keepdims=True)

    def stage(i, k):
        if i == 0:
            pl.when(k % GROUP == 0)(lambda: form(k))
            return
        chunks.stage(i, k)
        if i == 8:
            swap(k).start()

            @pl.when(k % GROUP == GROUP - 1)
            def _():
                embed(k - GROUP + 1, core, gathered[pl.ds(k - GROUP + 1, GROUP)])

        if i == 9:
            swap(k).wait_recv()
            swap(k).wait_send()

            @pl.when(k % GROUP == GROUP - 1)
            def _():
                embed(k - GROUP + 1, 1 - core, g_peer[pl.ds(k - GROUP + 1, GROUP)])

    run_slots(PARTS, stage, lambda t: None)
    for c in range(PLANE):
        payload[JOBS, c, 2:3] = loss[:, c * TILE : (c + 1) * TILE]
    small.begin(JOBS)
    ea_copy().wait_send()
    eb_copy().wait_send()
    small.middle(JOBS)
    for k in range(0, PARTS, GROUP):
        for side in range(2):
            ge_copy(k, side).wait()
    small.last(JOBS)
    small.end(JOBS)

    def dz_tile(i):
        at_cols = rows(i * wide, wide)
        sums = jnp.concatenate([total[JOBS, i * (wide // TILE) + c] for c in range(wide // TILE)], axis=1) / row_count
        mean_gn, mean_g = sums[0:1], sums[1:2]
        inv = stats[JOBS - 2, 1, :, at_cols]

        def block(at, c):
            value = (u_buf[1, at, at_cols] - mean_g - u_buf[0, at, at_cols] * mean_gn) * inv
            x_buf[0, at, at_cols] = value.astype(jnp.bfloat16)
            return c

        row_loop(block, 0)

    loop(0, tiles, dz_tile)
    keep_act(dz).start()
    for c in range(PLANE):
        vec[8, :, c * TILE : (c + 1) * TILE] = total[JOBS, c, 2:3]
    keep_act(dz).wait()


def front(feat_a, feat_b, weights, affine, off_weight):
    rows_dev, width = feat_a.shape
    half = width // 2
    part_rows = half // PARTS
    any_spec = pl.BlockSpec(memory_space=pl.ANY)
    vmem_spec = pl.BlockSpec(memory_space=pltpu.VMEM)
    wide_f32 = jax.ShapeDtypeStruct((rows_dev, width), jnp.float32)
    wide_bf16 = jax.ShapeDtypeStruct((rows_dev, width), jnp.bfloat16)
    dma = pltpu.SemaphoreType.DMA
    return pl.pallas_call(
        front_kernel,
        name="front",
        out_shape=[wide_f32, wide_f32, wide_bf16, wide_bf16, wide_bf16, wide_f32]
        + [jax.ShapeDtypeStruct((9, 1, width), jnp.float32)],
        in_specs=[any_spec] * 8 + [vmem_spec] * 4 + [pl.BlockSpec(memory_space=pltpu.SMEM)],
        out_specs=[any_spec] * 6 + [vmem_spec],
        scratch_shapes=[
            pltpu.VMEM((2, rows_dev, width), jnp.bfloat16),
            pltpu.VMEM((2, rows_dev, width), jnp.float32),
            pltpu.VMEM((W_BUFS, width, WIDE), jnp.bfloat16),
            pltpu.VMEM((JOBS, 2, 1, width), jnp.float32),
            pltpu.VMEM((4, 1, width), jnp.float32),
            pltpu.VMEM((1, width), jnp.float32),
            pltpu.VMEM((2 * rows_dev, half), jnp.bfloat16),
            pltpu.VMEM((2 * rows_dev, width), jnp.bfloat16),
            pltpu.VMEM((PARTS, part_rows, width), jnp.bfloat16),
            dma((2,)),
            dma((W_BUFS,)),
            dma((2,)),
            dma((PARTS // GROUP, 2)),
            dma((2,)),
            dma((2,)),
        ]
        + small_scratch(JOBS + 1)
        + chunk_scratch(PARTS, part_rows, width, PARTS, jnp.bfloat16),
        compiler_params=pltpu.CompilerParams(collective_id=0, has_side_effects=True, vmem_limit_bytes=VMEM_BYTES),
    )(feat_a, feat_b, *weights, *affine, off_weight)


def back_kernel(dz_hbm, x2, x1, x0, w_out, w_mid, u2, u1, vec, out2, out1, out0, sums_out, *scratch):
    (dy, xs, w_buf, u_buf, dpre) = scratch[:5]
    (in_sem, tile_sem, peer_send, peer_recv, store_sem) = scratch[5:10]
    small_refs = scratch[10 : 10 + SMALL_REFS]
    acc, gathered, l1, l2, l3, l4, send, recv = scratch[10 + SMALL_REFS :]
    rows_dev, width = dz_hbm.shape
    wide = w_buf.shape[1]
    tiles = width // wide
    row_count = rows_dev * DEPTH * PLANE
    half = width // 2
    part_rows = half // PARTS
    count = MATS * PARTS
    mats_in, outs, weights, pres = (x2, x1, x0), (out2, out1, out0), (w_out, w_mid), (u2, u1)
    place = Place()
    core, other_core = place.core, place.other_core
    mine = rows(core * rows_dev, rows_dev)
    place.arrive()
    small = small_sum(place, small_refs)
    payload, sums = small.payload, small.total

    def own_x(w):
        return pltpu.make_async_copy(mats_in[w].at[:, rows(core * half, half)], xs.at[w % 2, mine], in_sem.at[w])

    def peer_x(w):
        return remote_copy(mats_in[w].at[:, rows((1 - core) * half, half)], xs.at[w % 2, mine], peer_send.at[w], peer_recv.at[w], other_core)

    def peer_dy(w):
        block = dy.at[w % 2, mine]
        return remote_copy(block, block, peer_send.at[MATS + w], peer_recv.at[MATS + w], other_core)

    def x_arrive(w):
        block = xs.at[w % 2, mine]
        pltpu.make_async_copy(block, block, in_sem.at[w]).wait()
        remote_copy(block, block, peer_send.at[w], peer_recv.at[w], other_core).wait_recv()

    def w_tile(ref, i):
        return pltpu.make_async_copy(ref.at[rows(i * wide, wide)], w_buf.at[i % 2], tile_sem.at[0, i % 2])

    def u_tile(ref, i):
        return pltpu.make_async_copy(ref.at[:, rows(i * wide, wide)], u_buf.at[i % 2], tile_sem.at[1, i % 2])

    def start_w(layer, i):
        pick(layer, weights, lambda ref: w_tile(ref, i).start())

    def start_u(layer, i):
        pick(layer, pres, lambda ref: u_tile(ref, i).start())

    dz_load = pltpu.make_async_copy(dz_hbm, dy.at[0, mine], in_sem.at[MATS])
    dz_load.start()
    for w in range(2):
        own_x(w).start()
    w_tile(weights[0], 0).start()
    u_tile(pres[0], 0).start()
    payload[...] = jnp.zeros_like(payload)
    place.all_here()
    peer_x(0).start()
    dz_load.wait()
    peer_dy(0).start()
    peer_x(1).start()

    def row_loop(body, carry):
        return lax.fori_loop(0, rows_dev // BLOCK, body, carry)

    def chain_tile(layer, i):
        w_tile(w_out, i).wait()
        u_tile(u2, i).wait()

        @pl.when(i + 1 < tiles)
        def _():
            start_w(layer, i + 1)
            start_u(layer, i + 1)

        at_cols = rows(i * wide, wide)
        dpre[:, at_cols] = contract_cols(dy[layer, mine], w_buf[i % 2])
        gain, bias, mean, inv = (vec[layer * 4 + j, :, at_cols] for j in range(4))

        def block(r, carry):
            at = rows(r * BLOCK, BLOCK)
            n = (u_buf[i % 2, at] - mean) * inv
            g = jnp.where(n * gain + bias > 0.0, dpre[at, at_cols], 0.0)
            dpre[at, at_cols] = g
            return carry[0] + fold(g * n), carry[1] + fold(g)

        zero = jnp.zeros((8, wide), jnp.float32)
        for row, value in enumerate(row_loop(block, (zero, zero))):
            value = jnp.sum(value, axis=0, keepdims=True)
            for c in range(wide // TILE):
                payload[layer, i * (wide // TILE) + c, row : row + 1] = value[:, c * TILE : (c + 1) * TILE]

    def du(layer):
        start_u(layer, 0)

        def tile(i):
            u_tile(u2, i).wait()
            pl.when(i + 1 < tiles)(lambda: start_u(layer, i + 1))
            at_cols = rows(i * wide, wide)
            gain, mean, inv = (vec[layer * 4 + j, :, at_cols] for j in (0, 2, 3))
            means = jnp.concatenate([sums[layer, i * (wide // TILE) + c] for c in range(wide // TILE)], axis=1) / row_count
            mean_gn, mean_g = means[0:1], means[1:2]
            scale = gain * inv

            def block(r, c):
                at = rows(r * BLOCK, BLOCK)
                n = (u_buf[i % 2, at] - mean) * inv
                value = (dpre[at, at_cols] - mean_g - n * mean_gn) * scale
                dy[1 - layer, rows(core * rows_dev + r * BLOCK, BLOCK), at_cols] = value.astype(jnp.bfloat16)
                return c

            row_loop(block, 0)

        loop(0, tiles, tile)

    def finish(k, off, size, buf):
        j = k % SLOTS
        gathered[j, rows(off, size)] = acc[j, rows(off, size)] + buf[j]

    chunks = ChunkSum(place, SLOTS, acc, gathered, (l1, l2, l3, l4), send, recv, finish)

    def form(k):
        w, j = k // PARTS, k % SLOTS

        @pl.when(k % PARTS == 0)
        def _():
            x_arrive(w)
            peer_dy(w).wait_recv()

        at = rows((k % PARTS) * part_rows, GROUP * part_rows)
        size = min(1024, width)

        def col(c):
            cs = rows(c * size, size)
            acc[pl.ds(j, GROUP), :, cs] = contract_rows(xs[w % 2, :, at], dy[w % 2, :, cs]).reshape(GROUP, part_rows, size)

        loop(0, width // size, col)

    def out_rows(k, side):
        return pl.ds(pl.multiple_of(side * half + (k % PARTS) * part_rows, part_rows), part_rows)

    def last_copy(out, k, side):
        return chunks.copy(gathered.at[k % SLOTS], out.at[out_rows(k, side)], 7, k, other_core)

    def store_copy(out, k):
        return pltpu.make_async_copy(gathered.at[k % SLOTS], out.at[out_rows(k, core)], store_sem.at[k])

    def stage(i, k):
        if i == 0:
            pl.when(k % GROUP == 0)(lambda: form(k))
            return
        chunks.stage(i, k)
        if i == 8:

            def emit(out):
                last_copy(out, k, core).start()
                store_copy(out, k).start()

            pick(k // PARTS, outs, emit)
        if i == 9:

            def close(out):
                last_copy(out, k, 1 - core).wait_recv()
                store_copy(out, k).wait()
                last_copy(out, k, core).wait_send()

            pick(k // PARTS, outs, close)

    def layer_work(t):
        layer = t // LAYER_SLOTS
        at = t - LAYER_SLOTS * layer
        pl.when(at < tiles)(lambda: chain_tile(layer, at))
        pl.when(at == tiles)(lambda: small.begin(layer))
        pl.when(at == tiles + 1)(lambda: small.middle(layer))
        pl.when(at == tiles + 2)(lambda: small.last(layer))

        @pl.when(at == tiles + 3)
        def _():
            small.end(layer)
            pl.when(layer == 1)(lambda: peer_dy(0).wait_send())
            du(layer)
            peer_dy(layer + 1).start()

            @pl.when(layer == 0)
            def _():
                w_tile(weights[1], 0).start()
                u_tile(pres[1], 0).start()

            @pl.when(layer == 1)
            def _():
                peer_x(0).wait_send()
                own_x(2).start()
                peer_x(2).start()

    run_slots(count, stage, lambda t: pl.when(t < 2 * LAYER_SLOTS)(lambda: layer_work(t)))
    for w in (1, 2):
        peer_x(w).wait_send()
        peer_dy(w).wait_send()
    for c in range(PLANE):
        for row in range(4):
            sums_out[row : row + 1, c * TILE : (c + 1) * TILE] = sums[row // 2, c, row % 2 : row % 2 + 1]
    sums_out[4:5] = jnp.full((1, width), jnp.sum(vec[8]))


def backward(grad_z, x2, x1, x0, w_out, w_mid, u2, u1, vec):
    rows_dev, width = grad_z.shape
    part_rows = width // 2 // PARTS
    count = MATS * PARTS
    any_spec = pl.BlockSpec(memory_space=pl.ANY)
    vmem_spec = pl.BlockSpec(memory_space=pltpu.VMEM)
    mat = jax.ShapeDtypeStruct((width, width), jnp.float32)
    dma = pltpu.SemaphoreType.DMA
    return pl.pallas_call(
        back_kernel,
        name="backward",
        out_shape=[mat, mat, mat, jax.ShapeDtypeStruct((5, width), jnp.float32)],
        in_specs=[any_spec] * 8 + [vmem_spec],
        out_specs=[any_spec] * 3 + [vmem_spec],
        scratch_shapes=[
            pltpu.VMEM((2, 2 * rows_dev, width), jnp.bfloat16),
            pltpu.VMEM((2, 2 * rows_dev, width // 2), jnp.bfloat16),
            pltpu.VMEM((2, WIDE, width), jnp.bfloat16),
            pltpu.VMEM((2, rows_dev, WIDE), jnp.float32),
            pltpu.VMEM((rows_dev, width), jnp.float32),
            dma((MATS + 1,)),
            dma((2, 2)),
            dma((2 * MATS,)),
            dma((2 * MATS,)),
            dma((count,)),
        ]
        + small_scratch(2)
        + chunk_scratch(SLOTS, part_rows, width, count, jnp.float32),
        compiler_params=pltpu.CompilerParams(collective_id=1, has_side_effects=True, vmem_limit_bytes=VMEM_BYTES),
    )(grad_z, x2, x1, x0, w_out, w_mid, u2, u1, vec)


def solution(mesh):
    row_part = P(DATA_AXIS, None)
    replicated = P()

    def local_step(feat_a, feat_b, w_in, w_mid, w_out, t_in, t_mid, t_out, gain_1, bias_1, gain_2, bias_2, off_weight):
        affine = [v.reshape(1, -1) for v in (gain_1, bias_1, gain_2, bias_2)]
        pre_1, pre_2, act_1, act_2, grad_z, grad_emb, vec = front(
            feat_a, feat_b, (w_in, t_in, w_mid, t_mid, w_out, t_out), affine, off_weight.reshape(1)
        )
        grad_w_out, grad_w_mid, grad_w_in, sums = backward(grad_z, act_2, act_1, feat_a, w_out, w_mid, pre_2, pre_1, vec)
        return (sums[4, 0], grad_emb, grad_w_in, grad_w_mid, grad_w_out, sums[2], sums[3], sums[0], sums[1])

    return jax.shard_map(local_step, mesh=mesh, in_specs=(row_part, row_part) + (replicated,) * 11, out_specs=(replicated, row_part) + (replicated,) * 7, check_vma=False)
```

```python
import functools

import jax
import jax.numpy as jnp
from jax import lax
from jax.experimental import pallas as pl
from jax.experimental.pallas import tpu as pltpu
from jax.sharding import PartitionSpec as P

NORM_EPS = 1e-5
DATA_AXIS = "data"
MESH = pl.DeviceIdType.MESH
VMEM_BYTES = 67_043_328
PLANE = 8
DEPTH = 4
TILE = 256
WIDE = 512
BLOCK = 128
SUM_ROWS = 4
PARTS = 16
GROUP = 4
MATS = 3
ACC_SLOTS = 20
GATHER_SLOTS = 16
JOBS = 6
W_BUFS = 3
LAYER_SLOTS = 8
FRONT_PLAN = ((0, 0, 3, 5, 7, 10, 11, 13, 17, 19), (0, 1, 3, 4, 6, 5, 2, 9, 8, 7), (5, 2))
BACK_PLAN = ((0, 0, 5, 7, 10, 12, 13, 16, 20, 23), (0, 1, 9, 5, 3, 2, 8, 7, 4, 6), (4, 2))


def contract_rows(left_op, right_op):
    return lax.dot_general(left_op, right_op, (((0,), (0,)), ((), ())), preferred_element_type=jnp.float32)


def contract_cols(left_op, right_op):
    return lax.dot_general(left_op, right_op, (((1,), (1,)), ((), ())), preferred_element_type=jnp.float32)


def rows(off, size):
    return pl.ds(pl.multiple_of(off, size), size)


def pick(index, choices, what):
    for i, c in enumerate(choices):
        pl.when(index == i)(functools.partial(what, c))


def loop(lo, hi, body):
    def step(i, carry):
        body(i)
        return carry

    lax.fori_loop(lo, hi, step, 0)


def remote_copy(src, dst, send, recv, mate):
    return pltpu.make_async_remote_copy(src, dst, send, recv, device_id=(mate,), device_id_type=MESH)


class Place:
    def __init__(self):
        me = lax.axis_index(DATA_AXIS)
        self.me = me
        self.pos, self.plane = me % PLANE, me // PLANE
        self.core, self.bx, self.by, self.bz0, self.bz1 = me % 2, (me // 2) % 2, (me // 4) % 2, (me // 8) % 2, (me // 16) % 2
        self.other_core = me + 1 - 2 * self.core
        self.mates = [(self.pos + d) % PLANE for d in range(1, PLANE)]
        self.levels = [(self.plane + d) % DEPTH for d in range(1, DEPTH)]

    def peers(self):
        return [self.plane * PLANE + m for m in self.mates] + [lv * PLANE + self.pos for lv in self.levels]

    def arrive(self):
        sem = pltpu.get_barrier_semaphore()
        for peer in self.peers():
            pl.semaphore_signal(sem, inc=1, device_id=(peer,), device_id_type=MESH)

    def all_here(self):
        pl.semaphore_wait(pltpu.get_barrier_semaphore(), PLANE + DEPTH - 2)


class SmallSum:
    def __init__(self, place, payload, total, plane_buf, depth_buf, own_buf, sems):
        self.p, self.payload, self.total = place, payload, total
        self.plane_buf, self.depth_buf, self.own_buf, self.sems = plane_buf, depth_buf, own_buf, sems

    def first(self, j, m, slot):
        s, r = self.sems[0], self.sems[1]
        return remote_copy(self.payload.at[j, m], self.plane_buf.at[j, slot], s.at[j, m], r.at[j, slot], self.p.plane * PLANE + m)

    def second(self, j, lv, slot):
        s, r = self.sems[2], self.sems[3]
        return remote_copy(self.own_buf.at[j, 0], self.depth_buf.at[j, slot], s.at[j, lv], r.at[j, slot], lv * PLANE + self.p.pos)

    def third(self, j, m, slot):
        s, r = self.sems[4], self.sems[5]
        return remote_copy(self.own_buf.at[j, 1], self.total.at[j, slot], s.at[j, m], r.at[j, slot], self.p.plane * PLANE + m)

    def begin(self, j):
        for m in self.p.mates:
            self.first(j, m, self.p.pos).start()
        self.plane_buf[j, self.p.pos] = self.payload[j, self.p.pos]

    def middle(self, j):
        for m in self.p.mates:
            self.first(j, m, m).wait_recv()
        total = self.plane_buf[j, 0]
        for i in range(1, PLANE):
            total = total + self.plane_buf[j, i]
        self.own_buf[j, 0] = total
        self.depth_buf[j, self.p.plane] = total
        for lv in self.p.levels:
            self.second(j, lv, self.p.plane).start()

    def last(self, j):
        for lv in self.p.levels:
            self.second(j, lv, lv).wait_recv()
        total = self.depth_buf[j, 0]
        for i in range(1, DEPTH):
            total = total + self.depth_buf[j, i]
        self.own_buf[j, 1] = total
        self.total[j, self.p.pos] = total
        for m in self.p.mates:
            self.third(j, m, self.p.pos).start()

    def end(self, j):
        for m in self.p.mates:
            self.third(j, m, m).wait_recv()
            self.first(j, m, self.p.pos).wait_send()
            self.third(j, m, self.p.pos).wait_send()
        for lv in self.p.levels:
            self.second(j, lv, self.p.plane).wait_send()


def small_scratch(count):
    def buf(*lead):
        return pltpu.VMEM((count, *lead, SUM_ROWS, TILE), jnp.float32)

    bufs = [buf(PLANE), buf(PLANE), buf(PLANE), buf(DEPTH), buf(2)]
    return bufs + [pltpu.SemaphoreType.DMA((count, n)) for n in (PLANE, PLANE, DEPTH, DEPTH, PLANE, PLANE)]


SMALL_REFS = 11


def small_sum(place, refs):
    payload, total, plane_buf, depth_buf, own_buf = refs[:5]
    return SmallSum(place, payload, total, plane_buf, depth_buf, own_buf, refs[5:])


class ChunkSum:
    def __init__(self, place, z_first, acc, gathered, landing, send, recv, finish):
        self.p, self.z_first_plan, self.slots, self.gather_slots = place, z_first, acc.shape[0], gathered.shape[0]
        self.acc, self.gathered, self.landing, self.send, self.recv, self.finish = acc, gathered, landing, send, recv, finish
        self.size = acc.shape[1]
        core, bx, by = place.core, place.bx, place.by
        self.xy = ((2 + 2 * core, core * by + (1 - core) * bx), (4 - 2 * core, core * bx + (1 - core) * by))
        self.zz = ((8, place.bz0), (16, place.bz1))
        self.is_mid = place.bz0 + place.bz1 - 2 * place.bz0 * place.bz1
        self.z_mate = place.me + 8 * (1 - 2 * place.bz0)
        self.mid_mate = place.me + 8 * (1 - 2 * place.bz1)

    def z_first(self, k):
        every, at = self.z_first_plan
        off = k % every - at
        return 1 - lax.min(off * off, 1)

    def steps(self, k):
        zf = self.z_first(k)
        pairs = []
        for a, b in zip(self.xy + self.zz, self.zz + self.xy):
            stride = zf * b[0] + (1 - zf) * a[0]
            bit = zf * b[1] + (1 - zf) * a[1]
            pairs.append((self.p.me + stride * (1 - 2 * bit), bit))
        s2, s4 = self.size // 2, self.size // 4
        offs = (0, pairs[0][1] * s2, pairs[0][1] * s2 + pairs[1][1] * s4)
        return zf, pairs, offs

    def copy(self, src, dst, stage, k, mate):
        return remote_copy(src, dst, self.send.at[stage, k], self.recv.at[stage, k], mate)

    def down(self, stage, k, off, size, mate):
        j = k % self.slots
        return self.copy(self.acc.at[j, rows(off, size)], self.landing[stage].at[j], stage, k, mate)

    def up(self, stage, k, off, size, mate):
        block = self.gathered.at[k % self.gather_slots, rows(off, size)]
        return self.copy(block, block, stage, k, mate)

    def add(self, k, off, size, buf):
        step = min(size, 16)
        j = k % self.slots

        def body(i):
            at = rows(off + i * step, step)
            self.acc[j, at] = self.acc[j, at] + buf[j, rows(i * step, step)]

        loop(0, size // step, body)

    def stage(self, i, k):
        zf, pairs, offs = self.steps(k)
        s2, s4 = self.size // 2, self.size // 4
        l1, l2, l3, l4 = self.landing
        z_first = zf == 1
        mid = (zf == 0) & (self.is_mid == 1)
        end = (zf == 0) & (self.is_mid == 0)

        half_copy = lambda: self.down(0, k, offs[0] + (1 - pairs[0][1]) * s2, s2, pairs[0][0])
        quarter_copy = lambda: self.down(1, k, offs[1] + (1 - pairs[1][1]) * s4, s4, pairs[1][0])
        inward = lambda: self.down(2, k, offs[2], s4, zf * pairs[2][0] + (1 - zf) * self.z_mate)
        across = lambda: self.down(3, k, offs[2], s4, zf * pairs[3][0] + (1 - zf) * self.mid_mate)
        outward = lambda: self.up(4, k, offs[2], s4, self.z_mate)
        back4 = lambda: self.up(5, k, offs[2], s4, pairs[1][0])
        back2 = lambda: self.up(6, k, offs[1], s2, pairs[0][0])

        if i == 1:
            half_copy().start()
        elif i == 2:
            half_copy().wait_recv()
            self.add(k, offs[1], s2, l1)
            quarter_copy().start()
        elif i == 3:
            quarter_copy().wait_recv()
            self.add(k, offs[2], s4, l2)
            pl.when(z_first | end)(lambda: inward().start())
        elif i == 4:

            @pl.when(z_first | mid)
            def _():
                inward().wait_recv()
                pl.when(z_first)(lambda: inward().wait_send())
                self.add(k, offs[2], s4, l3)
                across().start()

        elif i == 5:

            @pl.when(z_first | mid)
            def _():
                across().wait_recv()
                self.finish(k, offs[2], s4, l4)
                pl.when(mid)(lambda: outward().start())

        elif i == 6:
            pl.when(end)(lambda: outward().wait_recv())
            back4().start()
            half_copy().wait_send()
            quarter_copy().wait_send()
            pl.when(end)(lambda: inward().wait_send())
            pl.when(z_first | mid)(lambda: across().wait_send())
        elif i == 7:
            back4().wait_recv()
            back2().start()
        elif i == 8:
            back2().wait_recv()
        else:
            pl.when(mid)(lambda: outward().wait_send())
            back4().wait_send()
            back2().wait_send()


def run_slots(plan, count, stage, between):
    lags, order, _ = plan

    def slot(t):
        for i in order:
            k = t - lags[i]

            @pl.when((k >= 0) & (k < count))
            def _():
                stage(i, k)

            if i == 1:
                between(t)

    loop(0, count + lags[-1], slot)


def chunk_scratch(slots, gather_slots, part_rows, width, count, dtype):
    def buf(n):
        return pltpu.VMEM((slots, n, width), jnp.float32)

    gathered = pltpu.VMEM((gather_slots, part_rows, width), dtype)

    dma = pltpu.SemaphoreType.DMA
    return [buf(part_rows), gathered, buf(part_rows // 2), buf(part_rows // 4), buf(part_rows // 4), buf(part_rows // 4)] + [
        dma((8, count)),
        dma((8, count)),
    ]


CHUNK_REFS = 8


def fold(value):
    return jnp.sum(value.reshape(value.shape[0] // 8, 8, value.shape[1]), axis=0)


def front_kernel(feat_a, feat_b, w_in, t_in, w_mid, t_mid, w_out, t_out, gain1, bias1, gain2, bias2, off_weight, pre1, pre2, act1, act2, dz, grad_emb, vec, *scratch):
    (x_buf, u_buf, w_buf, stats, affine, loss, ea, eb, g_peer) = scratch[:9]
    (x_sem, w_sem, keep_sem, ge_sem, e_send, e_recv) = scratch[9:15]
    small_refs = scratch[15 : 15 + SMALL_REFS]
    acc, gathered, l1, l2, l3, l4, send, recv = scratch[15 + SMALL_REFS :]
    rows_dev, width = feat_a.shape
    wide = w_buf.shape[2]
    tiles = width // wide
    half = width // 2
    part_rows = half // PARTS
    row_count = rows_dev * DEPTH * PLANE
    weights, feats = (w_in, t_in, w_mid, t_mid, w_out, t_out), (feat_a, feat_b)
    place = Place()
    core = place.core
    mine = rows(core * rows_dev, rows_dev)
    place.arrive()
    small = small_sum(place, small_refs)
    payload, total = small.payload, small.total

    def feat(v):
        return pltpu.make_async_copy(feats[v], x_buf.at[v], x_sem.at[v])

    def w_tile(ref, g):
        return pltpu.make_async_copy(ref.at[:, rows((g % tiles) * wide, wide)], w_buf.at[g % W_BUFS], w_sem.at[g % W_BUFS])

    def start_w(g):
        pick(g // tiles, weights, lambda ref: w_tile(ref, g).start())

    feat(0).start()
    w_tile(weights[0], 0).start()
    feat(1).start()
    for g in range(1, W_BUFS - 1):
        start_w(g)
    for j, ref in enumerate((gain1, bias1, gain2, bias2)):
        affine[j] = ref[...]
    feat(0).wait()
    payload[...] = jnp.zeros_like(payload)

    def keep_pre(ref):
        return pltpu.make_async_copy(u_buf.at[0], ref, keep_sem.at[0])

    def keep_act(ref):
        return pltpu.make_async_copy(x_buf.at[0], ref, keep_sem.at[1])

    def row_loop(body, carry):
        return lax.fori_loop(0, rows_dev // BLOCK, lambda r, c: body(rows(r * BLOCK, BLOCK), c), carry)

    def put_sums(j, i, row, value):
        value = jnp.sum(value, axis=0, keepdims=True)
        for c in range(value.shape[1] // TILE):
            payload[j, i + c, row : row + 1] = value[:, c * TILE : (c + 1) * TILE]

    def product(g):
        job, i = g // tiles, g % tiles
        view = job % 2
        w_tile(w_in, g).wait()
        pl.when(g + W_BUFS - 1 < JOBS * tiles)(lambda: start_w(g + W_BUFS - 1))
        at_cols = rows(i * wide, wide)
        u_buf[view, :, at_cols] = jnp.dot(x_buf[view], w_buf[g % W_BUFS], preferred_element_type=jnp.float32)

        def block(at, sums):
            u = u_buf[view, at, at_cols]
            return sums[0] + fold(u), sums[1] + fold(u * u)

        zero = jnp.zeros((8, wide), jnp.float32)
        for row, value in enumerate(row_loop(block, (zero, zero))):
            put_sums(job, i * (wide // TILE), row, value)

    def begin(job):
        small.begin(job)

        @pl.when(job % 2 == 0)
        def _():
            pick(job // 2, (pre1, pre2), lambda ref: keep_pre(ref).start())

    def norm(job):
        layer, view = job // 2, job % 2
        small.end(job)
        for c in range(PLANE):
            at = slice(c * TILE, (c + 1) * TILE)
            means = total[job, c] / row_count
            stats[job, 0, :, at] = means[0:1]
            stats[job, 1, :, at] = lax.rsqrt(means[1:2] - means[0:1] * means[0:1] + NORM_EPS)

        @pl.when((view == 0) & (layer == 1))
        def _():
            keep_act(act1).wait()

        @pl.when((view == 0) & (layer == 2))
        def _():
            keep_act(act2).wait()

        def hidden(i):
            at_cols = rows(i * wide, wide)
            mean, inv = stats[job, 0, :, at_cols], stats[job, 1, :, at_cols]
            gain, bias = affine[layer * 2, :, at_cols], affine[layer * 2 + 1, :, at_cols]

            def block(at, c):
                n = (u_buf[view, at, at_cols] - mean) * inv
                x_buf[view, at, at_cols] = jnp.maximum(n * gain + bias, 0.0).astype(jnp.bfloat16)
                return c

            row_loop(block, 0)

        def student(i):
            at_cols = rows(i * wide, wide)
            mean, inv = stats[job, 0, :, at_cols], stats[job, 1, :, at_cols]

            def block(at, c):
                n = (u_buf[0, at, at_cols] - mean) * inv
                u_buf[0, at, at_cols] = n
                x_buf[0, at, at_cols] = n.astype(jnp.bfloat16)
                return c

            row_loop(block, 0)

        def student_own(i):
            def block(r, c):
                ea[rows(core * rows_dev + r * BLOCK, BLOCK), rows(i * wide, wide)] = x_buf[0, rows(r * BLOCK, BLOCK), rows(core * half + i * wide, wide)]
                return c

            lax.fori_loop(0, rows_dev // BLOCK, block, 0)

        def teacher(i):
            at_cols = rows(i * wide, wide)
            mean, inv = stats[job, 0, :, at_cols], stats[job, 1, :, at_cols]

            def block(r, c):
                n = (u_buf[1, rows(r * BLOCK, BLOCK), at_cols] - mean) * inv
                eb[rows(core * rows_dev + r * BLOCK, BLOCK), at_cols] = n.astype(jnp.bfloat16)
                return c

            lax.fori_loop(0, rows_dev // BLOCK, block, 0)

        @pl.when(layer < 2)
        def _():
            loop(0, tiles, hidden)

            @pl.when(view == 0)
            def _():
                pick(layer, (act1, act2), lambda ref: keep_act(ref).start())
                keep_pre(pre1).wait()

        @pl.when((layer == 2) & (view == 0))
        def _():
            loop(0, tiles, student)
            ea_copy().start()
            loop(0, tiles // 2, student_own)

        @pl.when((layer == 2) & (view == 1))
        def _():
            loop(0, tiles, teacher)
            eb_copy().start()

    ea_copy = lambda: remote_copy(x_buf.at[0, :, rows((1 - core) * half, half)], ea.at[mine], e_send.at[0], e_recv.at[0], place.other_core)
    eb_copy = lambda: remote_copy(eb.at[mine], eb.at[mine], e_send.at[1], e_recv.at[1], place.other_core)

    def step(g):
        job, i = g // tiles, g % tiles
        view = job % 2
        pl.when(g == tiles)(lambda: feat(1).wait())
        product(g)
        pl.when(g == tiles - 1)(lambda: place.all_here())

        @pl.when((view == 0) & (i == 0) & (job > 0))
        def _():
            small.last(job - 1)

        @pl.when((view == 1) & (i == tiles // 2 - 1))
        def _():
            small.middle(job - 1)

        @pl.when(i == tiles - 1)
        def _():
            begin(job)

            @pl.when(view == 1)
            def _():
                small.last(job - 1)
                small.middle(job)

            pl.when(job > 0)(lambda: norm(job - 1))

    loop(0, JOBS * tiles, step)
    small.last(JOBS - 1)
    norm(JOBS - 1)
    for j, source in enumerate((affine.at[2], affine.at[3], stats.at[2, 0], stats.at[2, 1], affine.at[0], affine.at[1], stats.at[0, 0], stats.at[0, 1])):
        vec[j] = source[...]

    loss[...] = jnp.zeros_like(loss)

    def finish(k, off, size, buf):
        share = 0.5 - 0.25 * chunks.z_first(k).astype(jnp.float32)
        at = rows(off, size)
        corr = (acc[k, at] + buf[k]) / row_count
        row = core * half + k * part_rows + off
        diag = (row + lax.broadcasted_iota(jnp.int32, (size, width), 0)) == lax.broadcasted_iota(jnp.int32, (size, width), 1)
        weight = off_weight[0]
        miss = 1.0 - corr
        loss[...] += share * jnp.sum(jnp.where(diag, miss * miss, weight * (corr * corr)), axis=0, keepdims=True)
        gathered[k, at] = jnp.where(diag, -2.0 * miss, 2.0 * weight * corr).astype(jnp.bfloat16)

    chunks = ChunkSum(place, FRONT_PLAN[2], acc, gathered, (l1, l2, l3, l4), send, recv, finish)

    def form(k):
        @pl.when(k == 0)
        def _():
            ea_copy().wait_recv()
            eb_copy().wait_recv()

        at = rows(k * part_rows, GROUP * part_rows)
        size = min(1024, width)

        def col(c):
            cs = rows(c * size, size)
            acc[pl.ds(k, GROUP), :, cs] = contract_rows(ea[:, at], eb[:, cs]).reshape(GROUP, part_rows, size)

        loop(0, width // size, col)

    def swap(k):
        return chunks.copy(gathered.at[k], g_peer.at[k], 7, k, place.other_core)

    def ge_cols(k, side):
        return rows(side * half + k * part_rows, GROUP * part_rows)

    def ge_copy(k, side):
        at = ge_cols(k, side)
        return pltpu.make_async_copy(u_buf.at[1, :, at], grad_emb.at[:, at], ge_sem.at[k // GROUP, side])

    def embed(k, side, g_rows):
        at_cols = ge_cols(k, side)
        grad = contract_cols(eb[mine], g_rows.reshape(GROUP * part_rows, width)) / row_count
        u_buf[1, :, at_cols] = grad
        ge_copy(k, side).start()

        def block(at, sums):
            g = u_buf[1, at, at_cols]
            return sums[0] + fold(g * u_buf[0, at, at_cols]), sums[1] + fold(g)

        zero = jnp.zeros((8, GROUP * part_rows), jnp.float32)
        for row, value in enumerate(row_loop(block, (zero, zero))):
            payload[JOBS, (side * half + k * part_rows) // TILE, row : row + 1] = jnp.sum(value, axis=0, keepdims=True)

    def stage(i, k):
        if i == 0:
            pl.when(k % GROUP == 0)(lambda: form(k))
            return
        chunks.stage(i, k)
        if i == 8:
            swap(k).start()

            @pl.when(k % GROUP == GROUP - 1)
            def _():
                embed(k - GROUP + 1, core, gathered[pl.ds(k - GROUP + 1, GROUP)])

        if i == 9:
            swap(k).wait_recv()
            swap(k).wait_send()

            @pl.when(k % GROUP == GROUP - 1)
            def _():
                embed(k - GROUP + 1, 1 - core, g_peer[pl.ds(k - GROUP + 1, GROUP)])

    run_slots(FRONT_PLAN, PARTS, stage, lambda t: None)
    for c in range(PLANE):
        payload[JOBS, c, 2:3] = loss[:, c * TILE : (c + 1) * TILE]
    small.begin(JOBS)
    ea_copy().wait_send()
    eb_copy().wait_send()
    small.middle(JOBS)
    for k in range(0, PARTS, GROUP):
        for side in range(2):
            ge_copy(k, side).wait()
    small.last(JOBS)
    small.end(JOBS)

    def dz_tile(i):
        at_cols = rows(i * wide, wide)
        sums = jnp.concatenate([total[JOBS, i * (wide // TILE) + c] for c in range(wide // TILE)], axis=1) / row_count
        mean_gn, mean_g = sums[0:1], sums[1:2]
        inv = stats[JOBS - 2, 1, :, at_cols]

        def block(at, c):
            value = (u_buf[1, at, at_cols] - mean_g - u_buf[0, at, at_cols] * mean_gn) * inv
            x_buf[0, at, at_cols] = value.astype(jnp.bfloat16)
            return c

        row_loop(block, 0)

    loop(0, tiles, dz_tile)
    keep_act(dz).start()
    for c in range(PLANE):
        vec[8, :, c * TILE : (c + 1) * TILE] = total[JOBS, c, 2:3]
    keep_act(dz).wait()


def front(feat_a, feat_b, weights, affine, off_weight):
    rows_dev, width = feat_a.shape
    half = width // 2
    part_rows = half // PARTS
    any_spec = pl.BlockSpec(memory_space=pl.ANY)
    vmem_spec = pl.BlockSpec(memory_space=pltpu.VMEM)
    wide_f32 = jax.ShapeDtypeStruct((rows_dev, width), jnp.float32)
    wide_bf16 = jax.ShapeDtypeStruct((rows_dev, width), jnp.bfloat16)
    dma = pltpu.SemaphoreType.DMA
    return pl.pallas_call(
        front_kernel,
        name="front",
        out_shape=[wide_f32, wide_f32, wide_bf16, wide_bf16, wide_bf16, wide_f32]
        + [jax.ShapeDtypeStruct((9, 1, width), jnp.float32)],
        in_specs=[any_spec] * 8 + [vmem_spec] * 4 + [pl.BlockSpec(memory_space=pltpu.SMEM)],
        out_specs=[any_spec] * 6 + [vmem_spec],
        scratch_shapes=[
            pltpu.VMEM((2, rows_dev, width), jnp.bfloat16),
            pltpu.VMEM((2, rows_dev, width), jnp.float32),
            pltpu.VMEM((W_BUFS, width, WIDE), jnp.bfloat16),
            pltpu.VMEM((JOBS, 2, 1, width), jnp.float32),
            pltpu.VMEM((4, 1, width), jnp.float32),
            pltpu.VMEM((1, width), jnp.float32),
            pltpu.VMEM((2 * rows_dev, half), jnp.bfloat16),
            pltpu.VMEM((2 * rows_dev, width), jnp.bfloat16),
            pltpu.VMEM((PARTS, part_rows, width), jnp.bfloat16),
            dma((2,)),
            dma((W_BUFS,)),
            dma((2,)),
            dma((PARTS // GROUP, 2)),
            dma((2,)),
            dma((2,)),
        ]
        + small_scratch(JOBS + 1)
        + chunk_scratch(PARTS, PARTS, part_rows, width, PARTS, jnp.bfloat16),
        compiler_params=pltpu.CompilerParams(collective_id=0, has_side_effects=True, vmem_limit_bytes=VMEM_BYTES),
    )(feat_a, feat_b, *weights, *affine, off_weight)


def back_kernel(dz_hbm, x2, x1, x0, w_out, w_mid, u2, u1, vec, out2, out1, out0, sums_out, *scratch):
    (dy, xs, w_buf, u_buf, dpre) = scratch[:5]
    (in_sem, tile_sem, peer_send, peer_recv, store_sem) = scratch[5:10]
    small_refs = scratch[10 : 10 + SMALL_REFS]
    acc, gathered, l1, l2, l3, l4, send, recv = scratch[10 + SMALL_REFS :]
    rows_dev, width = dz_hbm.shape
    wide = w_buf.shape[1]
    tiles = width // wide
    row_count = rows_dev * DEPTH * PLANE
    half = width // 2
    part_rows = half // PARTS
    count = MATS * PARTS
    mats_in, outs, weights, pres = (x2, x1, x0), (out2, out1, out0), (w_out, w_mid), (u2, u1)
    place = Place()
    core, other_core = place.core, place.other_core
    mine = rows(core * rows_dev, rows_dev)
    place.arrive()
    small = small_sum(place, small_refs)
    payload, sums = small.payload, small.total

    def own_x(w):
        return pltpu.make_async_copy(mats_in[w].at[:, rows(core * half, half)], xs.at[w % 2, mine], in_sem.at[w])

    def peer_x(w):
        return remote_copy(mats_in[w].at[:, rows((1 - core) * half, half)], xs.at[w % 2, mine], peer_send.at[w], peer_recv.at[w], other_core)

    def peer_dy(w):
        block = dy.at[w % 2, mine]
        return remote_copy(block, block, peer_send.at[MATS + w], peer_recv.at[MATS + w], other_core)

    def x_arrive(w):
        block = xs.at[w % 2, mine]
        pltpu.make_async_copy(block, block, in_sem.at[w]).wait()
        remote_copy(block, block, peer_send.at[w], peer_recv.at[w], other_core).wait_recv()

    def w_tile(ref, i):
        return pltpu.make_async_copy(ref.at[rows(i * wide, wide)], w_buf.at[i % 2], tile_sem.at[0, i % 2])

    def u_tile(ref, i):
        return pltpu.make_async_copy(ref.at[:, rows(i * wide, wide)], u_buf.at[i % 2], tile_sem.at[1, i % 2])

    def start_w(layer, i):
        pick(layer, weights, lambda ref: w_tile(ref, i).start())

    def start_u(layer, i):
        pick(layer, pres, lambda ref: u_tile(ref, i).start())

    dz_load = pltpu.make_async_copy(dz_hbm, dy.at[0, mine], in_sem.at[MATS])
    dz_load.start()
    for w in range(2):
        own_x(w).start()
    w_tile(weights[0], 0).start()
    u_tile(pres[0], 0).start()
    payload[...] = jnp.zeros_like(payload)
    place.all_here()
    peer_x(0).start()
    dz_load.wait()
    peer_dy(0).start()
    peer_x(1).start()

    def row_loop(body, carry):
        return lax.fori_loop(0, rows_dev // BLOCK, body, carry)

    def chain_tile(layer, i):
        w_tile(w_out, i).wait()
        u_tile(u2, i).wait()

        @pl.when(i + 1 < tiles)
        def _():
            start_w(layer, i + 1)
            start_u(layer, i + 1)

        at_cols = rows(i * wide, wide)
        dpre[:, at_cols] = contract_cols(dy[layer, mine], w_buf[i % 2])
        gain, bias, mean, inv = (vec[layer * 4 + j, :, at_cols] for j in range(4))

        def block(r, carry):
            at = rows(r * BLOCK, BLOCK)
            n = (u_buf[i % 2, at] - mean) * inv
            g = jnp.where(n * gain + bias > 0.0, dpre[at, at_cols], 0.0)
            dpre[at, at_cols] = g
            return carry[0] + fold(g * n), carry[1] + fold(g)

        zero = jnp.zeros((8, wide), jnp.float32)
        for row, value in enumerate(row_loop(block, (zero, zero))):
            value = jnp.sum(value, axis=0, keepdims=True)
            for c in range(wide // TILE):
                payload[layer, i * (wide // TILE) + c, row : row + 1] = value[:, c * TILE : (c + 1) * TILE]

    def du(layer):
        start_u(layer, 0)

        def tile(i):
            u_tile(u2, i).wait()
            pl.when(i + 1 < tiles)(lambda: start_u(layer, i + 1))
            at_cols = rows(i * wide, wide)
            gain, mean, inv = (vec[layer * 4 + j, :, at_cols] for j in (0, 2, 3))
            means = jnp.concatenate([sums[layer, i * (wide // TILE) + c] for c in range(wide // TILE)], axis=1) / row_count
            mean_gn, mean_g = means[0:1], means[1:2]
            scale = gain * inv

            def block(r, c):
                at = rows(r * BLOCK, BLOCK)
                n = (u_buf[i % 2, at] - mean) * inv
                value = (dpre[at, at_cols] - mean_g - n * mean_gn) * scale
                dy[1 - layer, rows(core * rows_dev + r * BLOCK, BLOCK), at_cols] = value.astype(jnp.bfloat16)
                return c

            row_loop(block, 0)

        loop(0, tiles, tile)

    def finish(k, off, size, buf):
        j = k % ACC_SLOTS
        gathered[k % GATHER_SLOTS, rows(off, size)] = acc[j, rows(off, size)] + buf[j]

    chunks = ChunkSum(place, BACK_PLAN[2], acc, gathered, (l1, l2, l3, l4), send, recv, finish)

    def form(k):
        w, j = k // PARTS, k % ACC_SLOTS

        @pl.when(k % PARTS == 0)
        def _():
            x_arrive(w)
            peer_dy(w).wait_recv()

        at = rows((k % PARTS) * part_rows, GROUP * part_rows)
        size = min(1024, width)

        def col(c):
            cs = rows(c * size, size)
            acc[pl.ds(j, GROUP), :, cs] = contract_rows(xs[w % 2, :, at], dy[w % 2, :, cs]).reshape(GROUP, part_rows, size)

        loop(0, width // size, col)

    def out_rows(k, side):
        return pl.ds(pl.multiple_of(side * half + (k % PARTS) * part_rows, part_rows), part_rows)

    def last_copy(out, k, side):
        return chunks.copy(gathered.at[k % GATHER_SLOTS], out.at[out_rows(k, side)], 7, k, other_core)

    def store_copy(out, k):
        return pltpu.make_async_copy(gathered.at[k % GATHER_SLOTS], out.at[out_rows(k, core)], store_sem.at[k])

    def stage(i, k):
        if i == 0:
            pl.when(k % GROUP == 0)(lambda: form(k))
            return
        chunks.stage(i, k)
        if i == 8:

            def emit(out):
                last_copy(out, k, core).start()
                store_copy(out, k).start()

            pick(k // PARTS, outs, emit)
        if i == 9:

            def close(out):
                last_copy(out, k, 1 - core).wait_recv()
                store_copy(out, k).wait()
                last_copy(out, k, core).wait_send()

            pick(k // PARTS, outs, close)

    def layer_work(t):
        layer = t // LAYER_SLOTS
        at = t - LAYER_SLOTS * layer
        pl.when(at < tiles)(lambda: chain_tile(layer, at))
        pl.when(at == tiles)(lambda: small.begin(layer))
        pl.when(at == tiles + 1)(lambda: small.middle(layer))
        pl.when(at == tiles + 2)(lambda: small.last(layer))

        @pl.when(at == tiles + 3)
        def _():
            small.end(layer)
            pl.when(layer == 1)(lambda: peer_dy(0).wait_send())
            du(layer)
            peer_dy(layer + 1).start()

            @pl.when(layer == 0)
            def _():
                w_tile(weights[1], 0).start()
                u_tile(pres[1], 0).start()

            @pl.when(layer == 1)
            def _():
                peer_x(0).wait_send()
                own_x(2).start()
                peer_x(2).start()

    run_slots(BACK_PLAN, count, stage, lambda t: pl.when(t < 2 * LAYER_SLOTS)(lambda: layer_work(t)))
    for w in (1, 2):
        peer_x(w).wait_send()
        peer_dy(w).wait_send()
    for c in range(PLANE):
        for row in range(4):
            sums_out[row : row + 1, c * TILE : (c + 1) * TILE] = sums[row // 2, c, row % 2 : row % 2 + 1]
    sums_out[4:5] = jnp.full((1, width), jnp.sum(vec[8]))


def backward(grad_z, x2, x1, x0, w_out, w_mid, u2, u1, vec):
    rows_dev, width = grad_z.shape
    part_rows = width // 2 // PARTS
    count = MATS * PARTS
    any_spec = pl.BlockSpec(memory_space=pl.ANY)
    vmem_spec = pl.BlockSpec(memory_space=pltpu.VMEM)
    mat = jax.ShapeDtypeStruct((width, width), jnp.float32)
    dma = pltpu.SemaphoreType.DMA
    return pl.pallas_call(
        back_kernel,
        name="backward",
        out_shape=[mat, mat, mat, jax.ShapeDtypeStruct((5, width), jnp.float32)],
        in_specs=[any_spec] * 8 + [vmem_spec],
        out_specs=[any_spec] * 3 + [vmem_spec],
        scratch_shapes=[
            pltpu.VMEM((2, 2 * rows_dev, width), jnp.bfloat16),
            pltpu.VMEM((2, 2 * rows_dev, width // 2), jnp.bfloat16),
            pltpu.VMEM((2, WIDE, width), jnp.bfloat16),
            pltpu.VMEM((2, rows_dev, WIDE), jnp.float32),
            pltpu.VMEM((rows_dev, width), jnp.float32),
            dma((MATS + 1,)),
            dma((2, 2)),
            dma((2 * MATS,)),
            dma((2 * MATS,)),
            dma((count,)),
        ]
        + small_scratch(2)
        + chunk_scratch(ACC_SLOTS, GATHER_SLOTS, part_rows, width, count, jnp.float32),
        compiler_params=pltpu.CompilerParams(collective_id=1, has_side_effects=True, vmem_limit_bytes=VMEM_BYTES),
    )(grad_z, x2, x1, x0, w_out, w_mid, u2, u1, vec)


def solution(mesh):
    row_part = P(DATA_AXIS, None)
    replicated = P()

    def local_step(feat_a, feat_b, w_in, w_mid, w_out, t_in, t_mid, t_out, gain_1, bias_1, gain_2, bias_2, off_weight):
        affine = [v.reshape(1, -1) for v in (gain_1, bias_1, gain_2, bias_2)]
        pre_1, pre_2, act_1, act_2, grad_z, grad_emb, vec = front(
            feat_a, feat_b, (w_in, t_in, w_mid, t_mid, w_out, t_out), affine, off_weight.reshape(1)
        )
        grad_w_out, grad_w_mid, grad_w_in, sums = backward(grad_z, act_2, act_1, feat_a, w_out, w_mid, pre_2, pre_1, vec)
        return (sums[4, 0], grad_emb, grad_w_in, grad_w_mid, grad_w_out, sums[2], sums[3], sums[0], sums[1])

    return jax.shard_map(local_step, mesh=mesh, in_specs=(row_part, row_part) + (replicated,) * 11, out_specs=(replicated, row_part) + (replicated,) * 7, check_vma=False)
```

```python
import functools

import jax
import jax.numpy as jnp
from jax import lax
from jax.experimental import pallas as pl
from jax.experimental.pallas import tpu as pltpu
from jax.sharding import PartitionSpec as P

NORM_EPS = 1e-5
DATA_AXIS = "data"
MESH = pl.DeviceIdType.MESH
VMEM_BYTES = 67_043_328
PLANE = 8
DEPTH = 4
TILE = 256
WIDE = 512
BLOCK = 128
SUM_ROWS = 4
PARTS = 16
GROUP = 4
MATS = 3
ACC_SLOTS = 20
GATHER_SLOTS = 16
JOBS = 6
W_BUFS = 3
LAYER_SLOTS = 15
COPY_ROWS = 256
COPY_BUFS = 12
FRONT_PLAN = ((0, 0, 3, 5, 7, 10, 11, 13, 17, 19), (0, 1, 3, 4, 6, 5, 2, 9, 8, 7), (5, 2))
BACK_PLAN = ((0, 0, 5, 7, 10, 12, 13, 16, 20, 23), (0, 1, 9, 5, 3, 2, 8, 7, 4, 6), (4, 2))


def contract_rows(left_op, right_op):
    return lax.dot_general(left_op, right_op, (((0,), (0,)), ((), ())), preferred_element_type=jnp.float32)


def contract_cols(left_op, right_op):
    return lax.dot_general(left_op, right_op, (((1,), (1,)), ((), ())), preferred_element_type=jnp.float32)


def rows(off, size):
    return pl.ds(pl.multiple_of(off, size), size)


def pick(index, choices, what):
    for i, c in enumerate(choices):
        pl.when(index == i)(functools.partial(what, c))


def loop(lo, hi, body):
    def step(i, carry):
        body(i)
        return carry

    lax.fori_loop(lo, hi, step, 0)


def remote_copy(src, dst, send, recv, mate):
    return pltpu.make_async_remote_copy(src, dst, send, recv, device_id=(mate,), device_id_type=MESH)


class Place:
    def __init__(self):
        me = lax.axis_index(DATA_AXIS)
        self.me = me
        self.pos, self.plane = me % PLANE, me // PLANE
        self.core, self.bx, self.by, self.bz0, self.bz1 = me % 2, (me // 2) % 2, (me // 4) % 2, (me // 8) % 2, (me // 16) % 2
        self.other_core = me + 1 - 2 * self.core
        self.mates = [(self.pos + d) % PLANE for d in range(1, PLANE)]
        self.levels = [(self.plane + d) % DEPTH for d in range(1, DEPTH)]

    def peers(self):
        return [self.plane * PLANE + m for m in self.mates] + [lv * PLANE + self.pos for lv in self.levels]

    def arrive(self):
        sem = pltpu.get_barrier_semaphore()
        for peer in self.peers():
            pl.semaphore_signal(sem, inc=1, device_id=(peer,), device_id_type=MESH)

    def all_here(self):
        pl.semaphore_wait(pltpu.get_barrier_semaphore(), PLANE + DEPTH - 2)


class SmallSum:
    def __init__(self, place, payload, total, plane_buf, depth_buf, own_buf, sems):
        self.p, self.payload, self.total = place, payload, total
        self.plane_buf, self.depth_buf, self.own_buf, self.sems = plane_buf, depth_buf, own_buf, sems

    def first(self, j, m, slot):
        s, r = self.sems[0], self.sems[1]
        return remote_copy(self.payload.at[j, m], self.plane_buf.at[j, slot], s.at[j, m], r.at[j, slot], self.p.plane * PLANE + m)

    def second(self, j, lv, slot):
        s, r = self.sems[2], self.sems[3]
        return remote_copy(self.own_buf.at[j, 0], self.depth_buf.at[j, slot], s.at[j, lv], r.at[j, slot], lv * PLANE + self.p.pos)

    def third(self, j, m, slot):
        s, r = self.sems[4], self.sems[5]
        return remote_copy(self.own_buf.at[j, 1], self.total.at[j, slot], s.at[j, m], r.at[j, slot], self.p.plane * PLANE + m)

    def begin(self, j):
        for m in self.p.mates:
            self.first(j, m, self.p.pos).start()
        self.plane_buf[j, self.p.pos] = self.payload[j, self.p.pos]

    def middle(self, j):
        for m in self.p.mates:
            self.first(j, m, m).wait_recv()
        total = self.plane_buf[j, 0]
        for i in range(1, PLANE):
            total = total + self.plane_buf[j, i]
        self.own_buf[j, 0] = total
        self.depth_buf[j, self.p.plane] = total
        for lv in self.p.levels:
            self.second(j, lv, self.p.plane).start()

    def last(self, j):
        for lv in self.p.levels:
            self.second(j, lv, lv).wait_recv()
        total = self.depth_buf[j, 0]
        for i in range(1, DEPTH):
            total = total + self.depth_buf[j, i]
        self.own_buf[j, 1] = total
        self.total[j, self.p.pos] = total
        for m in self.p.mates:
            self.third(j, m, self.p.pos).start()

    def end(self, j):
        for m in self.p.mates:
            self.third(j, m, m).wait_recv()
            self.first(j, m, self.p.pos).wait_send()
            self.third(j, m, self.p.pos).wait_send()
        for lv in self.p.levels:
            self.second(j, lv, self.p.plane).wait_send()


def small_scratch(count):
    def buf(*lead):
        return pltpu.VMEM((count, *lead, SUM_ROWS, TILE), jnp.float32)

    bufs = [buf(PLANE), buf(PLANE), buf(PLANE), buf(DEPTH), buf(2)]
    return bufs + [pltpu.SemaphoreType.DMA((count, n)) for n in (PLANE, PLANE, DEPTH, DEPTH, PLANE, PLANE)]


SMALL_REFS = 11


def small_sum(place, refs):
    payload, total, plane_buf, depth_buf, own_buf = refs[:5]
    return SmallSum(place, payload, total, plane_buf, depth_buf, own_buf, refs[5:])


class ChunkSum:
    def __init__(self, place, z_first, acc, gathered, landing, send, recv, finish):
        self.p, self.z_first_plan, self.slots, self.gather_slots = place, z_first, acc.shape[0], gathered.shape[0]
        self.acc, self.gathered, self.landing, self.send, self.recv, self.finish = acc, gathered, landing, send, recv, finish
        self.size = acc.shape[1]
        core, bx, by = place.core, place.bx, place.by
        self.xy = ((2 + 2 * core, core * by + (1 - core) * bx), (4 - 2 * core, core * bx + (1 - core) * by))
        self.zz = ((8, place.bz0), (16, place.bz1))
        self.is_mid = place.bz0 + place.bz1 - 2 * place.bz0 * place.bz1
        self.z_mate = place.me + 8 * (1 - 2 * place.bz0)
        self.mid_mate = place.me + 8 * (1 - 2 * place.bz1)

    def z_first(self, k):
        every, at = self.z_first_plan
        off = k % every - at
        return 1 - lax.min(off * off, 1)

    def steps(self, k):
        zf = self.z_first(k)
        pairs = []
        for a, b in zip(self.xy + self.zz, self.zz + self.xy):
            stride = zf * b[0] + (1 - zf) * a[0]
            bit = zf * b[1] + (1 - zf) * a[1]
            pairs.append((self.p.me + stride * (1 - 2 * bit), bit))
        s2, s4 = self.size // 2, self.size // 4
        offs = (0, pairs[0][1] * s2, pairs[0][1] * s2 + pairs[1][1] * s4)
        return zf, pairs, offs

    def copy(self, src, dst, stage, k, mate):
        return remote_copy(src, dst, self.send.at[stage, k], self.recv.at[stage, k], mate)

    def down(self, stage, k, off, size, mate):
        j = k % self.slots
        return self.copy(self.acc.at[j, rows(off, size)], self.landing[stage].at[j], stage, k, mate)

    def up(self, stage, k, off, size, mate):
        block = self.gathered.at[k % self.gather_slots, rows(off, size)]
        return self.copy(block, block, stage, k, mate)

    def add(self, k, off, size, buf):
        step = min(size, 16)
        j = k % self.slots

        def body(i):
            at = rows(off + i * step, step)
            self.acc[j, at] = self.acc[j, at] + buf[j, rows(i * step, step)]

        loop(0, size // step, body)

    def stage(self, i, k):
        zf, pairs, offs = self.steps(k)
        s2, s4 = self.size // 2, self.size // 4
        l1, l2, l3, l4 = self.landing
        z_first = zf == 1
        mid = (zf == 0) & (self.is_mid == 1)
        end = (zf == 0) & (self.is_mid == 0)

        half_copy = lambda: self.down(0, k, offs[0] + (1 - pairs[0][1]) * s2, s2, pairs[0][0])
        quarter_copy = lambda: self.down(1, k, offs[1] + (1 - pairs[1][1]) * s4, s4, pairs[1][0])
        inward = lambda: self.down(2, k, offs[2], s4, zf * pairs[2][0] + (1 - zf) * self.z_mate)
        across = lambda: self.down(3, k, offs[2], s4, zf * pairs[3][0] + (1 - zf) * self.mid_mate)
        outward = lambda: self.up(4, k, offs[2], s4, self.z_mate)
        back4 = lambda: self.up(5, k, offs[2], s4, pairs[1][0])
        back2 = lambda: self.up(6, k, offs[1], s2, pairs[0][0])

        if i == 1:
            half_copy().start()
        elif i == 2:
            half_copy().wait_recv()
            self.add(k, offs[1], s2, l1)
            quarter_copy().start()
        elif i == 3:
            quarter_copy().wait_recv()
            self.add(k, offs[2], s4, l2)
            pl.when(z_first | end)(lambda: inward().start())
        elif i == 4:

            @pl.when(z_first | mid)
            def _():
                inward().wait_recv()
                pl.when(z_first)(lambda: inward().wait_send())
                self.add(k, offs[2], s4, l3)
                across().start()

        elif i == 5:

            @pl.when(z_first | mid)
            def _():
                across().wait_recv()
                self.finish(k, offs[2], s4, l4)
                pl.when(mid)(lambda: outward().start())

        elif i == 6:
            pl.when(end)(lambda: outward().wait_recv())
            back4().start()
            half_copy().wait_send()
            quarter_copy().wait_send()
            pl.when(end)(lambda: inward().wait_send())
            pl.when(z_first | mid)(lambda: across().wait_send())
        elif i == 7:
            back4().wait_recv()
            back2().start()
        elif i == 8:
            back2().wait_recv()
        else:
            pl.when(mid)(lambda: outward().wait_send())
            back4().wait_send()
            back2().wait_send()


def run_slots(plan, count, stage, between):
    lags, order, _ = plan

    def slot(t):
        for i in order:
            k = t - lags[i]

            @pl.when((k >= 0) & (k < count))
            def _():
                stage(i, k)

            if i == 1:
                between(t)

    loop(0, count + lags[-1], slot)


def chunk_scratch(slots, gather_slots, part_rows, width, count, dtype):
    def buf(n):
        return pltpu.VMEM((slots, n, width), jnp.float32)

    gathered = pltpu.VMEM((gather_slots, part_rows, width), dtype)

    dma = pltpu.SemaphoreType.DMA
    return [buf(part_rows), gathered, buf(part_rows // 2), buf(part_rows // 4), buf(part_rows // 4), buf(part_rows // 4)] + [
        dma((8, count)),
        dma((8, count)),
    ]


CHUNK_REFS = 8


def fold(value):
    return jnp.sum(value.reshape(value.shape[0] // 8, 8, value.shape[1]), axis=0)


def front_kernel(feat_a, feat_b, w_in, t_in, w_mid, t_mid, w_out, t_out, gain1, bias1, gain2, bias2, off_weight, pre1, pre2, xs2, xs1, xs0, dz, grad_emb, vec, *scratch):
    (x_buf, u_buf, w_buf, stats, affine, loss, ea, eb, g_peer) = scratch[:9]
    (x_sem, w_sem, pre_sem, keep_sem, keep_send, keep_recv, ge_sem, e_send, e_recv) = scratch[9:18]
    small_refs = scratch[18 : 18 + SMALL_REFS]
    acc, gathered, l1, l2, l3, l4, send, recv = scratch[18 + SMALL_REFS :]
    rows_dev, width = feat_a.shape
    wide = w_buf.shape[2]
    tiles = width // wide
    half = width // 2
    part_rows = half // PARTS
    row_count = rows_dev * DEPTH * PLANE
    weights, feats = (w_in, t_in, w_mid, t_mid, w_out, t_out), (feat_a, feat_b)
    place = Place()
    core = place.core
    mine = rows(core * rows_dev, rows_dev)
    place.arrive()
    small = small_sum(place, small_refs)
    payload, total = small.payload, small.total

    def feat(v):
        return pltpu.make_async_copy(feats[v], x_buf.at[v], x_sem.at[v])

    def w_tile(ref, g):
        return pltpu.make_async_copy(ref.at[:, rows((g % tiles) * wide, wide)], w_buf.at[g % W_BUFS], w_sem.at[g % W_BUFS])

    def start_w(g):
        pick(g // tiles, weights, lambda ref: w_tile(ref, g).start())

    feat(0).start()
    w_tile(weights[0], 0).start()
    feat(1).start()
    for g in range(1, W_BUFS - 1):
        start_w(g)
    for j, ref in enumerate((gain1, bias1, gain2, bias2)):
        affine[j] = ref[...]
    feat(0).wait()
    payload[...] = jnp.zeros_like(payload)

    def keep_pre(ref):
        return pltpu.make_async_copy(u_buf.at[0], ref, pre_sem.at[0])

    kept = (xs0, xs1, xs2)

    def keep_x(w):
        here = pltpu.make_async_copy(x_buf.at[0, :, rows(core * half, half)], kept[w].at[mine], keep_sem.at[w])
        there = remote_copy(x_buf.at[0, :, rows((1 - core) * half, half)], kept[w].at[mine], keep_send.at[w], keep_recv.at[w], place.other_core)
        return here, there

    def start_x(w):
        for c in keep_x(w):
            c.start()

    def free_x(w):
        here, there = keep_x(w)
        here.wait()
        there.wait_send()

    def keep_dz(i):
        at = (slice(None), rows(i * wide, wide))
        here = pltpu.make_async_copy(x_buf.at[(0, *at)], dz.at[mine, at[1]], keep_sem.at[3 + i])
        there = remote_copy(x_buf.at[(0, *at)], dz.at[mine, at[1]], keep_send.at[3 + i], keep_recv.at[3 + i], place.other_core)
        return here, there

    def row_loop(body, carry):
        return lax.fori_loop(0, rows_dev // BLOCK, lambda r, c: body(rows(r * BLOCK, BLOCK), c), carry)

    def put_sums(j, i, row, value):
        value = jnp.sum(value, axis=0, keepdims=True)
        for c in range(value.shape[1] // TILE):
            payload[j, i + c, row : row + 1] = value[:, c * TILE : (c + 1) * TILE]

    def product(g):
        job, i = g // tiles, g % tiles
        view = job % 2
        w_tile(w_in, g).wait()
        pl.when(g + W_BUFS - 1 < JOBS * tiles)(lambda: start_w(g + W_BUFS - 1))
        at_cols = rows(i * wide, wide)
        u_buf[view, :, at_cols] = jnp.dot(x_buf[view], w_buf[g % W_BUFS], preferred_element_type=jnp.float32)

        def block(at, sums):
            u = u_buf[view, at, at_cols]
            return sums[0] + fold(u), sums[1] + fold(u * u)

        zero = jnp.zeros((8, wide), jnp.float32)
        for row, value in enumerate(row_loop(block, (zero, zero))):
            put_sums(job, i * (wide // TILE), row, value)

    def begin(job):
        small.begin(job)

        @pl.when(job % 2 == 0)
        def _():
            pick(job // 2, (pre1, pre2), lambda ref: keep_pre(ref).start())

    def norm(job):
        layer, view = job // 2, job % 2
        small.end(job)
        for c in range(PLANE):
            at = slice(c * TILE, (c + 1) * TILE)
            means = total[job, c] / row_count
            stats[job, 0, :, at] = means[0:1]
            stats[job, 1, :, at] = lax.rsqrt(means[1:2] - means[0:1] * means[0:1] + NORM_EPS)

        pl.when(view == 0)(lambda: pick(layer, (0, 1, 2), free_x))

        def hidden(i):
            at_cols = rows(i * wide, wide)
            mean, inv = stats[job, 0, :, at_cols], stats[job, 1, :, at_cols]
            gain, bias = affine[layer * 2, :, at_cols], affine[layer * 2 + 1, :, at_cols]

            def block(at, c):
                n = (u_buf[view, at, at_cols] - mean) * inv
                x_buf[view, at, at_cols] = jnp.maximum(n * gain + bias, 0.0).astype(jnp.bfloat16)
                return c

            row_loop(block, 0)

        def student(i):
            at_cols = rows(i * wide, wide)
            mean, inv = stats[job, 0, :, at_cols], stats[job, 1, :, at_cols]

            def block(at, c):
                n = (u_buf[0, at, at_cols] - mean) * inv
                u_buf[0, at, at_cols] = n
                x_buf[0, at, at_cols] = n.astype(jnp.bfloat16)
                return c

            row_loop(block, 0)

        def student_own(i):
            def block(r, c):
                ea[rows(core * rows_dev + r * BLOCK, BLOCK), rows(i * wide, wide)] = x_buf[0, rows(r * BLOCK, BLOCK), rows(core * half + i * wide, wide)]
                return c

            lax.fori_loop(0, rows_dev // BLOCK, block, 0)

        def teacher(i):
            at_cols = rows(i * wide, wide)
            mean, inv = stats[job, 0, :, at_cols], stats[job, 1, :, at_cols]

            def block(r, c):
                n = (u_buf[1, rows(r * BLOCK, BLOCK), at_cols] - mean) * inv
                eb[rows(core * rows_dev + r * BLOCK, BLOCK), at_cols] = n.astype(jnp.bfloat16)
                return c

            lax.fori_loop(0, rows_dev // BLOCK, block, 0)

        @pl.when(layer < 2)
        def _():
            loop(0, tiles, hidden)

            @pl.when(view == 0)
            def _():
                pick(layer, (1, 2), start_x)
                keep_pre(pre1).wait()

        @pl.when((layer == 2) & (view == 0))
        def _():
            loop(0, tiles, student)
            ea_copy().start()
            loop(0, tiles // 2, student_own)

        @pl.when((layer == 2) & (view == 1))
        def _():
            loop(0, tiles, teacher)
            eb_copy().start()

    ea_copy = lambda: remote_copy(x_buf.at[0, :, rows((1 - core) * half, half)], ea.at[mine], e_send.at[0], e_recv.at[0], place.other_core)
    eb_copy = lambda: remote_copy(eb.at[mine], eb.at[mine], e_send.at[1], e_recv.at[1], place.other_core)

    def step(g):
        job, i = g // tiles, g % tiles
        view = job % 2
        pl.when(g == tiles)(lambda: feat(1).wait())
        product(g)

        @pl.when(g == 0)
        def _():
            place.all_here()
            start_x(0)

        pl.when((i == 0) & (job > 0))(lambda: small.middle(job - 1))
        pl.when((i == tiles - 2) & (job > 0))(lambda: small.last(job - 1))

        @pl.when(i == tiles - 1)
        def _():
            begin(job)
            pl.when(job > 0)(lambda: norm(job - 1))

    loop(0, JOBS * tiles, step)
    small.middle(JOBS - 1)
    small.last(JOBS - 1)
    norm(JOBS - 1)
    for j, source in enumerate((affine.at[2], affine.at[3], stats.at[2, 0], stats.at[2, 1], affine.at[0], affine.at[1], stats.at[0, 0], stats.at[0, 1])):
        vec[j] = source[...]

    loss[...] = jnp.zeros_like(loss)

    def finish(k, off, size, buf):
        share = 0.5 - 0.25 * chunks.z_first(k).astype(jnp.float32)
        at = rows(off, size)
        corr = (acc[k, at] + buf[k]) / row_count
        row = core * half + k * part_rows + off
        diag = (row + lax.broadcasted_iota(jnp.int32, (size, width), 0)) == lax.broadcasted_iota(jnp.int32, (size, width), 1)
        weight = off_weight[0]
        miss = 1.0 - corr
        loss[...] += share * jnp.sum(jnp.where(diag, miss * miss, weight * (corr * corr)), axis=0, keepdims=True)
        gathered[k, at] = jnp.where(diag, -2.0 * miss, 2.0 * weight * corr).astype(jnp.bfloat16)

    chunks = ChunkSum(place, FRONT_PLAN[2], acc, gathered, (l1, l2, l3, l4), send, recv, finish)

    def form(k):
        @pl.when(k == 0)
        def _():
            ea_copy().wait_recv()
            eb_copy().wait_recv()

        at = rows(k * part_rows, GROUP * part_rows)
        size = min(1024, width)

        def col(c):
            cs = rows(c * size, size)
            acc[pl.ds(k, GROUP), :, cs] = contract_rows(ea[:, at], eb[:, cs]).reshape(GROUP, part_rows, size)

        loop(0, width // size, col)

    def swap(k):
        return chunks.copy(gathered.at[k], g_peer.at[k], 7, k, place.other_core)

    def ge_cols(k, side):
        return rows(side * half + k * part_rows, GROUP * part_rows)

    def ge_copy(k, side):
        at = ge_cols(k, side)
        return pltpu.make_async_copy(u_buf.at[1, :, at], grad_emb.at[:, at], ge_sem.at[k // GROUP, side])

    def embed(k, side, g_rows):
        at_cols = ge_cols(k, side)
        grad = contract_cols(eb[mine], g_rows.reshape(GROUP * part_rows, width)) / row_count
        u_buf[1, :, at_cols] = grad
        ge_copy(k, side).start()

        def block(at, sums):
            g = u_buf[1, at, at_cols]
            return sums[0] + fold(g * u_buf[0, at, at_cols]), sums[1] + fold(g)

        zero = jnp.zeros((8, GROUP * part_rows), jnp.float32)
        for row, value in enumerate(row_loop(block, (zero, zero))):
            payload[JOBS, (side * half + k * part_rows) // TILE, row : row + 1] = jnp.sum(value, axis=0, keepdims=True)

    def stage(i, k):
        if i == 0:
            pl.when(k % GROUP == 0)(lambda: form(k))
            return
        chunks.stage(i, k)
        if i == 8:
            swap(k).start()

            @pl.when(k % GROUP == GROUP - 1)
            def _():
                embed(k - GROUP + 1, core, gathered[pl.ds(k - GROUP + 1, GROUP)])

        if i == 9:
            swap(k).wait_recv()
            swap(k).wait_send()

            @pl.when(k % GROUP == GROUP - 1)
            def _():
                embed(k - GROUP + 1, 1 - core, g_peer[pl.ds(k - GROUP + 1, GROUP)])

    run_slots(FRONT_PLAN, PARTS, stage, lambda t: None)
    for c in range(PLANE):
        payload[JOBS, c, 2:3] = loss[:, c * TILE : (c + 1) * TILE]
    small.begin(JOBS)
    ea_copy().wait_send()
    eb_copy().wait_send()
    small.middle(JOBS)
    for k in range(0, PARTS, GROUP):
        for side in range(2):
            ge_copy(k, side).wait()
    small.last(JOBS)
    small.end(JOBS)

    def dz_tile(i):
        at_cols = rows(i * wide, wide)
        sums = jnp.concatenate([total[JOBS, i * (wide // TILE) + c] for c in range(wide // TILE)], axis=1) / row_count
        mean_gn, mean_g = sums[0:1], sums[1:2]
        inv = stats[JOBS - 2, 1, :, at_cols]

        def block(at, c):
            value = (u_buf[1, at, at_cols] - mean_g - u_buf[0, at, at_cols] * mean_gn) * inv
            x_buf[0, at, at_cols] = value.astype(jnp.bfloat16)
            return c

        row_loop(block, 0)
        for c in keep_dz(i):
            c.start()

    loop(0, tiles, dz_tile)
    for c in range(PLANE):
        vec[8, :, c * TILE : (c + 1) * TILE] = total[JOBS, c, 2:3]
    for w in range(3):
        keep_x(w)[1].wait_recv()
    for i in range(tiles):
        here, there = keep_dz(i)
        here.wait()
        there.wait()


def front(feat_a, feat_b, weights, affine, off_weight):
    rows_dev, width = feat_a.shape
    half = width // 2
    part_rows = half // PARTS
    any_spec = pl.BlockSpec(memory_space=pl.ANY)
    vmem_spec = pl.BlockSpec(memory_space=pltpu.VMEM)
    wide_f32 = jax.ShapeDtypeStruct((rows_dev, width), jnp.float32)
    kept = jax.ShapeDtypeStruct((2 * rows_dev, half), jnp.bfloat16)
    both_dz = jax.ShapeDtypeStruct((2 * rows_dev, width), jnp.bfloat16)
    keeps = 3 + width // WIDE
    dma = pltpu.SemaphoreType.DMA
    return pl.pallas_call(
        front_kernel,
        name="front",
        out_shape=[wide_f32, wide_f32, kept, kept, kept, both_dz, wide_f32]
        + [jax.ShapeDtypeStruct((9, 1, width), jnp.float32)],
        in_specs=[any_spec] * 8 + [vmem_spec] * 4 + [pl.BlockSpec(memory_space=pltpu.SMEM)],
        out_specs=[any_spec] * 7 + [vmem_spec],
        scratch_shapes=[
            pltpu.VMEM((2, rows_dev, width), jnp.bfloat16),
            pltpu.VMEM((2, rows_dev, width), jnp.float32),
            pltpu.VMEM((W_BUFS, width, WIDE), jnp.bfloat16),
            pltpu.VMEM((JOBS, 2, 1, width), jnp.float32),
            pltpu.VMEM((4, 1, width), jnp.float32),
            pltpu.VMEM((1, width), jnp.float32),
            pltpu.VMEM((2 * rows_dev, half), jnp.bfloat16),
            pltpu.VMEM((2 * rows_dev, width), jnp.bfloat16),
            pltpu.VMEM((PARTS, part_rows, width), jnp.bfloat16),
            dma((2,)),
            dma((W_BUFS,)),
            dma((1,)),
            dma((keeps,)),
            dma((keeps,)),
            dma((keeps,)),
            dma((PARTS // GROUP, 2)),
            dma((2,)),
            dma((2,)),
        ]
        + small_scratch(JOBS + 1)
        + chunk_scratch(PARTS, PARTS, part_rows, width, PARTS, jnp.bfloat16),
        compiler_params=pltpu.CompilerParams(collective_id=0, has_side_effects=True, vmem_limit_bytes=VMEM_BYTES),
    )(feat_a, feat_b, *weights, *affine, off_weight)


def back_kernel(dz_hbm, x2, x1, x0, w_out, w_mid, u2, u1, vec, out2, out1, out0, sums_out, *scratch):
    (dy, xs, w_buf, u_buf, dpre) = scratch[:5]
    (in_sem, tile_sem, peer_send, peer_recv, store_sem) = scratch[5:10]
    small_refs = scratch[10 : 10 + SMALL_REFS]
    acc, gathered, l1, l2, l3, l4, send, recv = scratch[10 + SMALL_REFS :]
    rows_dev, width = dpre.shape
    wide = w_buf.shape[1]
    tiles = width // wide
    row_count = rows_dev * DEPTH * PLANE
    half = width // 2
    part_rows = half // PARTS
    count = MATS * PARTS
    mats_in, outs, weights, pres = (x2, x1, x0), (out2, out1, out0), (w_out, w_mid), (u2, u1)
    place = Place()
    core, other_core = place.core, place.other_core
    mine = rows(core * rows_dev, rows_dev)
    place.arrive()
    small = small_sum(place, small_refs)
    payload, sums = small.payload, small.total

    def load_x(w):
        return pltpu.make_async_copy(mats_in[w], xs.at[w % 2], in_sem.at[w])

    def peer_dy(w):
        block = dy.at[w % 2, mine]
        return remote_copy(block, block, peer_send.at[w], peer_recv.at[w], other_core)

    def w_tile(ref, i):
        return pltpu.make_async_copy(ref.at[rows(i * wide, wide)], w_buf.at[i % 2], tile_sem.at[0, i % 2])

    def u_tile(ref, i):
        return pltpu.make_async_copy(ref.at[:, rows(i * wide, wide)], u_buf.at[i % 2], tile_sem.at[1, i % 2])

    def start_w(layer, i):
        pick(layer, weights, lambda ref: w_tile(ref, i).start())

    def start_u(layer, i):
        pick(layer, pres, lambda ref: u_tile(ref, i).start())

    dz_load = pltpu.make_async_copy(dz_hbm, dy.at[0], in_sem.at[MATS])
    dz_load.start()
    load_x(0).start()
    w_tile(weights[0], 0).start()
    u_tile(pres[0], 0).start()
    load_x(1).start()
    payload[...] = jnp.zeros_like(payload)

    def row_loop(body, carry):
        return lax.fori_loop(0, rows_dev // BLOCK, body, carry)

    def chain_tile(layer, i):
        w_tile(w_out, i).wait()
        u_tile(u2, i).wait()

        @pl.when(i + 1 < tiles)
        def _():
            start_w(layer, i + 1)
            start_u(layer, i + 1)

        at_cols = rows(i * wide, wide)
        dpre[:, at_cols] = contract_cols(dy[layer, mine], w_buf[i % 2])
        gain, bias, mean, inv = (vec[layer * 4 + j, :, at_cols] for j in range(4))

        def block(r, carry):
            at = rows(r * BLOCK, BLOCK)
            n = (u_buf[i % 2, at] - mean) * inv
            g = jnp.where(n * gain + bias > 0.0, dpre[at, at_cols], 0.0)
            dpre[at, at_cols] = g
            return carry[0] + fold(g * n), carry[1] + fold(g)

        zero = jnp.zeros((8, wide), jnp.float32)
        for row, value in enumerate(row_loop(block, (zero, zero))):
            value = jnp.sum(value, axis=0, keepdims=True)
            for c in range(wide // TILE):
                payload[layer, i * (wide // TILE) + c, row : row + 1] = value[:, c * TILE : (c + 1) * TILE]

    def du_tile(layer, i):
        u_tile(u2, i).wait()
        pl.when(i + 1 < tiles)(lambda: start_u(layer, i + 1))
        at_cols = rows(i * wide, wide)
        gain, mean, inv = (vec[layer * 4 + j, :, at_cols] for j in (0, 2, 3))
        means = jnp.concatenate([sums[layer, i * (wide // TILE) + c] for c in range(wide // TILE)], axis=1) / row_count
        mean_gn, mean_g = means[0:1], means[1:2]
        scale = gain * inv

        def block(r, c):
            at = rows(r * BLOCK, BLOCK)
            n = (u_buf[i % 2, at] - mean) * inv
            value = (dpre[at, at_cols] - mean_g - n * mean_gn) * scale
            dy[1 - layer, rows(core * rows_dev + r * BLOCK, BLOCK), at_cols] = value.astype(jnp.bfloat16)
            return c

        row_loop(block, 0)

    def finish(k, off, size, buf):
        j = k % ACC_SLOTS
        gathered[k % GATHER_SLOTS, rows(off, size)] = acc[j, rows(off, size)] + buf[j]

    chunks = ChunkSum(place, BACK_PLAN[2], acc, gathered, (l1, l2, l3, l4), send, recv, finish)

    def form(k):
        w, j = k // PARTS, k % ACC_SLOTS

        @pl.when(k % PARTS == 0)
        def _():
            pltpu.make_async_copy(xs.at[w % 2], xs.at[w % 2], in_sem.at[w]).wait()
            pl.when(w > 0)(lambda: peer_dy(w).wait_recv())

        at = rows((k % PARTS) * part_rows, GROUP * part_rows)
        size = min(1024, width)

        def col(c):
            cs = rows(c * size, size)
            acc[pl.ds(j, GROUP), :, cs] = contract_rows(xs[w % 2, :, at], dy[w % 2, :, cs]).reshape(GROUP, part_rows, size)

        loop(0, width // size, col)

    def out_rows(k, side):
        return pl.ds(pl.multiple_of(side * half + (k % PARTS) * part_rows, part_rows), part_rows)

    def last_copy(out, k, side):
        return chunks.copy(gathered.at[k % GATHER_SLOTS], out.at[out_rows(k, side)], 7, k, other_core)

    def store_copy(out, k):
        return pltpu.make_async_copy(gathered.at[k % GATHER_SLOTS], out.at[out_rows(k, core)], store_sem.at[k])

    def stage(i, k):
        if i == 0:
            pl.when((k % GROUP == 0) & (k > 0))(lambda: form(k))
            return
        chunks.stage(i, k)
        if i == 8:

            def emit(out):
                last_copy(out, k, core).start()
                store_copy(out, k).start()

            pick(k // PARTS, outs, emit)
        if i == 9:

            def close(out):
                last_copy(out, k, 1 - core).wait_recv()
                store_copy(out, k).wait()
                last_copy(out, k, core).wait_send()

            pick(k // PARTS, outs, close)

    def layer_work(t):
        layer = t // LAYER_SLOTS
        at = t - LAYER_SLOTS * layer
        first_du = 2 * tiles + 3
        pl.when((at < 2 * tiles) & (at % 2 == 1))(lambda: chain_tile(layer, at // 2))
        pl.when(at == 2 * tiles)(lambda: small.begin(layer))
        pl.when(at == 2 * tiles + 1)(lambda: small.middle(layer))

        @pl.when(at == 2 * tiles + 2)
        def _():
            small.last(layer)
            start_u(layer, 0)

        pl.when(at == first_du)(lambda: small.end(layer))
        pl.when(at >= first_du)(lambda: du_tile(layer, at - first_du))

        @pl.when(at == LAYER_SLOTS - 1)
        def _():
            peer_dy(layer + 1).start()

            @pl.when(layer == 0)
            def _():
                w_tile(weights[1], 0).start()
                u_tile(pres[1], 0).start()

            pl.when(layer == 1)(lambda: load_x(2).start())

    dz_load.wait()
    form(0)
    place.all_here()
    run_slots(BACK_PLAN, count, stage, lambda t: pl.when(t < 2 * LAYER_SLOTS)(lambda: layer_work(t)))
    for w in (1, 2):
        peer_dy(w).wait_send()
    for c in range(PLANE):
        for row in range(4):
            sums_out[row : row + 1, c * TILE : (c + 1) * TILE] = sums[row // 2, c, row % 2 : row % 2 + 1]
    sums_out[4:5] = jnp.full((1, width), jnp.sum(vec[8]))


def backward(grad_z, x2, x1, x0, w_out, w_mid, u2, u1, vec):
    rows_dev, width = u2.shape
    part_rows = width // 2 // PARTS
    count = MATS * PARTS
    any_spec = pl.BlockSpec(memory_space=pl.ANY)
    vmem_spec = pl.BlockSpec(memory_space=pltpu.VMEM)
    mat = jax.ShapeDtypeStruct((width, width), jnp.float32)
    dma = pltpu.SemaphoreType.DMA
    return pl.pallas_call(
        back_kernel,
        name="backward",
        out_shape=[mat, mat, mat, jax.ShapeDtypeStruct((5, width), jnp.float32)],
        in_specs=[any_spec] * 8 + [vmem_spec],
        out_specs=[any_spec] * 3 + [vmem_spec],
        scratch_shapes=[
            pltpu.VMEM((2, 2 * rows_dev, width), jnp.bfloat16),
            pltpu.VMEM((2, 2 * rows_dev, width // 2), jnp.bfloat16),
            pltpu.VMEM((2, WIDE, width), jnp.bfloat16),
            pltpu.VMEM((2, rows_dev, WIDE), jnp.float32),
            pltpu.VMEM((rows_dev, width), jnp.float32),
            dma((MATS + 1,)),
            dma((2, 2)),
            dma((MATS,)),
            dma((MATS,)),
            dma((count,)),
        ]
        + small_scratch(2)
        + chunk_scratch(ACC_SLOTS, GATHER_SLOTS, part_rows, width, count, jnp.float32),
        compiler_params=pltpu.CompilerParams(collective_id=1, has_side_effects=True, vmem_limit_bytes=VMEM_BYTES),
    )(grad_z, x2, x1, x0, w_out, w_mid, u2, u1, vec)


def copy_kernel(*refs):
    pairs = len(refs[:-3]) // 2
    ins, outs, (buf, in_sem, out_sem) = refs[:pairs], refs[pairs : 2 * pairs], refs[2 * pairs :]
    blocks = [(i, r) for i in range(pairs) for r in range(0, ins[i].shape[0], COPY_ROWS)]

    def read(b):
        i, r = blocks[b]
        return pltpu.make_async_copy(ins[i].at[pl.ds(r, COPY_ROWS)], buf.at[b % COPY_BUFS], in_sem.at[b % COPY_BUFS])

    def write(b):
        i, r = blocks[b]
        return pltpu.make_async_copy(buf.at[b % COPY_BUFS], outs[i].at[pl.ds(r, COPY_ROWS)], out_sem.at[b % COPY_BUFS])

    ahead = COPY_BUFS // 2
    for b in range(min(ahead, len(blocks))):
        read(b).start()
    for b in range(len(blocks)):
        if b + ahead < len(blocks):
            if b + ahead >= COPY_BUFS:
                write(b + ahead - COPY_BUFS).wait()
            read(b + ahead).start()
        read(b).wait()
        write(b).start()
    for b in range(max(0, len(blocks) - COPY_BUFS), len(blocks)):
        write(b).wait()


def copy_out(*arrays):
    any_spec = pl.BlockSpec(memory_space=pl.ANY)
    dma = pltpu.SemaphoreType.DMA
    return pl.pallas_call(
        copy_kernel,
        name="copy_out",
        out_shape=[jax.ShapeDtypeStruct(a.shape, a.dtype) for a in arrays],
        in_specs=[any_spec] * len(arrays),
        out_specs=[any_spec] * len(arrays),
        scratch_shapes=[pltpu.VMEM((COPY_BUFS, COPY_ROWS, arrays[0].shape[1]), jnp.float32), dma((COPY_BUFS,)), dma((COPY_BUFS,))],
        compiler_params=pltpu.CompilerParams(vmem_limit_bytes=VMEM_BYTES),
    )(*arrays)


def solution(mesh):
    row_part = P(DATA_AXIS, None)
    replicated = P()

    def local_step(feat_a, feat_b, w_in, w_mid, w_out, t_in, t_mid, t_out, gain_1, bias_1, gain_2, bias_2, off_weight):
        affine = [v.reshape(1, -1) for v in (gain_1, bias_1, gain_2, bias_2)]
        pre_1, pre_2, xs_2, xs_1, xs_0, grad_z, grad_emb, vec = front(
            feat_a, feat_b, (w_in, t_in, w_mid, t_mid, w_out, t_out), affine, off_weight.reshape(1)
        )
        grad_w_out, grad_w_mid, grad_w_in, sums = backward(grad_z, xs_2, xs_1, xs_0, w_out, w_mid, pre_2, pre_1, vec)
        grad_emb, grad_w_out, grad_w_mid, grad_w_in = copy_out(grad_emb, grad_w_out, grad_w_mid, grad_w_in)
        return (sums[4, 0], grad_emb, grad_w_in, grad_w_mid, grad_w_out, sums[2], sums[3], sums[0], sums[1])

    return jax.shard_map(local_step, mesh=mesh, in_specs=(row_part, row_part) + (replicated,) * 11, out_specs=(replicated, row_part) + (replicated,) * 7, check_vma=False)
```

```python
import functools

import jax
import jax.numpy as jnp
from jax import lax
from jax.experimental import pallas as pl
from jax.experimental.pallas import tpu as pltpu
from jax.sharding import PartitionSpec as P

NORM_EPS = 1e-5
DATA_AXIS = "data"
MESH = pl.DeviceIdType.MESH
VMEM_BYTES = 67_043_328
PLANE = 8
DEPTH = 4
TILE = 256
WIDE = 512
BLOCK = 128
SUM_ROWS = 4
PARTS = 16
GROUP = 4
MATS = 3
ACC_SLOTS = 20
GATHER_SLOTS = 16
JOBS = 6
W_BUFS = 3
LAYER_SLOTS = 15
COPY_ROWS = 256
COPY_BUFS = 12
FRONT_PLAN = ((0, 0, 3, 5, 7, 9, 12, 13, 16, 17, 18), (0, 6, 3, 4, 9, 10, 8, 5, 2, 7, 1))
BACK_PLAN = ((0, 0, 3, 5, 7, 8, 9, 11, 14, 17, 19), (0, 4, 8, 7, 10, 1, 2, 3, 5, 6, 9))


def front_kind(kind, k):
    s, l = (k % 5 == 2) & (k > 2), k == 2
    return {"s": s, "l": l, "x": (k % 5 != 2)}[kind]


def back_kind(kind, k):
    l = ((k % 5 == 2) & (k < 43)) | ((k % 5 == 0) & (k >= 10) & (k < 36))
    return l if kind == "l" else jnp.logical_not(l)


def contract_rows(left_op, right_op):
    return lax.dot_general(left_op, right_op, (((0,), (0,)), ((), ())), preferred_element_type=jnp.float32)


def contract_cols(left_op, right_op):
    return lax.dot_general(left_op, right_op, (((1,), (1,)), ((), ())), preferred_element_type=jnp.float32)


def rows(off, size):
    return pl.ds(pl.multiple_of(off, size), size)


def pick(index, choices, what):
    for i, c in enumerate(choices):
        pl.when(index == i)(functools.partial(what, c))


def loop(lo, hi, body):
    def step(i, carry):
        body(i)
        return carry

    lax.fori_loop(lo, hi, step, 0)


def remote_copy(src, dst, send, recv, mate):
    return pltpu.make_async_remote_copy(src, dst, send, recv, device_id=(mate,), device_id_type=MESH)


class Place:
    def __init__(self):
        me = lax.axis_index(DATA_AXIS)
        self.me = me
        self.pos, self.plane = me % PLANE, me // PLANE
        self.core, self.bx, self.by, self.bz0, self.bz1 = me % 2, (me // 2) % 2, (me // 4) % 2, (me // 8) % 2, (me // 16) % 2
        self.other_core = me + 1 - 2 * self.core
        self.mates = [(self.pos + d) % PLANE for d in range(1, PLANE)]
        self.levels = [(self.plane + d) % DEPTH for d in range(1, DEPTH)]

    def peers(self):
        return [self.plane * PLANE + m for m in self.mates] + [lv * PLANE + self.pos for lv in self.levels]

    def arrive(self):
        sem = pltpu.get_barrier_semaphore()
        for peer in self.peers():
            pl.semaphore_signal(sem, inc=1, device_id=(peer,), device_id_type=MESH)

    def all_here(self):
        pl.semaphore_wait(pltpu.get_barrier_semaphore(), PLANE + DEPTH - 2)


class SmallSum:
    def __init__(self, place, payload, total, plane_buf, depth_buf, own_buf, sems):
        self.p, self.payload, self.total = place, payload, total
        self.plane_buf, self.depth_buf, self.own_buf, self.sems = plane_buf, depth_buf, own_buf, sems

    def first(self, j, m, slot):
        s, r = self.sems[0], self.sems[1]
        return remote_copy(self.payload.at[j, m], self.plane_buf.at[j, slot], s.at[j, m], r.at[j, slot], self.p.plane * PLANE + m)

    def second(self, j, lv, slot):
        s, r = self.sems[2], self.sems[3]
        return remote_copy(self.own_buf.at[j, 0], self.depth_buf.at[j, slot], s.at[j, lv], r.at[j, slot], lv * PLANE + self.p.pos)

    def third(self, j, m, slot):
        s, r = self.sems[4], self.sems[5]
        return remote_copy(self.own_buf.at[j, 1], self.total.at[j, slot], s.at[j, m], r.at[j, slot], self.p.plane * PLANE + m)

    def begin(self, j):
        for m in self.p.mates:
            self.first(j, m, self.p.pos).start()
        self.plane_buf[j, self.p.pos] = self.payload[j, self.p.pos]

    def middle(self, j):
        for m in self.p.mates:
            self.first(j, m, m).wait_recv()
        total = self.plane_buf[j, 0]
        for i in range(1, PLANE):
            total = total + self.plane_buf[j, i]
        self.own_buf[j, 0] = total
        self.depth_buf[j, self.p.plane] = total
        for lv in self.p.levels:
            self.second(j, lv, self.p.plane).start()

    def last(self, j):
        for lv in self.p.levels:
            self.second(j, lv, lv).wait_recv()
        total = self.depth_buf[j, 0]
        for i in range(1, DEPTH):
            total = total + self.depth_buf[j, i]
        self.own_buf[j, 1] = total
        self.total[j, self.p.pos] = total
        for m in self.p.mates:
            self.third(j, m, self.p.pos).start()

    def end(self, j):
        for m in self.p.mates:
            self.third(j, m, m).wait_recv()
            self.first(j, m, self.p.pos).wait_send()
            self.third(j, m, self.p.pos).wait_send()
        for lv in self.p.levels:
            self.second(j, lv, self.p.plane).wait_send()


def small_scratch(count):
    def buf(*lead):
        return pltpu.VMEM((count, *lead, SUM_ROWS, TILE), jnp.float32)

    bufs = [buf(PLANE), buf(PLANE), buf(PLANE), buf(DEPTH), buf(2)]
    return bufs + [pltpu.SemaphoreType.DMA((count, n)) for n in (PLANE, PLANE, DEPTH, DEPTH, PLANE, PLANE)]


SMALL_REFS = 11


def small_sum(place, refs):
    payload, total, plane_buf, depth_buf, own_buf = refs[:5]
    return SmallSum(place, payload, total, plane_buf, depth_buf, own_buf, refs[5:])


class ChunkSum:
    def __init__(self, place, kinds, is_kind, acc, gathered, landing, send, recv, finish):
        self.p, self.kinds, self.is_kind, self.slots, self.gather_slots = place, kinds, is_kind, acc.shape[0], gathered.shape[0]
        self.acc, self.gathered, self.landing, self.send, self.recv, self.finish = acc, gathered, landing, send, recv, finish
        self.size = acc.shape[1]
        self.s2, self.s4 = self.size // 2, self.size // 4
        core, bx, by, me = place.core, place.bx, place.by, place.me
        first, second = core * by + (1 - core) * bx, core * bx + (1 - core) * by
        self.xy = ((me + (2 + 2 * core) * (1 - 2 * first), first), (me + (4 - 2 * core) * (1 - 2 * second), second))
        self.zz = ((me + 8 * (1 - 2 * place.bz0), place.bz0), (me + 16 * (1 - 2 * place.bz1), place.bz1))
        self.is_mid = place.bz0 + place.bz1 - 2 * place.bz0 * place.bz1
        self.mid, self.end = self.is_mid == 1, self.is_mid == 0
        self.z_mate = self.zz[0][0]
        self.mid_mate = me + 8 * (1 - 2 * place.bz1)

    def copy(self, src, dst, stage, k, mate):
        return remote_copy(src, dst, self.send.at[stage, k], self.recv.at[stage, k], mate)

    def span(self, off, size):
        return pl.ds(pl.multiple_of(off, self.s4), size)

    def down(self, stage, k, off, size, mate, buf=None):
        j = k % self.slots
        buf = self.landing[stage] if buf is None else buf
        return self.copy(self.acc.at[j, self.span(off, size)], buf.at[j, pl.ds(0, size)], stage, k, mate)

    def up(self, stage, k, off, size, mate):
        block = self.gathered.at[k % self.gather_slots, self.span(off, size)]
        return self.copy(block, block, stage, k, mate)

    def add(self, k, off, size, buf):
        step = min(size, 16)
        j = k % self.slots

        def body(i):
            at = pl.ds(pl.multiple_of(off + i * step, step), step)
            self.acc[j, at] = self.acc[j, at] + buf[j, rows(i * step, step)]

        loop(0, size // step, body)

    def stage(self, i, k):
        for kind in self.kinds:
            run = {"x": self.stage_x, "s": self.stage_s, "l": self.stage_l}[kind]
            pl.when(self.is_kind(kind, k))(functools.partial(run, i, k))

    def stage_x(self, i, k):
        (m1, b1), (m2, b2), s2, s4 = *self.xy, self.s2, self.s4
        off1, off2 = b1 * s2, b1 * s2 + b2 * s4
        half = lambda: self.down(0, k, (1 - b1) * s2, s2, m1)
        quarter = lambda: self.down(1, k, off1 + (1 - b2) * s4, s4, m2)
        inward = lambda: self.down(2, k, off2, s4, self.z_mate)
        across = lambda: self.down(3, k, off2, s4, self.mid_mate)
        outward = lambda: self.up(4, k, off2, s4, self.z_mate)
        back4 = lambda: self.up(5, k, off2, s4, m2)
        back2 = lambda: self.up(6, k, off1, s2, m1)
        if i == 1:
            half().start()
        elif i == 2:
            half().wait_recv()
            self.add(k, off1, s2, self.landing[0])
            quarter().start()
        elif i == 3:
            quarter().wait_recv()
            self.add(k, off2, s4, self.landing[1])
            pl.when(self.end)(lambda: inward().start())
        elif i == 4:

            @pl.when(self.mid)
            def _():
                inward().wait_recv()
                self.add(k, off2, s4, self.landing[2])
                across().start()

        elif i == 5:

            @pl.when(self.mid)
            def _():
                across().wait_recv()
                self.finish(k, off2, s4, self.landing[3])
                outward().start()

        elif i == 6:
            pl.when(self.end)(lambda: outward().wait_recv())
            back4().start()
            half().wait_send()
            quarter().wait_send()
            pl.when(self.end)(lambda: inward().wait_send())
            pl.when(self.mid)(lambda: across().wait_send())
        elif i == 7:
            back4().wait_recv()
            back2().start()
        elif i == 8:
            back2().wait_recv()
        elif i == 10:
            pl.when(self.mid)(lambda: outward().wait_send())
            back4().wait_send()
            back2().wait_send()

    def stage_s(self, i, k):
        (m1, b1), (m2, b2), s2, s4 = *self.zz, self.s2, self.s4
        off1, off2 = b1 * s2, b1 * s2 + b2 * s4
        half = lambda: self.down(0, k, (1 - b1) * s2, s2, m1)
        quarter = lambda: self.down(1, k, off1 + (1 - b2) * s4, s4, m2)
        whole_1 = lambda: self.down(2, k, off2, s4, self.xy[0][0])
        whole_2 = lambda: self.down(3, k, off2, s4, self.xy[1][0])
        back4 = lambda: self.up(5, k, off2, s4, m2)
        back2 = lambda: self.up(6, k, off1, s2, m1)
        if i == 1:
            half().start()
        elif i == 2:
            half().wait_recv()
            self.add(k, off1, s2, self.landing[0])
            quarter().start()
        elif i == 3:
            quarter().wait_recv()
            self.add(k, off2, s4, self.landing[1])
            whole_1().start()
        elif i == 4:
            whole_1().wait_recv()
            whole_1().wait_send()
            self.add(k, off2, s4, self.landing[2])
            whole_2().start()
        elif i == 5:
            whole_2().wait_recv()
            self.finish(k, off2, s4, self.landing[3])
        elif i == 6:
            back4().start()
            half().wait_send()
            quarter().wait_send()
            whole_2().wait_send()
        elif i == 7:
            back4().wait_recv()
            back2().start()
        elif i == 8:
            back2().wait_recv()
        elif i == 10:
            back4().wait_send()
            back2().wait_send()

    def stage_l(self, i, k):
        s2, s4 = self.s2, self.s4
        s3 = s2 + s4
        b0, b1 = self.p.bz0, self.p.bz1
        own, side, tip, rest = (2 * b1 + b0) * s4, b1 * s2, 3 * b1 * s4, (1 - b1) * s4
        inward = lambda: self.down(0, k, rest, s3, self.z_mate)
        across = lambda: self.down(1, k, (1 - b1) * s2, s2, self.mid_mate)
        outward = lambda: self.down(2, k, tip, s4, self.z_mate)
        whole_1 = lambda: self.down(3, k, own, s4, self.xy[0][0])
        whole_2 = lambda: self.down(8, k, own, s4, self.xy[1][0], self.landing[4])
        tip_back = lambda: self.up(4, k, tip, s4, self.z_mate)
        side_back = lambda: self.up(5, k, side, s2, self.mid_mate)
        rest_back = lambda: self.up(6, k, rest, s3, self.z_mate)
        if i == 1:
            pl.when(self.end)(lambda: inward().start())
        elif i == 2:

            @pl.when(self.mid)
            def _():
                inward().wait_recv()
                self.add(k, rest, s3, self.landing[0])
                across().start()

        elif i == 3:

            @pl.when(self.mid)
            def _():
                across().wait_recv()
                self.add(k, side, s2, self.landing[1])
                outward().start()

        elif i == 4:

            @pl.when(self.end)
            def _():
                outward().wait_recv()
                self.add(k, own, s4, self.landing[2])

            whole_1().start()
        elif i == 5:
            whole_1().wait_recv()
            whole_1().wait_send()
            pl.when(self.mid)(lambda: outward().wait_send())
            self.add(k, own, s4, self.landing[3])
            whole_2().start()
        elif i == 6:
            whole_2().wait_recv()
            self.finish(k, own, s4, self.landing[4])
            pl.when(self.end)(lambda: tip_back().start())
            whole_2().wait_send()
            pl.when(self.end)(lambda: inward().wait_send())
            pl.when(self.mid)(lambda: across().wait_send())
        elif i == 7:

            @pl.when(self.mid)
            def _():
                tip_back().wait_recv()
                side_back().start()

        elif i == 8:

            @pl.when(self.mid)
            def _():
                side_back().wait_recv()
                rest_back().start()

        elif i == 9:
            pl.when(self.end)(lambda: rest_back().wait_recv())
        elif i == 10:
            pl.when(self.end)(lambda: tip_back().wait_send())

            @pl.when(self.mid)
            def _():
                side_back().wait_send()
                rest_back().wait_send()


def run_slots(plan, count, stage, between):
    lags, order = plan

    def slot(t):
        for i in order:
            k = t - lags[i]

            @pl.when((k >= 0) & (k < count))
            def _():
                stage(i, k)

            if i == 1:
                between(t)

    loop(0, count + lags[-1], slot)


def chunk_scratch(slots, gather_slots, part_rows, width, count, dtype):
    def buf(n):
        return pltpu.VMEM((slots, n, width), jnp.float32)

    gathered = pltpu.VMEM((gather_slots, part_rows, width), dtype)

    dma = pltpu.SemaphoreType.DMA
    quarter = part_rows // 4
    return [buf(part_rows), gathered, *(buf(n * quarter) for n in (3, 2, 1, 1, 1)), dma((9, count)), dma((9, count))]


def fold(value):
    return jnp.sum(value.reshape(value.shape[0] // 8, 8, value.shape[1]), axis=0)


def front_kernel(feat_a, feat_b, w_in, t_in, w_mid, t_mid, w_out, t_out, gain1, bias1, gain2, bias2, off_weight, pre1, pre2, xs2, xs1, xs0, dz, grad_emb, vec, *scratch):
    (x_buf, u_buf, w_buf, stats, affine, loss, ea, eb, g_peer) = scratch[:9]
    (x_sem, w_sem, pre_sem, keep_sem, keep_send, keep_recv, ge_sem, e_send, e_recv) = scratch[9:18]
    small_refs = scratch[18 : 18 + SMALL_REFS]
    acc, gathered, *landing, send, recv = scratch[18 + SMALL_REFS :]
    rows_dev, width = feat_a.shape
    wide = w_buf.shape[2]
    tiles = width // wide
    half = width // 2
    part_rows = half // PARTS
    row_count = rows_dev * DEPTH * PLANE
    weights, feats = (w_in, t_in, w_mid, t_mid, w_out, t_out), (feat_a, feat_b)
    place = Place()
    core = place.core
    mine = rows(core * rows_dev, rows_dev)
    place.arrive()
    small = small_sum(place, small_refs)
    payload, total = small.payload, small.total

    def feat(v):
        return pltpu.make_async_copy(feats[v], x_buf.at[v], x_sem.at[v])

    def w_tile(ref, g):
        return pltpu.make_async_copy(ref.at[:, rows((g % tiles) * wide, wide)], w_buf.at[g % W_BUFS], w_sem.at[g % W_BUFS])

    def start_w(g):
        pick(g // tiles, weights, lambda ref: w_tile(ref, g).start())

    feat(0).start()
    w_tile(weights[0], 0).start()
    feat(1).start()
    for g in range(1, W_BUFS - 1):
        start_w(g)
    for j, ref in enumerate((gain1, bias1, gain2, bias2)):
        affine[j] = ref[...]
    feat(0).wait()
    payload[...] = jnp.zeros_like(payload)

    def keep_pre(ref):
        return pltpu.make_async_copy(u_buf.at[0], ref, pre_sem.at[0])

    kept = (xs0, xs1, xs2)

    def keep_x(w):
        here = pltpu.make_async_copy(x_buf.at[0, :, rows(core * half, half)], kept[w].at[mine], keep_sem.at[w])
        there = remote_copy(x_buf.at[0, :, rows((1 - core) * half, half)], kept[w].at[mine], keep_send.at[w], keep_recv.at[w], place.other_core)
        return here, there

    def start_x(w):
        for c in keep_x(w):
            c.start()

    def free_x(w):
        here, there = keep_x(w)
        here.wait()
        there.wait_send()

    def keep_dz(i):
        at = (slice(None), rows(i * wide, wide))
        here = pltpu.make_async_copy(x_buf.at[(0, *at)], dz.at[mine, at[1]], keep_sem.at[3 + i])
        there = remote_copy(x_buf.at[(0, *at)], dz.at[mine, at[1]], keep_send.at[3 + i], keep_recv.at[3 + i], place.other_core)
        return here, there

    def row_loop(body, carry):
        return lax.fori_loop(0, rows_dev // BLOCK, lambda r, c: body(rows(r * BLOCK, BLOCK), c), carry)

    def put_sums(j, i, row, value):
        value = jnp.sum(value, axis=0, keepdims=True)
        for c in range(value.shape[1] // TILE):
            payload[j, i + c, row : row + 1] = value[:, c * TILE : (c + 1) * TILE]

    def product(g):
        job, i = g // tiles, g % tiles
        view = job % 2
        w_tile(w_in, g).wait()
        pl.when(g + W_BUFS - 1 < JOBS * tiles)(lambda: start_w(g + W_BUFS - 1))
        at_cols = rows(i * wide, wide)
        u_buf[view, :, at_cols] = jnp.dot(x_buf[view], w_buf[g % W_BUFS], preferred_element_type=jnp.float32)

        def block(at, sums):
            u = u_buf[view, at, at_cols]
            return sums[0] + fold(u), sums[1] + fold(u * u)

        zero = jnp.zeros((8, wide), jnp.float32)
        for row, value in enumerate(row_loop(block, (zero, zero))):
            put_sums(job, i * (wide // TILE), row, value)

    def begin(job):
        small.begin(job)

        @pl.when(job % 2 == 0)
        def _():
            pick(job // 2, (pre1, pre2), lambda ref: keep_pre(ref).start())

    def norm(job):
        layer, view = job // 2, job % 2
        small.end(job)
        for c in range(PLANE):
            at = slice(c * TILE, (c + 1) * TILE)
            means = total[job, c] / row_count
            stats[job, 0, :, at] = means[0:1]
            stats[job, 1, :, at] = lax.rsqrt(means[1:2] - means[0:1] * means[0:1] + NORM_EPS)

        pl.when(view == 0)(lambda: pick(layer, (0, 1, 2), free_x))

        def hidden(i):
            at_cols = rows(i * wide, wide)
            mean, inv = stats[job, 0, :, at_cols], stats[job, 1, :, at_cols]
            gain, bias = affine[layer * 2, :, at_cols], affine[layer * 2 + 1, :, at_cols]

            def block(at, c):
                n = (u_buf[view, at, at_cols] - mean) * inv
                x_buf[view, at, at_cols] = jnp.maximum(n * gain + bias, 0.0).astype(jnp.bfloat16)
                return c

            row_loop(block, 0)

        def student(i):
            at_cols = rows(i * wide, wide)
            mean, inv = stats[job, 0, :, at_cols], stats[job, 1, :, at_cols]

            def block(at, c):
                n = (u_buf[0, at, at_cols] - mean) * inv
                u_buf[0, at, at_cols] = n
                x_buf[0, at, at_cols] = n.astype(jnp.bfloat16)
                return c

            row_loop(block, 0)

        def student_own(i):
            def block(r, c):
                ea[rows(core * rows_dev + r * BLOCK, BLOCK), rows(i * wide, wide)] = x_buf[0, rows(r * BLOCK, BLOCK), rows(core * half + i * wide, wide)]
                return c

            lax.fori_loop(0, rows_dev // BLOCK, block, 0)

        def teacher(i):
            at_cols = rows(i * wide, wide)
            mean, inv = stats[job, 0, :, at_cols], stats[job, 1, :, at_cols]

            def block(r, c):
                n = (u_buf[1, rows(r * BLOCK, BLOCK), at_cols] - mean) * inv
                eb[rows(core * rows_dev + r * BLOCK, BLOCK), at_cols] = n.astype(jnp.bfloat16)
                return c

            lax.fori_loop(0, rows_dev // BLOCK, block, 0)

        @pl.when(layer < 2)
        def _():
            loop(0, tiles, hidden)

            @pl.when(view == 0)
            def _():
                pick(layer, (1, 2), start_x)
                keep_pre(pre1).wait()

        @pl.when((layer == 2) & (view == 0))
        def _():
            loop(0, tiles, student)
            ea_copy().start()
            loop(0, tiles // 2, student_own)

        @pl.when((layer == 2) & (view == 1))
        def _():
            loop(0, tiles, teacher)
            eb_copy().start()

    ea_copy = lambda: remote_copy(x_buf.at[0, :, rows((1 - core) * half, half)], ea.at[mine], e_send.at[0], e_recv.at[0], place.other_core)
    eb_copy = lambda: remote_copy(eb.at[mine], eb.at[mine], e_send.at[1], e_recv.at[1], place.other_core)

    def step(g):
        job, i = g // tiles, g % tiles
        view = job % 2
        pl.when(g == tiles)(lambda: feat(1).wait())
        product(g)

        @pl.when(g == 0)
        def _():
            place.all_here()
            start_x(0)

        pl.when((i == 0) & (job > 0))(lambda: small.middle(job - 1))
        pl.when((i == tiles - 2) & (job > 0))(lambda: small.last(job - 1))

        @pl.when(i == tiles - 1)
        def _():
            begin(job)
            pl.when(job > 0)(lambda: norm(job - 1))

    loop(0, JOBS * tiles, step)
    small.middle(JOBS - 1)
    small.last(JOBS - 1)
    norm(JOBS - 1)
    for j, source in enumerate((affine.at[2], affine.at[3], stats.at[2, 0], stats.at[2, 1], affine.at[0], affine.at[1], stats.at[0, 0], stats.at[0, 1])):
        vec[j] = source[...]

    loss[...] = jnp.zeros_like(loss)

    def finish(k, off, size, buf):
        share = jnp.where(front_kind("x", k), 0.5, 0.25)
        at = rows(off, size)
        corr = (acc[k, at] + buf[k]) / row_count
        row = core * half + k * part_rows + off
        diag = (row + lax.broadcasted_iota(jnp.int32, (size, width), 0)) == lax.broadcasted_iota(jnp.int32, (size, width), 1)
        weight = off_weight[0]
        miss = 1.0 - corr
        loss[...] += share * jnp.sum(jnp.where(diag, miss * miss, weight * (corr * corr)), axis=0, keepdims=True)
        gathered[k, at] = jnp.where(diag, -2.0 * miss, 2.0 * weight * corr).astype(jnp.bfloat16)

    chunks = ChunkSum(place, "xsl", front_kind, acc, gathered, landing, send, recv, finish)

    def form(k):
        @pl.when(k == 0)
        def _():
            ea_copy().wait_recv()
            eb_copy().wait_recv()

        at = rows(k * part_rows, GROUP * part_rows)
        size = min(1024, width)

        def col(c):
            cs = rows(c * size, size)
            acc[pl.ds(k, GROUP), :, cs] = contract_rows(ea[:, at], eb[:, cs]).reshape(GROUP, part_rows, size)

        loop(0, width // size, col)

    def swap(k):
        return chunks.copy(gathered.at[k], g_peer.at[k], 7, k, place.other_core)

    def ge_cols(k, side):
        return rows(side * half + k * part_rows, GROUP * part_rows)

    def ge_copy(k, side):
        at = ge_cols(k, side)
        return pltpu.make_async_copy(u_buf.at[1, :, at], grad_emb.at[:, at], ge_sem.at[k // GROUP, side])

    def embed(k, side, g_rows):
        at_cols = ge_cols(k, side)
        grad = contract_cols(eb[mine], g_rows.reshape(GROUP * part_rows, width)) / row_count
        u_buf[1, :, at_cols] = grad
        ge_copy(k, side).start()

        def block(at, sums):
            g = u_buf[1, at, at_cols]
            return sums[0] + fold(g * u_buf[0, at, at_cols]), sums[1] + fold(g)

        zero = jnp.zeros((8, GROUP * part_rows), jnp.float32)
        for row, value in enumerate(row_loop(block, (zero, zero))):
            payload[JOBS, (side * half + k * part_rows) // TILE, row : row + 1] = jnp.sum(value, axis=0, keepdims=True)

    def stage(i, k):
        if i == 0:
            pl.when(k % GROUP == 0)(lambda: form(k))
            return
        chunks.stage(i, k)
        if i == 8:
            pl.when(jnp.logical_not(front_kind("l", k)))(lambda: swap(k).start())
        if i == 9:
            pl.when(front_kind("l", k))(lambda: swap(k).start())

            @pl.when(k % GROUP == GROUP - 1)
            def _():
                embed(k - GROUP + 1, core, gathered[pl.ds(k - GROUP + 1, GROUP)])

        if i == 10:
            swap(k).wait_recv()
            swap(k).wait_send()

            @pl.when(k % GROUP == GROUP - 1)
            def _():
                embed(k - GROUP + 1, 1 - core, g_peer[pl.ds(k - GROUP + 1, GROUP)])

    run_slots(FRONT_PLAN, PARTS, stage, lambda t: None)
    for c in range(PLANE):
        payload[JOBS, c, 2:3] = loss[:, c * TILE : (c + 1) * TILE]
    small.begin(JOBS)
    ea_copy().wait_send()
    eb_copy().wait_send()
    small.middle(JOBS)
    for k in range(0, PARTS, GROUP):
        for side in range(2):
            ge_copy(k, side).wait()
    small.last(JOBS)
    small.end(JOBS)

    def dz_tile(i):
        at_cols = rows(i * wide, wide)
        sums = jnp.concatenate([total[JOBS, i * (wide // TILE) + c] for c in range(wide // TILE)], axis=1) / row_count
        mean_gn, mean_g = sums[0:1], sums[1:2]
        inv = stats[JOBS - 2, 1, :, at_cols]

        def block(at, c):
            value = (u_buf[1, at, at_cols] - mean_g - u_buf[0, at, at_cols] * mean_gn) * inv
            x_buf[0, at, at_cols] = value.astype(jnp.bfloat16)
            return c

        row_loop(block, 0)
        for c in keep_dz(i):
            c.start()

    loop(0, tiles, dz_tile)
    for c in range(PLANE):
        vec[8, :, c * TILE : (c + 1) * TILE] = total[JOBS, c, 2:3]
    for w in range(3):
        keep_x(w)[1].wait_recv()
    for i in range(tiles):
        here, there = keep_dz(i)
        here.wait()
        there.wait()


def front(feat_a, feat_b, weights, affine, off_weight):
    rows_dev, width = feat_a.shape
    half = width // 2
    part_rows = half // PARTS
    any_spec = pl.BlockSpec(memory_space=pl.ANY)
    vmem_spec = pl.BlockSpec(memory_space=pltpu.VMEM)
    wide_f32 = jax.ShapeDtypeStruct((rows_dev, width), jnp.float32)
    kept = jax.ShapeDtypeStruct((2 * rows_dev, half), jnp.bfloat16)
    both_dz = jax.ShapeDtypeStruct((2 * rows_dev, width), jnp.bfloat16)
    keeps = 3 + width // WIDE
    dma = pltpu.SemaphoreType.DMA
    return pl.pallas_call(
        front_kernel,
        name="front",
        out_shape=[wide_f32, wide_f32, kept, kept, kept, both_dz, wide_f32]
        + [jax.ShapeDtypeStruct((9, 1, width), jnp.float32)],
        in_specs=[any_spec] * 8 + [vmem_spec] * 4 + [pl.BlockSpec(memory_space=pltpu.SMEM)],
        out_specs=[any_spec] * 7 + [vmem_spec],
        scratch_shapes=[
            pltpu.VMEM((2, rows_dev, width), jnp.bfloat16),
            pltpu.VMEM((2, rows_dev, width), jnp.float32),
            pltpu.VMEM((W_BUFS, width, WIDE), jnp.bfloat16),
            pltpu.VMEM((JOBS, 2, 1, width), jnp.float32),
            pltpu.VMEM((4, 1, width), jnp.float32),
            pltpu.VMEM((1, width), jnp.float32),
            pltpu.VMEM((2 * rows_dev, half), jnp.bfloat16),
            pltpu.VMEM((2 * rows_dev, width), jnp.bfloat16),
            pltpu.VMEM((PARTS, part_rows, width), jnp.bfloat16),
            dma((2,)),
            dma((W_BUFS,)),
            dma((1,)),
            dma((keeps,)),
            dma((keeps,)),
            dma((keeps,)),
            dma((PARTS // GROUP, 2)),
            dma((2,)),
            dma((2,)),
        ]
        + small_scratch(JOBS + 1)
        + chunk_scratch(PARTS, PARTS, part_rows, width, PARTS, jnp.bfloat16),
        compiler_params=pltpu.CompilerParams(collective_id=0, has_side_effects=True, vmem_limit_bytes=VMEM_BYTES),
    )(feat_a, feat_b, *weights, *affine, off_weight)


def back_kernel(dz_hbm, x2, x1, x0, w_out, w_mid, u2, u1, vec, out2, out1, out0, sums_out, *scratch):
    (dy, xs, w_buf, u_buf, dpre) = scratch[:5]
    (in_sem, tile_sem, peer_send, peer_recv, store_sem) = scratch[5:10]
    small_refs = scratch[10 : 10 + SMALL_REFS]
    acc, gathered, *landing, send, recv = scratch[10 + SMALL_REFS :]
    rows_dev, width = dpre.shape
    wide = w_buf.shape[1]
    tiles = width // wide
    row_count = rows_dev * DEPTH * PLANE
    half = width // 2
    part_rows = half // PARTS
    count = MATS * PARTS
    mats_in, outs, weights, pres = (x2, x1, x0), (out2, out1, out0), (w_out, w_mid), (u2, u1)
    place = Place()
    core, other_core = place.core, place.other_core
    mine = rows(core * rows_dev, rows_dev)
    place.arrive()
    small = small_sum(place, small_refs)
    payload, sums = small.payload, small.total

    def load_x(w):
        return pltpu.make_async_copy(mats_in[w], xs.at[w % 2], in_sem.at[w])

    def peer_dy(w):
        block = dy.at[w % 2, mine]
        return remote_copy(block, block, peer_send.at[w], peer_recv.at[w], other_core)

    def w_tile(ref, i):
        return pltpu.make_async_copy(ref.at[rows(i * wide, wide)], w_buf.at[i % 2], tile_sem.at[0, i % 2])

    def u_tile(ref, i):
        return pltpu.make_async_copy(ref.at[:, rows(i * wide, wide)], u_buf.at[i % 2], tile_sem.at[1, i % 2])

    def start_w(layer, i):
        pick(layer, weights, lambda ref: w_tile(ref, i).start())

    def start_u(layer, i):
        pick(layer, pres, lambda ref: u_tile(ref, i).start())

    dz_load = pltpu.make_async_copy(dz_hbm, dy.at[0], in_sem.at[MATS])
    dz_load.start()
    load_x(0).start()
    w_tile(weights[0], 0).start()
    u_tile(pres[0], 0).start()
    load_x(1).start()
    payload[...] = jnp.zeros_like(payload)

    def row_loop(body, carry):
        return lax.fori_loop(0, rows_dev // BLOCK, body, carry)

    def chain_tile(layer, i):
        w_tile(w_out, i).wait()
        u_tile(u2, i).wait()

        @pl.when(i + 1 < tiles)
        def _():
            start_w(layer, i + 1)
            start_u(layer, i + 1)

        at_cols = rows(i * wide, wide)
        dpre[:, at_cols] = contract_cols(dy[layer, mine], w_buf[i % 2])
        gain, bias, mean, inv = (vec[layer * 4 + j, :, at_cols] for j in range(4))

        def block(r, carry):
            at = rows(r * BLOCK, BLOCK)
            n = (u_buf[i % 2, at] - mean) * inv
            g = jnp.where(n * gain + bias > 0.0, dpre[at, at_cols], 0.0)
            dpre[at, at_cols] = g
            return carry[0] + fold(g * n), carry[1] + fold(g)

        zero = jnp.zeros((8, wide), jnp.float32)
        for row, value in enumerate(row_loop(block, (zero, zero))):
            value = jnp.sum(value, axis=0, keepdims=True)
            for c in range(wide // TILE):
                payload[layer, i * (wide // TILE) + c, row : row + 1] = value[:, c * TILE : (c + 1) * TILE]

    def du_tile(layer, i):
        u_tile(u2, i).wait()
        pl.when(i + 1 < tiles)(lambda: start_u(layer, i + 1))
        at_cols = rows(i * wide, wide)
        gain, mean, inv = (vec[layer * 4 + j, :, at_cols] for j in (0, 2, 3))
        means = jnp.concatenate([sums[layer, i * (wide // TILE) + c] for c in range(wide // TILE)], axis=1) / row_count
        mean_gn, mean_g = means[0:1], means[1:2]
        scale = gain * inv

        def block(r, c):
            at = rows(r * BLOCK, BLOCK)
            n = (u_buf[i % 2, at] - mean) * inv
            value = (dpre[at, at_cols] - mean_g - n * mean_gn) * scale
            dy[1 - layer, rows(core * rows_dev + r * BLOCK, BLOCK), at_cols] = value.astype(jnp.bfloat16)
            return c

        row_loop(block, 0)

    def finish(k, off, size, buf):
        j = k % ACC_SLOTS
        gathered[k % GATHER_SLOTS, rows(off, size)] = acc[j, rows(off, size)] + buf[j]

    chunks = ChunkSum(place, "xl", back_kind, acc, gathered, landing, send, recv, finish)

    def form(k):
        w, j = k // PARTS, k % ACC_SLOTS

        @pl.when(k % PARTS == 0)
        def _():
            pltpu.make_async_copy(xs.at[w % 2], xs.at[w % 2], in_sem.at[w]).wait()
            pl.when(w > 0)(lambda: peer_dy(w).wait_recv())

        at = rows((k % PARTS) * part_rows, GROUP * part_rows)
        size = min(1024, width)

        def col(c):
            cs = rows(c * size, size)
            acc[pl.ds(j, GROUP), :, cs] = contract_rows(xs[w % 2, :, at], dy[w % 2, :, cs]).reshape(GROUP, part_rows, size)

        loop(0, width // size, col)

    def out_rows(k, side):
        return pl.ds(pl.multiple_of(side * half + (k % PARTS) * part_rows, part_rows), part_rows)

    def last_copy(out, k, side):
        return chunks.copy(gathered.at[k % GATHER_SLOTS], out.at[out_rows(k, side)], 7, k, other_core)

    def store_copy(out, k):
        return pltpu.make_async_copy(gathered.at[k % GATHER_SLOTS], out.at[out_rows(k, core)], store_sem.at[k])

    def stage(i, k):
        if i == 0:
            pl.when((k % GROUP == 0) & (k > 0))(lambda: form(k))
            return
        chunks.stage(i, k)
        def emit(out):
            last_copy(out, k, core).start()
            store_copy(out, k).start()

        if i == 8:
            pl.when(back_kind("x", k))(lambda: pick(k // PARTS, outs, emit))
        if i == 9:
            pl.when(back_kind("l", k))(lambda: pick(k // PARTS, outs, emit))
        if i == 10:

            def close(out):
                last_copy(out, k, 1 - core).wait_recv()
                store_copy(out, k).wait()
                last_copy(out, k, core).wait_send()

            pick(k // PARTS, outs, close)

    def layer_work(t):
        layer = t // LAYER_SLOTS
        at = t - LAYER_SLOTS * layer
        first_du = 2 * tiles + 3
        pl.when((at < 2 * tiles) & (at % 2 == 1))(lambda: chain_tile(layer, at // 2))
        pl.when(at == 2 * tiles)(lambda: small.begin(layer))
        pl.when(at == 2 * tiles + 1)(lambda: small.middle(layer))

        @pl.when(at == 2 * tiles + 2)
        def _():
            small.last(layer)
            start_u(layer, 0)

        pl.when(at == first_du)(lambda: small.end(layer))
        pl.when(at >= first_du)(lambda: du_tile(layer, at - first_du))

        @pl.when(at == LAYER_SLOTS - 1)
        def _():
            peer_dy(layer + 1).start()

            @pl.when(layer == 0)
            def _():
                w_tile(weights[1], 0).start()
                u_tile(pres[1], 0).start()

            pl.when(layer == 1)(lambda: load_x(2).start())

    dz_load.wait()
    form(0)
    place.all_here()
    run_slots(BACK_PLAN, count, stage, lambda t: pl.when(t < 2 * LAYER_SLOTS)(lambda: layer_work(t)))
    for w in (1, 2):
        peer_dy(w).wait_send()
    for c in range(PLANE):
        for row in range(4):
            sums_out[row : row + 1, c * TILE : (c + 1) * TILE] = sums[row // 2, c, row % 2 : row % 2 + 1]
    sums_out[4:5] = jnp.full((1, width), jnp.sum(vec[8]))


def backward(grad_z, x2, x1, x0, w_out, w_mid, u2, u1, vec):
    rows_dev, width = u2.shape
    part_rows = width // 2 // PARTS
    count = MATS * PARTS
    any_spec = pl.BlockSpec(memory_space=pl.ANY)
    vmem_spec = pl.BlockSpec(memory_space=pltpu.VMEM)
    mat = jax.ShapeDtypeStruct((width, width), jnp.float32)
    dma = pltpu.SemaphoreType.DMA
    return pl.pallas_call(
        back_kernel,
        name="backward",
        out_shape=[mat, mat, mat, jax.ShapeDtypeStruct((5, width), jnp.float32)],
        in_specs=[any_spec] * 8 + [vmem_spec],
        out_specs=[any_spec] * 3 + [vmem_spec],
        scratch_shapes=[
            pltpu.VMEM((2, 2 * rows_dev, width), jnp.bfloat16),
            pltpu.VMEM((2, 2 * rows_dev, width // 2), jnp.bfloat16),
            pltpu.VMEM((2, WIDE, width), jnp.bfloat16),
            pltpu.VMEM((2, rows_dev, WIDE), jnp.float32),
            pltpu.VMEM((rows_dev, width), jnp.float32),
            dma((MATS + 1,)),
            dma((2, 2)),
            dma((MATS,)),
            dma((MATS,)),
            dma((count,)),
        ]
        + small_scratch(2)
        + chunk_scratch(ACC_SLOTS, GATHER_SLOTS, part_rows, width, count, jnp.float32),
        compiler_params=pltpu.CompilerParams(collective_id=1, has_side_effects=True, vmem_limit_bytes=VMEM_BYTES),
    )(grad_z, x2, x1, x0, w_out, w_mid, u2, u1, vec)


def copy_kernel(*refs):
    pairs = len(refs[:-3]) // 2
    ins, outs, (buf, in_sem, out_sem) = refs[:pairs], refs[pairs : 2 * pairs], refs[2 * pairs :]
    blocks = [(i, r) for i in range(pairs) for r in range(0, ins[i].shape[0], COPY_ROWS)]

    def read(b):
        i, r = blocks[b]
        return pltpu.make_async_copy(ins[i].at[pl.ds(r, COPY_ROWS)], buf.at[b % COPY_BUFS], in_sem.at[b % COPY_BUFS])

    def write(b):
        i, r = blocks[b]
        return pltpu.make_async_copy(buf.at[b % COPY_BUFS], outs[i].at[pl.ds(r, COPY_ROWS)], out_sem.at[b % COPY_BUFS])

    ahead = COPY_BUFS // 2
    for b in range(min(ahead, len(blocks))):
        read(b).start()
    for b in range(len(blocks)):
        if b + ahead < len(blocks):
            if b + ahead >= COPY_BUFS:
                write(b + ahead - COPY_BUFS).wait()
            read(b + ahead).start()
        read(b).wait()
        write(b).start()
    for b in range(max(0, len(blocks) - COPY_BUFS), len(blocks)):
        write(b).wait()


def copy_out(*arrays):
    any_spec = pl.BlockSpec(memory_space=pl.ANY)
    dma = pltpu.SemaphoreType.DMA
    return pl.pallas_call(
        copy_kernel,
        name="copy_out",
        out_shape=[jax.ShapeDtypeStruct(a.shape, a.dtype) for a in arrays],
        in_specs=[any_spec] * len(arrays),
        out_specs=[any_spec] * len(arrays),
        scratch_shapes=[pltpu.VMEM((COPY_BUFS, COPY_ROWS, arrays[0].shape[1]), jnp.float32), dma((COPY_BUFS,)), dma((COPY_BUFS,))],
        compiler_params=pltpu.CompilerParams(vmem_limit_bytes=VMEM_BYTES),
    )(*arrays)


def solution(mesh):
    row_part = P(DATA_AXIS, None)
    replicated = P()

    def local_step(feat_a, feat_b, w_in, w_mid, w_out, t_in, t_mid, t_out, gain_1, bias_1, gain_2, bias_2, off_weight):
        affine = [v.reshape(1, -1) for v in (gain_1, bias_1, gain_2, bias_2)]
        pre_1, pre_2, xs_2, xs_1, xs_0, grad_z, grad_emb, vec = front(
            feat_a, feat_b, (w_in, t_in, w_mid, t_mid, w_out, t_out), affine, off_weight.reshape(1)
        )
        grad_w_out, grad_w_mid, grad_w_in, sums = backward(grad_z, xs_2, xs_1, xs_0, w_out, w_mid, pre_2, pre_1, vec)
        grad_emb, grad_w_out, grad_w_mid, grad_w_in = copy_out(grad_emb, grad_w_out, grad_w_mid, grad_w_in)
        return (sums[4, 0], grad_emb, grad_w_in, grad_w_mid, grad_w_out, sums[2], sums[3], sums[0], sums[1])

    return jax.shard_map(local_step, mesh=mesh, in_specs=(row_part, row_part) + (replicated,) * 11, out_specs=(replicated, row_part) + (replicated,) * 7, check_vma=False)
```

```python
import functools

import jax
import jax.numpy as jnp
from jax import lax
from jax.experimental import pallas as pl
from jax.experimental.pallas import tpu as pltpu
from jax.sharding import PartitionSpec as P

NORM_EPS = 1e-5
DATA_AXIS = "data"
MESH = pl.DeviceIdType.MESH
VMEM_BYTES = 67_043_328
PLANE = 8
DEPTH = 4
TILE = 256
WIDE = 512
BLOCK = 128
SUM_ROWS = 4
PARTS = 16
GROUP = 4
MATS = 3
ACC_SLOTS = 20
GATHER_SLOTS = 16
JOBS = 6
W_BUFS = 3
LAYER_SLOTS = 15
COPY_ROWS = 256
COPY_BUFS = 20
FRONT_PLAN = ((0, 0, 3, 5, 7, 9, 12, 13, 16, 17, 18), (0, 6, 3, 4, 9, 10, 8, 5, 2, 7, 1))
BACK_PLAN = ((0, 0, 3, 5, 7, 8, 9, 11, 14, 17, 19), (0, 4, 8, 7, 10, 1, 2, 3, 5, 6, 9))


def front_kind(kind, k):
    s, l = (k % 5 == 2) & (k > 2), k == 2
    return {"s": s, "l": l, "x": (k % 5 != 2)}[kind]


def back_kind(kind, k):
    l = ((k % 5 == 2) & (k < 43)) | ((k % 5 == 0) & (k >= 10) & (k < 36))
    return l if kind == "l" else jnp.logical_not(l)


def contract_rows(left_op, right_op):
    return lax.dot_general(left_op, right_op, (((0,), (0,)), ((), ())), preferred_element_type=jnp.float32)


def contract_cols(left_op, right_op):
    return lax.dot_general(left_op, right_op, (((1,), (1,)), ((), ())), preferred_element_type=jnp.float32)


def rows(off, size):
    return pl.ds(pl.multiple_of(off, size), size)


def pick(index, choices, what):
    for i, c in enumerate(choices):
        pl.when(index == i)(functools.partial(what, c))


def loop(lo, hi, body):
    def step(i, carry):
        body(i)
        return carry

    lax.fori_loop(lo, hi, step, 0)


def remote_copy(src, dst, send, recv, mate):
    return pltpu.make_async_remote_copy(src, dst, send, recv, device_id=(mate,), device_id_type=MESH)


class Place:
    def __init__(self):
        me = lax.axis_index(DATA_AXIS)
        self.me = me
        self.pos, self.plane = me % PLANE, me // PLANE
        self.core, self.bx, self.by, self.bz0, self.bz1 = me % 2, (me // 2) % 2, (me // 4) % 2, (me // 8) % 2, (me // 16) % 2
        self.other_core = me + 1 - 2 * self.core
        self.mates = [(self.pos + d) % PLANE for d in range(1, PLANE)]
        self.levels = [(self.plane + d) % DEPTH for d in range(1, DEPTH)]

    def peers(self):
        return [self.plane * PLANE + m for m in self.mates] + [lv * PLANE + self.pos for lv in self.levels]

    def arrive(self):
        sem = pltpu.get_barrier_semaphore()
        for peer in self.peers():
            pl.semaphore_signal(sem, inc=1, device_id=(peer,), device_id_type=MESH)

    def all_here(self):
        pl.semaphore_wait(pltpu.get_barrier_semaphore(), PLANE + DEPTH - 2)


class SmallSum:
    def __init__(self, place, payload, total, plane_buf, depth_buf, own_buf, sems):
        self.p, self.payload, self.total = place, payload, total
        self.plane_buf, self.depth_buf, self.own_buf, self.sems = plane_buf, depth_buf, own_buf, sems

    def first(self, j, m, slot):
        s, r = self.sems[0], self.sems[1]
        return remote_copy(self.payload.at[j, m], self.plane_buf.at[j, slot], s.at[j, m], r.at[j, slot], self.p.plane * PLANE + m)

    def second(self, j, lv, slot):
        s, r = self.sems[2], self.sems[3]
        return remote_copy(self.own_buf.at[j, 0], self.depth_buf.at[j, slot], s.at[j, lv], r.at[j, slot], lv * PLANE + self.p.pos)

    def third(self, j, m, slot):
        s, r = self.sems[4], self.sems[5]
        return remote_copy(self.own_buf.at[j, 1], self.total.at[j, slot], s.at[j, m], r.at[j, slot], self.p.plane * PLANE + m)

    def begin(self, j):
        for m in self.p.mates:
            self.first(j, m, self.p.pos).start()
        self.plane_buf[j, self.p.pos] = self.payload[j, self.p.pos]

    def middle(self, j):
        for m in self.p.mates:
            self.first(j, m, m).wait_recv()
        total = self.plane_buf[j, 0]
        for i in range(1, PLANE):
            total = total + self.plane_buf[j, i]
        self.own_buf[j, 0] = total
        self.depth_buf[j, self.p.plane] = total
        for lv in self.p.levels:
            self.second(j, lv, self.p.plane).start()

    def last(self, j):
        for lv in self.p.levels:
            self.second(j, lv, lv).wait_recv()
        total = self.depth_buf[j, 0]
        for i in range(1, DEPTH):
            total = total + self.depth_buf[j, i]
        self.own_buf[j, 1] = total
        self.total[j, self.p.pos] = total
        for m in self.p.mates:
            self.third(j, m, self.p.pos).start()

    def end(self, j):
        for m in self.p.mates:
            self.third(j, m, m).wait_recv()
            self.first(j, m, self.p.pos).wait_send()
            self.third(j, m, self.p.pos).wait_send()
        for lv in self.p.levels:
            self.second(j, lv, self.p.plane).wait_send()


def small_scratch(count):
    def buf(*lead):
        return pltpu.VMEM((count, *lead, SUM_ROWS, TILE), jnp.float32)

    bufs = [buf(PLANE), buf(PLANE), buf(PLANE), buf(DEPTH), buf(2)]
    return bufs + [pltpu.SemaphoreType.DMA((count, n)) for n in (PLANE, PLANE, DEPTH, DEPTH, PLANE, PLANE)]


SMALL_REFS = 11


def small_sum(place, refs):
    payload, total, plane_buf, depth_buf, own_buf = refs[:5]
    return SmallSum(place, payload, total, plane_buf, depth_buf, own_buf, refs[5:])


class ChunkSum:
    def __init__(self, place, kinds, is_kind, acc, gathered, landing, send, recv, finish):
        self.p, self.kinds, self.is_kind, self.slots, self.gather_slots = place, kinds, is_kind, acc.shape[0], gathered.shape[0]
        self.acc, self.gathered, self.landing, self.send, self.recv, self.finish = acc, gathered, landing, send, recv, finish
        self.size = acc.shape[1]
        self.s2, self.s4 = self.size // 2, self.size // 4
        core, bx, by, me = place.core, place.bx, place.by, place.me
        first, second = core * by + (1 - core) * bx, core * bx + (1 - core) * by
        self.xy = ((me + (2 + 2 * core) * (1 - 2 * first), first), (me + (4 - 2 * core) * (1 - 2 * second), second))
        self.zz = ((me + 8 * (1 - 2 * place.bz0), place.bz0), (me + 16 * (1 - 2 * place.bz1), place.bz1))
        self.is_mid = place.bz0 + place.bz1 - 2 * place.bz0 * place.bz1
        self.mid, self.end = self.is_mid == 1, self.is_mid == 0
        self.z_mate = self.zz[0][0]
        self.mid_mate = me + 8 * (1 - 2 * place.bz1)

    def copy(self, src, dst, stage, k, mate):
        return remote_copy(src, dst, self.send.at[stage, k], self.recv.at[stage, k], mate)

    def span(self, off, size):
        return pl.ds(pl.multiple_of(off, self.s4), size)

    def down(self, stage, k, off, size, mate, buf=None):
        j = k % self.slots
        buf = self.landing[stage] if buf is None else buf
        return self.copy(self.acc.at[j, self.span(off, size)], buf.at[j, pl.ds(0, size)], stage, k, mate)

    def up(self, stage, k, off, size, mate):
        block = self.gathered.at[k % self.gather_slots, self.span(off, size)]
        return self.copy(block, block, stage, k, mate)

    def add(self, k, off, size, buf):
        step = min(size, 16)
        j = k % self.slots

        def body(i):
            at = pl.ds(pl.multiple_of(off + i * step, step), step)
            self.acc[j, at] = self.acc[j, at] + buf[j, rows(i * step, step)]

        loop(0, size // step, body)

    def stage(self, i, k):
        for kind in self.kinds:
            run = {"x": self.stage_x, "s": self.stage_s, "l": self.stage_l}[kind]
            pl.when(self.is_kind(kind, k))(functools.partial(run, i, k))

    def stage_x(self, i, k):
        (m1, b1), (m2, b2), s2, s4 = *self.xy, self.s2, self.s4
        off1, off2 = b1 * s2, b1 * s2 + b2 * s4
        half = lambda: self.down(0, k, (1 - b1) * s2, s2, m1)
        quarter = lambda: self.down(1, k, off1 + (1 - b2) * s4, s4, m2)
        inward = lambda: self.down(2, k, off2, s4, self.z_mate)
        across = lambda: self.down(3, k, off2, s4, self.mid_mate)
        outward = lambda: self.up(4, k, off2, s4, self.z_mate)
        back4 = lambda: self.up(5, k, off2, s4, m2)
        back2 = lambda: self.up(6, k, off1, s2, m1)
        if i == 1:
            half().start()
        elif i == 2:
            half().wait_recv()
            self.add(k, off1, s2, self.landing[0])
            quarter().start()
        elif i == 3:
            quarter().wait_recv()
            self.add(k, off2, s4, self.landing[1])
            pl.when(self.end)(lambda: inward().start())
        elif i == 4:

            @pl.when(self.mid)
            def _():
                inward().wait_recv()
                self.add(k, off2, s4, self.landing[2])
                across().start()

        elif i == 5:

            @pl.when(self.mid)
            def _():
                across().wait_recv()
                self.finish(k, off2, s4, self.landing[3])
                outward().start()

        elif i == 6:
            pl.when(self.end)(lambda: outward().wait_recv())
            back4().start()
            half().wait_send()
            quarter().wait_send()
            pl.when(self.end)(lambda: inward().wait_send())
            pl.when(self.mid)(lambda: across().wait_send())
        elif i == 7:
            back4().wait_recv()
            back2().start()
        elif i == 8:
            back2().wait_recv()
        elif i == 10:
            pl.when(self.mid)(lambda: outward().wait_send())
            back4().wait_send()
            back2().wait_send()

    def stage_s(self, i, k):
        (m1, b1), (m2, b2), s2, s4 = *self.zz, self.s2, self.s4
        off1, off2 = b1 * s2, b1 * s2 + b2 * s4
        half = lambda: self.down(0, k, (1 - b1) * s2, s2, m1)
        quarter = lambda: self.down(1, k, off1 + (1 - b2) * s4, s4, m2)
        whole_1 = lambda: self.down(2, k, off2, s4, self.xy[0][0])
        whole_2 = lambda: self.down(3, k, off2, s4, self.xy[1][0])
        back4 = lambda: self.up(5, k, off2, s4, m2)
        back2 = lambda: self.up(6, k, off1, s2, m1)
        if i == 1:
            half().start()
        elif i == 2:
            half().wait_recv()
            self.add(k, off1, s2, self.landing[0])
            quarter().start()
        elif i == 3:
            quarter().wait_recv()
            self.add(k, off2, s4, self.landing[1])
            whole_1().start()
        elif i == 4:
            whole_1().wait_recv()
            whole_1().wait_send()
            self.add(k, off2, s4, self.landing[2])
            whole_2().start()
        elif i == 5:
            whole_2().wait_recv()
            self.finish(k, off2, s4, self.landing[3])
        elif i == 6:
            back4().start()
            half().wait_send()
            quarter().wait_send()
            whole_2().wait_send()
        elif i == 7:
            back4().wait_recv()
            back2().start()
        elif i == 8:
            back2().wait_recv()
        elif i == 10:
            back4().wait_send()
            back2().wait_send()

    def stage_l(self, i, k):
        s2, s4 = self.s2, self.s4
        s3 = s2 + s4
        b0, b1 = self.p.bz0, self.p.bz1
        own, side, tip, rest = (2 * b1 + b0) * s4, b1 * s2, 3 * b1 * s4, (1 - b1) * s4
        inward = lambda: self.down(0, k, rest, s3, self.z_mate)
        across = lambda: self.down(1, k, (1 - b1) * s2, s2, self.mid_mate)
        outward = lambda: self.down(2, k, tip, s4, self.z_mate)
        whole_1 = lambda: self.down(3, k, own, s4, self.xy[0][0])
        whole_2 = lambda: self.down(8, k, own, s4, self.xy[1][0], self.landing[4])
        tip_back = lambda: self.up(4, k, tip, s4, self.z_mate)
        side_back = lambda: self.up(5, k, side, s2, self.mid_mate)
        rest_back = lambda: self.up(6, k, rest, s3, self.z_mate)
        if i == 1:
            pl.when(self.end)(lambda: inward().start())
        elif i == 2:

            @pl.when(self.mid)
            def _():
                inward().wait_recv()
                self.add(k, rest, s3, self.landing[0])
                across().start()

        elif i == 3:

            @pl.when(self.mid)
            def _():
                across().wait_recv()
                self.add(k, side, s2, self.landing[1])
                outward().start()

        elif i == 4:

            @pl.when(self.end)
            def _():
                outward().wait_recv()
                self.add(k, own, s4, self.landing[2])

            whole_1().start()
        elif i == 5:
            whole_1().wait_recv()
            whole_1().wait_send()
            pl.when(self.mid)(lambda: outward().wait_send())
            self.add(k, own, s4, self.landing[3])
            whole_2().start()
        elif i == 6:
            whole_2().wait_recv()
            self.finish(k, own, s4, self.landing[4])
            pl.when(self.end)(lambda: tip_back().start())
            whole_2().wait_send()
            pl.when(self.end)(lambda: inward().wait_send())
            pl.when(self.mid)(lambda: across().wait_send())
        elif i == 7:

            @pl.when(self.mid)
            def _():
                tip_back().wait_recv()
                side_back().start()

        elif i == 8:

            @pl.when(self.mid)
            def _():
                side_back().wait_recv()
                rest_back().start()

        elif i == 9:
            pl.when(self.end)(lambda: rest_back().wait_recv())
        elif i == 10:
            pl.when(self.end)(lambda: tip_back().wait_send())

            @pl.when(self.mid)
            def _():
                side_back().wait_send()
                rest_back().wait_send()


def form_next(k, form):
    pl.when(k == 1)(lambda: form(GROUP // 2, GROUP // 2))
    pl.when((k % GROUP == 0) & (k > 0))(lambda: form(k, GROUP))


def run_slots(plan, count, stage, between):
    lags, order = plan

    def slot(t):
        for i in order:
            k = t - lags[i]

            @pl.when((k >= 0) & (k < count))
            def _():
                stage(i, k)

            if i == 1:
                between(t)

    loop(0, count + lags[-1], slot)


def chunk_scratch(slots, gather_slots, part_rows, width, count, dtype):
    def buf(n):
        return pltpu.VMEM((slots, n, width), jnp.float32)

    gathered = pltpu.VMEM((gather_slots, part_rows, width), dtype)

    dma = pltpu.SemaphoreType.DMA
    quarter = part_rows // 4
    return [buf(part_rows), gathered, *(buf(n * quarter) for n in (3, 2, 1, 1, 1)), dma((9, count)), dma((9, count))]


def fold(value):
    return jnp.sum(value.reshape(value.shape[0] // 8, 8, value.shape[1]), axis=0)


def front_kernel(feat_a, feat_b, w_in, t_in, w_mid, t_mid, w_out, t_out, gain1, bias1, gain2, bias2, off_weight, pre1, pre2, xs2, xs1, xs0, dz, grad_emb, vec, *scratch):
    (x_buf, u_buf, w_buf, stats, affine, loss, ea, eb, g_peer) = scratch[:9]
    (x_sem, w_sem, pre_sem, keep_sem, keep_send, keep_recv, ge_sem, e_send, e_recv) = scratch[9:18]
    small_refs = scratch[18 : 18 + SMALL_REFS]
    acc, gathered, *landing, send, recv = scratch[18 + SMALL_REFS :]
    rows_dev, width = feat_a.shape
    wide = w_buf.shape[2]
    tiles = width // wide
    half = width // 2
    part_rows = half // PARTS
    row_count = rows_dev * DEPTH * PLANE
    weights, feats = (w_in, t_in, w_mid, t_mid, w_out, t_out), (feat_a, feat_b)
    place = Place()
    core = place.core
    mine = rows(core * rows_dev, rows_dev)
    place.arrive()
    small = small_sum(place, small_refs)
    payload, total = small.payload, small.total

    def feat(v):
        return pltpu.make_async_copy(feats[v], x_buf.at[v], x_sem.at[v])

    def w_tile(ref, g):
        return pltpu.make_async_copy(ref.at[:, rows((g % tiles) * wide, wide)], w_buf.at[g % W_BUFS], w_sem.at[g % W_BUFS])

    def start_w(g):
        pick(g // tiles, weights, lambda ref: w_tile(ref, g).start())

    feat(0).start()
    w_tile(weights[0], 0).start()
    feat(1).start()
    for g in range(1, W_BUFS - 1):
        start_w(g)
    for j, ref in enumerate((gain1, bias1, gain2, bias2)):
        affine[j] = ref[...]
    feat(0).wait()
    payload[...] = jnp.zeros_like(payload)

    def keep_pre(ref):
        return pltpu.make_async_copy(u_buf.at[0], ref, pre_sem.at[0])

    kept = (xs0, xs1, xs2)

    def keep_x(w):
        here = pltpu.make_async_copy(x_buf.at[0, :, rows(core * half, half)], kept[w].at[mine], keep_sem.at[w])
        there = remote_copy(x_buf.at[0, :, rows((1 - core) * half, half)], kept[w].at[mine], keep_send.at[w], keep_recv.at[w], place.other_core)
        return here, there

    def start_x(w):
        for c in keep_x(w):
            c.start()

    def free_x(w):
        here, there = keep_x(w)
        here.wait()
        there.wait_send()

    def keep_dz(i):
        at = (slice(None), rows(i * wide, wide))
        here = pltpu.make_async_copy(x_buf.at[(0, *at)], dz.at[mine, at[1]], keep_sem.at[3 + i])
        there = remote_copy(x_buf.at[(0, *at)], dz.at[mine, at[1]], keep_send.at[3 + i], keep_recv.at[3 + i], place.other_core)
        return here, there

    def row_loop(body, carry):
        return lax.fori_loop(0, rows_dev // BLOCK, lambda r, c: body(rows(r * BLOCK, BLOCK), c), carry)

    def put_sums(j, i, row, value):
        value = jnp.sum(value, axis=0, keepdims=True)
        for c in range(value.shape[1] // TILE):
            payload[j, i + c, row : row + 1] = value[:, c * TILE : (c + 1) * TILE]

    def product(g):
        job, i = g // tiles, g % tiles
        view = job % 2
        w_tile(w_in, g).wait()
        pl.when(g + W_BUFS - 1 < JOBS * tiles)(lambda: start_w(g + W_BUFS - 1))
        at_cols = rows(i * wide, wide)
        u_buf[view, :, at_cols] = jnp.dot(x_buf[view], w_buf[g % W_BUFS], preferred_element_type=jnp.float32)

        def block(at, sums):
            u = u_buf[view, at, at_cols]
            return sums[0] + fold(u), sums[1] + fold(u * u)

        zero = jnp.zeros((8, wide), jnp.float32)
        for row, value in enumerate(row_loop(block, (zero, zero))):
            put_sums(job, i * (wide // TILE), row, value)

    def begin(job):
        small.begin(job)

        @pl.when(job % 2 == 0)
        def _():
            pick(job // 2, (pre1, pre2), lambda ref: keep_pre(ref).start())

    def norm(job):
        layer, view = job // 2, job % 2
        small.end(job)
        for c in range(PLANE):
            at = slice(c * TILE, (c + 1) * TILE)
            means = total[job, c] / row_count
            stats[job, 0, :, at] = means[0:1]
            stats[job, 1, :, at] = lax.rsqrt(means[1:2] - means[0:1] * means[0:1] + NORM_EPS)

        pl.when(view == 0)(lambda: pick(layer, (0, 1, 2), free_x))

        def hidden(i):
            at_cols = rows(i * wide, wide)
            mean, inv = stats[job, 0, :, at_cols], stats[job, 1, :, at_cols]
            gain, bias = affine[layer * 2, :, at_cols], affine[layer * 2 + 1, :, at_cols]

            def block(at, c):
                n = (u_buf[view, at, at_cols] - mean) * inv
                x_buf[view, at, at_cols] = jnp.maximum(n * gain + bias, 0.0).astype(jnp.bfloat16)
                return c

            row_loop(block, 0)

        def student(i):
            at_cols = rows(i * wide, wide)
            mean, inv = stats[job, 0, :, at_cols], stats[job, 1, :, at_cols]

            def block(at, c):
                n = (u_buf[0, at, at_cols] - mean) * inv
                u_buf[0, at, at_cols] = n
                x_buf[0, at, at_cols] = n.astype(jnp.bfloat16)
                return c

            row_loop(block, 0)

        def student_own(i):
            def block(r, c):
                ea[rows(core * rows_dev + r * BLOCK, BLOCK), rows(i * wide, wide)] = x_buf[0, rows(r * BLOCK, BLOCK), rows(core * half + i * wide, wide)]
                return c

            lax.fori_loop(0, rows_dev // BLOCK, block, 0)

        def teacher(i):
            at_cols = rows(i * wide, wide)
            mean, inv = stats[job, 0, :, at_cols], stats[job, 1, :, at_cols]

            def block(r, c):
                n = (u_buf[1, rows(r * BLOCK, BLOCK), at_cols] - mean) * inv
                eb[rows(core * rows_dev + r * BLOCK, BLOCK), at_cols] = n.astype(jnp.bfloat16)
                return c

            lax.fori_loop(0, rows_dev // BLOCK, block, 0)
            eb_copy(i).start()

        @pl.when(layer < 2)
        def _():
            loop(0, tiles, hidden)

            @pl.when(view == 0)
            def _():
                pick(layer, (1, 2), start_x)
                keep_pre(pre1).wait()

        @pl.when((layer == 2) & (view == 0))
        def _():
            loop(0, tiles, student)
            ea_copy().start()
            loop(0, tiles // 2, student_own)

        @pl.when((layer == 2) & (view == 1))
        def _():
            loop(0, tiles, teacher)

    ea_copy = lambda: remote_copy(x_buf.at[0, :, rows((1 - core) * half, half)], ea.at[mine], e_send.at[0], e_recv.at[0], place.other_core)

    def eb_copy(i):
        block = eb.at[mine, rows(i * wide, wide)]
        return remote_copy(block, block, e_send.at[1 + i], e_recv.at[1 + i], place.other_core)

    def step(g):
        job, i = g // tiles, g % tiles
        view = job % 2
        pl.when(g == tiles)(lambda: feat(1).wait())
        product(g)

        @pl.when(g == 0)
        def _():
            place.all_here()
            start_x(0)

        pl.when((i == 0) & (job > 0))(lambda: small.middle(job - 1))
        pl.when((i == tiles - 2) & (job > 0))(lambda: small.last(job - 1))

        @pl.when(i == tiles - 1)
        def _():
            begin(job)
            pl.when(job > 0)(lambda: norm(job - 1))

    loop(0, JOBS * tiles, step)
    small.middle(JOBS - 1)
    small.last(JOBS - 1)
    norm(JOBS - 1)
    for j, source in enumerate((affine.at[2], affine.at[3], stats.at[2, 0], stats.at[2, 1], affine.at[0], affine.at[1], stats.at[0, 0], stats.at[0, 1])):
        vec[j] = source[...]

    loss[...] = jnp.zeros_like(loss)

    def finish(k, off, size, buf):
        share = jnp.where(front_kind("x", k), 0.5, 0.25)
        at = rows(off, size)
        corr = (acc[k, at] + buf[k]) / row_count
        row = core * half + k * part_rows + off
        diag = (row + lax.broadcasted_iota(jnp.int32, (size, width), 0)) == lax.broadcasted_iota(jnp.int32, (size, width), 1)
        weight = off_weight[0]
        miss = 1.0 - corr
        loss[...] += share * jnp.sum(jnp.where(diag, miss * miss, weight * (corr * corr)), axis=0, keepdims=True)
        gathered[k, at] = jnp.where(diag, -2.0 * miss, 2.0 * weight * corr).astype(jnp.bfloat16)

    chunks = ChunkSum(place, "xsl", front_kind, acc, gathered, landing, send, recv, finish)

    def form(k, group):
        at = rows(k * part_rows, group * part_rows)
        size = min(1024, width)

        def col(c):
            @pl.when(k == 0)
            def _():
                for i in range(size // wide):
                    eb_copy(c * (size // wide) + i).wait_recv()

            cs = rows(c * size, size)
            acc[pl.ds(k, group), :, cs] = contract_rows(ea[:, at], eb[:, cs]).reshape(group, part_rows, size)

        loop(0, width // size, col)

    def swap(k):
        return chunks.copy(gathered.at[k], g_peer.at[k], 7, k, place.other_core)

    def ge_cols(k, side):
        return rows(side * half + k * part_rows, GROUP * part_rows)

    def ge_copy(k, side):
        at = ge_cols(k, side)
        return pltpu.make_async_copy(u_buf.at[1, :, at], grad_emb.at[:, at], ge_sem.at[k // GROUP, side])

    def embed(k, side, g_rows):
        at_cols = ge_cols(k, side)
        grad = contract_cols(eb[mine], g_rows.reshape(GROUP * part_rows, width)) / row_count
        u_buf[1, :, at_cols] = grad
        ge_copy(k, side).start()

        def block(at, sums):
            g = u_buf[1, at, at_cols]
            return sums[0] + fold(g * u_buf[0, at, at_cols]), sums[1] + fold(g)

        zero = jnp.zeros((8, GROUP * part_rows), jnp.float32)
        for row, value in enumerate(row_loop(block, (zero, zero))):
            payload[JOBS, (side * half + k * part_rows) // TILE, row : row + 1] = jnp.sum(value, axis=0, keepdims=True)

    def stage(i, k):
        if i == 0:
            form_next(k, form)
            return
        chunks.stage(i, k)
        if i == 8:
            pl.when(jnp.logical_not(front_kind("l", k)))(lambda: swap(k).start())
        if i == 9:
            pl.when(front_kind("l", k))(lambda: swap(k).start())

            @pl.when(k % GROUP == GROUP - 1)
            def _():
                embed(k - GROUP + 1, core, gathered[pl.ds(k - GROUP + 1, GROUP)])

        if i == 10:
            swap(k).wait_recv()
            swap(k).wait_send()

            @pl.when(k % GROUP == GROUP - 1)
            def _():
                embed(k - GROUP + 1, 1 - core, g_peer[pl.ds(k - GROUP + 1, GROUP)])

    ea_copy().wait_recv()
    form(0, GROUP // 2)
    run_slots(FRONT_PLAN, PARTS, stage, lambda t: None)
    for c in range(PLANE):
        payload[JOBS, c, 2:3] = loss[:, c * TILE : (c + 1) * TILE]
    small.begin(JOBS)
    ea_copy().wait_send()
    for i in range(tiles):
        eb_copy(i).wait_send()
    small.middle(JOBS)
    for k in range(0, PARTS, GROUP):
        for side in range(2):
            ge_copy(k, side).wait()
    small.last(JOBS)
    small.end(JOBS)

    def dz_tile(i):
        at_cols = rows(i * wide, wide)
        sums = jnp.concatenate([total[JOBS, i * (wide // TILE) + c] for c in range(wide // TILE)], axis=1) / row_count
        mean_gn, mean_g = sums[0:1], sums[1:2]
        inv = stats[JOBS - 2, 1, :, at_cols]

        def block(at, c):
            value = (u_buf[1, at, at_cols] - mean_g - u_buf[0, at, at_cols] * mean_gn) * inv
            x_buf[0, at, at_cols] = value.astype(jnp.bfloat16)
            return c

        row_loop(block, 0)
        for c in keep_dz(i):
            c.start()

    loop(0, tiles, dz_tile)
    for c in range(PLANE):
        vec[8, :, c * TILE : (c + 1) * TILE] = total[JOBS, c, 2:3]
    for w in range(3):
        keep_x(w)[1].wait_recv()
    for i in range(tiles):
        here, there = keep_dz(i)
        here.wait()
        there.wait()


def front(feat_a, feat_b, weights, affine, off_weight):
    rows_dev, width = feat_a.shape
    half = width // 2
    part_rows = half // PARTS
    any_spec = pl.BlockSpec(memory_space=pl.ANY)
    vmem_spec = pl.BlockSpec(memory_space=pltpu.VMEM)
    wide_f32 = jax.ShapeDtypeStruct((rows_dev, width), jnp.float32)
    kept = jax.ShapeDtypeStruct((2 * rows_dev, half), jnp.bfloat16)
    both_dz = jax.ShapeDtypeStruct((2 * rows_dev, width), jnp.bfloat16)
    keeps = 3 + width // WIDE
    dma = pltpu.SemaphoreType.DMA
    return pl.pallas_call(
        front_kernel,
        name="front",
        out_shape=[wide_f32, wide_f32, kept, kept, kept, both_dz, wide_f32]
        + [jax.ShapeDtypeStruct((9, 1, width), jnp.float32)],
        in_specs=[any_spec] * 8 + [vmem_spec] * 4 + [pl.BlockSpec(memory_space=pltpu.SMEM)],
        out_specs=[any_spec] * 7 + [vmem_spec],
        scratch_shapes=[
            pltpu.VMEM((2, rows_dev, width), jnp.bfloat16),
            pltpu.VMEM((2, rows_dev, width), jnp.float32),
            pltpu.VMEM((W_BUFS, width, WIDE), jnp.bfloat16),
            pltpu.VMEM((JOBS, 2, 1, width), jnp.float32),
            pltpu.VMEM((4, 1, width), jnp.float32),
            pltpu.VMEM((1, width), jnp.float32),
            pltpu.VMEM((2 * rows_dev, half), jnp.bfloat16),
            pltpu.VMEM((2 * rows_dev, width), jnp.bfloat16),
            pltpu.VMEM((PARTS, part_rows, width), jnp.bfloat16),
            dma((2,)),
            dma((W_BUFS,)),
            dma((1,)),
            dma((keeps,)),
            dma((keeps,)),
            dma((keeps,)),
            dma((PARTS // GROUP, 2)),
            dma((1 + width // WIDE,)),
            dma((1 + width // WIDE,)),
        ]
        + small_scratch(JOBS + 1)
        + chunk_scratch(PARTS, PARTS, part_rows, width, PARTS, jnp.bfloat16),
        compiler_params=pltpu.CompilerParams(collective_id=0, has_side_effects=True, vmem_limit_bytes=VMEM_BYTES),
    )(feat_a, feat_b, *weights, *affine, off_weight)


def back_kernel(dz_hbm, x2, x1, x0, w_out, w_mid, u2, u1, vec, out2, out1, out0, sums_out, *scratch):
    (dy, xs, w_buf, u_buf, dpre) = scratch[:5]
    (in_sem, tile_sem, peer_send, peer_recv, store_sem) = scratch[5:10]
    small_refs = scratch[10 : 10 + SMALL_REFS]
    acc, gathered, *landing, send, recv = scratch[10 + SMALL_REFS :]
    rows_dev, width = dpre.shape
    wide = w_buf.shape[1]
    tiles = width // wide
    row_count = rows_dev * DEPTH * PLANE
    half = width // 2
    part_rows = half // PARTS
    count = MATS * PARTS
    mats_in, outs, weights, pres = (x2, x1, x0), (out2, out1, out0), (w_out, w_mid), (u2, u1)
    place = Place()
    core, other_core = place.core, place.other_core
    mine = rows(core * rows_dev, rows_dev)
    place.arrive()
    small = small_sum(place, small_refs)
    payload, sums = small.payload, small.total

    def load_x(w):
        return pltpu.make_async_copy(mats_in[w], xs.at[w % 2], in_sem.at[w])

    def peer_dy(w):
        block = dy.at[w % 2, mine]
        return remote_copy(block, block, peer_send.at[w], peer_recv.at[w], other_core)

    def w_tile(ref, i):
        return pltpu.make_async_copy(ref.at[rows(i * wide, wide)], w_buf.at[i % 2], tile_sem.at[0, i % 2])

    def u_tile(ref, i):
        return pltpu.make_async_copy(ref.at[:, rows(i * wide, wide)], u_buf.at[i % 2], tile_sem.at[1, i % 2])

    def start_w(layer, i):
        pick(layer, weights, lambda ref: w_tile(ref, i).start())

    def start_u(layer, i):
        pick(layer, pres, lambda ref: u_tile(ref, i).start())

    size = min(1024, width)

    def load_dz(c):
        return pltpu.make_async_copy(dz_hbm.at[:, rows(c * size, size)], dy.at[0, :, rows(c * size, size)], in_sem.at[MATS + c])

    load_x(0).start()
    for c in range(width // size):
        load_dz(c).start()
    w_tile(weights[0], 0).start()
    u_tile(pres[0], 0).start()
    load_x(1).start()
    payload[...] = jnp.zeros_like(payload)

    def row_loop(body, carry):
        return lax.fori_loop(0, rows_dev // BLOCK, body, carry)

    def chain_tile(layer, i):
        w_tile(w_out, i).wait()
        u_tile(u2, i).wait()

        @pl.when(i + 1 < tiles)
        def _():
            start_w(layer, i + 1)
            start_u(layer, i + 1)

        at_cols = rows(i * wide, wide)
        dpre[:, at_cols] = contract_cols(dy[layer, mine], w_buf[i % 2])
        gain, bias, mean, inv = (vec[layer * 4 + j, :, at_cols] for j in range(4))

        def block(r, carry):
            at = rows(r * BLOCK, BLOCK)
            n = (u_buf[i % 2, at] - mean) * inv
            g = jnp.where(n * gain + bias > 0.0, dpre[at, at_cols], 0.0)
            dpre[at, at_cols] = g
            return carry[0] + fold(g * n), carry[1] + fold(g)

        zero = jnp.zeros((8, wide), jnp.float32)
        for row, value in enumerate(row_loop(block, (zero, zero))):
            value = jnp.sum(value, axis=0, keepdims=True)
            for c in range(wide // TILE):
                payload[layer, i * (wide // TILE) + c, row : row + 1] = value[:, c * TILE : (c + 1) * TILE]

    def du_tile(layer, i):
        u_tile(u2, i).wait()
        pl.when(i + 1 < tiles)(lambda: start_u(layer, i + 1))
        at_cols = rows(i * wide, wide)
        gain, mean, inv = (vec[layer * 4 + j, :, at_cols] for j in (0, 2, 3))
        means = jnp.concatenate([sums[layer, i * (wide // TILE) + c] for c in range(wide // TILE)], axis=1) / row_count
        mean_gn, mean_g = means[0:1], means[1:2]
        scale = gain * inv

        def block(r, c):
            at = rows(r * BLOCK, BLOCK)
            n = (u_buf[i % 2, at] - mean) * inv
            value = (dpre[at, at_cols] - mean_g - n * mean_gn) * scale
            dy[1 - layer, rows(core * rows_dev + r * BLOCK, BLOCK), at_cols] = value.astype(jnp.bfloat16)
            return c

        row_loop(block, 0)

    def finish(k, off, size, buf):
        j = k % ACC_SLOTS
        gathered[k % GATHER_SLOTS, rows(off, size)] = acc[j, rows(off, size)] + buf[j]

    chunks = ChunkSum(place, "xl", back_kind, acc, gathered, landing, send, recv, finish)

    def form(k, group):
        w, j = k // PARTS, k % ACC_SLOTS

        @pl.when(k % PARTS == 0)
        def _():
            pltpu.make_async_copy(xs.at[w % 2], xs.at[w % 2], in_sem.at[w]).wait()
            pl.when(w > 0)(lambda: peer_dy(w).wait_recv())

        at = rows((k % PARTS) * part_rows, group * part_rows)

        def col(c):
            pl.when(k == 0)(lambda: load_dz(c).wait())
            cs = rows(c * size, size)
            acc[pl.ds(j, group), :, cs] = contract_rows(xs[w % 2, :, at], dy[w % 2, :, cs]).reshape(group, part_rows, size)

        loop(0, width // size, col)

    def out_rows(k, side):
        return pl.ds(pl.multiple_of(side * half + (k % PARTS) * part_rows, part_rows), part_rows)

    def last_copy(out, k, side):
        return chunks.copy(gathered.at[k % GATHER_SLOTS], out.at[out_rows(k, side)], 7, k, other_core)

    def store_copy(out, k):
        return pltpu.make_async_copy(gathered.at[k % GATHER_SLOTS], out.at[out_rows(k, core)], store_sem.at[k])

    def stage(i, k):
        if i == 0:
            form_next(k, form)
            return
        chunks.stage(i, k)
        def emit(out):
            last_copy(out, k, core).start()
            store_copy(out, k).start()

        if i == 8:
            pl.when(back_kind("x", k))(lambda: pick(k // PARTS, outs, emit))
        if i == 9:
            pl.when(back_kind("l", k))(lambda: pick(k // PARTS, outs, emit))
        if i == 10:

            def close(out):
                last_copy(out, k, 1 - core).wait_recv()
                store_copy(out, k).wait()
                last_copy(out, k, core).wait_send()

            pick(k // PARTS, outs, close)

    def layer_work(t):
        layer = t // LAYER_SLOTS
        at = t - LAYER_SLOTS * layer
        first_du = 2 * tiles + 3
        pl.when((at < 2 * tiles) & (at % 2 == 1))(lambda: chain_tile(layer, at // 2))
        pl.when(at == 2 * tiles)(lambda: small.begin(layer))
        pl.when(at == 2 * tiles + 1)(lambda: small.middle(layer))

        @pl.when(at == 2 * tiles + 2)
        def _():
            small.last(layer)
            start_u(layer, 0)

        pl.when(at == first_du)(lambda: small.end(layer))
        pl.when(at >= first_du)(lambda: du_tile(layer, at - first_du))

        @pl.when(at == LAYER_SLOTS - 1)
        def _():
            peer_dy(layer + 1).start()

            @pl.when(layer == 0)
            def _():
                w_tile(weights[1], 0).start()
                u_tile(pres[1], 0).start()

            pl.when(layer == 1)(lambda: load_x(2).start())

    form(0, GROUP // 2)
    place.all_here()
    run_slots(BACK_PLAN, count, stage, lambda t: pl.when(t < 2 * LAYER_SLOTS)(lambda: layer_work(t)))
    for w in (1, 2):
        peer_dy(w).wait_send()
    for c in range(PLANE):
        for row in range(4):
            sums_out[row : row + 1, c * TILE : (c + 1) * TILE] = sums[row // 2, c, row % 2 : row % 2 + 1]
    sums_out[4:5] = jnp.full((1, width), jnp.sum(vec[8]))


def backward(grad_z, x2, x1, x0, w_out, w_mid, u2, u1, vec):
    rows_dev, width = u2.shape
    part_rows = width // 2 // PARTS
    count = MATS * PARTS
    any_spec = pl.BlockSpec(memory_space=pl.ANY)
    vmem_spec = pl.BlockSpec(memory_space=pltpu.VMEM)
    mat = jax.ShapeDtypeStruct((width, width), jnp.float32)
    dma = pltpu.SemaphoreType.DMA
    return pl.pallas_call(
        back_kernel,
        name="backward",
        out_shape=[mat, mat, mat, jax.ShapeDtypeStruct((5, width), jnp.float32)],
        in_specs=[any_spec] * 8 + [vmem_spec],
        out_specs=[any_spec] * 3 + [vmem_spec],
        scratch_shapes=[
            pltpu.VMEM((2, 2 * rows_dev, width), jnp.bfloat16),
            pltpu.VMEM((2, 2 * rows_dev, width // 2), jnp.bfloat16),
            pltpu.VMEM((2, WIDE, width), jnp.bfloat16),
            pltpu.VMEM((2, rows_dev, WIDE), jnp.float32),
            pltpu.VMEM((rows_dev, width), jnp.float32),
            dma((MATS + 2,)),
            dma((2, 2)),
            dma((MATS,)),
            dma((MATS,)),
            dma((count,)),
        ]
        + small_scratch(2)
        + chunk_scratch(ACC_SLOTS, GATHER_SLOTS, part_rows, width, count, jnp.float32),
        compiler_params=pltpu.CompilerParams(collective_id=1, has_side_effects=True, vmem_limit_bytes=VMEM_BYTES),
    )(grad_z, x2, x1, x0, w_out, w_mid, u2, u1, vec)


def copy_kernel(*refs):
    pairs = (len(refs) - 3 - 6) // 2
    ins, small, outs, small_outs, (buf, in_sem, out_sem) = refs[:pairs], refs[pairs], refs[pairs + 1 : 2 * pairs + 1], refs[2 * pairs + 1 : -3], refs[-3:]
    blocks = [(i, r) for i in range(pairs) for r in range(0, ins[i].shape[0], COPY_ROWS)]

    def read(b):
        i, r = blocks[b]
        return pltpu.make_async_copy(ins[i].at[pl.ds(r, COPY_ROWS)], buf.at[b % COPY_BUFS], in_sem.at[b % COPY_BUFS])

    def write(b):
        i, r = blocks[b]
        return pltpu.make_async_copy(buf.at[b % COPY_BUFS], outs[i].at[pl.ds(r, COPY_ROWS)], out_sem.at[b % COPY_BUFS])

    ahead = COPY_BUFS // 2
    for b in range(min(ahead, len(blocks))):
        read(b).start()
    for row in range(4):
        small_outs[row][...] = small[row : row + 1]
    small_outs[4][...] = small[4:5, :1]
    for b in range(len(blocks)):
        if b + ahead < len(blocks):
            if b + ahead >= COPY_BUFS:
                write(b + ahead - COPY_BUFS).wait()
            read(b + ahead).start()
        read(b).wait()
        write(b).start()
    for b in range(max(0, len(blocks) - COPY_BUFS), len(blocks)):
        write(b).wait()


def copy_out(arrays, small):
    any_spec = pl.BlockSpec(memory_space=pl.ANY)
    vmem_spec = pl.BlockSpec(memory_space=pltpu.VMEM)
    dma = pltpu.SemaphoreType.DMA
    width = small.shape[1]
    row = jax.ShapeDtypeStruct((1, width), jnp.float32)
    return pl.pallas_call(
        copy_kernel,
        name="copy_out",
        out_shape=[jax.ShapeDtypeStruct(a.shape, a.dtype) for a in arrays] + [row] * 4 + [jax.ShapeDtypeStruct((1, 1), jnp.float32)],
        in_specs=[any_spec] * len(arrays) + [vmem_spec],
        out_specs=[any_spec] * len(arrays) + [vmem_spec] * 5,
        scratch_shapes=[pltpu.VMEM((COPY_BUFS, COPY_ROWS, width), jnp.float32), dma((COPY_BUFS,)), dma((COPY_BUFS,))],
        compiler_params=pltpu.CompilerParams(vmem_limit_bytes=VMEM_BYTES),
    )(*arrays, small)


def solution(mesh):
    row_part = P(DATA_AXIS, None)
    replicated = P()

    def local_step(feat_a, feat_b, w_in, w_mid, w_out, t_in, t_mid, t_out, gain_1, bias_1, gain_2, bias_2, off_weight):
        affine = [v.reshape(1, -1) for v in (gain_1, bias_1, gain_2, bias_2)]
        pre_1, pre_2, xs_2, xs_1, xs_0, grad_z, grad_emb, vec = front(
            feat_a, feat_b, (w_in, t_in, w_mid, t_mid, w_out, t_out), affine, off_weight.reshape(1)
        )
        grad_w_out, grad_w_mid, grad_w_in, sums = backward(grad_z, xs_2, xs_1, xs_0, w_out, w_mid, pre_2, pre_1, vec)
        (grad_emb, grad_w_out, grad_w_mid, grad_w_in, gain_2, bias_2, gain_1, bias_1, loss) = copy_out((grad_emb, grad_w_out, grad_w_mid, grad_w_in), sums)
        gain_1, bias_1, gain_2, bias_2 = (v.reshape(-1) for v in (gain_1, bias_1, gain_2, bias_2))
        return (loss.reshape(()), grad_emb, grad_w_in, grad_w_mid, grad_w_out, gain_1, bias_1, gain_2, bias_2)

    return jax.shard_map(local_step, mesh=mesh, in_specs=(row_part, row_part) + (replicated,) * 11, out_specs=(replicated, row_part) + (replicated,) * 7, check_vma=False)
```

```python
import functools

import jax
import jax.numpy as jnp
from jax import lax
from jax.experimental import pallas as pl
from jax.experimental.pallas import tpu as pltpu
from jax.sharding import PartitionSpec as P

NORM_EPS = 1e-5
DATA_AXIS = "data"
MESH = pl.DeviceIdType.MESH
VMEM_BYTES = 67_043_328
PLANE = 8
DEPTH = 4
TILE = 256
WIDE = 512
BLOCK = 128
SUM_ROWS = 2
PARTS = 16
GROUP = 4
MATS = 3
ACC_SLOTS = 20
GATHER_SLOTS = 16
JOBS = 6
W_BUFS = 3
LAYER_SLOTS = 15
COPY_ROWS = 256
COPY_BUFS = 20
FRONT_PLAN = ((0, 0, 3, 5, 7, 9, 12, 13, 16, 17, 18), (0, 6, 3, 4, 9, 10, 8, 5, 2, 7, 1))
BACK_PLAN = ((0, 0, 3, 5, 7, 8, 9, 11, 14, 17, 19), (0, 4, 8, 7, 10, 1, 2, 3, 5, 6, 9))


def front_kind(kind, k):
    s, l = (k % 5 == 2) & (k > 2), k == 2
    return {"s": s, "l": l, "x": (k % 5 != 2)}[kind]


def back_kind(kind, k):
    l = ((k % 5 == 2) & (k < 43)) | ((k % 5 == 0) & (k >= 10) & (k < 36))
    return l if kind == "l" else jnp.logical_not(l)


def contract_rows(left_op, right_op):
    return lax.dot_general(left_op, right_op, (((0,), (0,)), ((), ())), preferred_element_type=jnp.float32)


def contract_cols(left_op, right_op):
    return lax.dot_general(left_op, right_op, (((1,), (1,)), ((), ())), preferred_element_type=jnp.float32)


def rows(off, size):
    return pl.ds(pl.multiple_of(off, size), size)


def pick(index, choices, what):
    for i, c in enumerate(choices):
        pl.when(index == i)(functools.partial(what, c))


def loop(lo, hi, body):
    def step(i, carry):
        body(i)
        return carry

    lax.fori_loop(lo, hi, step, 0)


def remote_copy(src, dst, send, recv, mate):
    return pltpu.make_async_remote_copy(src, dst, send, recv, device_id=(mate,), device_id_type=MESH)


class Place:
    def __init__(self):
        me = lax.axis_index(DATA_AXIS)
        self.me = me
        self.pos, self.plane = me % PLANE, me // PLANE
        self.core, self.bx, self.by, self.bz0, self.bz1 = me % 2, (me // 2) % 2, (me // 4) % 2, (me // 8) % 2, (me // 16) % 2
        self.other_core = me + 1 - 2 * self.core
        self.mates = [(self.pos + d) % PLANE for d in range(1, PLANE)]
        self.levels = [(self.plane + d) % DEPTH for d in range(1, DEPTH)]

    def peers(self):
        return [self.plane * PLANE + m for m in self.mates] + [lv * PLANE + self.pos for lv in self.levels]

    def arrive(self):
        sem = pltpu.get_barrier_semaphore()
        for peer in self.peers():
            pl.semaphore_signal(sem, inc=1, device_id=(peer,), device_id_type=MESH)

    def all_here(self):
        pl.semaphore_wait(pltpu.get_barrier_semaphore(), PLANE + DEPTH - 2)


class SmallSum:
    def __init__(self, place, payload, total, depth_buf, line_sum, plane_buf, sems):
        self.p, self.payload, self.total = place, payload, total
        self.depth_buf, self.line_sum, self.plane_buf, self.sems = depth_buf, line_sum, plane_buf, sems

    def along(self, j, lv, slot):
        s, r = self.sems[0], self.sems[1]
        return remote_copy(self.payload.at[j], self.depth_buf.at[j, slot], s.at[j, lv], r.at[j, slot], lv * PLANE + self.p.pos)

    def within(self, j, m, slot):
        s, r = self.sems[2], self.sems[3]
        return remote_copy(self.line_sum.at[j], self.plane_buf.at[j, slot], s.at[j, m], r.at[j, slot], self.p.plane * PLANE + m)

    def begin(self, j):
        for lv in self.p.levels:
            self.along(j, lv, self.p.plane).start()
        self.depth_buf[j, self.p.plane] = self.payload[j]

    def middle(self, j):
        for lv in self.p.levels:
            self.along(j, lv, lv).wait_recv()
        total = self.depth_buf[j, 0]
        for i in range(1, DEPTH):
            total = total + self.depth_buf[j, i]
        self.line_sum[j] = total
        for m in self.p.mates:
            self.within(j, m, self.p.pos).start()
        self.plane_buf[j, self.p.pos] = total

    def end(self, j):
        for m in self.p.mates:
            self.within(j, m, m).wait_recv()
        total = self.plane_buf[j, 0]
        for i in range(1, PLANE):
            total = total + self.plane_buf[j, i]
        self.total[j] = total
        for lv in self.p.levels:
            self.along(j, lv, self.p.plane).wait_send()
        for m in self.p.mates:
            self.within(j, m, self.p.pos).wait_send()


def small_scratch(count):
    def buf(*lead):
        return pltpu.VMEM((count, *lead, PLANE, SUM_ROWS, TILE), jnp.float32)

    return [buf(), buf(), buf(DEPTH), buf(), buf(PLANE)] + [pltpu.SemaphoreType.DMA((count, n)) for n in (DEPTH, DEPTH, PLANE, PLANE)]


SMALL_REFS = 9


def small_sum(place, refs):
    return SmallSum(place, *refs[:5], refs[5:])


class ChunkSum:
    def __init__(self, place, kinds, is_kind, acc, gathered, landing, send, recv, finish):
        self.p, self.kinds, self.is_kind, self.slots, self.gather_slots = place, kinds, is_kind, acc.shape[0], gathered.shape[0]
        self.acc, self.gathered, self.landing, self.send, self.recv, self.finish = acc, gathered, landing, send, recv, finish
        self.size = acc.shape[1]
        self.s2, self.s4 = self.size // 2, self.size // 4
        core, bx, by, me = place.core, place.bx, place.by, place.me
        first, second = core * by + (1 - core) * bx, core * bx + (1 - core) * by
        self.xy = ((me + (2 + 2 * core) * (1 - 2 * first), first), (me + (4 - 2 * core) * (1 - 2 * second), second))
        self.zz = ((me + 8 * (1 - 2 * place.bz0), place.bz0), (me + 16 * (1 - 2 * place.bz1), place.bz1))
        self.is_mid = place.bz0 + place.bz1 - 2 * place.bz0 * place.bz1
        self.mid, self.end = self.is_mid == 1, self.is_mid == 0
        self.z_mate = self.zz[0][0]
        self.mid_mate = me + 8 * (1 - 2 * place.bz1)

    def copy(self, src, dst, stage, k, mate):
        return remote_copy(src, dst, self.send.at[stage, k], self.recv.at[stage, k], mate)

    def span(self, off, size):
        return pl.ds(pl.multiple_of(off, self.s4), size)

    def down(self, stage, k, off, size, mate, buf=None):
        j = k % self.slots
        buf = self.landing[stage] if buf is None else buf
        return self.copy(self.acc.at[j, self.span(off, size)], buf.at[j, pl.ds(0, size)], stage, k, mate)

    def up(self, stage, k, off, size, mate):
        block = self.gathered.at[k % self.gather_slots, self.span(off, size)]
        return self.copy(block, block, stage, k, mate)

    def add(self, k, off, size, buf):
        step = min(size, 16)
        j = k % self.slots

        def body(i):
            at = pl.ds(pl.multiple_of(off + i * step, step), step)
            self.acc[j, at] = self.acc[j, at] + buf[j, rows(i * step, step)]

        loop(0, size // step, body)

    def stage(self, i, k):
        for kind in self.kinds:
            run = {"x": self.stage_x, "s": self.stage_s, "l": self.stage_l}[kind]
            pl.when(self.is_kind(kind, k))(functools.partial(run, i, k))

    def stage_x(self, i, k):
        (m1, b1), (m2, b2), s2, s4 = *self.xy, self.s2, self.s4
        off1, off2 = b1 * s2, b1 * s2 + b2 * s4
        half = lambda: self.down(0, k, (1 - b1) * s2, s2, m1)
        quarter = lambda: self.down(1, k, off1 + (1 - b2) * s4, s4, m2)
        inward = lambda: self.down(2, k, off2, s4, self.z_mate)
        across = lambda: self.down(3, k, off2, s4, self.mid_mate)
        outward = lambda: self.up(4, k, off2, s4, self.z_mate)
        back4 = lambda: self.up(5, k, off2, s4, m2)
        back2 = lambda: self.up(6, k, off1, s2, m1)
        if i == 1:
            half().start()
        elif i == 2:
            half().wait_recv()
            self.add(k, off1, s2, self.landing[0])
            quarter().start()
        elif i == 3:
            quarter().wait_recv()
            self.add(k, off2, s4, self.landing[1])
            pl.when(self.end)(lambda: inward().start())
        elif i == 4:

            @pl.when(self.mid)
            def _():
                inward().wait_recv()
                self.add(k, off2, s4, self.landing[2])
                across().start()

        elif i == 5:

            @pl.when(self.mid)
            def _():
                across().wait_recv()
                self.finish(k, off2, s4, self.landing[3])
                outward().start()

        elif i == 6:
            pl.when(self.end)(lambda: outward().wait_recv())
            back4().start()
            half().wait_send()
            quarter().wait_send()
            pl.when(self.end)(lambda: inward().wait_send())
            pl.when(self.mid)(lambda: across().wait_send())
        elif i == 7:
            back4().wait_recv()
            back2().start()
        elif i == 8:
            back2().wait_recv()
        elif i == 10:
            pl.when(self.mid)(lambda: outward().wait_send())
            back4().wait_send()
            back2().wait_send()

    def stage_s(self, i, k):
        (m1, b1), (m2, b2), s2, s4 = *self.zz, self.s2, self.s4
        off1, off2 = b1 * s2, b1 * s2 + b2 * s4
        half = lambda: self.down(0, k, (1 - b1) * s2, s2, m1)
        quarter = lambda: self.down(1, k, off1 + (1 - b2) * s4, s4, m2)
        whole_1 = lambda: self.down(2, k, off2, s4, self.xy[0][0])
        whole_2 = lambda: self.down(3, k, off2, s4, self.xy[1][0])
        back4 = lambda: self.up(5, k, off2, s4, m2)
        back2 = lambda: self.up(6, k, off1, s2, m1)
        if i == 1:
            half().start()
        elif i == 2:
            half().wait_recv()
            self.add(k, off1, s2, self.landing[0])
            quarter().start()
        elif i == 3:
            quarter().wait_recv()
            self.add(k, off2, s4, self.landing[1])
            whole_1().start()
        elif i == 4:
            whole_1().wait_recv()
            whole_1().wait_send()
            self.add(k, off2, s4, self.landing[2])
            whole_2().start()
        elif i == 5:
            whole_2().wait_recv()
            self.finish(k, off2, s4, self.landing[3])
        elif i == 6:
            back4().start()
            half().wait_send()
            quarter().wait_send()
            whole_2().wait_send()
        elif i == 7:
            back4().wait_recv()
            back2().start()
        elif i == 8:
            back2().wait_recv()
        elif i == 10:
            back4().wait_send()
            back2().wait_send()

    def stage_l(self, i, k):
        s2, s4 = self.s2, self.s4
        s3 = s2 + s4
        b0, b1 = self.p.bz0, self.p.bz1
        own, side, tip, rest = (2 * b1 + b0) * s4, b1 * s2, 3 * b1 * s4, (1 - b1) * s4
        inward = lambda: self.down(0, k, rest, s3, self.z_mate)
        across = lambda: self.down(1, k, (1 - b1) * s2, s2, self.mid_mate)
        outward = lambda: self.down(2, k, tip, s4, self.z_mate)
        whole_1 = lambda: self.down(3, k, own, s4, self.xy[0][0])
        whole_2 = lambda: self.down(8, k, own, s4, self.xy[1][0], self.landing[4])
        tip_back = lambda: self.up(4, k, tip, s4, self.z_mate)
        side_back = lambda: self.up(5, k, side, s2, self.mid_mate)
        rest_back = lambda: self.up(6, k, rest, s3, self.z_mate)
        if i == 1:
            pl.when(self.end)(lambda: inward().start())
        elif i == 2:

            @pl.when(self.mid)
            def _():
                inward().wait_recv()
                self.add(k, rest, s3, self.landing[0])
                across().start()

        elif i == 3:

            @pl.when(self.mid)
            def _():
                across().wait_recv()
                self.add(k, side, s2, self.landing[1])
                outward().start()

        elif i == 4:

            @pl.when(self.end)
            def _():
                outward().wait_recv()
                self.add(k, own, s4, self.landing[2])

            whole_1().start()
        elif i == 5:
            whole_1().wait_recv()
            whole_1().wait_send()
            pl.when(self.mid)(lambda: outward().wait_send())
            self.add(k, own, s4, self.landing[3])
            whole_2().start()
        elif i == 6:
            whole_2().wait_recv()
            self.finish(k, own, s4, self.landing[4])
            pl.when(self.end)(lambda: tip_back().start())
            whole_2().wait_send()
            pl.when(self.end)(lambda: inward().wait_send())
            pl.when(self.mid)(lambda: across().wait_send())
        elif i == 7:

            @pl.when(self.mid)
            def _():
                tip_back().wait_recv()
                side_back().start()

        elif i == 8:

            @pl.when(self.mid)
            def _():
                side_back().wait_recv()
                rest_back().start()

        elif i == 9:
            pl.when(self.end)(lambda: rest_back().wait_recv())
        elif i == 10:
            pl.when(self.end)(lambda: tip_back().wait_send())

            @pl.when(self.mid)
            def _():
                side_back().wait_send()
                rest_back().wait_send()


def form_next(k, form):
    pl.when(k == 1)(lambda: form(GROUP // 2, GROUP // 2))
    pl.when((k % GROUP == 0) & (k > 0))(lambda: form(k, GROUP))


def run_slots(plan, count, stage, between):
    lags, order = plan

    def slot(t):
        for i in order:
            k = t - lags[i]

            @pl.when((k >= 0) & (k < count))
            def _():
                stage(i, k)

            if i == 1:
                between(t)

    loop(0, count + lags[-1], slot)


def chunk_scratch(slots, gather_slots, part_rows, width, count, dtype):
    def buf(n):
        return pltpu.VMEM((slots, n, width), jnp.float32)

    gathered = pltpu.VMEM((gather_slots, part_rows, width), dtype)

    dma = pltpu.SemaphoreType.DMA
    quarter = part_rows // 4
    return [buf(part_rows), gathered, *(buf(n * quarter) for n in (3, 2, 1, 1, 1)), dma((9, count)), dma((9, count))]


def fold(value):
    return jnp.sum(value.reshape(value.shape[0] // 8, 8, value.shape[1]), axis=0)


def front_kernel(feat_a, feat_b, w_in, t_in, w_mid, t_mid, w_out, t_out, gain1, bias1, gain2, bias2, off_weight, pre1, pre2, xs2, xs1, xs0, dz, grad_emb, vec, *scratch):
    (x_buf, u_buf, w_buf, stats, affine, loss, ea, eb, g_peer) = scratch[:9]
    (x_sem, w_sem, pre_sem, keep_sem, keep_send, keep_recv, ge_sem, e_send, e_recv) = scratch[9:18]
    small_refs = scratch[18 : 18 + SMALL_REFS]
    acc, gathered, *landing, send, recv = scratch[18 + SMALL_REFS :]
    rows_dev, width = feat_a.shape
    wide = w_buf.shape[2]
    tiles = width // wide
    half = width // 2
    part_rows = half // PARTS
    row_count = rows_dev * DEPTH * PLANE
    weights, feats = (w_in, t_in, w_mid, t_mid, w_out, t_out), (feat_a, feat_b)
    place = Place()
    core = place.core
    mine = rows(core * rows_dev, rows_dev)
    place.arrive()
    small = small_sum(place, small_refs)
    payload, total = small.payload, small.total

    def feat(v):
        return pltpu.make_async_copy(feats[v], x_buf.at[v], x_sem.at[v])

    def w_tile(ref, g):
        return pltpu.make_async_copy(ref.at[:, rows((g % tiles) * wide, wide)], w_buf.at[g % W_BUFS], w_sem.at[g % W_BUFS])

    def start_w(g):
        pick(g // tiles, weights, lambda ref: w_tile(ref, g).start())

    feat(0).start()
    w_tile(weights[0], 0).start()
    feat(1).start()
    for g in range(1, W_BUFS - 1):
        start_w(g)
    for j, ref in enumerate((gain1, bias1, gain2, bias2)):
        affine[j] = ref[...]
    feat(0).wait()
    payload[...] = jnp.zeros_like(payload)

    def keep_pre(ref):
        return pltpu.make_async_copy(u_buf.at[0], ref, pre_sem.at[0])

    kept = (xs0, xs1, xs2)

    def keep_x(w):
        here = pltpu.make_async_copy(x_buf.at[0, :, rows(core * half, half)], kept[w].at[mine], keep_sem.at[w])
        there = remote_copy(x_buf.at[0, :, rows((1 - core) * half, half)], kept[w].at[mine], keep_send.at[w], keep_recv.at[w], place.other_core)
        return here, there

    def start_x(w):
        for c in keep_x(w):
            c.start()

    def free_x(w):
        here, there = keep_x(w)
        here.wait()
        there.wait_send()

    def keep_dz(i):
        at = (slice(None), rows(i * wide, wide))
        here = pltpu.make_async_copy(x_buf.at[(0, *at)], dz.at[mine, at[1]], keep_sem.at[3 + i])
        there = remote_copy(x_buf.at[(0, *at)], dz.at[mine, at[1]], keep_send.at[3 + i], keep_recv.at[3 + i], place.other_core)
        return here, there

    def row_loop(body, carry):
        return lax.fori_loop(0, rows_dev // BLOCK, lambda r, c: body(rows(r * BLOCK, BLOCK), c), carry)

    def put_sums(j, i, row, value):
        value = jnp.sum(value, axis=0, keepdims=True)
        for c in range(value.shape[1] // TILE):
            payload[j, i + c, row : row + 1] = value[:, c * TILE : (c + 1) * TILE]

    def product(g):
        job, i = g // tiles, g % tiles
        view = job % 2
        w_tile(w_in, g).wait()
        pl.when(g + W_BUFS - 1 < JOBS * tiles)(lambda: start_w(g + W_BUFS - 1))
        at_cols = rows(i * wide, wide)
        u_buf[view, :, at_cols] = jnp.dot(x_buf[view], w_buf[g % W_BUFS], preferred_element_type=jnp.float32)

        def block(at, sums):
            u = u_buf[view, at, at_cols]
            return sums[0] + fold(u), sums[1] + fold(u * u)

        zero = jnp.zeros((8, wide), jnp.float32)
        for row, value in enumerate(row_loop(block, (zero, zero))):
            put_sums(job, i * (wide // TILE), row, value)

    def begin(job):
        small.begin(job)

        @pl.when(job % 2 == 0)
        def _():
            pick(job // 2, (pre1, pre2), lambda ref: keep_pre(ref).start())

    def norm(job):
        layer, view = job // 2, job % 2
        small.end(job)
        for c in range(PLANE):
            at = slice(c * TILE, (c + 1) * TILE)
            means = total[job, c] / row_count
            stats[job, 0, :, at] = means[0:1]
            stats[job, 1, :, at] = lax.rsqrt(means[1:2] - means[0:1] * means[0:1] + NORM_EPS)

        pl.when(view == 0)(lambda: pick(layer, (0, 1, 2), free_x))

        def hidden(i):
            at_cols = rows(i * wide, wide)
            mean, inv = stats[job, 0, :, at_cols], stats[job, 1, :, at_cols]
            gain, bias = affine[layer * 2, :, at_cols], affine[layer * 2 + 1, :, at_cols]

            def block(at, c):
                n = (u_buf[view, at, at_cols] - mean) * inv
                x_buf[view, at, at_cols] = jnp.maximum(n * gain + bias, 0.0).astype(jnp.bfloat16)
                return c

            row_loop(block, 0)

        def student(i):
            at_cols = rows(i * wide, wide)
            mean, inv = stats[job, 0, :, at_cols], stats[job, 1, :, at_cols]

            def block(at, c):
                n = (u_buf[0, at, at_cols] - mean) * inv
                u_buf[0, at, at_cols] = n
                x_buf[0, at, at_cols] = n.astype(jnp.bfloat16)
                return c

            row_loop(block, 0)

        def student_own(i):
            def block(r, c):
                ea[rows(core * rows_dev + r * BLOCK, BLOCK), rows(i * wide, wide)] = x_buf[0, rows(r * BLOCK, BLOCK), rows(core * half + i * wide, wide)]
                return c

            lax.fori_loop(0, rows_dev // BLOCK, block, 0)

        def teacher(i):
            at_cols = rows(i * wide, wide)
            mean, inv = stats[job, 0, :, at_cols], stats[job, 1, :, at_cols]

            def block(r, c):
                n = (u_buf[1, rows(r * BLOCK, BLOCK), at_cols] - mean) * inv
                eb[rows(core * rows_dev + r * BLOCK, BLOCK), at_cols] = n.astype(jnp.bfloat16)
                return c

            lax.fori_loop(0, rows_dev // BLOCK, block, 0)
            eb_copy(i).start()

        @pl.when(layer < 2)
        def _():
            loop(0, tiles, hidden)

            @pl.when(view == 0)
            def _():
                pick(layer, (1, 2), start_x)
                keep_pre(pre1).wait()

        @pl.when((layer == 2) & (view == 0))
        def _():
            loop(0, tiles, student)
            ea_copy().start()
            loop(0, tiles // 2, student_own)

        @pl.when((layer == 2) & (view == 1))
        def _():
            loop(0, tiles, teacher)

    ea_copy = lambda: remote_copy(x_buf.at[0, :, rows((1 - core) * half, half)], ea.at[mine], e_send.at[0], e_recv.at[0], place.other_core)

    def eb_copy(i):
        block = eb.at[mine, rows(i * wide, wide)]
        return remote_copy(block, block, e_send.at[1 + i], e_recv.at[1 + i], place.other_core)

    def step(g):
        job, i = g // tiles, g % tiles
        view = job % 2
        pl.when(g == tiles)(lambda: feat(1).wait())
        product(g)

        @pl.when(g == 0)
        def _():
            place.all_here()
            start_x(0)

        pl.when((i == 1) & (job > 0))(lambda: small.middle(job - 1))

        @pl.when(i == tiles - 1)
        def _():
            begin(job)
            pl.when(job > 0)(lambda: norm(job - 1))

    loop(0, JOBS * tiles, step)
    small.middle(JOBS - 1)
    norm(JOBS - 1)
    for j, source in enumerate((affine.at[2], affine.at[3], stats.at[2, 0], stats.at[2, 1], affine.at[0], affine.at[1], stats.at[0, 0], stats.at[0, 1])):
        vec[j] = source[...]

    loss[...] = jnp.zeros_like(loss)

    def finish(k, off, size, buf):
        share = jnp.where(front_kind("x", k), 0.5, 0.25)
        at = rows(off, size)
        corr = (acc[k, at] + buf[k]) / row_count
        row = core * half + k * part_rows + off
        diag = (row + lax.broadcasted_iota(jnp.int32, (size, width), 0)) == lax.broadcasted_iota(jnp.int32, (size, width), 1)
        weight = off_weight[0]
        miss = 1.0 - corr
        loss[...] += share * jnp.sum(jnp.where(diag, miss * miss, weight * (corr * corr)), axis=0, keepdims=True)
        gathered[k, at] = jnp.where(diag, -2.0 * miss, 2.0 * weight * corr).astype(jnp.bfloat16)

    chunks = ChunkSum(place, "xsl", front_kind, acc, gathered, landing, send, recv, finish)

    def form(k, group):
        at = rows(k * part_rows, group * part_rows)
        size = min(1024, width)

        def col(c):
            @pl.when(k == 0)
            def _():
                for i in range(size // wide):
                    eb_copy(c * (size // wide) + i).wait_recv()

            cs = rows(c * size, size)
            acc[pl.ds(k, group), :, cs] = contract_rows(ea[:, at], eb[:, cs]).reshape(group, part_rows, size)

        loop(0, width // size, col)

    def swap(k):
        return chunks.copy(gathered.at[k], g_peer.at[k], 7, k, place.other_core)

    def ge_cols(k, side):
        return rows(side * half + k * part_rows, GROUP * part_rows)

    def ge_copy(k, side):
        at = ge_cols(k, side)
        return pltpu.make_async_copy(u_buf.at[1, :, at], grad_emb.at[:, at], ge_sem.at[k // GROUP, side])

    def embed(k, side, g_rows):
        at_cols = ge_cols(k, side)
        grad = contract_cols(eb[mine], g_rows.reshape(GROUP * part_rows, width)) / row_count
        u_buf[1, :, at_cols] = grad
        ge_copy(k, side).start()

        def block(at, sums):
            g = u_buf[1, at, at_cols]
            return sums[0] + fold(g * u_buf[0, at, at_cols]), sums[1] + fold(g)

        zero = jnp.zeros((8, GROUP * part_rows), jnp.float32)
        for row, value in enumerate(row_loop(block, (zero, zero))):
            payload[JOBS, (side * half + k * part_rows) // TILE, row : row + 1] = jnp.sum(value, axis=0, keepdims=True)

    def stage(i, k):
        if i == 0:
            form_next(k, form)
            return
        chunks.stage(i, k)
        if i == 8:
            pl.when(jnp.logical_not(front_kind("l", k)))(lambda: swap(k).start())
        if i == 9:
            pl.when(front_kind("l", k))(lambda: swap(k).start())

            @pl.when(k % GROUP == GROUP - 1)
            def _():
                embed(k - GROUP + 1, core, gathered[pl.ds(k - GROUP + 1, GROUP)])

        if i == 10:
            swap(k).wait_recv()
            swap(k).wait_send()

            @pl.when(k % GROUP == GROUP - 1)
            def _():
                embed(k - GROUP + 1, 1 - core, g_peer[pl.ds(k - GROUP + 1, GROUP)])

    ea_copy().wait_recv()
    form(0, GROUP // 2)
    run_slots(FRONT_PLAN, PARTS, stage, lambda t: None)
    small.begin(JOBS)
    for c in range(PLANE):
        payload[JOBS + 1, c, 0:1] = loss[:, c * TILE : (c + 1) * TILE]
    small.begin(JOBS + 1)
    ea_copy().wait_send()
    for i in range(tiles):
        eb_copy(i).wait_send()
    small.middle(JOBS)
    small.middle(JOBS + 1)
    for k in range(0, PARTS, GROUP):
        for side in range(2):
            ge_copy(k, side).wait()
    small.end(JOBS)

    def dz_tile(i):
        at_cols = rows(i * wide, wide)
        sums = jnp.concatenate([total[JOBS, i * (wide // TILE) + c] for c in range(wide // TILE)], axis=1) / row_count
        mean_gn, mean_g = sums[0:1], sums[1:2]
        inv = stats[JOBS - 2, 1, :, at_cols]

        def block(at, c):
            value = (u_buf[1, at, at_cols] - mean_g - u_buf[0, at, at_cols] * mean_gn) * inv
            x_buf[0, at, at_cols] = value.astype(jnp.bfloat16)
            return c

        row_loop(block, 0)
        for c in keep_dz(i):
            c.start()

    loop(0, tiles, dz_tile)
    small.end(JOBS + 1)
    for c in range(PLANE):
        vec[8, :, c * TILE : (c + 1) * TILE] = total[JOBS + 1, c, 0:1]
    for w in range(3):
        keep_x(w)[1].wait_recv()
    for i in range(tiles):
        here, there = keep_dz(i)
        here.wait()
        there.wait()


def front(feat_a, feat_b, weights, affine, off_weight):
    rows_dev, width = feat_a.shape
    half = width // 2
    part_rows = half // PARTS
    any_spec = pl.BlockSpec(memory_space=pl.ANY)
    vmem_spec = pl.BlockSpec(memory_space=pltpu.VMEM)
    wide_f32 = jax.ShapeDtypeStruct((rows_dev, width), jnp.float32)
    kept = jax.ShapeDtypeStruct((2 * rows_dev, half), jnp.bfloat16)
    both_dz = jax.ShapeDtypeStruct((2 * rows_dev, width), jnp.bfloat16)
    keeps = 3 + width // WIDE
    dma = pltpu.SemaphoreType.DMA
    return pl.pallas_call(
        front_kernel,
        name="front",
        out_shape=[wide_f32, wide_f32, kept, kept, kept, both_dz, wide_f32]
        + [jax.ShapeDtypeStruct((9, 1, width), jnp.float32)],
        in_specs=[any_spec] * 8 + [vmem_spec] * 4 + [pl.BlockSpec(memory_space=pltpu.SMEM)],
        out_specs=[any_spec] * 7 + [vmem_spec],
        scratch_shapes=[
            pltpu.VMEM((2, rows_dev, width), jnp.bfloat16),
            pltpu.VMEM((2, rows_dev, width), jnp.float32),
            pltpu.VMEM((W_BUFS, width, WIDE), jnp.bfloat16),
            pltpu.VMEM((JOBS, 2, 1, width), jnp.float32),
            pltpu.VMEM((4, 1, width), jnp.float32),
            pltpu.VMEM((1, width), jnp.float32),
            pltpu.VMEM((2 * rows_dev, half), jnp.bfloat16),
            pltpu.VMEM((2 * rows_dev, width), jnp.bfloat16),
            pltpu.VMEM((PARTS, part_rows, width), jnp.bfloat16),
            dma((2,)),
            dma((W_BUFS,)),
            dma((1,)),
            dma((keeps,)),
            dma((keeps,)),
            dma((keeps,)),
            dma((PARTS // GROUP, 2)),
            dma((1 + width // WIDE,)),
            dma((1 + width // WIDE,)),
        ]
        + small_scratch(JOBS + 2)
        + chunk_scratch(PARTS, PARTS, part_rows, width, PARTS, jnp.bfloat16),
        compiler_params=pltpu.CompilerParams(collective_id=0, has_side_effects=True, vmem_limit_bytes=VMEM_BYTES),
    )(feat_a, feat_b, *weights, *affine, off_weight)


def back_kernel(dz_hbm, x2, x1, x0, w_out, w_mid, u2, u1, vec, out2, out1, out0, sums_out, *scratch):
    (dy, xs, w_buf, u_buf, dpre) = scratch[:5]
    (in_sem, tile_sem, peer_send, peer_recv, store_sem) = scratch[5:10]
    small_refs = scratch[10 : 10 + SMALL_REFS]
    acc, gathered, *landing, send, recv = scratch[10 + SMALL_REFS :]
    rows_dev, width = dpre.shape
    wide = w_buf.shape[1]
    tiles = width // wide
    row_count = rows_dev * DEPTH * PLANE
    half = width // 2
    part_rows = half // PARTS
    count = MATS * PARTS
    mats_in, outs, weights, pres = (x2, x1, x0), (out2, out1, out0), (w_out, w_mid), (u2, u1)
    place = Place()
    core, other_core = place.core, place.other_core
    mine = rows(core * rows_dev, rows_dev)
    place.arrive()
    small = small_sum(place, small_refs)
    payload, sums = small.payload, small.total

    def load_x(w):
        return pltpu.make_async_copy(mats_in[w], xs.at[w % 2], in_sem.at[w])

    def peer_dy(w):
        block = dy.at[w % 2, mine]
        return remote_copy(block, block, peer_send.at[w], peer_recv.at[w], other_core)

    def w_tile(ref, i):
        return pltpu.make_async_copy(ref.at[rows(i * wide, wide)], w_buf.at[i % 2], tile_sem.at[0, i % 2])

    def u_tile(ref, i):
        return pltpu.make_async_copy(ref.at[:, rows(i * wide, wide)], u_buf.at[i % 2], tile_sem.at[1, i % 2])

    def start_w(layer, i):
        pick(layer, weights, lambda ref: w_tile(ref, i).start())

    def start_u(layer, i):
        pick(layer, pres, lambda ref: u_tile(ref, i).start())

    size = min(1024, width)

    def load_dz(c):
        return pltpu.make_async_copy(dz_hbm.at[:, rows(c * size, size)], dy.at[0, :, rows(c * size, size)], in_sem.at[MATS + c])

    load_x(0).start()
    for c in range(width // size):
        load_dz(c).start()
    w_tile(weights[0], 0).start()
    u_tile(pres[0], 0).start()
    load_x(1).start()
    payload[...] = jnp.zeros_like(payload)

    def row_loop(body, carry):
        return lax.fori_loop(0, rows_dev // BLOCK, body, carry)

    def chain_tile(layer, i):
        w_tile(w_out, i).wait()
        u_tile(u2, i).wait()

        @pl.when(i + 1 < tiles)
        def _():
            start_w(layer, i + 1)
            start_u(layer, i + 1)

        at_cols = rows(i * wide, wide)
        dpre[:, at_cols] = contract_cols(dy[layer, mine], w_buf[i % 2])
        gain, bias, mean, inv = (vec[layer * 4 + j, :, at_cols] for j in range(4))

        def block(r, carry):
            at = rows(r * BLOCK, BLOCK)
            n = (u_buf[i % 2, at] - mean) * inv
            g = jnp.where(n * gain + bias > 0.0, dpre[at, at_cols], 0.0)
            dpre[at, at_cols] = g
            return carry[0] + fold(g * n), carry[1] + fold(g)

        zero = jnp.zeros((8, wide), jnp.float32)
        for row, value in enumerate(row_loop(block, (zero, zero))):
            value = jnp.sum(value, axis=0, keepdims=True)
            for c in range(wide // TILE):
                payload[layer, i * (wide // TILE) + c, row : row + 1] = value[:, c * TILE : (c + 1) * TILE]

    def du_tile(layer, i):
        u_tile(u2, i).wait()
        pl.when(i + 1 < tiles)(lambda: start_u(layer, i + 1))
        at_cols = rows(i * wide, wide)
        gain, mean, inv = (vec[layer * 4 + j, :, at_cols] for j in (0, 2, 3))
        means = jnp.concatenate([sums[layer, i * (wide // TILE) + c] for c in range(wide // TILE)], axis=1) / row_count
        mean_gn, mean_g = means[0:1], means[1:2]
        scale = gain * inv

        def block(r, c):
            at = rows(r * BLOCK, BLOCK)
            n = (u_buf[i % 2, at] - mean) * inv
            value = (dpre[at, at_cols] - mean_g - n * mean_gn) * scale
            dy[1 - layer, rows(core * rows_dev + r * BLOCK, BLOCK), at_cols] = value.astype(jnp.bfloat16)
            return c

        row_loop(block, 0)

    def finish(k, off, size, buf):
        j = k % ACC_SLOTS
        gathered[k % GATHER_SLOTS, rows(off, size)] = acc[j, rows(off, size)] + buf[j]

    chunks = ChunkSum(place, "xl", back_kind, acc, gathered, landing, send, recv, finish)

    def form(k, group):
        w, j = k // PARTS, k % ACC_SLOTS

        @pl.when(k % PARTS == 0)
        def _():
            pltpu.make_async_copy(xs.at[w % 2], xs.at[w % 2], in_sem.at[w]).wait()
            pl.when(w > 0)(lambda: peer_dy(w).wait_recv())

        at = rows((k % PARTS) * part_rows, group * part_rows)

        def col(c):
            pl.when(k == 0)(lambda: load_dz(c).wait())
            cs = rows(c * size, size)
            acc[pl.ds(j, group), :, cs] = contract_rows(xs[w % 2, :, at], dy[w % 2, :, cs]).reshape(group, part_rows, size)

        loop(0, width // size, col)

    def out_rows(k, side):
        return pl.ds(pl.multiple_of(side * half + (k % PARTS) * part_rows, part_rows), part_rows)

    def last_copy(out, k, side):
        return chunks.copy(gathered.at[k % GATHER_SLOTS], out.at[out_rows(k, side)], 7, k, other_core)

    def store_copy(out, k):
        return pltpu.make_async_copy(gathered.at[k % GATHER_SLOTS], out.at[out_rows(k, core)], store_sem.at[k])

    def stage(i, k):
        if i == 0:
            form_next(k, form)
            return
        chunks.stage(i, k)
        def emit(out):
            last_copy(out, k, core).start()
            store_copy(out, k).start()

        if i == 8:
            pl.when(back_kind("x", k))(lambda: pick(k // PARTS, outs, emit))
        if i == 9:
            pl.when(back_kind("l", k))(lambda: pick(k // PARTS, outs, emit))
        if i == 10:

            def close(out):
                last_copy(out, k, 1 - core).wait_recv()
                store_copy(out, k).wait()
                last_copy(out, k, core).wait_send()

            pick(k // PARTS, outs, close)

    def layer_work(t):
        layer = t // LAYER_SLOTS
        at = t - LAYER_SLOTS * layer
        first_du = 2 * tiles + 3
        pl.when((at < 2 * tiles) & (at % 2 == 1))(lambda: chain_tile(layer, at // 2))
        pl.when(at == 2 * tiles)(lambda: small.begin(layer))
        pl.when(at == 2 * tiles + 1)(lambda: small.middle(layer))

        pl.when(at == 2 * tiles + 2)(lambda: start_u(layer, 0))

        pl.when(at == first_du)(lambda: small.end(layer))
        pl.when(at >= first_du)(lambda: du_tile(layer, at - first_du))

        @pl.when(at == LAYER_SLOTS - 1)
        def _():
            peer_dy(layer + 1).start()

            @pl.when(layer == 0)
            def _():
                w_tile(weights[1], 0).start()
                u_tile(pres[1], 0).start()

            pl.when(layer == 1)(lambda: load_x(2).start())

    form(0, GROUP // 2)
    place.all_here()
    run_slots(BACK_PLAN, count, stage, lambda t: pl.when(t < 2 * LAYER_SLOTS)(lambda: layer_work(t)))
    for w in (1, 2):
        peer_dy(w).wait_send()
    for c in range(PLANE):
        for row in range(4):
            sums_out[row : row + 1, c * TILE : (c + 1) * TILE] = sums[row // 2, c, row % 2 : row % 2 + 1]
    sums_out[4:5] = jnp.full((1, width), jnp.sum(vec[8]))


def backward(grad_z, x2, x1, x0, w_out, w_mid, u2, u1, vec):
    rows_dev, width = u2.shape
    part_rows = width // 2 // PARTS
    count = MATS * PARTS
    any_spec = pl.BlockSpec(memory_space=pl.ANY)
    vmem_spec = pl.BlockSpec(memory_space=pltpu.VMEM)
    mat = jax.ShapeDtypeStruct((width, width), jnp.float32)
    dma = pltpu.SemaphoreType.DMA
    return pl.pallas_call(
        back_kernel,
        name="backward",
        out_shape=[mat, mat, mat, jax.ShapeDtypeStruct((5, width), jnp.float32)],
        in_specs=[any_spec] * 8 + [vmem_spec],
        out_specs=[any_spec] * 3 + [vmem_spec],
        scratch_shapes=[
            pltpu.VMEM((2, 2 * rows_dev, width), jnp.bfloat16),
            pltpu.VMEM((2, 2 * rows_dev, width // 2), jnp.bfloat16),
            pltpu.VMEM((2, WIDE, width), jnp.bfloat16),
            pltpu.VMEM((2, rows_dev, WIDE), jnp.float32),
            pltpu.VMEM((rows_dev, width), jnp.float32),
            dma((MATS + 2,)),
            dma((2, 2)),
            dma((MATS,)),
            dma((MATS,)),
            dma((count,)),
        ]
        + small_scratch(2)
        + chunk_scratch(ACC_SLOTS, GATHER_SLOTS, part_rows, width, count, jnp.float32),
        compiler_params=pltpu.CompilerParams(collective_id=1, has_side_effects=True, vmem_limit_bytes=VMEM_BYTES),
    )(grad_z, x2, x1, x0, w_out, w_mid, u2, u1, vec)


def copy_kernel(*refs):
    pairs = (len(refs) - 3 - 6) // 2
    ins, small, outs, small_outs, (buf, in_sem, out_sem) = refs[:pairs], refs[pairs], refs[pairs + 1 : 2 * pairs + 1], refs[2 * pairs + 1 : -3], refs[-3:]
    blocks = [(i, r) for i in range(pairs) for r in range(0, ins[i].shape[0], COPY_ROWS)]

    def read(b):
        i, r = blocks[b]
        return pltpu.make_async_copy(ins[i].at[pl.ds(r, COPY_ROWS)], buf.at[b % COPY_BUFS], in_sem.at[b % COPY_BUFS])

    def write(b):
        i, r = blocks[b]
        return pltpu.make_async_copy(buf.at[b % COPY_BUFS], outs[i].at[pl.ds(r, COPY_ROWS)], out_sem.at[b % COPY_BUFS])

    ahead = COPY_BUFS // 2
    for b in range(min(ahead, len(blocks))):
        read(b).start()
    for row in range(4):
        small_outs[row][...] = small[row : row + 1]
    small_outs[4][...] = small[4:5, :1]
    for b in range(len(blocks)):
        if b + ahead < len(blocks):
            if b + ahead >= COPY_BUFS:
                write(b + ahead - COPY_BUFS).wait()
            read(b + ahead).start()
        read(b).wait()
        write(b).start()
    for b in range(max(0, len(blocks) - COPY_BUFS), len(blocks)):
        write(b).wait()


def copy_out(arrays, small):
    any_spec = pl.BlockSpec(memory_space=pl.ANY)
    vmem_spec = pl.BlockSpec(memory_space=pltpu.VMEM)
    dma = pltpu.SemaphoreType.DMA
    width = small.shape[1]
    row = jax.ShapeDtypeStruct((1, width), jnp.float32)
    return pl.pallas_call(
        copy_kernel,
        name="copy_out",
        out_shape=[jax.ShapeDtypeStruct(a.shape, a.dtype) for a in arrays] + [row] * 4 + [jax.ShapeDtypeStruct((1, 1), jnp.float32)],
        in_specs=[any_spec] * len(arrays) + [vmem_spec],
        out_specs=[any_spec] * len(arrays) + [vmem_spec] * 5,
        scratch_shapes=[pltpu.VMEM((COPY_BUFS, COPY_ROWS, width), jnp.float32), dma((COPY_BUFS,)), dma((COPY_BUFS,))],
        compiler_params=pltpu.CompilerParams(vmem_limit_bytes=VMEM_BYTES),
    )(*arrays, small)


def solution(mesh):
    row_part = P(DATA_AXIS, None)
    replicated = P()

    def local_step(feat_a, feat_b, w_in, w_mid, w_out, t_in, t_mid, t_out, gain_1, bias_1, gain_2, bias_2, off_weight):
        affine = [v.reshape(1, -1) for v in (gain_1, bias_1, gain_2, bias_2)]
        pre_1, pre_2, xs_2, xs_1, xs_0, grad_z, grad_emb, vec = front(
            feat_a, feat_b, (w_in, t_in, w_mid, t_mid, w_out, t_out), affine, off_weight.reshape(1)
        )
        grad_w_out, grad_w_mid, grad_w_in, sums = backward(grad_z, xs_2, xs_1, xs_0, w_out, w_mid, pre_2, pre_1, vec)
        (grad_emb, grad_w_out, grad_w_mid, grad_w_in, gain_2, bias_2, gain_1, bias_1, loss) = copy_out((grad_emb, grad_w_out, grad_w_mid, grad_w_in), sums)
        gain_1, bias_1, gain_2, bias_2 = (v.reshape(-1) for v in (gain_1, bias_1, gain_2, bias_2))
        return (loss.reshape(()), grad_emb, grad_w_in, grad_w_mid, grad_w_out, gain_1, bias_1, gain_2, bias_2)

    return jax.shard_map(local_step, mesh=mesh, in_specs=(row_part, row_part) + (replicated,) * 11, out_specs=(replicated, row_part) + (replicated,) * 7, check_vma=False)
```

```python
import functools

import jax
import jax.numpy as jnp
from jax import lax
from jax.experimental import pallas as pl
from jax.experimental.pallas import tpu as pltpu
from jax.sharding import PartitionSpec as P

NORM_EPS = 1e-5
DATA_AXIS = "data"
MESH = pl.DeviceIdType.MESH
VMEM_BYTES = 67_043_328
PLANE = 8
DEPTH = 4
TILE = 256
WIDE = 512
BLOCK = 128
SUM_ROWS = 2
PARTS = 16
GROUP = 4
MATS = 3
ACC_SLOTS = 20
GATHER_SLOTS = 16
JOBS = 6
W_BUFS = 3
LAYER_SLOTS = 15
COPY_ROWS = 256
COPY_BUFS = 20
FRONT_PLAN = ((0, 0, 3, 5, 7, 9, 12, 13, 16, 17, 18), (0, 6, 3, 4, 9, 10, 8, 5, 2, 7, 1))
BACK_PLAN = ((0, 0, 3, 5, 7, 8, 9, 11, 14, 17, 19), (0, 4, 8, 7, 10, 1, 2, 3, 5, 6, 9))


def front_kind(kind, k):
    s, l = (k % 5 == 2) & (k > 2), k == 2
    return {"s": s, "l": l, "x": (k % 5 != 2)}[kind]


def back_kind(kind, k):
    l = ((k % 5 == 2) & (k < 43)) | ((k % 5 == 0) & (k >= 10) & (k < 36))
    return l if kind == "l" else jnp.logical_not(l)


def contract_rows(left_op, right_op):
    return lax.dot_general(left_op, right_op, (((0,), (0,)), ((), ())), preferred_element_type=jnp.float32)


def contract_cols(left_op, right_op):
    return lax.dot_general(left_op, right_op, (((1,), (1,)), ((), ())), preferred_element_type=jnp.float32)


def rows(off, size):
    return pl.ds(pl.multiple_of(off, size), size)


def pick(index, choices, what):
    for i, c in enumerate(choices):
        pl.when(index == i)(functools.partial(what, c))


def loop(lo, hi, body):
    def step(i, carry):
        body(i)
        return carry

    lax.fori_loop(lo, hi, step, 0)


def remote_copy(src, dst, send, recv, mate):
    return pltpu.make_async_remote_copy(src, dst, send, recv, device_id=(mate,), device_id_type=MESH)


class Place:
    def __init__(self):
        me = lax.axis_index(DATA_AXIS)
        self.me = me
        self.pos, self.plane = me % PLANE, me // PLANE
        self.core, self.bx, self.by, self.bz0, self.bz1 = me % 2, (me // 2) % 2, (me // 4) % 2, (me // 8) % 2, (me // 16) % 2
        self.other_core = me + 1 - 2 * self.core
        self.mates = [(self.pos + d) % PLANE for d in range(1, PLANE)]
        self.levels = [(self.plane + d) % DEPTH for d in range(1, DEPTH)]

    def peers(self):
        return [self.plane * PLANE + m for m in self.mates] + [lv * PLANE + self.pos for lv in self.levels]

    def arrive(self):
        sem = pltpu.get_barrier_semaphore()
        for peer in self.peers():
            pl.semaphore_signal(sem, inc=1, device_id=(peer,), device_id_type=MESH)

    def all_here(self):
        pl.semaphore_wait(pltpu.get_barrier_semaphore(), PLANE + DEPTH - 2)


class SmallSum:
    def __init__(self, place, payload, total, depth_buf, line_sum, plane_buf, sems):
        self.p, self.payload, self.total = place, payload, total
        self.depth_buf, self.line_sum, self.plane_buf, self.sems = depth_buf, line_sum, plane_buf, sems

    def along(self, j, lv, slot):
        s, r = self.sems[0], self.sems[1]
        return remote_copy(self.payload.at[j], self.depth_buf.at[j, slot], s.at[j, lv], r.at[j, slot], lv * PLANE + self.p.pos)

    def within(self, j, m, slot):
        s, r = self.sems[2], self.sems[3]
        return remote_copy(self.line_sum.at[j], self.plane_buf.at[j, slot], s.at[j, m], r.at[j, slot], self.p.plane * PLANE + m)

    def begin(self, j):
        for lv in self.p.levels:
            self.along(j, lv, self.p.plane).start()
        self.depth_buf[j, self.p.plane] = self.payload[j]

    def middle(self, j):
        for lv in self.p.levels:
            self.along(j, lv, lv).wait_recv()
        total = self.depth_buf[j, 0]
        for i in range(1, DEPTH):
            total = total + self.depth_buf[j, i]
        self.line_sum[j] = total
        for m in self.p.mates:
            self.within(j, m, self.p.pos).start()
        self.plane_buf[j, self.p.pos] = total

    def end(self, j):
        for m in self.p.mates:
            self.within(j, m, m).wait_recv()
        total = self.plane_buf[j, 0]
        for i in range(1, PLANE):
            total = total + self.plane_buf[j, i]
        self.total[j] = total
        for lv in self.p.levels:
            self.along(j, lv, self.p.plane).wait_send()
        for m in self.p.mates:
            self.within(j, m, self.p.pos).wait_send()


def small_scratch(count):
    def buf(*lead):
        return pltpu.VMEM((count, *lead, PLANE, SUM_ROWS, TILE), jnp.float32)

    return [buf(), buf(), buf(DEPTH), buf(), buf(PLANE)] + [pltpu.SemaphoreType.DMA((count, n)) for n in (DEPTH, DEPTH, PLANE, PLANE)]


SMALL_REFS = 9


def small_sum(place, refs):
    return SmallSum(place, *refs[:5], refs[5:])


class ChunkSum:
    def __init__(self, place, kinds, is_kind, acc, gathered, landing, send, recv, finish):
        self.p, self.kinds, self.is_kind, self.slots, self.gather_slots = place, kinds, is_kind, acc.shape[0], gathered.shape[0]
        self.acc, self.gathered, self.landing, self.send, self.recv, self.finish = acc, gathered, landing, send, recv, finish
        self.size = acc.shape[1]
        self.s2, self.s4 = self.size // 2, self.size // 4
        core, bx, by, me = place.core, place.bx, place.by, place.me
        first, second = core * by + (1 - core) * bx, core * bx + (1 - core) * by
        self.xy = ((me + (2 + 2 * core) * (1 - 2 * first), first), (me + (4 - 2 * core) * (1 - 2 * second), second))
        self.zz = ((me + 8 * (1 - 2 * place.bz0), place.bz0), (me + 16 * (1 - 2 * place.bz1), place.bz1))
        self.is_mid = place.bz0 + place.bz1 - 2 * place.bz0 * place.bz1
        self.mid, self.end = self.is_mid == 1, self.is_mid == 0
        self.z_mate = self.zz[0][0]
        self.mid_mate = me + 8 * (1 - 2 * place.bz1)

    def copy(self, src, dst, stage, k, mate):
        return remote_copy(src, dst, self.send.at[stage, k], self.recv.at[stage, k], mate)

    def span(self, off, size):
        return pl.ds(pl.multiple_of(off, self.s4), size)

    def down(self, stage, k, off, size, mate, buf=None):
        j = k % self.slots
        buf = self.landing[stage] if buf is None else buf
        return self.copy(self.acc.at[j, self.span(off, size)], buf.at[j, pl.ds(0, size)], stage, k, mate)

    def up(self, stage, k, off, size, mate):
        block = self.gathered.at[k % self.gather_slots, self.span(off, size)]
        return self.copy(block, block, stage, k, mate)

    def add(self, k, off, size, buf):
        step = min(size, 16)
        j = k % self.slots

        def body(i):
            at = pl.ds(pl.multiple_of(off + i * step, step), step)
            self.acc[j, at] = self.acc[j, at] + buf[j, rows(i * step, step)]

        loop(0, size // step, body)

    def stage(self, i, k):
        for kind in self.kinds:
            run = {"x": self.stage_x, "s": self.stage_s, "l": self.stage_l}[kind]
            pl.when(self.is_kind(kind, k))(functools.partial(run, i, k))

    def stage_x(self, i, k):
        (m1, b1), (m2, b2), s2, s4 = *self.xy, self.s2, self.s4
        off1, off2 = b1 * s2, b1 * s2 + b2 * s4
        half = lambda: self.down(0, k, (1 - b1) * s2, s2, m1)
        quarter = lambda: self.down(1, k, off1 + (1 - b2) * s4, s4, m2)
        inward = lambda: self.down(2, k, off2, s4, self.z_mate)
        across = lambda: self.down(3, k, off2, s4, self.mid_mate)
        outward = lambda: self.up(4, k, off2, s4, self.z_mate)
        back4 = lambda: self.up(5, k, off2, s4, m2)
        back2 = lambda: self.up(6, k, off1, s2, m1)
        if i == 1:
            half().start()
        elif i == 2:
            half().wait_recv()
            self.add(k, off1, s2, self.landing[0])
            quarter().start()
        elif i == 3:
            quarter().wait_recv()
            self.add(k, off2, s4, self.landing[1])
            pl.when(self.end)(lambda: inward().start())
        elif i == 4:

            @pl.when(self.mid)
            def _():
                inward().wait_recv()
                self.add(k, off2, s4, self.landing[2])
                across().start()

        elif i == 5:

            @pl.when(self.mid)
            def _():
                across().wait_recv()
                self.finish(k, off2, s4, self.landing[3])
                outward().start()

        elif i == 6:
            pl.when(self.end)(lambda: outward().wait_recv())
            back4().start()
            half().wait_send()
            quarter().wait_send()
            pl.when(self.end)(lambda: inward().wait_send())
            pl.when(self.mid)(lambda: across().wait_send())
        elif i == 7:
            back4().wait_recv()
            back2().start()
        elif i == 8:
            back2().wait_recv()
        elif i == 10:
            pl.when(self.mid)(lambda: outward().wait_send())
            back4().wait_send()
            back2().wait_send()

    def stage_s(self, i, k):
        (m1, b1), (m2, b2), s2, s4 = *self.zz, self.s2, self.s4
        off1, off2 = b1 * s2, b1 * s2 + b2 * s4
        half = lambda: self.down(0, k, (1 - b1) * s2, s2, m1)
        quarter = lambda: self.down(1, k, off1 + (1 - b2) * s4, s4, m2)
        whole_1 = lambda: self.down(2, k, off2, s4, self.xy[0][0])
        whole_2 = lambda: self.down(3, k, off2, s4, self.xy[1][0])
        back4 = lambda: self.up(5, k, off2, s4, m2)
        back2 = lambda: self.up(6, k, off1, s2, m1)
        if i == 1:
            half().start()
        elif i == 2:
            half().wait_recv()
            self.add(k, off1, s2, self.landing[0])
            quarter().start()
        elif i == 3:
            quarter().wait_recv()
            self.add(k, off2, s4, self.landing[1])
            whole_1().start()
        elif i == 4:
            whole_1().wait_recv()
            whole_1().wait_send()
            self.add(k, off2, s4, self.landing[2])
            whole_2().start()
        elif i == 5:
            whole_2().wait_recv()
            self.finish(k, off2, s4, self.landing[3])
        elif i == 6:
            back4().start()
            half().wait_send()
            quarter().wait_send()
            whole_2().wait_send()
        elif i == 7:
            back4().wait_recv()
            back2().start()
        elif i == 8:
            back2().wait_recv()
        elif i == 10:
            back4().wait_send()
            back2().wait_send()

    def stage_l(self, i, k):
        s2, s4 = self.s2, self.s4
        s3 = s2 + s4
        b0, b1 = self.p.bz0, self.p.bz1
        own, side, tip, rest = (2 * b1 + b0) * s4, b1 * s2, 3 * b1 * s4, (1 - b1) * s4
        inward = lambda: self.down(0, k, rest, s3, self.z_mate)
        across = lambda: self.down(1, k, (1 - b1) * s2, s2, self.mid_mate)
        outward = lambda: self.down(2, k, tip, s4, self.z_mate)
        whole_1 = lambda: self.down(3, k, own, s4, self.xy[0][0])
        whole_2 = lambda: self.down(8, k, own, s4, self.xy[1][0], self.landing[4])
        tip_back = lambda: self.up(4, k, tip, s4, self.z_mate)
        side_back = lambda: self.up(5, k, side, s2, self.mid_mate)
        rest_back = lambda: self.up(6, k, rest, s3, self.z_mate)
        if i == 1:
            pl.when(self.end)(lambda: inward().start())
        elif i == 2:

            @pl.when(self.mid)
            def _():
                inward().wait_recv()
                self.add(k, rest, s3, self.landing[0])
                across().start()

        elif i == 3:

            @pl.when(self.mid)
            def _():
                across().wait_recv()
                self.add(k, side, s2, self.landing[1])
                outward().start()

        elif i == 4:

            @pl.when(self.end)
            def _():
                outward().wait_recv()
                self.add(k, own, s4, self.landing[2])

            whole_1().start()
        elif i == 5:
            whole_1().wait_recv()
            whole_1().wait_send()
            pl.when(self.mid)(lambda: outward().wait_send())
            self.add(k, own, s4, self.landing[3])
            whole_2().start()
        elif i == 6:
            whole_2().wait_recv()
            self.finish(k, own, s4, self.landing[4])
            pl.when(self.end)(lambda: tip_back().start())
            whole_2().wait_send()
            pl.when(self.end)(lambda: inward().wait_send())
            pl.when(self.mid)(lambda: across().wait_send())
        elif i == 7:

            @pl.when(self.mid)
            def _():
                tip_back().wait_recv()
                side_back().start()

        elif i == 8:

            @pl.when(self.mid)
            def _():
                side_back().wait_recv()
                rest_back().start()

        elif i == 9:
            pl.when(self.end)(lambda: rest_back().wait_recv())
        elif i == 10:
            pl.when(self.end)(lambda: tip_back().wait_send())

            @pl.when(self.mid)
            def _():
                side_back().wait_send()
                rest_back().wait_send()


def form_next(k, form):
    pl.when(k == 1)(lambda: form(GROUP // 2, GROUP // 2))
    pl.when((k % GROUP == 0) & (k > 0))(lambda: form(k, GROUP))


def run_slots(plan, count, stage, between):
    lags, order = plan

    def slot(t):
        for i in order:
            k = t - lags[i]

            @pl.when((k >= 0) & (k < count))
            def _():
                stage(i, k)

            if i == 1:
                between(t)

    loop(0, count + lags[-1], slot)


def chunk_scratch(slots, gather_slots, part_rows, width, count, dtype):
    def buf(n):
        return pltpu.VMEM((slots, n, width), jnp.float32)

    gathered = pltpu.VMEM((gather_slots, part_rows, width), dtype)

    dma = pltpu.SemaphoreType.DMA
    quarter = part_rows // 4
    return [buf(part_rows), gathered, *(buf(n * quarter) for n in (3, 2, 1, 1, 1)), dma((9, count)), dma((9, count))]


def fold(value):
    return jnp.sum(value.reshape(value.shape[0] // 8, 8, value.shape[1]), axis=0)


def front_kernel(feat_a, feat_b, w_in, t_in, w_mid, t_mid, w_out, t_out, gain1, bias1, gain2, bias2, off_weight, pre1, pre2, xs2, xs1, xs0, dz, grad_emb, vec, *scratch):
    (x_buf, u_buf, w_buf, stats, affine, loss, ea, eb, g_peer) = scratch[:9]
    (x_sem, w_sem, pre_sem, keep_sem, keep_send, keep_recv, ge_sem, e_send, e_recv) = scratch[9:18]
    small_refs = scratch[18 : 18 + SMALL_REFS]
    acc, gathered, *landing, send, recv = scratch[18 + SMALL_REFS :]
    rows_dev, width = feat_a.shape
    wide = w_buf.shape[2]
    tiles = width // wide
    half = width // 2
    part_rows = half // PARTS
    row_count = rows_dev * DEPTH * PLANE
    weights, feats = (w_in, t_in, w_mid, t_mid, w_out, t_out), (feat_a, feat_b)
    place = Place()
    core = place.core
    mine = rows(core * rows_dev, rows_dev)
    place.arrive()
    small = small_sum(place, small_refs)
    payload, total = small.payload, small.total

    def feat(v):
        return pltpu.make_async_copy(feats[v], x_buf.at[v], x_sem.at[v])

    def w_tile(ref, g):
        return pltpu.make_async_copy(ref.at[:, rows((g % tiles) * wide, wide)], w_buf.at[g % W_BUFS], w_sem.at[g % W_BUFS])

    def start_w(g):
        pick(g // tiles, weights, lambda ref: w_tile(ref, g).start())

    feat(0).start()
    w_tile(weights[0], 0).start()
    feat(1).start()
    for g in range(1, W_BUFS - 1):
        start_w(g)
    for j, ref in enumerate((gain1, bias1, gain2, bias2)):
        affine[j] = ref[...]
    feat(0).wait()
    payload[...] = jnp.zeros_like(payload)

    def keep_pre(ref):
        return pltpu.make_async_copy(u_buf.at[0], ref, pre_sem.at[0])

    kept = (xs0, xs1, xs2)

    def keep_x(w):
        here = pltpu.make_async_copy(x_buf.at[0, :, rows(core * half, half)], kept[w].at[mine], keep_sem.at[w])
        there = remote_copy(x_buf.at[0, :, rows((1 - core) * half, half)], kept[w].at[mine], keep_send.at[w], keep_recv.at[w], place.other_core)
        return here, there

    def start_x(w):
        for c in keep_x(w):
            c.start()

    def free_x(w):
        here, there = keep_x(w)
        here.wait()
        there.wait_send()

    def keep_dz(i):
        at = (slice(None), rows(i * wide, wide))
        here = pltpu.make_async_copy(x_buf.at[(0, *at)], dz.at[mine, at[1]], keep_sem.at[3 + i])
        there = remote_copy(x_buf.at[(0, *at)], dz.at[mine, at[1]], keep_send.at[3 + i], keep_recv.at[3 + i], place.other_core)
        return here, there

    def row_loop(body, carry):
        return lax.fori_loop(0, rows_dev // BLOCK, lambda r, c: body(rows(r * BLOCK, BLOCK), c), carry)

    def put_sums(j, i, row, value):
        value = jnp.sum(value, axis=0, keepdims=True)
        for c in range(value.shape[1] // TILE):
            payload[j, i + c, row : row + 1] = value[:, c * TILE : (c + 1) * TILE]

    def product(g):
        job, i = g // tiles, g % tiles
        view = job % 2
        w_tile(w_in, g).wait()
        pl.when(g + W_BUFS - 1 < JOBS * tiles)(lambda: start_w(g + W_BUFS - 1))
        at_cols = rows(i * wide, wide)
        u_buf[view, :, at_cols] = jnp.dot(x_buf[view], w_buf[g % W_BUFS], preferred_element_type=jnp.float32)

        def block(at, sums):
            u = u_buf[view, at, at_cols]
            return sums[0] + fold(u), sums[1] + fold(u * u)

        zero = jnp.zeros((8, wide), jnp.float32)
        for row, value in enumerate(row_loop(block, (zero, zero))):
            put_sums(job, i * (wide // TILE), row, value)

    def begin(job):
        small.begin(job)

        @pl.when(job % 2 == 0)
        def _():
            pick(job // 2, (pre1, pre2), lambda ref: keep_pre(ref).start())

    def norm(job):
        layer, view = job // 2, job % 2
        small.end(job)
        for c in range(PLANE):
            at = slice(c * TILE, (c + 1) * TILE)
            means = total[job, c] / row_count
            stats[job, 0, :, at] = means[0:1]
            stats[job, 1, :, at] = lax.rsqrt(means[1:2] - means[0:1] * means[0:1] + NORM_EPS)

        pl.when(view == 0)(lambda: pick(layer, (0, 1, 2), free_x))

        def hidden(i):
            at_cols = rows(i * wide, wide)
            mean, inv = stats[job, 0, :, at_cols], stats[job, 1, :, at_cols]
            gain, bias = affine[layer * 2, :, at_cols], affine[layer * 2 + 1, :, at_cols]

            def block(at, c):
                n = (u_buf[view, at, at_cols] - mean) * inv
                x_buf[view, at, at_cols] = jnp.maximum(n * gain + bias, 0.0).astype(jnp.bfloat16)
                return c

            row_loop(block, 0)

        def student(i):
            at_cols = rows(i * wide, wide)
            mean, inv = stats[job, 0, :, at_cols], stats[job, 1, :, at_cols]

            def block(at, c):
                n = (u_buf[0, at, at_cols] - mean) * inv
                u_buf[0, at, at_cols] = n
                x_buf[0, at, at_cols] = n.astype(jnp.bfloat16)
                return c

            row_loop(block, 0)

        def student_own(i):
            def block(r, c):
                ea[rows(core * rows_dev + r * BLOCK, BLOCK), rows(i * wide, wide)] = x_buf[0, rows(r * BLOCK, BLOCK), rows(core * half + i * wide, wide)]
                return c

            lax.fori_loop(0, rows_dev // BLOCK, block, 0)

        def teacher(i):
            at_cols = rows(i * wide, wide)
            mean, inv = stats[job, 0, :, at_cols], stats[job, 1, :, at_cols]

            def block(r, c):
                n = (u_buf[1, rows(r * BLOCK, BLOCK), at_cols] - mean) * inv
                eb[rows(core * rows_dev + r * BLOCK, BLOCK), at_cols] = n.astype(jnp.bfloat16)
                return c

            lax.fori_loop(0, rows_dev // BLOCK, block, 0)
            eb_copy(i).start()

        @pl.when(layer < 2)
        def _():
            loop(0, tiles, hidden)

            @pl.when(view == 0)
            def _():
                pick(layer, (1, 2), start_x)
                keep_pre(pre1).wait()

        @pl.when((layer == 2) & (view == 0))
        def _():
            loop(0, tiles, student)
            ea_copy().start()
            loop(0, tiles // 2, student_own)

        @pl.when((layer == 2) & (view == 1))
        def _():
            loop(0, tiles, teacher)

    ea_copy = lambda: remote_copy(x_buf.at[0, :, rows((1 - core) * half, half)], ea.at[mine], e_send.at[0], e_recv.at[0], place.other_core)

    def eb_copy(i):
        block = eb.at[mine, rows(i * wide, wide)]
        return remote_copy(block, block, e_send.at[1 + i], e_recv.at[1 + i], place.other_core)

    def step(g):
        job, i = g // tiles, g % tiles
        view = job % 2
        pl.when(g == tiles)(lambda: feat(1).wait())
        product(g)

        @pl.when(g == 0)
        def _():
            place.all_here()
            start_x(0)

        pl.when((i == 0) & (job > 0))(lambda: small.middle(job - 1))

        @pl.when(i == tiles - 1)
        def _():
            begin(job)
            pl.when(job > 0)(lambda: norm(job - 1))

    loop(0, JOBS * tiles, step)
    small.middle(JOBS - 1)
    norm(JOBS - 1)
    for j, source in enumerate((affine.at[2], affine.at[3], stats.at[2, 0], stats.at[2, 1], affine.at[0], affine.at[1], stats.at[0, 0], stats.at[0, 1])):
        vec[j] = source[...]

    loss[...] = jnp.zeros_like(loss)

    def finish(k, off, size, buf):
        share = jnp.where(front_kind("x", k), 0.5, 0.25)
        at = rows(off, size)
        corr = (acc[k, at] + buf[k]) / row_count
        row = core * half + k * part_rows + off
        diag = (row + lax.broadcasted_iota(jnp.int32, (size, width), 0)) == lax.broadcasted_iota(jnp.int32, (size, width), 1)
        weight = off_weight[0]
        miss = 1.0 - corr
        loss[...] += share * jnp.sum(jnp.where(diag, miss * miss, weight * (corr * corr)), axis=0, keepdims=True)
        gathered[k, at] = jnp.where(diag, -2.0 * miss, 2.0 * weight * corr).astype(jnp.bfloat16)

    chunks = ChunkSum(place, "xsl", front_kind, acc, gathered, landing, send, recv, finish)

    def form(k, group):
        at = rows(k * part_rows, group * part_rows)
        size = min(1024, width)

        def col(c):
            @pl.when(k == 0)
            def _():
                for i in range(size // wide):
                    eb_copy(c * (size // wide) + i).wait_recv()

            cs = rows(c * size, size)
            acc[pl.ds(k, group), :, cs] = contract_rows(ea[:, at], eb[:, cs]).reshape(group, part_rows, size)

        loop(0, width // size, col)

    def swap(k):
        return chunks.copy(gathered.at[k], g_peer.at[k], 7, k, place.other_core)

    def ge_cols(k, side):
        return rows(side * half + k * part_rows, GROUP * part_rows)

    def ge_copy(k, side):
        at = ge_cols(k, side)
        return pltpu.make_async_copy(u_buf.at[1, :, at], grad_emb.at[:, at], ge_sem.at[k // GROUP, side])

    def embed(k, side, g_rows):
        at_cols = ge_cols(k, side)
        grad = contract_cols(eb[mine], g_rows.reshape(GROUP * part_rows, width)) / row_count
        u_buf[1, :, at_cols] = grad
        ge_copy(k, side).start()

        def block(at, sums):
            g = u_buf[1, at, at_cols]
            return sums[0] + fold(g * u_buf[0, at, at_cols]), sums[1] + fold(g)

        zero = jnp.zeros((8, GROUP * part_rows), jnp.float32)
        for row, value in enumerate(row_loop(block, (zero, zero))):
            payload[JOBS, (side * half + k * part_rows) // TILE, row : row + 1] = jnp.sum(value, axis=0, keepdims=True)

    def stage(i, k):
        if i == 0:
            form_next(k, form)
            return
        chunks.stage(i, k)
        if i == 8:
            pl.when(jnp.logical_not(front_kind("l", k)))(lambda: swap(k).start())
        if i == 9:
            pl.when(front_kind("l", k))(lambda: swap(k).start())

            @pl.when(k % GROUP == GROUP - 1)
            def _():
                embed(k - GROUP + 1, core, gathered[pl.ds(k - GROUP + 1, GROUP)])

        if i == 10:
            swap(k).wait_recv()
            swap(k).wait_send()

            @pl.when(k % GROUP == GROUP - 1)
            def _():
                embed(k - GROUP + 1, 1 - core, g_peer[pl.ds(k - GROUP + 1, GROUP)])

    ea_copy().wait_recv()
    form(0, GROUP // 2)
    run_slots(FRONT_PLAN, PARTS, stage, lambda t: None)
    small.begin(JOBS)
    for c in range(PLANE):
        payload[JOBS + 1, c, 0:1] = loss[:, c * TILE : (c + 1) * TILE]
    small.begin(JOBS + 1)
    ea_copy().wait_send()
    for i in range(tiles):
        eb_copy(i).wait_send()
    small.middle(JOBS)
    small.middle(JOBS + 1)
    for k in range(0, PARTS, GROUP):
        for side in range(2):
            ge_copy(k, side).wait()
    small.end(JOBS)

    def dz_tile(i):
        at_cols = rows(i * wide, wide)
        sums = jnp.concatenate([total[JOBS, i * (wide // TILE) + c] for c in range(wide // TILE)], axis=1) / row_count
        mean_gn, mean_g = sums[0:1], sums[1:2]
        inv = stats[JOBS - 2, 1, :, at_cols]

        def block(at, c):
            value = (u_buf[1, at, at_cols] - mean_g - u_buf[0, at, at_cols] * mean_gn) * inv
            x_buf[0, at, at_cols] = value.astype(jnp.bfloat16)
            return c

        row_loop(block, 0)
        for c in keep_dz(i):
            c.start()

    loop(0, tiles, dz_tile)
    small.end(JOBS + 1)
    for c in range(PLANE):
        vec[8, :, c * TILE : (c + 1) * TILE] = total[JOBS + 1, c, 0:1]
    for w in range(3):
        keep_x(w)[1].wait_recv()
    for i in range(tiles):
        here, there = keep_dz(i)
        here.wait()
        there.wait()


def front(feat_a, feat_b, weights, affine, off_weight):
    rows_dev, width = feat_a.shape
    half = width // 2
    part_rows = half // PARTS
    any_spec = pl.BlockSpec(memory_space=pl.ANY)
    vmem_spec = pl.BlockSpec(memory_space=pltpu.VMEM)
    wide_f32 = jax.ShapeDtypeStruct((rows_dev, width), jnp.float32)
    kept = jax.ShapeDtypeStruct((2 * rows_dev, half), jnp.bfloat16)
    both_dz = jax.ShapeDtypeStruct((2 * rows_dev, width), jnp.bfloat16)
    keeps = 3 + width // WIDE
    dma = pltpu.SemaphoreType.DMA
    return pl.pallas_call(
        front_kernel,
        name="front",
        out_shape=[wide_f32, wide_f32, kept, kept, kept, both_dz, wide_f32]
        + [jax.ShapeDtypeStruct((9, 1, width), jnp.float32)],
        in_specs=[any_spec] * 8 + [vmem_spec] * 4 + [pl.BlockSpec(memory_space=pltpu.SMEM)],
        out_specs=[any_spec] * 7 + [vmem_spec],
        scratch_shapes=[
            pltpu.VMEM((2, rows_dev, width), jnp.bfloat16),
            pltpu.VMEM((2, rows_dev, width), jnp.float32),
            pltpu.VMEM((W_BUFS, width, WIDE), jnp.bfloat16),
            pltpu.VMEM((JOBS, 2, 1, width), jnp.float32),
            pltpu.VMEM((4, 1, width), jnp.float32),
            pltpu.VMEM((1, width), jnp.float32),
            pltpu.VMEM((2 * rows_dev, half), jnp.bfloat16),
            pltpu.VMEM((2 * rows_dev, width), jnp.bfloat16),
            pltpu.VMEM((PARTS, part_rows, width), jnp.bfloat16),
            dma((2,)),
            dma((W_BUFS,)),
            dma((1,)),
            dma((keeps,)),
            dma((keeps,)),
            dma((keeps,)),
            dma((PARTS // GROUP, 2)),
            dma((1 + width // WIDE,)),
            dma((1 + width // WIDE,)),
        ]
        + small_scratch(JOBS + 2)
        + chunk_scratch(PARTS, PARTS, part_rows, width, PARTS, jnp.bfloat16),
        compiler_params=pltpu.CompilerParams(collective_id=0, has_side_effects=True, vmem_limit_bytes=VMEM_BYTES),
    )(feat_a, feat_b, *weights, *affine, off_weight)


def back_kernel(dz_hbm, x2, x1, x0, w_out, w_mid, u2, u1, vec, out2, out1, out0, sums_out, *scratch):
    (dy, xs, w_buf, u_buf, dpre) = scratch[:5]
    (in_sem, tile_sem, peer_send, peer_recv, store_sem) = scratch[5:10]
    small_refs = scratch[10 : 10 + SMALL_REFS]
    acc, gathered, *landing, send, recv = scratch[10 + SMALL_REFS :]
    rows_dev, width = dpre.shape
    wide = w_buf.shape[1]
    tiles = width // wide
    row_count = rows_dev * DEPTH * PLANE
    half = width // 2
    part_rows = half // PARTS
    count = MATS * PARTS
    mats_in, outs, weights, pres = (x2, x1, x0), (out2, out1, out0), (w_out, w_mid), (u2, u1)
    place = Place()
    core, other_core = place.core, place.other_core
    mine = rows(core * rows_dev, rows_dev)
    place.arrive()
    small = small_sum(place, small_refs)
    payload, sums = small.payload, small.total

    def load_x(w):
        return pltpu.make_async_copy(mats_in[w], xs.at[w % 2], in_sem.at[w])

    def peer_dy(w):
        block = dy.at[w % 2, mine]
        return remote_copy(block, block, peer_send.at[w], peer_recv.at[w], other_core)

    def w_tile(ref, i):
        return pltpu.make_async_copy(ref.at[rows(i * wide, wide)], w_buf.at[i % 2], tile_sem.at[0, i % 2])

    def u_tile(ref, i):
        return pltpu.make_async_copy(ref.at[:, rows(i * wide, wide)], u_buf.at[i % 2], tile_sem.at[1, i % 2])

    def start_w(layer, i):
        pick(layer, weights, lambda ref: w_tile(ref, i).start())

    def start_u(layer, i):
        pick(layer, pres, lambda ref: u_tile(ref, i).start())

    size = min(1024, width)

    def load_dz(c):
        return pltpu.make_async_copy(dz_hbm.at[:, rows(c * size, size)], dy.at[0, :, rows(c * size, size)], in_sem.at[MATS + c])

    load_x(0).start()
    for c in range(width // size):
        load_dz(c).start()
    w_tile(weights[0], 0).start()
    u_tile(pres[0], 0).start()
    load_x(1).start()
    payload[...] = jnp.zeros_like(payload)

    def row_loop(body, carry):
        return lax.fori_loop(0, rows_dev // BLOCK, body, carry)

    def chain_tile(layer, i):
        w_tile(w_out, i).wait()
        u_tile(u2, i).wait()

        @pl.when(i + 1 < tiles)
        def _():
            start_w(layer, i + 1)
            start_u(layer, i + 1)

        at_cols = rows(i * wide, wide)
        dpre[:, at_cols] = contract_cols(dy[layer, mine], w_buf[i % 2])
        gain, bias, mean, inv = (vec[layer * 4 + j, :, at_cols] for j in range(4))

        def block(r, carry):
            at = rows(r * BLOCK, BLOCK)
            n = (u_buf[i % 2, at] - mean) * inv
            g = jnp.where(n * gain + bias > 0.0, dpre[at, at_cols], 0.0)
            dpre[at, at_cols] = g
            return carry[0] + fold(g * n), carry[1] + fold(g)

        zero = jnp.zeros((8, wide), jnp.float32)
        for row, value in enumerate(row_loop(block, (zero, zero))):
            value = jnp.sum(value, axis=0, keepdims=True)
            for c in range(wide // TILE):
                payload[layer, i * (wide // TILE) + c, row : row + 1] = value[:, c * TILE : (c + 1) * TILE]

    def du_tile(layer, i):
        u_tile(u2, i).wait()
        pl.when(i + 1 < tiles)(lambda: start_u(layer, i + 1))
        at_cols = rows(i * wide, wide)
        gain, mean, inv = (vec[layer * 4 + j, :, at_cols] for j in (0, 2, 3))
        means = jnp.concatenate([sums[layer, i * (wide // TILE) + c] for c in range(wide // TILE)], axis=1) / row_count
        mean_gn, mean_g = means[0:1], means[1:2]
        scale = gain * inv

        def block(r, c):
            at = rows(r * BLOCK, BLOCK)
            n = (u_buf[i % 2, at] - mean) * inv
            value = (dpre[at, at_cols] - mean_g - n * mean_gn) * scale
            dy[1 - layer, rows(core * rows_dev + r * BLOCK, BLOCK), at_cols] = value.astype(jnp.bfloat16)
            return c

        row_loop(block, 0)

    def finish(k, off, size, buf):
        j = k % ACC_SLOTS
        gathered[k % GATHER_SLOTS, rows(off, size)] = acc[j, rows(off, size)] + buf[j]

    chunks = ChunkSum(place, "xl", back_kind, acc, gathered, landing, send, recv, finish)

    def form(k, group):
        w, j = k // PARTS, k % ACC_SLOTS

        @pl.when(k % PARTS == 0)
        def _():
            pltpu.make_async_copy(xs.at[w % 2], xs.at[w % 2], in_sem.at[w]).wait()
            pl.when(w > 0)(lambda: peer_dy(w).wait_recv())

        at = rows((k % PARTS) * part_rows, group * part_rows)

        def col(c):
            pl.when(k == 0)(lambda: load_dz(c).wait())
            cs = rows(c * size, size)
            acc[pl.ds(j, group), :, cs] = contract_rows(xs[w % 2, :, at], dy[w % 2, :, cs]).reshape(group, part_rows, size)

        loop(0, width // size, col)

    def out_rows(k, side):
        return pl.ds(pl.multiple_of(side * half + (k % PARTS) * part_rows, part_rows), part_rows)

    def last_copy(out, k, side):
        return chunks.copy(gathered.at[k % GATHER_SLOTS], out.at[out_rows(k, side)], 7, k, other_core)

    def store_copy(out, k):
        return pltpu.make_async_copy(gathered.at[k % GATHER_SLOTS], out.at[out_rows(k, core)], store_sem.at[k])

    def stage(i, k):
        if i == 0:
            form_next(k, form)
            return
        chunks.stage(i, k)
        def emit(out):
            last_copy(out, k, core).start()
            store_copy(out, k).start()

        if i == 8:
            pl.when(back_kind("x", k))(lambda: pick(k // PARTS, outs, emit))
        if i == 9:
            pl.when(back_kind("l", k))(lambda: pick(k // PARTS, outs, emit))
        if i == 10:

            def close(out):
                last_copy(out, k, 1 - core).wait_recv()
                store_copy(out, k).wait()
                last_copy(out, k, core).wait_send()

            pick(k // PARTS, outs, close)

    def layer_work(t):
        layer = t // LAYER_SLOTS
        at = t - LAYER_SLOTS * layer
        first_du = 2 * tiles + 3
        pl.when((at < 2 * tiles) & (at % 2 == 1))(lambda: chain_tile(layer, at // 2))
        pl.when(at == 2 * tiles)(lambda: small.begin(layer))
        pl.when(at == 2 * tiles + 1)(lambda: small.middle(layer))

        pl.when(at == 2 * tiles + 2)(lambda: start_u(layer, 0))

        pl.when(at == first_du)(lambda: small.end(layer))
        pl.when(at >= first_du)(lambda: du_tile(layer, at - first_du))

        @pl.when(at == LAYER_SLOTS - 1)
        def _():
            peer_dy(layer + 1).start()

            @pl.when(layer == 0)
            def _():
                w_tile(weights[1], 0).start()
                u_tile(pres[1], 0).start()

            pl.when(layer == 1)(lambda: load_x(2).start())

    form(0, GROUP // 2)
    place.all_here()
    run_slots(BACK_PLAN, count, stage, lambda t: pl.when(t < 2 * LAYER_SLOTS)(lambda: layer_work(t)))
    for w in (1, 2):
        peer_dy(w).wait_send()
    for c in range(PLANE):
        for row in range(4):
            sums_out[row : row + 1, c * TILE : (c + 1) * TILE] = sums[row // 2, c, row % 2 : row % 2 + 1]
    sums_out[4:5] = jnp.full((1, width), jnp.sum(vec[8]))


def backward(grad_z, x2, x1, x0, w_out, w_mid, u2, u1, vec):
    rows_dev, width = u2.shape
    part_rows = width // 2 // PARTS
    count = MATS * PARTS
    any_spec = pl.BlockSpec(memory_space=pl.ANY)
    vmem_spec = pl.BlockSpec(memory_space=pltpu.VMEM)
    mat = jax.ShapeDtypeStruct((width, width), jnp.float32)
    dma = pltpu.SemaphoreType.DMA
    return pl.pallas_call(
        back_kernel,
        name="backward",
        out_shape=[mat, mat, mat, jax.ShapeDtypeStruct((5, width), jnp.float32)],
        in_specs=[any_spec] * 8 + [vmem_spec],
        out_specs=[any_spec] * 3 + [vmem_spec],
        scratch_shapes=[
            pltpu.VMEM((2, 2 * rows_dev, width), jnp.bfloat16),
            pltpu.VMEM((2, 2 * rows_dev, width // 2), jnp.bfloat16),
            pltpu.VMEM((2, WIDE, width), jnp.bfloat16),
            pltpu.VMEM((2, rows_dev, WIDE), jnp.float32),
            pltpu.VMEM((rows_dev, width), jnp.float32),
            dma((MATS + 2,)),
            dma((2, 2)),
            dma((MATS,)),
            dma((MATS,)),
            dma((count,)),
        ]
        + small_scratch(2)
        + chunk_scratch(ACC_SLOTS, GATHER_SLOTS, part_rows, width, count, jnp.float32),
        compiler_params=pltpu.CompilerParams(collective_id=1, has_side_effects=True, vmem_limit_bytes=VMEM_BYTES),
    )(grad_z, x2, x1, x0, w_out, w_mid, u2, u1, vec)


def copy_kernel(*refs):
    pairs = (len(refs) - 5 - 6) // 2
    ins, small, outs, small_outs = refs[:pairs], refs[pairs], refs[pairs + 1 : 2 * pairs + 1], refs[2 * pairs + 1 : -5]
    buf, small_buf, in_sem, out_sem, small_sem = refs[-5:]
    blocks = [(i, r) for i in range(pairs) for r in range(0, ins[i].shape[0], COPY_ROWS)]

    def read(b):
        i, r = blocks[b]
        return pltpu.make_async_copy(ins[i].at[pl.ds(r, COPY_ROWS)], buf.at[b % COPY_BUFS], in_sem.at[b % COPY_BUFS])

    def write(b):
        i, r = blocks[b]
        return pltpu.make_async_copy(buf.at[b % COPY_BUFS], outs[i].at[pl.ds(r, COPY_ROWS)], out_sem.at[b % COPY_BUFS])

    ahead = COPY_BUFS // 2
    for b in range(min(ahead, len(blocks))):
        read(b).start()
    pltpu.make_async_copy(small, small_buf, small_sem.at[4]).start()

    def small_write(row):
        return pltpu.make_async_copy(small_buf.at[pl.ds(row, 1)], small_outs[row], small_sem.at[row])

    for b in range(len(blocks)):
        if b + ahead < len(blocks):
            if b + ahead >= COPY_BUFS:
                write(b + ahead - COPY_BUFS).wait()
            read(b + ahead).start()
        read(b).wait()
        write(b).start()
        if b == 0:
            pltpu.make_async_copy(small, small_buf, small_sem.at[4]).wait()
            small_outs[4][...] = small_buf[4:5, :1]
            for row in range(4):
                small_write(row).start()
    for row in range(4):
        small_write(row).wait()
    for b in range(max(0, len(blocks) - COPY_BUFS), len(blocks)):
        write(b).wait()


def copy_out(arrays, small):
    any_spec = pl.BlockSpec(memory_space=pl.ANY)
    vmem_spec = pl.BlockSpec(memory_space=pltpu.VMEM)
    dma = pltpu.SemaphoreType.DMA
    width = small.shape[1]
    row = jax.ShapeDtypeStruct((1, width), jnp.float32)
    return pl.pallas_call(
        copy_kernel,
        name="copy_out",
        out_shape=[jax.ShapeDtypeStruct(a.shape, a.dtype) for a in arrays] + [row] * 4 + [jax.ShapeDtypeStruct((1, 1), jnp.float32)],
        in_specs=[any_spec] * (len(arrays) + 1),
        out_specs=[any_spec] * (len(arrays) + 4) + [vmem_spec],
        scratch_shapes=[
            pltpu.VMEM((COPY_BUFS, COPY_ROWS, width), jnp.float32),
            pltpu.VMEM(small.shape, jnp.float32),
            dma((COPY_BUFS,)),
            dma((COPY_BUFS,)),
            dma((5,)),
        ],
        compiler_params=pltpu.CompilerParams(vmem_limit_bytes=VMEM_BYTES),
    )(*arrays, small)


def solution(mesh):
    row_part = P(DATA_AXIS, None)
    replicated = P()

    def local_step(feat_a, feat_b, w_in, w_mid, w_out, t_in, t_mid, t_out, gain_1, bias_1, gain_2, bias_2, off_weight):
        affine = [v.reshape(1, -1) for v in (gain_1, bias_1, gain_2, bias_2)]
        pre_1, pre_2, xs_2, xs_1, xs_0, grad_z, grad_emb, vec = front(
            feat_a, feat_b, (w_in, t_in, w_mid, t_mid, w_out, t_out), affine, off_weight.reshape(1)
        )
        grad_w_out, grad_w_mid, grad_w_in, sums = backward(grad_z, xs_2, xs_1, xs_0, w_out, w_mid, pre_2, pre_1, vec)
        (grad_emb, grad_w_out, grad_w_mid, grad_w_in, gain_2, bias_2, gain_1, bias_1, loss) = copy_out((grad_emb, grad_w_out, grad_w_mid, grad_w_in), sums)
        gain_1, bias_1, gain_2, bias_2 = (v.reshape(-1) for v in (gain_1, bias_1, gain_2, bias_2))
        return (loss.reshape(()), grad_emb, grad_w_in, grad_w_mid, grad_w_out, gain_1, bias_1, gain_2, bias_2)

    return jax.shard_map(local_step, mesh=mesh, in_specs=(row_part, row_part) + (replicated,) * 11, out_specs=(replicated, row_part) + (replicated,) * 7, check_vma=False)
```

```python
import functools

import jax
import jax.numpy as jnp
from jax import lax
from jax.experimental import pallas as pl
from jax.experimental.pallas import tpu as pltpu
from jax.sharding import PartitionSpec as P

NORM_EPS = 1e-5
DATA_AXIS = "data"
MESH = pl.DeviceIdType.MESH
VMEM_BYTES = 67_043_328
PLANE = 8
DEPTH = 4
TILE = 256
WIDE = 512
BLOCK = 128
SUM_ROWS = 2
PARTS = 16
GROUP = 4
MATS = 3
ACC_SLOTS = 16
GATHER_SLOTS = 14
BACK_VMEM = 49_800_000
COPY_VMEM = 40 * 1024 * 1024
JOBS = 6
W_BUFS = 3
LAYER_SLOTS = 15
COPY_ROWS = 256
COPY_BUFS = 16
FRONT_PLAN = ((0, 0, 3, 5, 7, 9, 12, 13, 16, 17, 18), (0, 6, 3, 4, 9, 10, 8, 5, 2, 7, 1))
BACK_PLAN = ((0, 0, 3, 5, 7, 8, 9, 11, 14, 17, 19), (0, 4, 8, 7, 10, 1, 2, 3, 5, 6, 9))


def front_kind(kind, k):
    s, l = (k % 5 == 2) & (k > 2), k == 2
    return {"s": s, "l": l, "x": (k % 5 != 2)}[kind]


def back_kind(kind, k):
    l = ((k % 5 == 2) & (k < 43)) | ((k % 5 == 0) & (k >= 10) & (k < 36))
    return l if kind == "l" else jnp.logical_not(l)


def contract_rows(left_op, right_op):
    return lax.dot_general(left_op, right_op, (((0,), (0,)), ((), ())), preferred_element_type=jnp.float32)


def contract_cols(left_op, right_op):
    return lax.dot_general(left_op, right_op, (((1,), (1,)), ((), ())), preferred_element_type=jnp.float32)


def rows(off, size):
    return pl.ds(pl.multiple_of(off, size), size)


def pick(index, choices, what):
    for i, c in enumerate(choices):
        pl.when(index == i)(functools.partial(what, c))


def loop(lo, hi, body):
    def step(i, carry):
        body(i)
        return carry

    lax.fori_loop(lo, hi, step, 0)


def remote_copy(src, dst, send, recv, mate):
    return pltpu.make_async_remote_copy(src, dst, send, recv, device_id=(mate,), device_id_type=MESH)


class Place:
    def __init__(self):
        me = lax.axis_index(DATA_AXIS)
        self.me = me
        self.pos, self.plane = me % PLANE, me // PLANE
        self.core, self.bx, self.by, self.bz0, self.bz1 = me % 2, (me // 2) % 2, (me // 4) % 2, (me // 8) % 2, (me // 16) % 2
        self.other_core = me + 1 - 2 * self.core
        self.mates = [(self.pos + d) % PLANE for d in range(1, PLANE)]
        self.levels = [(self.plane + d) % DEPTH for d in range(1, DEPTH)]

    def peers(self):
        return [self.plane * PLANE + m for m in self.mates] + [lv * PLANE + self.pos for lv in self.levels]

    def arrive(self):
        sem = pltpu.get_barrier_semaphore()
        for peer in self.peers():
            pl.semaphore_signal(sem, inc=1, device_id=(peer,), device_id_type=MESH)

    def all_here(self):
        pl.semaphore_wait(pltpu.get_barrier_semaphore(), PLANE + DEPTH - 2)


class SmallSum:
    def __init__(self, place, payload, total, depth_buf, line_sum, plane_buf, sems):
        self.p, self.payload, self.total = place, payload, total
        self.depth_buf, self.line_sum, self.plane_buf, self.sems = depth_buf, line_sum, plane_buf, sems

    def along(self, j, lv, slot):
        s, r = self.sems[0], self.sems[1]
        return remote_copy(self.payload.at[j], self.depth_buf.at[j, slot], s.at[j, lv], r.at[j, slot], lv * PLANE + self.p.pos)

    def within(self, j, m, slot):
        s, r = self.sems[2], self.sems[3]
        return remote_copy(self.line_sum.at[j], self.plane_buf.at[j, slot], s.at[j, m], r.at[j, slot], self.p.plane * PLANE + m)

    def begin(self, j):
        for lv in self.p.levels:
            self.along(j, lv, self.p.plane).start()
        self.depth_buf[j, self.p.plane] = self.payload[j]

    def middle(self, j):
        for lv in self.p.levels:
            self.along(j, lv, lv).wait_recv()
        total = self.depth_buf[j, 0]
        for i in range(1, DEPTH):
            total = total + self.depth_buf[j, i]
        self.line_sum[j] = total
        for m in self.p.mates:
            self.within(j, m, self.p.pos).start()
        self.plane_buf[j, self.p.pos] = total

    def end(self, j):
        for m in self.p.mates:
            self.within(j, m, m).wait_recv()
        total = self.plane_buf[j, 0]
        for i in range(1, PLANE):
            total = total + self.plane_buf[j, i]
        self.total[j] = total
        for lv in self.p.levels:
            self.along(j, lv, self.p.plane).wait_send()
        for m in self.p.mates:
            self.within(j, m, self.p.pos).wait_send()


def small_scratch(count):
    def buf(*lead):
        return pltpu.VMEM((count, *lead, PLANE, SUM_ROWS, TILE), jnp.float32)

    return [buf(), buf(), buf(DEPTH), buf(), buf(PLANE)] + [pltpu.SemaphoreType.DMA((count, n)) for n in (DEPTH, DEPTH, PLANE, PLANE)]


SMALL_REFS = 9


def small_sum(place, refs):
    return SmallSum(place, *refs[:5], refs[5:])


class Homed:
    def __init__(self, homes, make):
        self.homes, self.make = homes, make

    def do(self, what):
        for when, home in self.homes:
            run = lambda home=home: getattr(self.make(home), what)()
            run() if when is None else pl.when(when)(run)

    def start(self):
        self.do("start")

    def wait_recv(self):
        self.do("wait_recv")

    def wait_send(self):
        self.do("wait_send")


class ChunkSum:
    def __init__(self, place, kinds, is_kind, acc, homes, landing, send, recv, finish):
        self.p, self.kinds, self.is_kind, self.slots, self.homes = place, kinds, is_kind, acc.shape[0], homes
        self.acc, self.landing, self.send, self.recv, self.finish = acc, landing, send, recv, finish
        self.size = acc.shape[1]
        self.s2, self.s4 = self.size // 2, self.size // 4
        core, bx, by, me = place.core, place.bx, place.by, place.me
        first, second = core * by + (1 - core) * bx, core * bx + (1 - core) * by
        self.xy = ((me + (2 + 2 * core) * (1 - 2 * first), first), (me + (4 - 2 * core) * (1 - 2 * second), second))
        self.zz = ((me + 8 * (1 - 2 * place.bz0), place.bz0), (me + 16 * (1 - 2 * place.bz1), place.bz1))
        self.is_mid = place.bz0 + place.bz1 - 2 * place.bz0 * place.bz1
        self.mid, self.end = self.is_mid == 1, self.is_mid == 0
        self.z_mate = self.zz[0][0]
        self.mid_mate = me + 8 * (1 - 2 * place.bz1)

    def copy(self, src, dst, stage, k, mate):
        return remote_copy(src, dst, self.send.at[stage, k], self.recv.at[stage, k], mate)

    def span(self, off, size):
        return pl.ds(pl.multiple_of(off, self.s4), size)

    def down(self, stage, k, off, size, mate, buf=None):
        j = k % self.slots
        buf = self.landing[stage] if buf is None else buf
        return self.copy(self.acc.at[j, self.span(off, size)], buf.at[j, pl.ds(0, size)], stage, k, mate)

    def up(self, stage, k, off, size, mate):
        return Homed(self.homes(k), lambda home: self.copy(home(off, size), home(off, size), stage, k, mate))

    def add(self, k, off, size, buf):
        step = min(size, 16)
        j = k % self.slots

        def body(i):
            at = pl.ds(pl.multiple_of(off + i * step, step), step)
            self.acc[j, at] = self.acc[j, at] + buf[j, rows(i * step, step)]

        loop(0, size // step, body)

    def stage(self, i, k):
        for kind in self.kinds:
            run = {"x": self.stage_x, "s": self.stage_s, "l": self.stage_l}[kind]
            pl.when(self.is_kind(kind, k))(functools.partial(run, i, k))

    def stage_x(self, i, k):
        (m1, b1), (m2, b2), s2, s4 = *self.xy, self.s2, self.s4
        off1, off2 = b1 * s2, b1 * s2 + b2 * s4
        half = lambda: self.down(0, k, (1 - b1) * s2, s2, m1)
        quarter = lambda: self.down(1, k, off1 + (1 - b2) * s4, s4, m2)
        inward = lambda: self.down(2, k, off2, s4, self.z_mate)
        across = lambda: self.down(3, k, off2, s4, self.mid_mate)
        outward = lambda: self.up(4, k, off2, s4, self.z_mate)
        back4 = lambda: self.up(5, k, off2, s4, m2)
        back2 = lambda: self.up(6, k, off1, s2, m1)
        if i == 1:
            half().start()
        elif i == 2:
            half().wait_recv()
            self.add(k, off1, s2, self.landing[0])
            quarter().start()
        elif i == 3:
            quarter().wait_recv()
            self.add(k, off2, s4, self.landing[1])
            pl.when(self.end)(lambda: inward().start())
        elif i == 4:

            @pl.when(self.mid)
            def _():
                inward().wait_recv()
                self.add(k, off2, s4, self.landing[2])
                across().start()

        elif i == 5:

            @pl.when(self.mid)
            def _():
                across().wait_recv()
                self.finish(k, off2, s4, self.landing[3])
                outward().start()

        elif i == 6:
            pl.when(self.end)(lambda: outward().wait_recv())
            back4().start()
            half().wait_send()
            quarter().wait_send()
            pl.when(self.end)(lambda: inward().wait_send())
            pl.when(self.mid)(lambda: across().wait_send())
        elif i == 7:
            back4().wait_recv()
            back2().start()
        elif i == 8:
            back2().wait_recv()
        elif i == 10:
            pl.when(self.mid)(lambda: outward().wait_send())
            back4().wait_send()
            back2().wait_send()

    def stage_s(self, i, k):
        (m1, b1), (m2, b2), s2, s4 = *self.zz, self.s2, self.s4
        off1, off2 = b1 * s2, b1 * s2 + b2 * s4
        half = lambda: self.down(0, k, (1 - b1) * s2, s2, m1)
        quarter = lambda: self.down(1, k, off1 + (1 - b2) * s4, s4, m2)
        whole_1 = lambda: self.down(2, k, off2, s4, self.xy[0][0])
        whole_2 = lambda: self.down(3, k, off2, s4, self.xy[1][0])
        back4 = lambda: self.up(5, k, off2, s4, m2)
        back2 = lambda: self.up(6, k, off1, s2, m1)
        if i == 1:
            half().start()
        elif i == 2:
            half().wait_recv()
            self.add(k, off1, s2, self.landing[0])
            quarter().start()
        elif i == 3:
            quarter().wait_recv()
            self.add(k, off2, s4, self.landing[1])
            whole_1().start()
        elif i == 4:
            whole_1().wait_recv()
            whole_1().wait_send()
            self.add(k, off2, s4, self.landing[2])
            whole_2().start()
        elif i == 5:
            whole_2().wait_recv()
            self.finish(k, off2, s4, self.landing[3])
        elif i == 6:
            back4().start()
            half().wait_send()
            quarter().wait_send()
            whole_2().wait_send()
        elif i == 7:
            back4().wait_recv()
            back2().start()
        elif i == 8:
            back2().wait_recv()
        elif i == 10:
            back4().wait_send()
            back2().wait_send()

    def stage_l(self, i, k):
        s2, s4 = self.s2, self.s4
        s3 = s2 + s4
        b0, b1 = self.p.bz0, self.p.bz1
        own, side, tip, rest = (2 * b1 + b0) * s4, b1 * s2, 3 * b1 * s4, (1 - b1) * s4
        inward = lambda: self.down(0, k, rest, s3, self.z_mate)
        across = lambda: self.down(1, k, (1 - b1) * s2, s2, self.mid_mate)
        outward = lambda: self.down(2, k, tip, s4, self.z_mate)
        whole_1 = lambda: self.down(3, k, own, s4, self.xy[0][0])
        whole_2 = lambda: self.down(8, k, own, s4, self.xy[1][0], self.landing[4])
        tip_back = lambda: self.up(4, k, tip, s4, self.z_mate)
        side_back = lambda: self.up(5, k, side, s2, self.mid_mate)
        rest_back = lambda: self.up(6, k, rest, s3, self.z_mate)
        if i == 1:
            pl.when(self.end)(lambda: inward().start())
        elif i == 2:

            @pl.when(self.mid)
            def _():
                inward().wait_recv()
                self.add(k, rest, s3, self.landing[0])
                across().start()

        elif i == 3:

            @pl.when(self.mid)
            def _():
                across().wait_recv()
                self.add(k, side, s2, self.landing[1])
                outward().start()

        elif i == 4:

            @pl.when(self.end)
            def _():
                outward().wait_recv()
                self.add(k, own, s4, self.landing[2])

            whole_1().start()
        elif i == 5:
            whole_1().wait_recv()
            whole_1().wait_send()
            pl.when(self.mid)(lambda: outward().wait_send())
            self.add(k, own, s4, self.landing[3])
            whole_2().start()
        elif i == 6:
            whole_2().wait_recv()
            self.finish(k, own, s4, self.landing[4])
            pl.when(self.end)(lambda: tip_back().start())
            whole_2().wait_send()
            pl.when(self.end)(lambda: inward().wait_send())
            pl.when(self.mid)(lambda: across().wait_send())
        elif i == 7:

            @pl.when(self.mid)
            def _():
                tip_back().wait_recv()
                side_back().start()

        elif i == 8:

            @pl.when(self.mid)
            def _():
                side_back().wait_recv()
                rest_back().start()

        elif i == 9:
            pl.when(self.end)(lambda: rest_back().wait_recv())
        elif i == 10:
            pl.when(self.end)(lambda: tip_back().wait_send())

            @pl.when(self.mid)
            def _():
                side_back().wait_send()
                rest_back().wait_send()


def form_next(k, form):
    pl.when(k == 1)(lambda: form(GROUP // 2, GROUP // 2))
    pl.when((k % GROUP == 0) & (k > 0))(lambda: form(k, GROUP))


def run_slots(plan, count, stage, between):
    lags, order = plan

    def slot(t):
        for i in order:
            k = t - lags[i]

            @pl.when((k >= 0) & (k < count))
            def _():
                stage(i, k)

            if i == 1:
                between(t)

    loop(0, count + lags[-1], slot)


def chunk_scratch(slots, gather_slots, part_rows, width, count, dtype):
    def buf(n):
        return pltpu.VMEM((slots, n, width), jnp.float32)

    gathered = pltpu.VMEM((gather_slots, part_rows, width), dtype)

    dma = pltpu.SemaphoreType.DMA
    quarter = part_rows // 4
    return [buf(part_rows), gathered, *(buf(n * quarter) for n in (3, 2, 1, 1, 1)), dma((9, count)), dma((9, count))]


def fold(value):
    return jnp.sum(value.reshape(value.shape[0] // 8, 8, value.shape[1]), axis=0)


def front_kernel(feat_a, feat_b, w_in, t_in, w_mid, t_mid, w_out, t_out, gain1, bias1, gain2, bias2, off_weight, pre1, pre2, xs2, xs1, xs0, dz, grad_emb, vec, *scratch):
    (x_buf, u_buf, w_buf, stats, affine, loss, ea, eb, g_peer) = scratch[:9]
    (x_sem, w_sem, pre_sem, keep_sem, keep_send, keep_recv, ge_sem, e_send, e_recv) = scratch[9:18]
    small_refs = scratch[18 : 18 + SMALL_REFS]
    acc, gathered, *landing, send, recv = scratch[18 + SMALL_REFS :]
    rows_dev, width = feat_a.shape
    wide = w_buf.shape[2]
    tiles = width // wide
    half = width // 2
    part_rows = half // PARTS
    row_count = rows_dev * DEPTH * PLANE
    weights, feats = (w_in, t_in, w_mid, t_mid, w_out, t_out), (feat_a, feat_b)
    place = Place()
    core = place.core
    mine = rows(core * rows_dev, rows_dev)
    place.arrive()
    small = small_sum(place, small_refs)
    payload, total = small.payload, small.total

    def feat(v):
        return pltpu.make_async_copy(feats[v], x_buf.at[v], x_sem.at[v])

    def w_tile(ref, g):
        return pltpu.make_async_copy(ref.at[:, rows((g % tiles) * wide, wide)], w_buf.at[g % W_BUFS], w_sem.at[g % W_BUFS])

    def start_w(g):
        pick(g // tiles, weights, lambda ref: w_tile(ref, g).start())

    feat(0).start()
    w_tile(weights[0], 0).start()
    feat(1).start()
    for g in range(1, W_BUFS - 1):
        start_w(g)
    for j, ref in enumerate((gain1, bias1, gain2, bias2)):
        affine[j] = ref[...]
    feat(0).wait()
    payload[...] = jnp.zeros_like(payload)

    def keep_pre(ref):
        return pltpu.make_async_copy(u_buf.at[0], ref, pre_sem.at[0])

    kept = (xs0, xs1, xs2)

    def keep_x(w):
        here = pltpu.make_async_copy(x_buf.at[0, :, rows(core * half, half)], kept[w].at[mine], keep_sem.at[w])
        there = remote_copy(x_buf.at[0, :, rows((1 - core) * half, half)], kept[w].at[mine], keep_send.at[w], keep_recv.at[w], place.other_core)
        return here, there

    def start_x(w):
        for c in keep_x(w):
            c.start()

    def free_x(w):
        here, there = keep_x(w)
        here.wait()
        there.wait_send()

    def keep_dz(i):
        at = (slice(None), rows(i * wide, wide))
        here = pltpu.make_async_copy(x_buf.at[(0, *at)], dz.at[mine, at[1]], keep_sem.at[3 + i])
        there = remote_copy(x_buf.at[(0, *at)], dz.at[mine, at[1]], keep_send.at[3 + i], keep_recv.at[3 + i], place.other_core)
        return here, there

    def row_loop(body, carry):
        return lax.fori_loop(0, rows_dev // BLOCK, lambda r, c: body(rows(r * BLOCK, BLOCK), c), carry)

    def put_sums(j, i, row, value):
        value = jnp.sum(value, axis=0, keepdims=True)
        for c in range(value.shape[1] // TILE):
            payload[j, i + c, row : row + 1] = value[:, c * TILE : (c + 1) * TILE]

    def product(g):
        job, i = g // tiles, g % tiles
        view = job % 2
        w_tile(w_in, g).wait()
        pl.when(g + W_BUFS - 1 < JOBS * tiles)(lambda: start_w(g + W_BUFS - 1))
        at_cols = rows(i * wide, wide)
        u_buf[view, :, at_cols] = jnp.dot(x_buf[view], w_buf[g % W_BUFS], preferred_element_type=jnp.float32)

        def block(at, sums):
            u = u_buf[view, at, at_cols]
            return sums[0] + fold(u), sums[1] + fold(u * u)

        zero = jnp.zeros((8, wide), jnp.float32)
        for row, value in enumerate(row_loop(block, (zero, zero))):
            put_sums(job, i * (wide // TILE), row, value)

    def begin(job):
        small.begin(job)

        @pl.when(job % 2 == 0)
        def _():
            pick(job // 2, (pre1, pre2), lambda ref: keep_pre(ref).start())

    def norm(job):
        layer, view = job // 2, job % 2
        small.end(job)
        for c in range(PLANE):
            at = slice(c * TILE, (c + 1) * TILE)
            means = total[job, c] / row_count
            stats[job, 0, :, at] = means[0:1]
            stats[job, 1, :, at] = lax.rsqrt(means[1:2] - means[0:1] * means[0:1] + NORM_EPS)

        pl.when(view == 0)(lambda: pick(layer, (0, 1, 2), free_x))

        def hidden(i):
            at_cols = rows(i * wide, wide)
            mean, inv = stats[job, 0, :, at_cols], stats[job, 1, :, at_cols]
            gain, bias = affine[layer * 2, :, at_cols], affine[layer * 2 + 1, :, at_cols]

            def block(at, c):
                n = (u_buf[view, at, at_cols] - mean) * inv
                x_buf[view, at, at_cols] = jnp.maximum(n * gain + bias, 0.0).astype(jnp.bfloat16)
                return c

            row_loop(block, 0)

        def student(i):
            at_cols = rows(i * wide, wide)
            mean, inv = stats[job, 0, :, at_cols], stats[job, 1, :, at_cols]

            def block(at, c):
                n = (u_buf[0, at, at_cols] - mean) * inv
                u_buf[0, at, at_cols] = n
                x_buf[0, at, at_cols] = n.astype(jnp.bfloat16)
                return c

            row_loop(block, 0)

        def student_own(i):
            def block(r, c):
                ea[rows(core * rows_dev + r * BLOCK, BLOCK), rows(i * wide, wide)] = x_buf[0, rows(r * BLOCK, BLOCK), rows(core * half + i * wide, wide)]
                return c

            lax.fori_loop(0, rows_dev // BLOCK, block, 0)

        def teacher(i):
            at_cols = rows(i * wide, wide)
            mean, inv = stats[job, 0, :, at_cols], stats[job, 1, :, at_cols]

            def block(r, c):
                n = (u_buf[1, rows(r * BLOCK, BLOCK), at_cols] - mean) * inv
                eb[rows(core * rows_dev + r * BLOCK, BLOCK), at_cols] = n.astype(jnp.bfloat16)
                return c

            lax.fori_loop(0, rows_dev // BLOCK, block, 0)
            eb_copy(i).start()

        @pl.when(layer < 2)
        def _():
            loop(0, tiles, hidden)

            @pl.when(view == 0)
            def _():
                pick(layer, (1, 2), start_x)
                keep_pre(pre1).wait()

        @pl.when((layer == 2) & (view == 0))
        def _():
            loop(0, tiles, student)
            ea_copy().start()
            loop(0, tiles // 2, student_own)

        @pl.when((layer == 2) & (view == 1))
        def _():
            loop(0, tiles, teacher)

    ea_copy = lambda: remote_copy(x_buf.at[0, :, rows((1 - core) * half, half)], ea.at[mine], e_send.at[0], e_recv.at[0], place.other_core)

    def eb_copy(i):
        block = eb.at[mine, rows(i * wide, wide)]
        return remote_copy(block, block, e_send.at[1 + i], e_recv.at[1 + i], place.other_core)

    def step(g):
        job, i = g // tiles, g % tiles
        view = job % 2
        pl.when(g == tiles)(lambda: feat(1).wait())
        product(g)

        @pl.when(g == 0)
        def _():
            place.all_here()
            start_x(0)

        pl.when((i == 1) & (job > 0))(lambda: small.middle(job - 1))

        @pl.when(i == tiles - 1)
        def _():
            begin(job)
            pl.when(job > 0)(lambda: norm(job - 1))

    loop(0, JOBS * tiles, step)
    small.middle(JOBS - 1)
    norm(JOBS - 1)
    for j, source in enumerate((affine.at[2], affine.at[3], stats.at[2, 0], stats.at[2, 1], affine.at[0], affine.at[1], stats.at[0, 0], stats.at[0, 1])):
        vec[j] = source[...]

    loss[...] = jnp.zeros_like(loss)

    def finish(k, off, size, buf):
        share = jnp.where(front_kind("x", k), 0.5, 0.25)
        at = rows(off, size)
        corr = (acc[k, at] + buf[k]) / row_count
        row = core * half + k * part_rows + off
        diag = (row + lax.broadcasted_iota(jnp.int32, (size, width), 0)) == lax.broadcasted_iota(jnp.int32, (size, width), 1)
        weight = off_weight[0]
        miss = 1.0 - corr
        loss[...] += share * jnp.sum(jnp.where(diag, miss * miss, weight * (corr * corr)), axis=0, keepdims=True)
        gathered[k, at] = jnp.where(diag, -2.0 * miss, 2.0 * weight * corr).astype(jnp.bfloat16)

    def homes(k):
        return [(None, lambda off, size: gathered.at[k, pl.ds(pl.multiple_of(off, part_rows // 4), size)])]

    chunks = ChunkSum(place, "xsl", front_kind, acc, homes, landing, send, recv, finish)

    def form(k, group):
        at = rows(k * part_rows, group * part_rows)
        size = min(1024, width)

        def col(c):
            @pl.when(k == 0)
            def _():
                for i in range(size // wide):
                    eb_copy(c * (size // wide) + i).wait_recv()

            cs = rows(c * size, size)
            acc[pl.ds(k, group), :, cs] = contract_rows(ea[:, at], eb[:, cs]).reshape(group, part_rows, size)

        loop(0, width // size, col)

    def swap(k):
        return chunks.copy(gathered.at[k], g_peer.at[k], 7, k, place.other_core)

    def ge_cols(k, side):
        return rows(side * half + k * part_rows, GROUP * part_rows)

    def ge_copy(k, side):
        at = ge_cols(k, side)
        return pltpu.make_async_copy(u_buf.at[1, :, at], grad_emb.at[:, at], ge_sem.at[k // GROUP, side])

    def embed(k, side, g_rows):
        at_cols = ge_cols(k, side)
        grad = contract_cols(eb[mine], g_rows.reshape(GROUP * part_rows, width)) / row_count
        u_buf[1, :, at_cols] = grad
        ge_copy(k, side).start()

        def block(at, sums):
            g = u_buf[1, at, at_cols]
            return sums[0] + fold(g * u_buf[0, at, at_cols]), sums[1] + fold(g)

        zero = jnp.zeros((8, GROUP * part_rows), jnp.float32)
        for row, value in enumerate(row_loop(block, (zero, zero))):
            payload[JOBS, (side * half + k * part_rows) // TILE, row : row + 1] = jnp.sum(value, axis=0, keepdims=True)

    def stage(i, k):
        if i == 0:
            form_next(k, form)
            return
        chunks.stage(i, k)
        if i == 8:
            pl.when(jnp.logical_not(front_kind("l", k)))(lambda: swap(k).start())
        if i == 9:
            pl.when(front_kind("l", k))(lambda: swap(k).start())

            @pl.when(k % GROUP == GROUP - 1)
            def _():
                embed(k - GROUP + 1, core, gathered[pl.ds(k - GROUP + 1, GROUP)])

        if i == 10:
            swap(k).wait_recv()
            swap(k).wait_send()

            @pl.when(k % GROUP == GROUP - 1)
            def _():
                embed(k - GROUP + 1, 1 - core, g_peer[pl.ds(k - GROUP + 1, GROUP)])

    ea_copy().wait_recv()
    form(0, GROUP // 2)
    run_slots(FRONT_PLAN, PARTS, stage, lambda t: None)
    small.begin(JOBS)
    for c in range(PLANE):
        payload[JOBS + 1, c, 0:1] = loss[:, c * TILE : (c + 1) * TILE]
    small.begin(JOBS + 1)
    ea_copy().wait_send()
    for i in range(tiles):
        eb_copy(i).wait_send()
    small.middle(JOBS)
    small.middle(JOBS + 1)
    for k in range(0, PARTS, GROUP):
        for side in range(2):
            ge_copy(k, side).wait()
    small.end(JOBS)

    def dz_tile(i):
        at_cols = rows(i * wide, wide)
        sums = jnp.concatenate([total[JOBS, i * (wide // TILE) + c] for c in range(wide // TILE)], axis=1) / row_count
        mean_gn, mean_g = sums[0:1], sums[1:2]
        inv = stats[JOBS - 2, 1, :, at_cols]

        def block(at, c):
            value = (u_buf[1, at, at_cols] - mean_g - u_buf[0, at, at_cols] * mean_gn) * inv
            x_buf[0, at, at_cols] = value.astype(jnp.bfloat16)
            return c

        row_loop(block, 0)
        for c in keep_dz(i):
            c.start()

    loop(0, tiles, dz_tile)
    small.end(JOBS + 1)
    for c in range(PLANE):
        vec[8, :, c * TILE : (c + 1) * TILE] = total[JOBS + 1, c, 0:1]
    for w in range(3):
        keep_x(w)[1].wait_recv()
    for i in range(tiles):
        here, there = keep_dz(i)
        here.wait()
        there.wait()


def front(feat_a, feat_b, weights, affine, off_weight):
    rows_dev, width = feat_a.shape
    half = width // 2
    part_rows = half // PARTS
    any_spec = pl.BlockSpec(memory_space=pl.ANY)
    vmem_spec = pl.BlockSpec(memory_space=pltpu.VMEM)
    wide_f32 = jax.ShapeDtypeStruct((rows_dev, width), jnp.float32)
    kept = jax.ShapeDtypeStruct((2 * rows_dev, half), jnp.bfloat16)
    both_dz = jax.ShapeDtypeStruct((2 * rows_dev, width), jnp.bfloat16)
    keeps = 3 + width // WIDE
    dma = pltpu.SemaphoreType.DMA
    return pl.pallas_call(
        front_kernel,
        name="front",
        out_shape=[wide_f32, wide_f32, kept, kept, kept, both_dz, wide_f32]
        + [jax.ShapeDtypeStruct((9, 1, width), jnp.float32)],
        in_specs=[any_spec] * 8 + [vmem_spec] * 4 + [pl.BlockSpec(memory_space=pltpu.SMEM)],
        out_specs=[any_spec] * 7 + [vmem_spec],
        scratch_shapes=[
            pltpu.VMEM((2, rows_dev, width), jnp.bfloat16),
            pltpu.VMEM((2, rows_dev, width), jnp.float32),
            pltpu.VMEM((W_BUFS, width, WIDE), jnp.bfloat16),
            pltpu.VMEM((JOBS, 2, 1, width), jnp.float32),
            pltpu.VMEM((4, 1, width), jnp.float32),
            pltpu.VMEM((1, width), jnp.float32),
            pltpu.VMEM((2 * rows_dev, half), jnp.bfloat16),
            pltpu.VMEM((2 * rows_dev, width), jnp.bfloat16),
            pltpu.VMEM((PARTS, part_rows, width), jnp.bfloat16),
            dma((2,)),
            dma((W_BUFS,)),
            dma((1,)),
            dma((keeps,)),
            dma((keeps,)),
            dma((keeps,)),
            dma((PARTS // GROUP, 2)),
            dma((1 + width // WIDE,)),
            dma((1 + width // WIDE,)),
        ]
        + small_scratch(JOBS + 2)
        + chunk_scratch(PARTS, PARTS, part_rows, width, PARTS, jnp.bfloat16),
        compiler_params=pltpu.CompilerParams(collective_id=0, has_side_effects=True, vmem_limit_bytes=VMEM_BYTES),
    )(feat_a, feat_b, *weights, *affine, off_weight)


def back_kernel(dz_hbm, x2, x1, x0, w_out, w_mid, u2, u1, vec, out2, out1, out0, sums_out, *scratch):
    (dy, xs, w_buf) = scratch[:3]
    (in_sem, tile_sem, peer_send, peer_recv, store_sem) = scratch[3:8]
    small_refs = scratch[8 : 8 + SMALL_REFS]
    acc, gathered, *landing, send, recv = scratch[8 + SMALL_REFS :]
    rows_dev, width = u2.shape
    wide = w_buf.shape[0]
    tiles = width // wide
    row_count = rows_dev * DEPTH * PLANE
    half = width // 2
    part_rows = half // PARTS
    count = MATS * PARTS
    mats_in, outs, weights, pres = (x2, x1, x0), (out2, out1), (w_out, w_mid), (u2, u1)
    dpre = out0.at[pl.ds(0, rows_dev)]

    def u_buf(i):
        return out0.at[pl.ds(rows_dev, rows_dev), rows((i % 2) * wide, wide)]

    place = Place()
    core, other_core = place.core, place.other_core
    mine = rows(core * rows_dev, rows_dev)
    place.arrive()
    small = small_sum(place, small_refs)
    payload, sums = small.payload, small.total

    def load_x(w):
        return pltpu.make_async_copy(mats_in[w], xs.at[w % 2], in_sem.at[w])

    def peer_dy(w):
        block = dy.at[w % 2, mine]
        return remote_copy(block, block, peer_send.at[w], peer_recv.at[w], other_core)

    def w_tile(ref, i):
        return pltpu.make_async_copy(ref.at[rows(i * wide, wide)], w_buf, tile_sem.at[0, 0])

    def u_tile(ref, i):
        return pltpu.make_async_copy(ref.at[:, rows(i * wide, wide)], u_buf(i), tile_sem.at[1, i % 2])

    def start_w(layer, i):
        pick(layer, weights, lambda ref: w_tile(ref, i).start())

    def start_u(layer, i):
        pick(layer, pres, lambda ref: u_tile(ref, i).start())

    size = min(1024, width)

    def load_dz(c):
        return pltpu.make_async_copy(dz_hbm.at[:, rows(c * size, size)], dy.at[0, :, rows(c * size, size)], in_sem.at[MATS + c])

    load_x(0).start()
    for c in range(width // size):
        load_dz(c).start()
    w_tile(weights[0], 0).start()
    u_tile(pres[0], 0).start()
    load_x(1).start()
    payload[...] = jnp.zeros_like(payload)

    def row_loop(body, carry):
        return lax.fori_loop(0, rows_dev // BLOCK, body, carry)

    def chain_tile(layer, i):
        w_tile(w_out, i).wait()
        u_tile(u2, i).wait()

        pl.when(i + 1 < tiles)(lambda: start_u(layer, i + 1))
        at_cols = rows(i * wide, wide)
        dpre[:, at_cols] = contract_cols(dy[layer, mine], w_buf[...])
        pl.when(i + 1 < tiles)(lambda: start_w(layer, i + 1))
        gain, bias, mean, inv = (vec[layer * 4 + j, :, at_cols] for j in range(4))

        def block(r, carry):
            at = rows(r * BLOCK, BLOCK)
            n = (out0[rows(rows_dev + r * BLOCK, BLOCK), rows((i % 2) * wide, wide)] - mean) * inv
            g = jnp.where(n * gain + bias > 0.0, dpre[at, at_cols], 0.0)
            dpre[at, at_cols] = g
            return carry[0] + fold(g * n), carry[1] + fold(g)

        zero = jnp.zeros((8, wide), jnp.float32)
        for row, value in enumerate(row_loop(block, (zero, zero))):
            value = jnp.sum(value, axis=0, keepdims=True)
            for c in range(wide // TILE):
                payload[layer, i * (wide // TILE) + c, row : row + 1] = value[:, c * TILE : (c + 1) * TILE]

    def du_tile(layer, i):
        u_tile(u2, i).wait()
        pl.when(i + 1 < tiles)(lambda: start_u(layer, i + 1))
        at_cols = rows(i * wide, wide)
        gain, mean, inv = (vec[layer * 4 + j, :, at_cols] for j in (0, 2, 3))
        means = jnp.concatenate([sums[layer, i * (wide // TILE) + c] for c in range(wide // TILE)], axis=1) / row_count
        mean_gn, mean_g = means[0:1], means[1:2]
        scale = gain * inv

        def block(r, c):
            at = rows(r * BLOCK, BLOCK)
            n = (out0[rows(rows_dev + r * BLOCK, BLOCK), rows((i % 2) * wide, wide)] - mean) * inv
            value = (dpre[at, at_cols] - mean_g - n * mean_gn) * scale
            dy[1 - layer, rows(core * rows_dev + r * BLOCK, BLOCK), at_cols] = value.astype(jnp.bfloat16)
            return c

        row_loop(block, 0)

    in_last = (MATS - 1) * PARTS
    quarter = part_rows // 4

    def home_row(k):
        return core * half + (k % PARTS) * part_rows

    def homes(k):
        return [
            (k < in_last, lambda off, size: gathered.at[k % GATHER_SLOTS, pl.ds(pl.multiple_of(off, quarter), size)]),
            (k >= in_last, lambda off, size: out0.at[pl.ds(pl.multiple_of(home_row(k) + off, quarter), size)]),
        ]

    def finish(k, off, size, buf):
        j = k % ACC_SLOTS
        value = acc[j, rows(off, size)] + buf[j]

        @pl.when(k < in_last)
        def _():
            gathered[k % GATHER_SLOTS, rows(off, size)] = value

        @pl.when(k >= in_last)
        def _():
            out0[rows(home_row(k) + off, size)] = value

    chunks = ChunkSum(place, "xl", back_kind, acc, homes, landing, send, recv, finish)

    def form(k, group):
        w, j = k // PARTS, k % ACC_SLOTS

        @pl.when(k % PARTS == 0)
        def _():
            pltpu.make_async_copy(xs.at[w % 2], xs.at[w % 2], in_sem.at[w]).wait()
            pl.when(w > 0)(lambda: peer_dy(w).wait_recv())

        at = rows((k % PARTS) * part_rows, group * part_rows)

        def col(c):
            pl.when(k == 0)(lambda: load_dz(c).wait())
            cs = rows(c * size, size)
            acc[pl.ds(j, group), :, cs] = contract_rows(xs[w % 2, :, at], dy[w % 2, :, cs]).reshape(group, part_rows, size)

        loop(0, width // size, col)

    def out_rows(k, side):
        return pl.ds(pl.multiple_of(side * half + (k % PARTS) * part_rows, part_rows), part_rows)

    def last_copy(out, k, side):
        return chunks.copy(gathered.at[k % GATHER_SLOTS], out.at[out_rows(k, side)], 7, k, other_core)

    def store_copy(out, k):
        return pltpu.make_async_copy(gathered.at[k % GATHER_SLOTS], out.at[out_rows(k, core)], store_sem.at[k])

    def stage(i, k):
        if i == 0:
            form_next(k, form)
            return
        chunks.stage(i, k)
        own_rows = out0.at[pl.ds(pl.multiple_of(home_row(k), part_rows), part_rows)]
        in_place = chunks.copy(own_rows, own_rows, 7, k, other_core)
        last = k // PARTS == MATS - 1

        def emit(out):
            last_copy(out, k, core).start()
            store_copy(out, k).start()

        def emit_any():
            pick(k // PARTS, outs, emit)
            pl.when(last)(lambda: in_place.start())

        if i == 8:
            pl.when(back_kind("x", k))(emit_any)
        if i == 9:
            pl.when(back_kind("l", k))(emit_any)
        if i == 10:

            def close(out):
                last_copy(out, k, 1 - core).wait_recv()
                store_copy(out, k).wait()
                last_copy(out, k, core).wait_send()

            pick(k // PARTS, outs, close)

            @pl.when(last)
            def _():
                in_place.wait_recv()
                in_place.wait_send()

    def layer_work(t):
        layer = t // LAYER_SLOTS
        at = t - LAYER_SLOTS * layer
        first_du = 2 * tiles + 3
        pl.when((at < 2 * tiles) & (at % 2 == 1))(lambda: chain_tile(layer, at // 2))
        pl.when(at == 2 * tiles)(lambda: small.begin(layer))
        pl.when(at == 2 * tiles + 1)(lambda: small.middle(layer))

        pl.when(at == 2 * tiles + 2)(lambda: start_u(layer, 0))

        pl.when(at == first_du)(lambda: small.end(layer))
        pl.when(at >= first_du)(lambda: du_tile(layer, at - first_du))

        @pl.when(at == LAYER_SLOTS - 1)
        def _():
            peer_dy(layer + 1).start()

            @pl.when(layer == 0)
            def _():
                w_tile(weights[1], 0).start()
                u_tile(pres[1], 0).start()

            pl.when(layer == 1)(lambda: load_x(2).start())

    form(0, GROUP // 2)
    place.all_here()
    run_slots(BACK_PLAN, count, stage, lambda t: pl.when(t < 2 * LAYER_SLOTS)(lambda: layer_work(t)))
    for w in (1, 2):
        peer_dy(w).wait_send()
    for c in range(PLANE):
        for row in range(4):
            sums_out[row : row + 1, c * TILE : (c + 1) * TILE] = sums[row // 2, c, row % 2 : row % 2 + 1]
    sums_out[4:5] = jnp.full((1, width), jnp.sum(vec[8]))


def backward(grad_z, x2, x1, x0, w_out, w_mid, u2, u1, vec):
    rows_dev, width = u2.shape
    part_rows = width // 2 // PARTS
    count = MATS * PARTS
    any_spec = pl.BlockSpec(memory_space=pl.ANY)
    vmem_spec = pl.BlockSpec(memory_space=pltpu.VMEM)
    mat = jax.ShapeDtypeStruct((width, width), jnp.float32)
    dma = pltpu.SemaphoreType.DMA
    return pl.pallas_call(
        back_kernel,
        name="backward",
        out_shape=[mat, mat, pltpu.VMEM((width, width), jnp.float32), jax.ShapeDtypeStruct((5, width), jnp.float32)],
        in_specs=[any_spec] * 8 + [vmem_spec],
        out_specs=[any_spec] * 2 + [vmem_spec] * 2,
        scratch_shapes=[
            pltpu.VMEM((2, 2 * rows_dev, width), jnp.bfloat16),
            pltpu.VMEM((2, 2 * rows_dev, width // 2), jnp.bfloat16),
            pltpu.VMEM((WIDE, width), jnp.bfloat16),
            dma((MATS + 2,)),
            dma((2, 2)),
            dma((MATS,)),
            dma((MATS,)),
            dma((count,)),
        ]
        + small_scratch(2)
        + chunk_scratch(ACC_SLOTS, GATHER_SLOTS, part_rows, width, count, jnp.float32),
        compiler_params=pltpu.CompilerParams(collective_id=1, has_side_effects=True, vmem_limit_bytes=BACK_VMEM),
    )(grad_z, x2, x1, x0, w_out, w_mid, u2, u1, vec)


def copy_kernel(*refs):
    pairs = (len(refs) - 6 - 6) // 2
    ins, small, outs, small_outs = refs[:pairs], refs[pairs], refs[pairs + 1 : 2 * pairs + 1], refs[2 * pairs + 1 : -6]
    buf, small_buf, in_sem, out_sem, small_sem, near_sem = refs[-6:]
    blocks = [(i, r) for i in range(pairs - 1) for r in range(0, ins[i].shape[0], COPY_ROWS)]
    near = pltpu.make_async_copy(ins[-1], outs[-1], near_sem.at[0])

    def read(b):
        i, r = blocks[b]
        return pltpu.make_async_copy(ins[i].at[pl.ds(r, COPY_ROWS)], buf.at[b % COPY_BUFS], in_sem.at[b % COPY_BUFS])

    def write(b):
        i, r = blocks[b]
        return pltpu.make_async_copy(buf.at[b % COPY_BUFS], outs[i].at[pl.ds(r, COPY_ROWS)], out_sem.at[b % COPY_BUFS])

    ahead = COPY_BUFS // 2
    for b in range(min(ahead, len(blocks))):
        read(b).start()
    near.start()
    pltpu.make_async_copy(small, small_buf, small_sem.at[4]).start()

    def small_write(row):
        return pltpu.make_async_copy(small_buf.at[pl.ds(row, 1)], small_outs[row], small_sem.at[row])

    for b in range(len(blocks)):
        if b + ahead < len(blocks):
            if b + ahead >= COPY_BUFS:
                write(b + ahead - COPY_BUFS).wait()
            read(b + ahead).start()
        read(b).wait()
        write(b).start()
        if b == 0:
            pltpu.make_async_copy(small, small_buf, small_sem.at[4]).wait()
            small_outs[4][...] = small_buf[4:5, :1]
            for row in range(4):
                small_write(row).start()
    for row in range(4):
        small_write(row).wait()
    near.wait()
    for b in range(max(0, len(blocks) - COPY_BUFS), len(blocks)):
        write(b).wait()


def copy_out(arrays, small):
    any_spec = pl.BlockSpec(memory_space=pl.ANY)
    vmem_spec = pl.BlockSpec(memory_space=pltpu.VMEM)
    dma = pltpu.SemaphoreType.DMA
    width = small.shape[1]
    row = jax.ShapeDtypeStruct((1, width), jnp.float32)
    return pl.pallas_call(
        copy_kernel,
        name="copy_out",
        out_shape=[jax.ShapeDtypeStruct(a.shape, a.dtype) for a in arrays] + [row] * 4 + [jax.ShapeDtypeStruct((1, 1), jnp.float32)],
        in_specs=[any_spec] * (len(arrays) - 1) + [vmem_spec, any_spec],
        out_specs=[any_spec] * (len(arrays) + 4) + [vmem_spec],
        scratch_shapes=[
            pltpu.VMEM((COPY_BUFS, COPY_ROWS, width), jnp.float32),
            pltpu.VMEM(small.shape, jnp.float32),
            dma((COPY_BUFS,)),
            dma((COPY_BUFS,)),
            dma((5,)),
            dma((1,)),
        ],
        compiler_params=pltpu.CompilerParams(vmem_limit_bytes=COPY_VMEM),
    )(*arrays[:-1], pltpu.with_memory_space_constraint(arrays[-1], pltpu.VMEM), small)


def solution(mesh):
    row_part = P(DATA_AXIS, None)
    replicated = P()

    def local_step(feat_a, feat_b, w_in, w_mid, w_out, t_in, t_mid, t_out, gain_1, bias_1, gain_2, bias_2, off_weight):
        affine = [v.reshape(1, -1) for v in (gain_1, bias_1, gain_2, bias_2)]
        pre_1, pre_2, xs_2, xs_1, xs_0, grad_z, grad_emb, vec = front(
            feat_a, feat_b, (w_in, t_in, w_mid, t_mid, w_out, t_out), affine, off_weight.reshape(1)
        )
        grad_w_out, grad_w_mid, grad_w_in, sums = backward(grad_z, xs_2, xs_1, xs_0, w_out, w_mid, pre_2, pre_1, vec)
        (grad_emb, grad_w_out, grad_w_mid, grad_w_in, gain_2, bias_2, gain_1, bias_1, loss) = copy_out((grad_emb, grad_w_out, grad_w_mid, grad_w_in), sums)
        gain_1, bias_1, gain_2, bias_2 = (v.reshape(-1) for v in (gain_1, bias_1, gain_2, bias_2))
        return (loss.reshape(()), grad_emb, grad_w_in, grad_w_mid, grad_w_out, gain_1, bias_1, gain_2, bias_2)

    return jax.shard_map(local_step, mesh=mesh, in_specs=(row_part, row_part) + (replicated,) * 11, out_specs=(replicated, row_part) + (replicated,) * 7, check_vma=False)
```

```python
import functools

import jax
import jax.numpy as jnp
from jax import lax
from jax.experimental import pallas as pl
from jax.experimental.pallas import tpu as pltpu
from jax.sharding import PartitionSpec as P

NORM_EPS = 1e-5
DATA_AXIS = "data"
MESH = pl.DeviceIdType.MESH
VMEM_BYTES = 67_043_328
PLANE = 8
DEPTH = 4
TILE = 256
WIDE = 512
BLOCK = 128
SUM_ROWS = 2
PARTS = 16
GROUP = 4
MATS = 3
BACK_PARTS = 32
BACK_GROUP = 8
ACC_SLOTS = 32
GATHER_SLOTS = 28
BACK_VMEM = 49_800_000
COPY_VMEM = 42 * 1024 * 1024
JOBS = 6
W_BUFS = 3
LAYER_SLOTS = 15
COPY_ROWS = 256
COPY_BUFS = 18
FRONT_PLAN = ((0, 0, 3, 5, 7, 9, 12, 13, 16, 17, 18), (0, 6, 3, 4, 9, 10, 8, 5, 2, 7, 1))
BACK_PLAN = ((0, 0, 6, 10, 14, 16, 19, 23, 27, 32, 34), (0, 4, 10, 2, 7, 8, 3, 1, 9, 5, 6))


def front_kind(kind, k):
    s, l = (k % 5 == 2) & (k > 2), k == 2
    return {"s": s, "l": l, "x": (k % 5 != 2)}[kind]


def back_kind(kind, k):
    p = k // 2
    l = ((p % 5 == 2) & (p < 43)) | ((p % 5 == 0) & (p >= 10) & (p < 36)) | (k == 58)
    return l if kind == "l" else jnp.logical_not(l)


def contract_rows(left_op, right_op):
    return lax.dot_general(left_op, right_op, (((0,), (0,)), ((), ())), preferred_element_type=jnp.float32)


def contract_cols(left_op, right_op):
    return lax.dot_general(left_op, right_op, (((1,), (1,)), ((), ())), preferred_element_type=jnp.float32)


def rows(off, size):
    return pl.ds(pl.multiple_of(off, size), size)


def pick(index, choices, what):
    for i, c in enumerate(choices):
        pl.when(index == i)(functools.partial(what, c))


def loop(lo, hi, body):
    def step(i, carry):
        body(i)
        return carry

    lax.fori_loop(lo, hi, step, 0)


def remote_copy(src, dst, send, recv, mate):
    return pltpu.make_async_remote_copy(src, dst, send, recv, device_id=(mate,), device_id_type=MESH)


class Place:
    def __init__(self):
        me = lax.axis_index(DATA_AXIS)
        self.me = me
        self.pos, self.plane = me % PLANE, me // PLANE
        self.core, self.bx, self.by, self.bz0, self.bz1 = me % 2, (me // 2) % 2, (me // 4) % 2, (me // 8) % 2, (me // 16) % 2
        self.other_core = me + 1 - 2 * self.core
        self.mates = [(self.pos + d) % PLANE for d in range(1, PLANE)]
        self.levels = [(self.plane + d) % DEPTH for d in range(1, DEPTH)]

    def peers(self):
        return [self.plane * PLANE + m for m in self.mates] + [lv * PLANE + self.pos for lv in self.levels]

    def arrive(self):
        sem = pltpu.get_barrier_semaphore()
        for peer in self.peers():
            pl.semaphore_signal(sem, inc=1, device_id=(peer,), device_id_type=MESH)

    def all_here(self):
        pl.semaphore_wait(pltpu.get_barrier_semaphore(), PLANE + DEPTH - 2)


class SmallSum:
    def __init__(self, place, payload, total, depth_buf, line_sum, plane_buf, sems):
        self.p, self.payload, self.total = place, payload, total
        self.depth_buf, self.line_sum, self.plane_buf, self.sems = depth_buf, line_sum, plane_buf, sems

    def along(self, j, lv, slot):
        s, r = self.sems[0], self.sems[1]
        return remote_copy(self.payload.at[j], self.depth_buf.at[j, slot], s.at[j, lv], r.at[j, slot], lv * PLANE + self.p.pos)

    def within(self, j, m, slot):
        s, r = self.sems[2], self.sems[3]
        return remote_copy(self.line_sum.at[j], self.plane_buf.at[j, slot], s.at[j, m], r.at[j, slot], self.p.plane * PLANE + m)

    def begin(self, j):
        for lv in self.p.levels:
            self.along(j, lv, self.p.plane).start()
        self.depth_buf[j, self.p.plane] = self.payload[j]

    def middle(self, j):
        for lv in self.p.levels:
            self.along(j, lv, lv).wait_recv()
        total = self.depth_buf[j, 0]
        for i in range(1, DEPTH):
            total = total + self.depth_buf[j, i]
        self.line_sum[j] = total
        for m in self.p.mates:
            self.within(j, m, self.p.pos).start()
        self.plane_buf[j, self.p.pos] = total

    def end(self, j):
        for m in self.p.mates:
            self.within(j, m, m).wait_recv()
        total = self.plane_buf[j, 0]
        for i in range(1, PLANE):
            total = total + self.plane_buf[j, i]
        self.total[j] = total
        for lv in self.p.levels:
            self.along(j, lv, self.p.plane).wait_send()
        for m in self.p.mates:
            self.within(j, m, self.p.pos).wait_send()


def small_scratch(count):
    def buf(*lead):
        return pltpu.VMEM((count, *lead, PLANE, SUM_ROWS, TILE), jnp.float32)

    return [buf(), buf(), buf(DEPTH), buf(), buf(PLANE)] + [pltpu.SemaphoreType.DMA((count, n)) for n in (DEPTH, DEPTH, PLANE, PLANE)]


SMALL_REFS = 9


def small_sum(place, refs):
    return SmallSum(place, *refs[:5], refs[5:])


class Homed:
    def __init__(self, homes, make):
        self.homes, self.make = homes, make

    def do(self, what):
        for when, home in self.homes:
            run = lambda home=home: getattr(self.make(home), what)()
            run() if when is None else pl.when(when)(run)

    def start(self):
        self.do("start")

    def wait_recv(self):
        self.do("wait_recv")

    def wait_send(self):
        self.do("wait_send")


class ChunkSum:
    def __init__(self, place, kinds, is_kind, acc, homes, landing, send, recv, finish):
        self.p, self.kinds, self.is_kind, self.slots, self.homes = place, kinds, is_kind, acc.shape[0], homes
        self.acc, self.landing, self.send, self.recv, self.finish = acc, landing, send, recv, finish
        self.size = acc.shape[1]
        self.s2, self.s4 = self.size // 2, self.size // 4
        core, bx, by, me = place.core, place.bx, place.by, place.me
        first, second = core * by + (1 - core) * bx, core * bx + (1 - core) * by
        self.xy = ((me + (2 + 2 * core) * (1 - 2 * first), first), (me + (4 - 2 * core) * (1 - 2 * second), second))
        self.zz = ((me + 8 * (1 - 2 * place.bz0), place.bz0), (me + 16 * (1 - 2 * place.bz1), place.bz1))
        self.is_mid = place.bz0 + place.bz1 - 2 * place.bz0 * place.bz1
        self.mid, self.end = self.is_mid == 1, self.is_mid == 0
        self.z_mate = self.zz[0][0]
        self.mid_mate = me + 8 * (1 - 2 * place.bz1)

    def copy(self, src, dst, stage, k, mate):
        return remote_copy(src, dst, self.send.at[stage, k], self.recv.at[stage, k], mate)

    def span(self, off, size):
        return pl.ds(pl.multiple_of(off, self.s4), size)

    def down(self, stage, k, off, size, mate, buf=None):
        j = k % self.slots
        buf = self.landing[stage] if buf is None else buf
        return self.copy(self.acc.at[j, self.span(off, size)], buf.at[j, pl.ds(0, size)], stage, k, mate)

    def up(self, stage, k, off, size, mate):
        return Homed(self.homes(k), lambda home: self.copy(home(off, size), home(off, size), stage, k, mate))

    def add(self, k, off, size, buf):
        step = min(self.s4, 16)
        j = k % self.slots

        def body(i):
            at = pl.ds(pl.multiple_of(off + i * step, step), step)
            self.acc[j, at] = self.acc[j, at] + buf[j, rows(i * step, step)]

        loop(0, size // step, body)

    def stage(self, i, k):
        for kind in self.kinds:
            run = {"x": self.stage_x, "s": self.stage_s, "l": self.stage_l}[kind]
            pl.when(self.is_kind(kind, k))(functools.partial(run, i, k))

    def stage_x(self, i, k):
        (m1, b1), (m2, b2), s2, s4 = *self.xy, self.s2, self.s4
        off1, off2 = b1 * s2, b1 * s2 + b2 * s4
        half = lambda: self.down(0, k, (1 - b1) * s2, s2, m1)
        quarter = lambda: self.down(1, k, off1 + (1 - b2) * s4, s4, m2)
        inward = lambda: self.down(2, k, off2, s4, self.z_mate)
        across = lambda: self.down(3, k, off2, s4, self.mid_mate)
        outward = lambda: self.up(4, k, off2, s4, self.z_mate)
        back4 = lambda: self.up(5, k, off2, s4, m2)
        back2 = lambda: self.up(6, k, off1, s2, m1)
        if i == 1:
            half().start()
        elif i == 2:
            half().wait_recv()
            self.add(k, off1, s2, self.landing[0])
            quarter().start()
        elif i == 3:
            quarter().wait_recv()
            self.add(k, off2, s4, self.landing[1])
            pl.when(self.end)(lambda: inward().start())
        elif i == 4:

            @pl.when(self.mid)
            def _():
                inward().wait_recv()
                self.add(k, off2, s4, self.landing[2])
                across().start()

        elif i == 5:

            @pl.when(self.mid)
            def _():
                across().wait_recv()
                self.finish(k, off2, s4, self.landing[3])
                outward().start()

        elif i == 6:
            pl.when(self.end)(lambda: outward().wait_recv())
            back4().start()
            half().wait_send()
            quarter().wait_send()
            pl.when(self.end)(lambda: inward().wait_send())
            pl.when(self.mid)(lambda: across().wait_send())
        elif i == 7:
            back4().wait_recv()
            back2().start()
        elif i == 8:
            back2().wait_recv()
        elif i == 10:
            pl.when(self.mid)(lambda: outward().wait_send())
            back4().wait_send()
            back2().wait_send()

    def stage_s(self, i, k):
        (m1, b1), (m2, b2), s2, s4 = *self.zz, self.s2, self.s4
        off1, off2 = b1 * s2, b1 * s2 + b2 * s4
        half = lambda: self.down(0, k, (1 - b1) * s2, s2, m1)
        quarter = lambda: self.down(1, k, off1 + (1 - b2) * s4, s4, m2)
        whole_1 = lambda: self.down(2, k, off2, s4, self.xy[0][0])
        whole_2 = lambda: self.down(3, k, off2, s4, self.xy[1][0])
        back4 = lambda: self.up(5, k, off2, s4, m2)
        back2 = lambda: self.up(6, k, off1, s2, m1)
        if i == 1:
            half().start()
        elif i == 2:
            half().wait_recv()
            self.add(k, off1, s2, self.landing[0])
            quarter().start()
        elif i == 3:
            quarter().wait_recv()
            self.add(k, off2, s4, self.landing[1])
            whole_1().start()
        elif i == 4:
            whole_1().wait_recv()
            whole_1().wait_send()
            self.add(k, off2, s4, self.landing[2])
            whole_2().start()
        elif i == 5:
            whole_2().wait_recv()
            self.finish(k, off2, s4, self.landing[3])
        elif i == 6:
            back4().start()
            half().wait_send()
            quarter().wait_send()
            whole_2().wait_send()
        elif i == 7:
            back4().wait_recv()
            back2().start()
        elif i == 8:
            back2().wait_recv()
        elif i == 10:
            back4().wait_send()
            back2().wait_send()

    def stage_l(self, i, k):
        s2, s4 = self.s2, self.s4
        s3 = s2 + s4
        b0, b1 = self.p.bz0, self.p.bz1
        own, side, tip, rest = (2 * b1 + b0) * s4, b1 * s2, 3 * b1 * s4, (1 - b1) * s4
        inward = lambda: self.down(0, k, rest, s3, self.z_mate)
        across = lambda: self.down(1, k, (1 - b1) * s2, s2, self.mid_mate)
        outward = lambda: self.down(2, k, tip, s4, self.z_mate)
        whole_1 = lambda: self.down(3, k, own, s4, self.xy[0][0])
        whole_2 = lambda: self.down(8, k, own, s4, self.xy[1][0], self.landing[4])
        tip_back = lambda: self.up(4, k, tip, s4, self.z_mate)
        side_back = lambda: self.up(5, k, side, s2, self.mid_mate)
        rest_back = lambda: self.up(6, k, rest, s3, self.z_mate)
        if i == 1:
            pl.when(self.end)(lambda: inward().start())
        elif i == 2:

            @pl.when(self.mid)
            def _():
                inward().wait_recv()
                self.add(k, rest, s3, self.landing[0])
                across().start()

        elif i == 3:

            @pl.when(self.mid)
            def _():
                across().wait_recv()
                self.add(k, side, s2, self.landing[1])
                outward().start()

        elif i == 4:

            @pl.when(self.end)
            def _():
                outward().wait_recv()
                self.add(k, own, s4, self.landing[2])

            whole_1().start()
        elif i == 5:
            whole_1().wait_recv()
            whole_1().wait_send()
            pl.when(self.mid)(lambda: outward().wait_send())
            self.add(k, own, s4, self.landing[3])
            whole_2().start()
        elif i == 6:
            whole_2().wait_recv()
            self.finish(k, own, s4, self.landing[4])
            pl.when(self.end)(lambda: tip_back().start())
            whole_2().wait_send()
            pl.when(self.end)(lambda: inward().wait_send())
            pl.when(self.mid)(lambda: across().wait_send())
        elif i == 7:

            @pl.when(self.mid)
            def _():
                tip_back().wait_recv()
                side_back().start()

        elif i == 8:

            @pl.when(self.mid)
            def _():
                side_back().wait_recv()
                rest_back().start()

        elif i == 9:
            pl.when(self.end)(lambda: rest_back().wait_recv())
        elif i == 10:
            pl.when(self.end)(lambda: tip_back().wait_send())

            @pl.when(self.mid)
            def _():
                side_back().wait_send()
                rest_back().wait_send()


def form_next(k, group, form):
    pl.when(k == 1)(lambda: form(group // 2, group // 2))
    pl.when((k % group == 0) & (k > 0))(lambda: form(k, group))


def run_slots(plan, count, stage, between):
    lags, order = plan

    def slot(t):
        for i in order:
            k = t - lags[i]

            @pl.when((k >= 0) & (k < count))
            def _():
                stage(i, k)

            if i == 1:
                between(t)

    loop(0, count + lags[-1], slot)


def chunk_scratch(slots, gather_slots, part_rows, width, count, dtype):
    def buf(n):
        return pltpu.VMEM((slots, n, width), jnp.float32)

    gathered = pltpu.VMEM((gather_slots, part_rows, width), dtype)

    dma = pltpu.SemaphoreType.DMA
    quarter = part_rows // 4
    return [buf(part_rows), gathered, *(buf(n * quarter) for n in (3, 2, 1, 1, 1)), dma((9, count)), dma((9, count))]


def fold(value):
    return jnp.sum(value.reshape(value.shape[0] // 8, 8, value.shape[1]), axis=0)


def front_kernel(feat_a, feat_b, w_in, t_in, w_mid, t_mid, w_out, t_out, gain1, bias1, gain2, bias2, off_weight, pre1, pre2, xs2, xs1, xs0, dz, grad_emb, vec, *scratch):
    (x_buf, u_buf, w_buf, stats, affine, loss, ea, eb, g_peer) = scratch[:9]
    (x_sem, w_sem, pre_sem, keep_sem, keep_send, keep_recv, ge_sem, e_send, e_recv) = scratch[9:18]
    small_refs = scratch[18 : 18 + SMALL_REFS]
    acc, gathered, *landing, send, recv = scratch[18 + SMALL_REFS :]
    rows_dev, width = feat_a.shape
    wide = w_buf.shape[2]
    tiles = width // wide
    half = width // 2
    part_rows = half // PARTS
    row_count = rows_dev * DEPTH * PLANE
    weights, feats = (w_in, t_in, w_mid, t_mid, w_out, t_out), (feat_a, feat_b)
    place = Place()
    core = place.core
    mine = rows(core * rows_dev, rows_dev)
    place.arrive()
    small = small_sum(place, small_refs)
    payload, total = small.payload, small.total

    def feat(v):
        return pltpu.make_async_copy(feats[v], x_buf.at[v], x_sem.at[v])

    def w_tile(ref, g):
        return pltpu.make_async_copy(ref.at[:, rows((g % tiles) * wide, wide)], w_buf.at[g % W_BUFS], w_sem.at[g % W_BUFS])

    def start_w(g):
        pick(g // tiles, weights, lambda ref: w_tile(ref, g).start())

    feat(0).start()
    w_tile(weights[0], 0).start()
    feat(1).start()
    for g in range(1, W_BUFS - 1):
        start_w(g)
    for j, ref in enumerate((gain1, bias1, gain2, bias2)):
        affine[j] = ref[...]
    feat(0).wait()
    payload[...] = jnp.zeros_like(payload)

    def keep_pre(ref):
        return pltpu.make_async_copy(u_buf.at[0], ref, pre_sem.at[0])

    kept = (xs0, xs1, xs2)

    def keep_x(w):
        here = pltpu.make_async_copy(x_buf.at[0, :, rows(core * half, half)], kept[w].at[mine], keep_sem.at[w])
        there = remote_copy(x_buf.at[0, :, rows((1 - core) * half, half)], kept[w].at[mine], keep_send.at[w], keep_recv.at[w], place.other_core)
        return here, there

    def start_x(w):
        for c in keep_x(w):
            c.start()

    def free_x(w):
        here, there = keep_x(w)
        here.wait()
        there.wait_send()

    def keep_dz(i):
        at = (slice(None), rows(i * wide, wide))
        here = pltpu.make_async_copy(x_buf.at[(0, *at)], dz.at[mine, at[1]], keep_sem.at[3 + i])
        there = remote_copy(x_buf.at[(0, *at)], dz.at[mine, at[1]], keep_send.at[3 + i], keep_recv.at[3 + i], place.other_core)
        return here, there

    def row_loop(body, carry):
        return lax.fori_loop(0, rows_dev // BLOCK, lambda r, c: body(rows(r * BLOCK, BLOCK), c), carry)

    def put_sums(j, i, row, value):
        value = jnp.sum(value, axis=0, keepdims=True)
        for c in range(value.shape[1] // TILE):
            payload[j, i + c, row : row + 1] = value[:, c * TILE : (c + 1) * TILE]

    def product(g):
        job, i = g // tiles, g % tiles
        view = job % 2
        w_tile(w_in, g).wait()
        pl.when(g + W_BUFS - 1 < JOBS * tiles)(lambda: start_w(g + W_BUFS - 1))
        at_cols = rows(i * wide, wide)
        u_buf[view, :, at_cols] = jnp.dot(x_buf[view], w_buf[g % W_BUFS], preferred_element_type=jnp.float32)

        def block(at, sums):
            u = u_buf[view, at, at_cols]
            return sums[0] + fold(u), sums[1] + fold(u * u)

        zero = jnp.zeros((8, wide), jnp.float32)
        for row, value in enumerate(row_loop(block, (zero, zero))):
            put_sums(job, i * (wide // TILE), row, value)

    def begin(job):
        small.begin(job)

        @pl.when(job % 2 == 0)
        def _():
            pick(job // 2, (pre1, pre2), lambda ref: keep_pre(ref).start())

    def norm(job):
        layer, view = job // 2, job % 2
        small.end(job)
        for c in range(PLANE):
            at = slice(c * TILE, (c + 1) * TILE)
            means = total[job, c] / row_count
            stats[job, 0, :, at] = means[0:1]
            stats[job, 1, :, at] = lax.rsqrt(means[1:2] - means[0:1] * means[0:1] + NORM_EPS)

        pl.when(view == 0)(lambda: pick(layer, (0, 1, 2), free_x))

        def hidden(i):
            at_cols = rows(i * wide, wide)
            mean, inv = stats[job, 0, :, at_cols], stats[job, 1, :, at_cols]
            gain, bias = affine[layer * 2, :, at_cols], affine[layer * 2 + 1, :, at_cols]

            def block(at, c):
                n = (u_buf[view, at, at_cols] - mean) * inv
                x_buf[view, at, at_cols] = jnp.maximum(n * gain + bias, 0.0).astype(jnp.bfloat16)
                return c

            row_loop(block, 0)

        def student(i):
            at_cols = rows(i * wide, wide)
            mean, inv = stats[job, 0, :, at_cols], stats[job, 1, :, at_cols]

            def block(at, c):
                n = (u_buf[0, at, at_cols] - mean) * inv
                u_buf[0, at, at_cols] = n
                x_buf[0, at, at_cols] = n.astype(jnp.bfloat16)
                return c

            row_loop(block, 0)

        def student_own(i):
            def block(r, c):
                ea[rows(core * rows_dev + r * BLOCK, BLOCK), rows(i * wide, wide)] = x_buf[0, rows(r * BLOCK, BLOCK), rows(core * half + i * wide, wide)]
                return c

            lax.fori_loop(0, rows_dev // BLOCK, block, 0)

        def teacher(i):
            at_cols = rows(i * wide, wide)
            mean, inv = stats[job, 0, :, at_cols], stats[job, 1, :, at_cols]

            def block(r, c):
                n = (u_buf[1, rows(r * BLOCK, BLOCK), at_cols] - mean) * inv
                eb[rows(core * rows_dev + r * BLOCK, BLOCK), at_cols] = n.astype(jnp.bfloat16)
                return c

            lax.fori_loop(0, rows_dev // BLOCK, block, 0)
            eb_copy(i).start()

        @pl.when(layer < 2)
        def _():
            loop(0, tiles, hidden)

            @pl.when(view == 0)
            def _():
                pick(layer, (1, 2), start_x)
                keep_pre(pre1).wait()

        @pl.when((layer == 2) & (view == 0))
        def _():
            loop(0, tiles, student)
            ea_copy().start()
            loop(0, tiles // 2, student_own)

        @pl.when((layer == 2) & (view == 1))
        def _():
            loop(0, tiles, teacher)

    ea_copy = lambda: remote_copy(x_buf.at[0, :, rows((1 - core) * half, half)], ea.at[mine], e_send.at[0], e_recv.at[0], place.other_core)

    def eb_copy(i):
        block = eb.at[mine, rows(i * wide, wide)]
        return remote_copy(block, block, e_send.at[1 + i], e_recv.at[1 + i], place.other_core)

    def step(g):
        job, i = g // tiles, g % tiles
        view = job % 2
        pl.when(g == tiles)(lambda: feat(1).wait())
        product(g)

        @pl.when(g == 0)
        def _():
            place.all_here()
            start_x(0)

        pl.when((i == 1) & (job > 0))(lambda: small.middle(job - 1))

        @pl.when(i == tiles - 1)
        def _():
            begin(job)
            pl.when(job > 0)(lambda: norm(job - 1))

    loop(0, JOBS * tiles, step)
    small.middle(JOBS - 1)
    norm(JOBS - 1)
    for j, source in enumerate((affine.at[2], affine.at[3], stats.at[2, 0], stats.at[2, 1], affine.at[0], affine.at[1], stats.at[0, 0], stats.at[0, 1])):
        vec[j] = source[...]

    loss[...] = jnp.zeros_like(loss)

    def finish(k, off, size, buf):
        share = jnp.where(front_kind("x", k), 0.5, 0.25)
        at = rows(off, size)
        corr = (acc[k, at] + buf[k]) / row_count
        row = core * half + k * part_rows + off
        diag = (row + lax.broadcasted_iota(jnp.int32, (size, width), 0)) == lax.broadcasted_iota(jnp.int32, (size, width), 1)
        weight = off_weight[0]
        miss = 1.0 - corr
        loss[...] += share * jnp.sum(jnp.where(diag, miss * miss, weight * (corr * corr)), axis=0, keepdims=True)
        gathered[k, at] = jnp.where(diag, -2.0 * miss, 2.0 * weight * corr).astype(jnp.bfloat16)

    def homes(k):
        return [(None, lambda off, size: gathered.at[k, pl.ds(pl.multiple_of(off, part_rows // 4), size)])]

    chunks = ChunkSum(place, "xsl", front_kind, acc, homes, landing, send, recv, finish)

    def form(k, group):
        at = rows(k * part_rows, group * part_rows)
        size = min(1024, width)

        def col(c):
            @pl.when(k == 0)
            def _():
                for i in range(size // wide):
                    eb_copy(c * (size // wide) + i).wait_recv()

            cs = rows(c * size, size)
            acc[pl.ds(k, group), :, cs] = contract_rows(ea[:, at], eb[:, cs]).reshape(group, part_rows, size)

        loop(0, width // size, col)

    def swap(k):
        return chunks.copy(gathered.at[k], g_peer.at[k], 7, k, place.other_core)

    def ge_cols(k, side):
        return rows(side * half + k * part_rows, GROUP * part_rows)

    def ge_copy(k, side):
        at = ge_cols(k, side)
        return pltpu.make_async_copy(u_buf.at[1, :, at], grad_emb.at[:, at], ge_sem.at[k // GROUP, side])

    def embed(k, side, g_rows):
        at_cols = ge_cols(k, side)
        grad = contract_cols(eb[mine], g_rows.reshape(GROUP * part_rows, width)) / row_count
        u_buf[1, :, at_cols] = grad
        ge_copy(k, side).start()

        def block(at, sums):
            g = u_buf[1, at, at_cols]
            return sums[0] + fold(g * u_buf[0, at, at_cols]), sums[1] + fold(g)

        zero = jnp.zeros((8, GROUP * part_rows), jnp.float32)
        for row, value in enumerate(row_loop(block, (zero, zero))):
            payload[JOBS, (side * half + k * part_rows) // TILE, row : row + 1] = jnp.sum(value, axis=0, keepdims=True)

    def stage(i, k):
        if i == 0:
            form_next(k, GROUP, form)
            return
        chunks.stage(i, k)
        if i == 8:
            pl.when(jnp.logical_not(front_kind("l", k)))(lambda: swap(k).start())
        if i == 9:
            pl.when(front_kind("l", k))(lambda: swap(k).start())

            @pl.when(k % GROUP == GROUP - 1)
            def _():
                embed(k - GROUP + 1, core, gathered[pl.ds(k - GROUP + 1, GROUP)])

        if i == 10:
            swap(k).wait_recv()
            swap(k).wait_send()

            @pl.when(k % GROUP == GROUP - 1)
            def _():
                embed(k - GROUP + 1, 1 - core, g_peer[pl.ds(k - GROUP + 1, GROUP)])

    ea_copy().wait_recv()
    form(0, GROUP // 2)
    run_slots(FRONT_PLAN, PARTS, stage, lambda t: None)
    small.begin(JOBS)
    for c in range(PLANE):
        payload[JOBS + 1, c, 0:1] = loss[:, c * TILE : (c + 1) * TILE]
    small.begin(JOBS + 1)
    ea_copy().wait_send()
    for i in range(tiles):
        eb_copy(i).wait_send()
    small.middle(JOBS)
    small.middle(JOBS + 1)
    for k in range(0, PARTS, GROUP):
        for side in range(2):
            ge_copy(k, side).wait()
    small.end(JOBS)

    def dz_tile(i):
        at_cols = rows(i * wide, wide)
        sums = jnp.concatenate([total[JOBS, i * (wide // TILE) + c] for c in range(wide // TILE)], axis=1) / row_count
        mean_gn, mean_g = sums[0:1], sums[1:2]
        inv = stats[JOBS - 2, 1, :, at_cols]

        def block(at, c):
            value = (u_buf[1, at, at_cols] - mean_g - u_buf[0, at, at_cols] * mean_gn) * inv
            x_buf[0, at, at_cols] = value.astype(jnp.bfloat16)
            return c

        row_loop(block, 0)
        for c in keep_dz(i):
            c.start()

    loop(0, tiles, dz_tile)
    small.end(JOBS + 1)
    for c in range(PLANE):
        vec[8, :, c * TILE : (c + 1) * TILE] = total[JOBS + 1, c, 0:1]
    for w in range(3):
        keep_x(w)[1].wait_recv()
    for i in range(tiles):
        here, there = keep_dz(i)
        here.wait()
        there.wait()


def front(feat_a, feat_b, weights, affine, off_weight):
    rows_dev, width = feat_a.shape
    half = width // 2
    part_rows = half // PARTS
    any_spec = pl.BlockSpec(memory_space=pl.ANY)
    vmem_spec = pl.BlockSpec(memory_space=pltpu.VMEM)
    wide_f32 = jax.ShapeDtypeStruct((rows_dev, width), jnp.float32)
    kept = jax.ShapeDtypeStruct((2 * rows_dev, half), jnp.bfloat16)
    both_dz = jax.ShapeDtypeStruct((2 * rows_dev, width), jnp.bfloat16)
    keeps = 3 + width // WIDE
    dma = pltpu.SemaphoreType.DMA
    return pl.pallas_call(
        front_kernel,
        name="front",
        out_shape=[wide_f32, wide_f32, kept, kept, kept, both_dz, wide_f32]
        + [jax.ShapeDtypeStruct((9, 1, width), jnp.float32)],
        in_specs=[any_spec] * 8 + [vmem_spec] * 4 + [pl.BlockSpec(memory_space=pltpu.SMEM)],
        out_specs=[any_spec] * 7 + [vmem_spec],
        scratch_shapes=[
            pltpu.VMEM((2, rows_dev, width), jnp.bfloat16),
            pltpu.VMEM((2, rows_dev, width), jnp.float32),
            pltpu.VMEM((W_BUFS, width, WIDE), jnp.bfloat16),
            pltpu.VMEM((JOBS, 2, 1, width), jnp.float32),
            pltpu.VMEM((4, 1, width), jnp.float32),
            pltpu.VMEM((1, width), jnp.float32),
            pltpu.VMEM((2 * rows_dev, half), jnp.bfloat16),
            pltpu.VMEM((2 * rows_dev, width), jnp.bfloat16),
            pltpu.VMEM((PARTS, part_rows, width), jnp.bfloat16),
            dma((2,)),
            dma((W_BUFS,)),
            dma((1,)),
            dma((keeps,)),
            dma((keeps,)),
            dma((keeps,)),
            dma((PARTS // GROUP, 2)),
            dma((1 + width // WIDE,)),
            dma((1 + width // WIDE,)),
        ]
        + small_scratch(JOBS + 2)
        + chunk_scratch(PARTS, PARTS, part_rows, width, PARTS, jnp.bfloat16),
        compiler_params=pltpu.CompilerParams(collective_id=0, has_side_effects=True, vmem_limit_bytes=VMEM_BYTES),
    )(feat_a, feat_b, *weights, *affine, off_weight)


def back_kernel(dz_hbm, x2, x1, x0, w_out, w_mid, u2, u1, vec, out2, out1, out0, sums_out, *scratch):
    (dy, xs, w_buf) = scratch[:3]
    (in_sem, tile_sem, peer_send, peer_recv, store_sem) = scratch[3:8]
    small_refs = scratch[8 : 8 + SMALL_REFS]
    acc, gathered, *landing, send, recv = scratch[8 + SMALL_REFS :]
    rows_dev, width = u2.shape
    wide = w_buf.shape[0]
    tiles = width // wide
    row_count = rows_dev * DEPTH * PLANE
    half = width // 2
    part_rows = half // BACK_PARTS
    count = MATS * BACK_PARTS
    mats_in, outs, weights, pres = (x2, x1, x0), (out2, out1), (w_out, w_mid), (u2, u1)
    dpre = out0.at[pl.ds(0, rows_dev)]

    def u_buf(i):
        return out0.at[pl.ds(rows_dev, rows_dev), rows((i % 2) * wide, wide)]

    place = Place()
    core, other_core = place.core, place.other_core
    mine = rows(core * rows_dev, rows_dev)
    place.arrive()
    small = small_sum(place, small_refs)
    payload, sums = small.payload, small.total

    def load_x(w):
        return pltpu.make_async_copy(mats_in[w], xs.at[w % 2], in_sem.at[w])

    def peer_dy(w):
        block = dy.at[w % 2, mine]
        return remote_copy(block, block, peer_send.at[w], peer_recv.at[w], other_core)

    def w_tile(ref, i):
        return pltpu.make_async_copy(ref.at[rows(i * wide, wide)], w_buf, tile_sem.at[0, 0])

    def u_tile(ref, i):
        return pltpu.make_async_copy(ref.at[:, rows(i * wide, wide)], u_buf(i), tile_sem.at[1, i % 2])

    def start_w(layer, i):
        pick(layer, weights, lambda ref: w_tile(ref, i).start())

    def start_u(layer, i):
        pick(layer, pres, lambda ref: u_tile(ref, i).start())

    size = min(1024, width)

    def load_dz(c):
        return pltpu.make_async_copy(dz_hbm.at[:, rows(c * size, size)], dy.at[0, :, rows(c * size, size)], in_sem.at[MATS + c])

    load_x(0).start()
    for c in range(width // size):
        load_dz(c).start()
    w_tile(weights[0], 0).start()
    u_tile(pres[0], 0).start()
    load_x(1).start()
    payload[...] = jnp.zeros_like(payload)

    def row_loop(body, carry):
        return lax.fori_loop(0, rows_dev // BLOCK, body, carry)

    def chain_tile(layer, i):
        w_tile(w_out, i).wait()
        u_tile(u2, i).wait()

        pl.when(i + 1 < tiles)(lambda: start_u(layer, i + 1))
        at_cols = rows(i * wide, wide)
        dpre[:, at_cols] = contract_cols(dy[layer, mine], w_buf[...])
        pl.when(i + 1 < tiles)(lambda: start_w(layer, i + 1))
        gain, bias, mean, inv = (vec[layer * 4 + j, :, at_cols] for j in range(4))

        def block(r, carry):
            at = rows(r * BLOCK, BLOCK)
            n = (out0[rows(rows_dev + r * BLOCK, BLOCK), rows((i % 2) * wide, wide)] - mean) * inv
            g = jnp.where(n * gain + bias > 0.0, dpre[at, at_cols], 0.0)
            dpre[at, at_cols] = g
            return carry[0] + fold(g * n), carry[1] + fold(g)

        zero = jnp.zeros((8, wide), jnp.float32)
        for row, value in enumerate(row_loop(block, (zero, zero))):
            value = jnp.sum(value, axis=0, keepdims=True)
            for c in range(wide // TILE):
                payload[layer, i * (wide // TILE) + c, row : row + 1] = value[:, c * TILE : (c + 1) * TILE]

    def du_tile(layer, i):
        u_tile(u2, i).wait()
        pl.when(i + 1 < tiles)(lambda: start_u(layer, i + 1))
        at_cols = rows(i * wide, wide)
        gain, mean, inv = (vec[layer * 4 + j, :, at_cols] for j in (0, 2, 3))
        means = jnp.concatenate([sums[layer, i * (wide // TILE) + c] for c in range(wide // TILE)], axis=1) / row_count
        mean_gn, mean_g = means[0:1], means[1:2]
        scale = gain * inv

        def block(r, c):
            at = rows(r * BLOCK, BLOCK)
            n = (out0[rows(rows_dev + r * BLOCK, BLOCK), rows((i % 2) * wide, wide)] - mean) * inv
            value = (dpre[at, at_cols] - mean_g - n * mean_gn) * scale
            dy[1 - layer, rows(core * rows_dev + r * BLOCK, BLOCK), at_cols] = value.astype(jnp.bfloat16)
            return c

        row_loop(block, 0)

    in_last = (MATS - 1) * BACK_PARTS
    quarter = part_rows // 4

    def home_row(k):
        return core * half + (k % BACK_PARTS) * part_rows

    def homes(k):
        return [
            (k < in_last, lambda off, size: gathered.at[k % GATHER_SLOTS, pl.ds(pl.multiple_of(off, quarter), size)]),
            (k >= in_last, lambda off, size: out0.at[pl.ds(pl.multiple_of(home_row(k) + off, quarter), size)]),
        ]

    def finish(k, off, size, buf):
        j = k % ACC_SLOTS
        value = acc[j, rows(off, size)] + buf[j]

        @pl.when(k < in_last)
        def _():
            gathered[k % GATHER_SLOTS, rows(off, size)] = value

        @pl.when(k >= in_last)
        def _():
            out0[rows(home_row(k) + off, size)] = value

    chunks = ChunkSum(place, "xl", back_kind, acc, homes, landing, send, recv, finish)

    def form(k, group):
        w, j = k // BACK_PARTS, k % ACC_SLOTS

        @pl.when(k % BACK_PARTS == 0)
        def _():
            pltpu.make_async_copy(xs.at[w % 2], xs.at[w % 2], in_sem.at[w]).wait()
            pl.when(w > 0)(lambda: peer_dy(w).wait_recv())

        at = rows((k % BACK_PARTS) * part_rows, group * part_rows)

        def col(c):
            pl.when(k == 0)(lambda: load_dz(c).wait())
            cs = rows(c * size, size)
            acc[pl.ds(j, group), :, cs] = contract_rows(xs[w % 2, :, at], dy[w % 2, :, cs]).reshape(group, part_rows, size)

        loop(0, width // size, col)

    def out_rows(k, side):
        return pl.ds(pl.multiple_of(side * half + (k % BACK_PARTS) * part_rows, part_rows), part_rows)

    def last_copy(out, k, side):
        return chunks.copy(gathered.at[k % GATHER_SLOTS], out.at[out_rows(k, side)], 7, k, other_core)

    def store_copy(out, k):
        return pltpu.make_async_copy(gathered.at[k % GATHER_SLOTS], out.at[out_rows(k, core)], store_sem.at[k])

    def stage(i, k):
        if i == 0:
            form_next(k, BACK_GROUP, form)
            return
        chunks.stage(i, k)
        own_rows = out0.at[pl.ds(pl.multiple_of(home_row(k), part_rows), part_rows)]
        in_place = chunks.copy(own_rows, own_rows, 7, k, other_core)
        last = k // BACK_PARTS == MATS - 1

        def emit(out):
            last_copy(out, k, core).start()
            store_copy(out, k).start()

        def emit_any():
            pick(k // BACK_PARTS, outs, emit)
            pl.when(last)(lambda: in_place.start())

        if i == 8:
            pl.when(back_kind("x", k))(emit_any)
        if i == 9:
            pl.when(back_kind("l", k))(emit_any)
        if i == 10:

            def close(out):
                last_copy(out, k, 1 - core).wait_recv()
                store_copy(out, k).wait()
                last_copy(out, k, core).wait_send()

            pick(k // BACK_PARTS, outs, close)

            @pl.when(last)
            def _():
                in_place.wait_recv()
                in_place.wait_send()

    def layer_work(t):
        layer = t // LAYER_SLOTS
        at = t - LAYER_SLOTS * layer
        first_du = 2 * tiles + 3
        pl.when((at < 2 * tiles) & (at % 2 == 1))(lambda: chain_tile(layer, at // 2))
        pl.when(at == 2 * tiles)(lambda: small.begin(layer))
        pl.when(at == 2 * tiles + 1)(lambda: small.middle(layer))

        pl.when(at == 2 * tiles + 2)(lambda: start_u(layer, 0))

        pl.when(at == first_du)(lambda: small.end(layer))
        pl.when(at >= first_du)(lambda: du_tile(layer, at - first_du))

        @pl.when(at == LAYER_SLOTS - 1)
        def _():
            peer_dy(layer + 1).start()

            @pl.when(layer == 0)
            def _():
                w_tile(weights[1], 0).start()
                u_tile(pres[1], 0).start()

            pl.when(layer == 1)(lambda: load_x(2).start())

    form(0, BACK_GROUP // 2)
    place.all_here()
    run_slots(BACK_PLAN, count, stage, lambda t: pl.when((t % 2 == 0) & (t < 4 * LAYER_SLOTS))(lambda: layer_work(t // 2)))
    for w in (1, 2):
        peer_dy(w).wait_send()
    for c in range(PLANE):
        for row in range(4):
            sums_out[row : row + 1, c * TILE : (c + 1) * TILE] = sums[row // 2, c, row % 2 : row % 2 + 1]
    sums_out[4:5] = jnp.full((1, width), jnp.sum(vec[8]))


def backward(grad_z, x2, x1, x0, w_out, w_mid, u2, u1, vec):
    rows_dev, width = u2.shape
    part_rows = width // 2 // BACK_PARTS
    count = MATS * BACK_PARTS
    any_spec = pl.BlockSpec(memory_space=pl.ANY)
    vmem_spec = pl.BlockSpec(memory_space=pltpu.VMEM)
    mat = jax.ShapeDtypeStruct((width, width), jnp.float32)
    dma = pltpu.SemaphoreType.DMA
    return pl.pallas_call(
        back_kernel,
        name="backward",
        out_shape=[mat, mat, pltpu.VMEM((width, width), jnp.float32), jax.ShapeDtypeStruct((5, width), jnp.float32)],
        in_specs=[any_spec] * 8 + [vmem_spec],
        out_specs=[any_spec] * 2 + [vmem_spec] * 2,
        scratch_shapes=[
            pltpu.VMEM((2, 2 * rows_dev, width), jnp.bfloat16),
            pltpu.VMEM((2, 2 * rows_dev, width // 2), jnp.bfloat16),
            pltpu.VMEM((WIDE, width), jnp.bfloat16),
            dma((MATS + 2,)),
            dma((2, 2)),
            dma((MATS,)),
            dma((MATS,)),
            dma((count,)),
        ]
        + small_scratch(2)
        + chunk_scratch(ACC_SLOTS, GATHER_SLOTS, part_rows, width, count, jnp.float32),
        compiler_params=pltpu.CompilerParams(collective_id=1, has_side_effects=True, vmem_limit_bytes=BACK_VMEM),
    )(grad_z, x2, x1, x0, w_out, w_mid, u2, u1, vec)


def copy_kernel(*refs):
    pairs = (len(refs) - 6 - 6) // 2
    ins, small, outs, small_outs = refs[:pairs], refs[pairs], refs[pairs + 1 : 2 * pairs + 1], refs[2 * pairs + 1 : -6]
    buf, small_buf, in_sem, out_sem, small_sem, near_sem = refs[-6:]
    blocks = [(i, r) for i in range(pairs - 1) for r in range(0, ins[i].shape[0], COPY_ROWS)]
    near = pltpu.make_async_copy(ins[-1], outs[-1], near_sem.at[0])

    def read(b):
        i, r = blocks[b]
        return pltpu.make_async_copy(ins[i].at[pl.ds(r, COPY_ROWS)], buf.at[b % COPY_BUFS], in_sem.at[b % COPY_BUFS])

    def write(b):
        i, r = blocks[b]
        return pltpu.make_async_copy(buf.at[b % COPY_BUFS], outs[i].at[pl.ds(r, COPY_ROWS)], out_sem.at[b % COPY_BUFS])

    for b in range(len(blocks)):
        read(b).start()
    small_read = pltpu.make_async_copy(small, small_buf, small_sem.at[4])
    small_read.start()

    def small_write(row):
        return pltpu.make_async_copy(small_buf.at[pl.ds(row, 1)], small_outs[row], small_sem.at[row])

    for b in range(len(blocks)):
        read(b).wait()
    near.start()
    for b in range(len(blocks)):
        write(b).start()
    small_read.wait()
    small_outs[4][...] = small_buf[4:5, :1]
    for row in range(4):
        small_write(row).start()
    for row in range(4):
        small_write(row).wait()
    near.wait()
    for b in range(len(blocks)):
        write(b).wait()


def copy_out(arrays, small):
    any_spec = pl.BlockSpec(memory_space=pl.ANY)
    vmem_spec = pl.BlockSpec(memory_space=pltpu.VMEM)
    dma = pltpu.SemaphoreType.DMA
    width = small.shape[1]
    row = jax.ShapeDtypeStruct((1, width), jnp.float32)
    return pl.pallas_call(
        copy_kernel,
        name="copy_out",
        out_shape=[jax.ShapeDtypeStruct(a.shape, a.dtype) for a in arrays] + [row] * 4 + [jax.ShapeDtypeStruct((1, 1), jnp.float32)],
        in_specs=[any_spec] * (len(arrays) - 1) + [vmem_spec, any_spec],
        out_specs=[any_spec] * (len(arrays) + 4) + [vmem_spec],
        scratch_shapes=[
            pltpu.VMEM((COPY_BUFS, COPY_ROWS, width), jnp.float32),
            pltpu.VMEM(small.shape, jnp.float32),
            dma((COPY_BUFS,)),
            dma((COPY_BUFS,)),
            dma((5,)),
            dma((1,)),
        ],
        compiler_params=pltpu.CompilerParams(vmem_limit_bytes=COPY_VMEM),
    )(*arrays[:-1], pltpu.with_memory_space_constraint(arrays[-1], pltpu.VMEM), small)


def solution(mesh):
    row_part = P(DATA_AXIS, None)
    replicated = P()

    def local_step(feat_a, feat_b, w_in, w_mid, w_out, t_in, t_mid, t_out, gain_1, bias_1, gain_2, bias_2, off_weight):
        affine = [v.reshape(1, -1) for v in (gain_1, bias_1, gain_2, bias_2)]
        pre_1, pre_2, xs_2, xs_1, xs_0, grad_z, grad_emb, vec = front(
            feat_a, feat_b, (w_in, t_in, w_mid, t_mid, w_out, t_out), affine, off_weight.reshape(1)
        )
        grad_w_out, grad_w_mid, grad_w_in, sums = backward(grad_z, xs_2, xs_1, xs_0, w_out, w_mid, pre_2, pre_1, vec)
        (grad_emb, grad_w_out, grad_w_mid, grad_w_in, gain_2, bias_2, gain_1, bias_1, loss) = copy_out((grad_emb, grad_w_out, grad_w_mid, grad_w_in), sums)
        gain_1, bias_1, gain_2, bias_2 = (v.reshape(-1) for v in (gain_1, bias_1, gain_2, bias_2))
        return (loss.reshape(()), grad_emb, grad_w_in, grad_w_mid, grad_w_out, gain_1, bias_1, gain_2, bias_2)

    return jax.shard_map(local_step, mesh=mesh, in_specs=(row_part, row_part) + (replicated,) * 11, out_specs=(replicated, row_part) + (replicated,) * 7, check_vma=False)
```

```python
import functools

import jax
import jax.numpy as jnp
from jax import lax
from jax.experimental import pallas as pl
from jax.experimental.pallas import tpu as pltpu
from jax.sharding import PartitionSpec as P

NORM_EPS = 1e-5
DATA_AXIS = "data"
MESH = pl.DeviceIdType.MESH
VMEM_BYTES = 67_043_328
PLANE = 8
DEPTH = 4
TILE = 256
WIDE = 512
BLOCK = 128
SUM_ROWS = 2
SUM_PARTS = ((0, 6), (6, 2))
PARTS = 16
GROUP = 4
MATS = 3
ACC_SLOTS = 16
GATHER_SLOTS = 14
BACK_VMEM = 49_800_000
COPY_VMEM = 42 * 1024 * 1024
JOBS = 6
W_BUFS = 3
LAYER_SLOTS = 15
COPY_ROWS = 256
COPY_BUFS = 18
FRONT_PLAN = ((0, 0, 3, 5, 7, 9, 12, 13, 16, 17, 18), (0, 6, 3, 4, 9, 10, 8, 5, 2, 7, 1))
BACK_PLAN = ((0, 0, 3, 5, 7, 8, 9, 11, 14, 17, 19), (0, 4, 8, 7, 10, 1, 2, 3, 5, 6, 9))


def front_kind(kind, k):
    s, l = (k % 5 == 2) & (k > 2), k == 2
    return {"s": s, "l": l, "x": (k % 5 != 2)}[kind]


def back_kind(kind, k):
    l = ((k % 5 == 2) & (k < 43)) | ((k % 5 == 0) & (k >= 10) & (k < 36))
    return l if kind == "l" else jnp.logical_not(l)


def contract_rows(left_op, right_op):
    return lax.dot_general(left_op, right_op, (((0,), (0,)), ((), ())), preferred_element_type=jnp.float32)


def contract_cols(left_op, right_op):
    return lax.dot_general(left_op, right_op, (((1,), (1,)), ((), ())), preferred_element_type=jnp.float32)


def rows(off, size):
    return pl.ds(pl.multiple_of(off, size), size)


def pick(index, choices, what):
    for i, c in enumerate(choices):
        pl.when(index == i)(functools.partial(what, c))


def loop(lo, hi, body):
    def step(i, carry):
        body(i)
        return carry

    lax.fori_loop(lo, hi, step, 0)


def remote_copy(src, dst, send, recv, mate):
    return pltpu.make_async_remote_copy(src, dst, send, recv, device_id=(mate,), device_id_type=MESH)


class Place:
    def __init__(self):
        me = lax.axis_index(DATA_AXIS)
        self.me = me
        self.pos, self.plane = me % PLANE, me // PLANE
        self.core, self.bx, self.by, self.bz0, self.bz1 = me % 2, (me // 2) % 2, (me // 4) % 2, (me // 8) % 2, (me // 16) % 2
        self.other_core = me + 1 - 2 * self.core
        self.mates = [(self.pos + d) % PLANE for d in range(1, PLANE)]
        self.levels = [(self.plane + d) % DEPTH for d in range(1, DEPTH)]

    def peers(self):
        return [self.plane * PLANE + m for m in self.mates] + [lv * PLANE + self.pos for lv in self.levels]

    def arrive(self):
        sem = pltpu.get_barrier_semaphore()
        for peer in self.peers():
            pl.semaphore_signal(sem, inc=1, device_id=(peer,), device_id_type=MESH)

    def all_here(self):
        pl.semaphore_wait(pltpu.get_barrier_semaphore(), PLANE + DEPTH - 2)


class SmallSum:
    def __init__(self, place, payload, total, depth_buf, line_sum, plane_buf, sems):
        self.p, self.payload, self.total = place, payload, total
        self.depth_buf, self.line_sum, self.plane_buf, self.sems = depth_buf, line_sum, plane_buf, sems

    def along(self, j, part, lv, slot):
        (s, r), at = self.sems[:2], pl.ds(*SUM_PARTS[part])
        n = part * DEPTH
        return remote_copy(self.payload.at[j, at], self.depth_buf.at[j, slot, at], s.at[j, n + lv], r.at[j, n + slot], lv * PLANE + self.p.pos)

    def within(self, j, part, m, slot):
        (s, r), at = self.sems[2:], pl.ds(*SUM_PARTS[part])
        n = part * PLANE
        return remote_copy(self.line_sum.at[j, at], self.plane_buf.at[j, slot, at], s.at[j, n + m], r.at[j, n + slot], self.p.plane * PLANE + m)

    def begin(self, j, part):
        at = pl.ds(*SUM_PARTS[part])
        for lv in self.p.levels:
            self.along(j, part, lv, self.p.plane).start()
        self.depth_buf[j, self.p.plane, at] = self.payload[j, at]

    def middle(self, j, part):
        at = pl.ds(*SUM_PARTS[part])
        for lv in self.p.levels:
            self.along(j, part, lv, lv).wait_recv()
        total = self.depth_buf[j, 0, at]
        for i in range(1, DEPTH):
            total = total + self.depth_buf[j, i, at]
        self.line_sum[j, at] = total
        for m in self.p.mates:
            self.within(j, part, m, self.p.pos).start()
        self.plane_buf[j, self.p.pos, at] = total

    def end(self, j):
        for part in range(len(SUM_PARTS)):
            for m in self.p.mates:
                self.within(j, part, m, m).wait_recv()
        total = self.plane_buf[j, 0]
        for i in range(1, PLANE):
            total = total + self.plane_buf[j, i]
        self.total[j] = total
        for part in range(len(SUM_PARTS)):
            for lv in self.p.levels:
                self.along(j, part, lv, self.p.plane).wait_send()
            for m in self.p.mates:
                self.within(j, part, m, self.p.pos).wait_send()


def small_scratch(count):
    def buf(*lead):
        return pltpu.VMEM((count, *lead, PLANE, SUM_ROWS, TILE), jnp.float32)

    return [buf(), buf(), buf(DEPTH), buf(), buf(PLANE)] + [pltpu.SemaphoreType.DMA((count, n * len(SUM_PARTS))) for n in (DEPTH, DEPTH, PLANE, PLANE)]


SMALL_REFS = 9


def small_sum(place, refs):
    return SmallSum(place, *refs[:5], refs[5:])


class Homed:
    def __init__(self, homes, make):
        self.homes, self.make = homes, make

    def do(self, what):
        for when, home in self.homes:
            run = lambda home=home: getattr(self.make(home), what)()
            run() if when is None else pl.when(when)(run)

    def start(self):
        self.do("start")

    def wait_recv(self):
        self.do("wait_recv")

    def wait_send(self):
        self.do("wait_send")


class ChunkSum:
    def __init__(self, place, kinds, is_kind, acc, homes, landing, send, recv, finish):
        self.p, self.kinds, self.is_kind, self.slots, self.homes = place, kinds, is_kind, acc.shape[0], homes
        self.acc, self.landing, self.send, self.recv, self.finish = acc, landing, send, recv, finish
        self.size = acc.shape[1]
        self.s2, self.s4 = self.size // 2, self.size // 4
        core, bx, by, me = place.core, place.bx, place.by, place.me
        first, second = core * by + (1 - core) * bx, core * bx + (1 - core) * by
        self.xy = ((me + (2 + 2 * core) * (1 - 2 * first), first), (me + (4 - 2 * core) * (1 - 2 * second), second))
        self.zz = ((me + 8 * (1 - 2 * place.bz0), place.bz0), (me + 16 * (1 - 2 * place.bz1), place.bz1))
        self.is_mid = place.bz0 + place.bz1 - 2 * place.bz0 * place.bz1
        self.mid, self.end = self.is_mid == 1, self.is_mid == 0
        self.z_mate = self.zz[0][0]
        self.mid_mate = me + 8 * (1 - 2 * place.bz1)

    def copy(self, src, dst, stage, k, mate):
        return remote_copy(src, dst, self.send.at[stage, k], self.recv.at[stage, k], mate)

    def span(self, off, size):
        return pl.ds(pl.multiple_of(off, self.s4), size)

    def down(self, stage, k, off, size, mate, buf=None):
        j = k % self.slots
        buf = self.landing[stage] if buf is None else buf
        return self.copy(self.acc.at[j, self.span(off, size)], buf.at[j, pl.ds(0, size)], stage, k, mate)

    def up(self, stage, k, off, size, mate):
        return Homed(self.homes(k), lambda home: self.copy(home(off, size), home(off, size), stage, k, mate))

    def add(self, k, off, size, buf):
        step = min(size, 16)
        j = k % self.slots

        def body(i):
            at = pl.ds(pl.multiple_of(off + i * step, step), step)
            self.acc[j, at] = self.acc[j, at] + buf[j, rows(i * step, step)]

        loop(0, size // step, body)

    def stage(self, i, k):
        for kind in self.kinds:
            run = {"x": self.stage_x, "s": self.stage_s, "l": self.stage_l}[kind]
            pl.when(self.is_kind(kind, k))(functools.partial(run, i, k))

    def stage_x(self, i, k):
        (m1, b1), (m2, b2), s2, s4 = *self.xy, self.s2, self.s4
        off1, off2 = b1 * s2, b1 * s2 + b2 * s4
        half = lambda: self.down(0, k, (1 - b1) * s2, s2, m1)
        quarter = lambda: self.down(1, k, off1 + (1 - b2) * s4, s4, m2)
        inward = lambda: self.down(2, k, off2, s4, self.z_mate)
        across = lambda: self.down(3, k, off2, s4, self.mid_mate)
        outward = lambda: self.up(4, k, off2, s4, self.z_mate)
        back4 = lambda: self.up(5, k, off2, s4, m2)
        back2 = lambda: self.up(6, k, off1, s2, m1)
        if i == 1:
            half().start()
        elif i == 2:
            half().wait_recv()
            self.add(k, off1, s2, self.landing[0])
            quarter().start()
        elif i == 3:
            quarter().wait_recv()
            self.add(k, off2, s4, self.landing[1])
            pl.when(self.end)(lambda: inward().start())
        elif i == 4:

            @pl.when(self.mid)
            def _():
                inward().wait_recv()
                self.add(k, off2, s4, self.landing[2])
                across().start()

        elif i == 5:

            @pl.when(self.mid)
            def _():
                across().wait_recv()
                self.finish(k, off2, s4, self.landing[3])
                outward().start()

        elif i == 6:
            pl.when(self.end)(lambda: outward().wait_recv())
            back4().start()
            half().wait_send()
            quarter().wait_send()
            pl.when(self.end)(lambda: inward().wait_send())
            pl.when(self.mid)(lambda: across().wait_send())
        elif i == 7:
            back4().wait_recv()
            back2().start()
        elif i == 8:
            back2().wait_recv()
        elif i == 10:
            pl.when(self.mid)(lambda: outward().wait_send())
            back4().wait_send()
            back2().wait_send()

    def stage_s(self, i, k):
        (m1, b1), (m2, b2), s2, s4 = *self.zz, self.s2, self.s4
        off1, off2 = b1 * s2, b1 * s2 + b2 * s4
        half = lambda: self.down(0, k, (1 - b1) * s2, s2, m1)
        quarter = lambda: self.down(1, k, off1 + (1 - b2) * s4, s4, m2)
        whole_1 = lambda: self.down(2, k, off2, s4, self.xy[0][0])
        whole_2 = lambda: self.down(3, k, off2, s4, self.xy[1][0])
        back4 = lambda: self.up(5, k, off2, s4, m2)
        back2 = lambda: self.up(6, k, off1, s2, m1)
        if i == 1:
            half().start()
        elif i == 2:
            half().wait_recv()
            self.add(k, off1, s2, self.landing[0])
            quarter().start()
        elif i == 3:
            quarter().wait_recv()
            self.add(k, off2, s4, self.landing[1])
            whole_1().start()
        elif i == 4:
            whole_1().wait_recv()
            whole_1().wait_send()
            self.add(k, off2, s4, self.landing[2])
            whole_2().start()
        elif i == 5:
            whole_2().wait_recv()
            self.finish(k, off2, s4, self.landing[3])
        elif i == 6:
            back4().start()
            half().wait_send()
            quarter().wait_send()
            whole_2().wait_send()
        elif i == 7:
            back4().wait_recv()
            back2().start()
        elif i == 8:
            back2().wait_recv()
        elif i == 10:
            back4().wait_send()
            back2().wait_send()

    def stage_l(self, i, k):
        s2, s4 = self.s2, self.s4
        s3 = s2 + s4
        b0, b1 = self.p.bz0, self.p.bz1
        own, side, tip, rest = (2 * b1 + b0) * s4, b1 * s2, 3 * b1 * s4, (1 - b1) * s4
        inward = lambda: self.down(0, k, rest, s3, self.z_mate)
        across = lambda: self.down(1, k, (1 - b1) * s2, s2, self.mid_mate)
        outward = lambda: self.down(2, k, tip, s4, self.z_mate)
        whole_1 = lambda: self.down(3, k, own, s4, self.xy[0][0])
        whole_2 = lambda: self.down(8, k, own, s4, self.xy[1][0], self.landing[4])
        tip_back = lambda: self.up(4, k, tip, s4, self.z_mate)
        side_back = lambda: self.up(5, k, side, s2, self.mid_mate)
        rest_back = lambda: self.up(6, k, rest, s3, self.z_mate)
        if i == 1:
            pl.when(self.end)(lambda: inward().start())
        elif i == 2:

            @pl.when(self.mid)
            def _():
                inward().wait_recv()
                self.add(k, rest, s3, self.landing[0])
                across().start()

        elif i == 3:

            @pl.when(self.mid)
            def _():
                across().wait_recv()
                self.add(k, side, s2, self.landing[1])
                outward().start()

        elif i == 4:

            @pl.when(self.end)
            def _():
                outward().wait_recv()
                self.add(k, own, s4, self.landing[2])

            whole_1().start()
        elif i == 5:
            whole_1().wait_recv()
            whole_1().wait_send()
            pl.when(self.mid)(lambda: outward().wait_send())
            self.add(k, own, s4, self.landing[3])
            whole_2().start()
        elif i == 6:
            whole_2().wait_recv()
            self.finish(k, own, s4, self.landing[4])
            pl.when(self.end)(lambda: tip_back().start())
            whole_2().wait_send()
            pl.when(self.end)(lambda: inward().wait_send())
            pl.when(self.mid)(lambda: across().wait_send())
        elif i == 7:

            @pl.when(self.mid)
            def _():
                tip_back().wait_recv()
                side_back().start()

        elif i == 8:

            @pl.when(self.mid)
            def _():
                side_back().wait_recv()
                rest_back().start()

        elif i == 9:
            pl.when(self.end)(lambda: rest_back().wait_recv())
        elif i == 10:
            pl.when(self.end)(lambda: tip_back().wait_send())

            @pl.when(self.mid)
            def _():
                side_back().wait_send()
                rest_back().wait_send()


def form_next(k, form):
    pl.when(k == 1)(lambda: form(GROUP // 2, GROUP // 2))
    pl.when((k % GROUP == 0) & (k > 0))(lambda: form(k, GROUP))


def run_slots(plan, count, stage, between):
    lags, order = plan

    def slot(t):
        for i in order:
            k = t - lags[i]

            @pl.when((k >= 0) & (k < count))
            def _():
                stage(i, k)

            if i == 1:
                between(t)

    loop(0, count + lags[-1], slot)


def chunk_scratch(slots, gather_slots, part_rows, width, count, dtype):
    def buf(n):
        return pltpu.VMEM((slots, n, width), jnp.float32)

    gathered = pltpu.VMEM((gather_slots, part_rows, width), dtype)

    dma = pltpu.SemaphoreType.DMA
    quarter = part_rows // 4
    return [buf(part_rows), gathered, *(buf(n * quarter) for n in (3, 2, 1, 1, 1)), dma((9, count)), dma((9, count))]


def fold(value):
    return jnp.sum(value.reshape(value.shape[0] // 8, 8, value.shape[1]), axis=0)


def front_kernel(feat_a, feat_b, w_in, t_in, w_mid, t_mid, w_out, t_out, gain1, bias1, gain2, bias2, off_weight, pre1, pre2, xs2, xs1, xs0, dz, grad_emb, vec, *scratch):
    (x_buf, u_buf, w_buf, stats, affine, loss, ea, eb, g_peer) = scratch[:9]
    (x_sem, w_sem, pre_sem, keep_sem, keep_send, keep_recv, ge_sem, e_send, e_recv) = scratch[9:18]
    small_refs = scratch[18 : 18 + SMALL_REFS]
    acc, gathered, *landing, send, recv = scratch[18 + SMALL_REFS :]
    rows_dev, width = feat_a.shape
    wide = w_buf.shape[2]
    tiles = width // wide
    half = width // 2
    part_rows = half // PARTS
    row_count = rows_dev * DEPTH * PLANE
    weights, feats = (w_in, t_in, w_mid, t_mid, w_out, t_out), (feat_a, feat_b)
    place = Place()
    core = place.core
    mine = rows(core * rows_dev, rows_dev)
    place.arrive()
    small = small_sum(place, small_refs)
    payload, total = small.payload, small.total

    def feat(v):
        return pltpu.make_async_copy(feats[v], x_buf.at[v], x_sem.at[v])

    def w_tile(ref, g):
        return pltpu.make_async_copy(ref.at[:, rows((g % tiles) * wide, wide)], w_buf.at[g % W_BUFS], w_sem.at[g % W_BUFS])

    def start_w(g):
        pick(g // tiles, weights, lambda ref: w_tile(ref, g).start())

    feat(0).start()
    w_tile(weights[0], 0).start()
    feat(1).start()
    for g in range(1, W_BUFS - 1):
        start_w(g)
    for j, ref in enumerate((gain1, bias1, gain2, bias2)):
        affine[j] = ref[...]
    feat(0).wait()
    payload[...] = jnp.zeros_like(payload)

    def keep_pre(ref):
        return pltpu.make_async_copy(u_buf.at[0], ref, pre_sem.at[0])

    kept = (xs0, xs1, xs2)

    def keep_x(w):
        here = pltpu.make_async_copy(x_buf.at[0, :, rows(core * half, half)], kept[w].at[mine], keep_sem.at[w])
        there = remote_copy(x_buf.at[0, :, rows((1 - core) * half, half)], kept[w].at[mine], keep_send.at[w], keep_recv.at[w], place.other_core)
        return here, there

    def start_x(w):
        for c in keep_x(w):
            c.start()

    def free_x(w):
        here, there = keep_x(w)
        here.wait()
        there.wait_send()

    def keep_dz(i):
        at = (slice(None), rows(i * wide, wide))
        here = pltpu.make_async_copy(x_buf.at[(0, *at)], dz.at[mine, at[1]], keep_sem.at[3 + i])
        there = remote_copy(x_buf.at[(0, *at)], dz.at[mine, at[1]], keep_send.at[3 + i], keep_recv.at[3 + i], place.other_core)
        return here, there

    def row_loop(body, carry):
        return lax.fori_loop(0, rows_dev // BLOCK, lambda r, c: body(rows(r * BLOCK, BLOCK), c), carry)

    def put_sums(j, i, row, value):
        value = jnp.sum(value, axis=0, keepdims=True)
        for c in range(value.shape[1] // TILE):
            payload[j, i + c, row : row + 1] = value[:, c * TILE : (c + 1) * TILE]

    def product(g):
        job, i = g // tiles, g % tiles
        view = job % 2
        w_tile(w_in, g).wait()
        pl.when(g + W_BUFS - 1 < JOBS * tiles)(lambda: start_w(g + W_BUFS - 1))
        at_cols = rows(i * wide, wide)
        u_buf[view, :, at_cols] = jnp.dot(x_buf[view], w_buf[g % W_BUFS], preferred_element_type=jnp.float32)

        def block(at, sums):
            u = u_buf[view, at, at_cols]
            return sums[0] + fold(u), sums[1] + fold(u * u)

        zero = jnp.zeros((8, wide), jnp.float32)
        for row, value in enumerate(row_loop(block, (zero, zero))):
            put_sums(job, i * (wide // TILE), row, value)

    def keep(job):
        @pl.when(job % 2 == 0)
        def _():
            pick(job // 2, (pre1, pre2), lambda ref: keep_pre(ref).start())

    def norm(job):
        layer, view = job // 2, job % 2
        small.end(job)
        for c in range(PLANE):
            at = slice(c * TILE, (c + 1) * TILE)
            means = total[job, c] / row_count
            stats[job, 0, :, at] = means[0:1]
            stats[job, 1, :, at] = lax.rsqrt(means[1:2] - means[0:1] * means[0:1] + NORM_EPS)

        pl.when(view == 0)(lambda: pick(layer, (0, 1, 2), free_x))

        def hidden(i):
            at_cols = rows(i * wide, wide)
            mean, inv = stats[job, 0, :, at_cols], stats[job, 1, :, at_cols]
            gain, bias = affine[layer * 2, :, at_cols], affine[layer * 2 + 1, :, at_cols]

            def block(at, c):
                n = (u_buf[view, at, at_cols] - mean) * inv
                x_buf[view, at, at_cols] = jnp.maximum(n * gain + bias, 0.0).astype(jnp.bfloat16)
                return c

            row_loop(block, 0)

        def student(i):
            at_cols = rows(i * wide, wide)
            mean, inv = stats[job, 0, :, at_cols], stats[job, 1, :, at_cols]

            def block(at, c):
                n = (u_buf[0, at, at_cols] - mean) * inv
                u_buf[0, at, at_cols] = n
                x_buf[0, at, at_cols] = n.astype(jnp.bfloat16)
                return c

            row_loop(block, 0)

        def student_own(i):
            def block(r, c):
                ea[rows(core * rows_dev + r * BLOCK, BLOCK), rows(i * wide, wide)] = x_buf[0, rows(r * BLOCK, BLOCK), rows(core * half + i * wide, wide)]
                return c

            lax.fori_loop(0, rows_dev // BLOCK, block, 0)

        def teacher(i):
            at_cols = rows(i * wide, wide)
            mean, inv = stats[job, 0, :, at_cols], stats[job, 1, :, at_cols]

            def block(r, c):
                n = (u_buf[1, rows(r * BLOCK, BLOCK), at_cols] - mean) * inv
                eb[rows(core * rows_dev + r * BLOCK, BLOCK), at_cols] = n.astype(jnp.bfloat16)
                return c

            lax.fori_loop(0, rows_dev // BLOCK, block, 0)
            eb_copy(i).start()

        @pl.when(layer < 2)
        def _():
            loop(0, tiles, hidden)

            @pl.when(view == 0)
            def _():
                pick(layer, (1, 2), start_x)
                keep_pre(pre1).wait()

        @pl.when((layer == 2) & (view == 0))
        def _():
            loop(0, tiles, student)
            ea_copy().start()
            loop(0, tiles // 2, student_own)

        @pl.when((layer == 2) & (view == 1))
        def _():
            loop(0, tiles, teacher)

    ea_copy = lambda: remote_copy(x_buf.at[0, :, rows((1 - core) * half, half)], ea.at[mine], e_send.at[0], e_recv.at[0], place.other_core)

    def eb_copy(i):
        block = eb.at[mine, rows(i * wide, wide)]
        return remote_copy(block, block, e_send.at[1 + i], e_recv.at[1 + i], place.other_core)

    def step(g):
        job, i = g // tiles, g % tiles
        view = job % 2
        pl.when(g == tiles)(lambda: feat(1).wait())
        product(g)

        @pl.when(g == 0)
        def _():
            place.all_here()
            start_x(0)

        pl.when(i == tiles - 2)(lambda: small.begin(job, 0))
        pl.when((i == 0) & (job > 0))(lambda: small.middle(job - 1, 0))
        pl.when((i == 1) & (job > 0))(lambda: small.middle(job - 1, 1))

        @pl.when(i == tiles - 1)
        def _():
            small.begin(job, 1)
            keep(job)
            pl.when(job == JOBS - 1)(lambda: small.middle(job, 0))
            pl.when(job > 0)(lambda: norm(job - 1))

    loop(0, JOBS * tiles, step)
    small.middle(JOBS - 1, 1)
    norm(JOBS - 1)
    for j, source in enumerate((affine.at[2], affine.at[3], stats.at[2, 0], stats.at[2, 1], affine.at[0], affine.at[1], stats.at[0, 0], stats.at[0, 1])):
        vec[j] = source[...]

    loss[...] = jnp.zeros_like(loss)

    def finish(k, off, size, buf):
        share = jnp.where(front_kind("x", k), 0.5, 0.25)
        at = rows(off, size)
        corr = (acc[k, at] + buf[k]) / row_count
        row = core * half + k * part_rows + off
        diag = (row + lax.broadcasted_iota(jnp.int32, (size, width), 0)) == lax.broadcasted_iota(jnp.int32, (size, width), 1)
        weight = off_weight[0]
        miss = 1.0 - corr
        loss[...] += share * jnp.sum(jnp.where(diag, miss * miss, weight * (corr * corr)), axis=0, keepdims=True)
        gathered[k, at] = jnp.where(diag, -2.0 * miss, 2.0 * weight * corr).astype(jnp.bfloat16)

    def homes(k):
        return [(None, lambda off, size: gathered.at[k, pl.ds(pl.multiple_of(off, part_rows // 4), size)])]

    chunks = ChunkSum(place, "xsl", front_kind, acc, homes, landing, send, recv, finish)

    def form(k, group):
        at = rows(k * part_rows, group * part_rows)
        size = min(1024, width)

        def col(c):
            @pl.when(k == 0)
            def _():
                for i in range(size // wide):
                    eb_copy(c * (size // wide) + i).wait_recv()

            cs = rows(c * size, size)
            acc[pl.ds(k, group), :, cs] = contract_rows(ea[:, at], eb[:, cs]).reshape(group, part_rows, size)

        loop(0, width // size, col)

    def swap(k):
        return chunks.copy(gathered.at[k], g_peer.at[k], 7, k, place.other_core)

    def ge_cols(k, side):
        return rows(side * half + k * part_rows, GROUP * part_rows)

    def ge_copy(k, side):
        at = ge_cols(k, side)
        return pltpu.make_async_copy(u_buf.at[1, :, at], grad_emb.at[:, at], ge_sem.at[k // GROUP, side])

    def embed(k, side, g_rows):
        at_cols = ge_cols(k, side)
        grad = contract_cols(eb[mine], g_rows.reshape(GROUP * part_rows, width)) / row_count
        u_buf[1, :, at_cols] = grad
        ge_copy(k, side).start()

        def block(at, sums):
            g = u_buf[1, at, at_cols]
            return sums[0] + fold(g * u_buf[0, at, at_cols]), sums[1] + fold(g)

        zero = jnp.zeros((8, GROUP * part_rows), jnp.float32)
        for row, value in enumerate(row_loop(block, (zero, zero))):
            payload[JOBS, 2 * (k // GROUP) + side, row : row + 1] = jnp.sum(value, axis=0, keepdims=True)

    def stage(i, k):
        if i == 0:
            form_next(k, form)
            return
        chunks.stage(i, k)
        if i == 8:
            pl.when(jnp.logical_not(front_kind("l", k)))(lambda: swap(k).start())
        if i == 9:
            pl.when(front_kind("l", k))(lambda: swap(k).start())

            @pl.when(k % GROUP == GROUP - 1)
            def _():
                embed(k - GROUP + 1, core, gathered[pl.ds(k - GROUP + 1, GROUP)])

        if i == 10:
            swap(k).wait_recv()
            swap(k).wait_send()

            @pl.when(k % GROUP == GROUP - 1)
            def _():
                embed(k - GROUP + 1, 1 - core, g_peer[pl.ds(k - GROUP + 1, GROUP)])

            pl.when(k == PARTS - GROUP - 1)(lambda: small.begin(JOBS, 0))
            pl.when(k == PARTS - 2)(lambda: small.middle(JOBS, 0))

    ea_copy().wait_recv()
    form(0, GROUP // 2)
    run_slots(FRONT_PLAN, PARTS, stage, lambda t: None)
    small.begin(JOBS, 1)
    for c in range(PLANE):
        payload[JOBS + 1, c, 0:1] = loss[:, c * TILE : (c + 1) * TILE]
    ea_copy().wait_send()
    for i in range(tiles):
        eb_copy(i).wait_send()
    small.middle(JOBS, 1)
    for part in range(len(SUM_PARTS)):
        small.begin(JOBS + 1, part)
    for k in range(0, PARTS, GROUP):
        for side in range(2):
            ge_copy(k, side).wait()
    small.end(JOBS)

    def dz_tile(i):
        at_cols = rows(i * wide, wide)
        groups, side = tiles // 2, i // (tiles // 2)
        first = (i % groups) * (wide // TILE)
        sums = jnp.concatenate([total[JOBS, 2 * (first + c) + side] for c in range(wide // TILE)], axis=1) / row_count
        mean_gn, mean_g = sums[0:1], sums[1:2]
        inv = stats[JOBS - 2, 1, :, at_cols]

        def block(at, c):
            value = (u_buf[1, at, at_cols] - mean_g - u_buf[0, at, at_cols] * mean_gn) * inv
            x_buf[0, at, at_cols] = value.astype(jnp.bfloat16)
            return c

        row_loop(block, 0)
        for c in keep_dz(i):
            c.start()

    loop(0, tiles, dz_tile)
    for part in range(len(SUM_PARTS)):
        small.middle(JOBS + 1, part)
    small.end(JOBS + 1)
    for c in range(PLANE):
        vec[8, :, c * TILE : (c + 1) * TILE] = total[JOBS + 1, c, 0:1]
    for w in range(3):
        keep_x(w)[1].wait_recv()
    for i in range(tiles):
        here, there = keep_dz(i)
        here.wait()
        there.wait()


def front(feat_a, feat_b, weights, affine, off_weight):
    rows_dev, width = feat_a.shape
    half = width // 2
    part_rows = half // PARTS
    any_spec = pl.BlockSpec(memory_space=pl.ANY)
    vmem_spec = pl.BlockSpec(memory_space=pltpu.VMEM)
    wide_f32 = jax.ShapeDtypeStruct((rows_dev, width), jnp.float32)
    kept = jax.ShapeDtypeStruct((2 * rows_dev, half), jnp.bfloat16)
    both_dz = jax.ShapeDtypeStruct((2 * rows_dev, width), jnp.bfloat16)
    keeps = 3 + width // WIDE
    dma = pltpu.SemaphoreType.DMA
    return pl.pallas_call(
        front_kernel,
        name="front",
        out_shape=[wide_f32, wide_f32, kept, kept, kept, both_dz, wide_f32]
        + [jax.ShapeDtypeStruct((9, 1, width), jnp.float32)],
        in_specs=[any_spec] * 8 + [vmem_spec] * 4 + [pl.BlockSpec(memory_space=pltpu.SMEM)],
        out_specs=[any_spec] * 7 + [vmem_spec],
        scratch_shapes=[
            pltpu.VMEM((2, rows_dev, width), jnp.bfloat16),
            pltpu.VMEM((2, rows_dev, width), jnp.float32),
            pltpu.VMEM((W_BUFS, width, WIDE), jnp.bfloat16),
            pltpu.VMEM((JOBS, 2, 1, width), jnp.float32),
            pltpu.VMEM((4, 1, width), jnp.float32),
            pltpu.VMEM((1, width), jnp.float32),
            pltpu.VMEM((2 * rows_dev, half), jnp.bfloat16),
            pltpu.VMEM((2 * rows_dev, width), jnp.bfloat16),
            pltpu.VMEM((PARTS, part_rows, width), jnp.bfloat16),
            dma((2,)),
            dma((W_BUFS,)),
            dma((1,)),
            dma((keeps,)),
            dma((keeps,)),
            dma((keeps,)),
            dma((PARTS // GROUP, 2)),
            dma((1 + width // WIDE,)),
            dma((1 + width // WIDE,)),
        ]
        + small_scratch(JOBS + 2)
        + chunk_scratch(PARTS, PARTS, part_rows, width, PARTS, jnp.bfloat16),
        compiler_params=pltpu.CompilerParams(collective_id=0, has_side_effects=True, vmem_limit_bytes=VMEM_BYTES),
    )(feat_a, feat_b, *weights, *affine, off_weight)


def back_kernel(dz_hbm, x2, x1, x0, w_out, w_mid, u2, u1, vec, out2, out1, out0, sums_out, *scratch):
    (dy, xs, w_buf) = scratch[:3]
    (in_sem, tile_sem, peer_send, peer_recv, store_sem) = scratch[3:8]
    small_refs = scratch[8 : 8 + SMALL_REFS]
    acc, gathered, *landing, send, recv = scratch[8 + SMALL_REFS :]
    rows_dev, width = u2.shape
    wide = w_buf.shape[0]
    tiles = width // wide
    row_count = rows_dev * DEPTH * PLANE
    half = width // 2
    part_rows = half // PARTS
    count = MATS * PARTS
    mats_in, outs, weights, pres = (x2, x1, x0), (out2, out1), (w_out, w_mid), (u2, u1)
    dpre = out0.at[pl.ds(0, rows_dev)]

    def u_buf(i):
        return out0.at[pl.ds(rows_dev, rows_dev), rows((i % 2) * wide, wide)]

    place = Place()
    core, other_core = place.core, place.other_core
    mine = rows(core * rows_dev, rows_dev)
    place.arrive()
    small = small_sum(place, small_refs)
    payload, sums = small.payload, small.total

    def load_x(w):
        return pltpu.make_async_copy(mats_in[w], xs.at[w % 2], in_sem.at[w])

    def peer_dy(w):
        block = dy.at[w % 2, mine]
        return remote_copy(block, block, peer_send.at[w], peer_recv.at[w], other_core)

    def w_tile(ref, i):
        return pltpu.make_async_copy(ref.at[rows(i * wide, wide)], w_buf, tile_sem.at[0, 0])

    def u_tile(ref, i):
        return pltpu.make_async_copy(ref.at[:, rows(i * wide, wide)], u_buf(i), tile_sem.at[1, i % 2])

    def start_w(layer, i):
        pick(layer, weights, lambda ref: w_tile(ref, i).start())

    def start_u(layer, i):
        pick(layer, pres, lambda ref: u_tile(ref, i).start())

    size = min(1024, width)

    def load_dz(c):
        return pltpu.make_async_copy(dz_hbm.at[:, rows(c * size, size)], dy.at[0, :, rows(c * size, size)], in_sem.at[MATS + c])

    load_x(0).start()
    for c in range(width // size):
        load_dz(c).start()
    w_tile(weights[0], 0).start()
    u_tile(pres[0], 0).start()
    load_x(1).start()
    payload[...] = jnp.zeros_like(payload)

    def row_loop(body, carry):
        return lax.fori_loop(0, rows_dev // BLOCK, body, carry)

    def chain_tile(layer, i):
        w_tile(w_out, i).wait()
        u_tile(u2, i).wait()

        pl.when(i + 1 < tiles)(lambda: start_u(layer, i + 1))
        at_cols = rows(i * wide, wide)
        dpre[:, at_cols] = contract_cols(dy[layer, mine], w_buf[...])
        pl.when(i + 1 < tiles)(lambda: start_w(layer, i + 1))
        gain, bias, mean, inv = (vec[layer * 4 + j, :, at_cols] for j in range(4))

        def block(r, carry):
            at = rows(r * BLOCK, BLOCK)
            n = (out0[rows(rows_dev + r * BLOCK, BLOCK), rows((i % 2) * wide, wide)] - mean) * inv
            g = jnp.where(n * gain + bias > 0.0, dpre[at, at_cols], 0.0)
            dpre[at, at_cols] = g
            return carry[0] + fold(g * n), carry[1] + fold(g)

        zero = jnp.zeros((8, wide), jnp.float32)
        for row, value in enumerate(row_loop(block, (zero, zero))):
            value = jnp.sum(value, axis=0, keepdims=True)
            for c in range(wide // TILE):
                payload[layer, i * (wide // TILE) + c, row : row + 1] = value[:, c * TILE : (c + 1) * TILE]

    def du_tile(layer, i):
        u_tile(u2, i).wait()
        pl.when(i + 1 < tiles)(lambda: start_u(layer, i + 1))
        at_cols = rows(i * wide, wide)
        gain, mean, inv = (vec[layer * 4 + j, :, at_cols] for j in (0, 2, 3))
        means = jnp.concatenate([sums[layer, i * (wide // TILE) + c] for c in range(wide // TILE)], axis=1) / row_count
        mean_gn, mean_g = means[0:1], means[1:2]
        scale = gain * inv

        def block(r, c):
            at = rows(r * BLOCK, BLOCK)
            n = (out0[rows(rows_dev + r * BLOCK, BLOCK), rows((i % 2) * wide, wide)] - mean) * inv
            value = (dpre[at, at_cols] - mean_g - n * mean_gn) * scale
            dy[1 - layer, rows(core * rows_dev + r * BLOCK, BLOCK), at_cols] = value.astype(jnp.bfloat16)
            return c

        row_loop(block, 0)

    in_last = (MATS - 1) * PARTS
    quarter = part_rows // 4

    def home_row(k):
        return core * half + (k % PARTS) * part_rows

    def homes(k):
        return [
            (k < in_last, lambda off, size: gathered.at[k % GATHER_SLOTS, pl.ds(pl.multiple_of(off, quarter), size)]),
            (k >= in_last, lambda off, size: out0.at[pl.ds(pl.multiple_of(home_row(k) + off, quarter), size)]),
        ]

    def finish(k, off, size, buf):
        j = k % ACC_SLOTS
        value = acc[j, rows(off, size)] + buf[j]

        @pl.when(k < in_last)
        def _():
            gathered[k % GATHER_SLOTS, rows(off, size)] = value

        @pl.when(k >= in_last)
        def _():
            out0[rows(home_row(k) + off, size)] = value

    chunks = ChunkSum(place, "xl", back_kind, acc, homes, landing, send, recv, finish)

    def form(k, group):
        w, j = k // PARTS, k % ACC_SLOTS

        @pl.when(k % PARTS == 0)
        def _():
            pltpu.make_async_copy(xs.at[w % 2], xs.at[w % 2], in_sem.at[w]).wait()
            pl.when(w > 0)(lambda: peer_dy(w).wait_recv())

        at = rows((k % PARTS) * part_rows, group * part_rows)

        def col(c):
            pl.when(k == 0)(lambda: load_dz(c).wait())
            cs = rows(c * size, size)
            acc[pl.ds(j, group), :, cs] = contract_rows(xs[w % 2, :, at], dy[w % 2, :, cs]).reshape(group, part_rows, size)

        loop(0, width // size, col)

    def out_rows(k, side):
        return pl.ds(pl.multiple_of(side * half + (k % PARTS) * part_rows, part_rows), part_rows)

    def last_copy(out, k, side):
        return chunks.copy(gathered.at[k % GATHER_SLOTS], out.at[out_rows(k, side)], 7, k, other_core)

    def store_copy(out, k):
        return pltpu.make_async_copy(gathered.at[k % GATHER_SLOTS], out.at[out_rows(k, core)], store_sem.at[k])

    def stage(i, k):
        if i == 0:
            form_next(k, form)
            return
        chunks.stage(i, k)
        own_rows = out0.at[pl.ds(pl.multiple_of(home_row(k), part_rows), part_rows)]
        in_place = chunks.copy(own_rows, own_rows, 7, k, other_core)
        last = k // PARTS == MATS - 1

        def emit(out):
            last_copy(out, k, core).start()
            store_copy(out, k).start()

        def emit_any():
            pick(k // PARTS, outs, emit)
            pl.when(last)(lambda: in_place.start())

        if i == 8:
            pl.when(back_kind("x", k))(emit_any)
        if i == 9:
            pl.when(back_kind("l", k))(emit_any)
        if i == 10:

            def close(out):
                last_copy(out, k, 1 - core).wait_recv()
                store_copy(out, k).wait()
                last_copy(out, k, core).wait_send()

            pick(k // PARTS, outs, close)

            @pl.when(last)
            def _():
                in_place.wait_recv()
                in_place.wait_send()

    def layer_work(t):
        layer = t // LAYER_SLOTS
        at = t - LAYER_SLOTS * layer
        first_du = 2 * tiles + 3
        pl.when((at < 2 * tiles) & (at % 2 == 1))(lambda: chain_tile(layer, at // 2))
        @pl.when(at == 2 * tiles)
        def _():
            for part in range(len(SUM_PARTS)):
                small.begin(layer, part)

        @pl.when(at == 2 * tiles + 1)
        def _():
            for part in range(len(SUM_PARTS)):
                small.middle(layer, part)


        pl.when(at == 2 * tiles + 2)(lambda: start_u(layer, 0))

        pl.when(at == first_du)(lambda: small.end(layer))
        pl.when(at >= first_du)(lambda: du_tile(layer, at - first_du))

        @pl.when(at == LAYER_SLOTS - 1)
        def _():
            peer_dy(layer + 1).start()

            @pl.when(layer == 0)
            def _():
                w_tile(weights[1], 0).start()
                u_tile(pres[1], 0).start()

            pl.when(layer == 1)(lambda: load_x(2).start())

    form(0, GROUP // 2)
    place.all_here()
    run_slots(BACK_PLAN, count, stage, lambda t: pl.when(t < 2 * LAYER_SLOTS)(lambda: layer_work(t)))
    for w in (1, 2):
        peer_dy(w).wait_send()
    for c in range(PLANE):
        for row in range(4):
            sums_out[row : row + 1, c * TILE : (c + 1) * TILE] = sums[row // 2, c, row % 2 : row % 2 + 1]
    sums_out[4:5] = jnp.full((1, width), jnp.sum(vec[8]))


def backward(grad_z, x2, x1, x0, w_out, w_mid, u2, u1, vec):
    rows_dev, width = u2.shape
    part_rows = width // 2 // PARTS
    count = MATS * PARTS
    any_spec = pl.BlockSpec(memory_space=pl.ANY)
    vmem_spec = pl.BlockSpec(memory_space=pltpu.VMEM)
    mat = jax.ShapeDtypeStruct((width, width), jnp.float32)
    dma = pltpu.SemaphoreType.DMA
    return pl.pallas_call(
        back_kernel,
        name="backward",
        out_shape=[mat, mat, pltpu.VMEM((width, width), jnp.float32), jax.ShapeDtypeStruct((5, width), jnp.float32)],
        in_specs=[any_spec] * 8 + [vmem_spec],
        out_specs=[any_spec] * 2 + [vmem_spec] * 2,
        scratch_shapes=[
            pltpu.VMEM((2, 2 * rows_dev, width), jnp.bfloat16),
            pltpu.VMEM((2, 2 * rows_dev, width // 2), jnp.bfloat16),
            pltpu.VMEM((WIDE, width), jnp.bfloat16),
            dma((MATS + 2,)),
            dma((2, 2)),
            dma((MATS,)),
            dma((MATS,)),
            dma((count,)),
        ]
        + small_scratch(2)
        + chunk_scratch(ACC_SLOTS, GATHER_SLOTS, part_rows, width, count, jnp.float32),
        compiler_params=pltpu.CompilerParams(collective_id=1, has_side_effects=True, vmem_limit_bytes=BACK_VMEM),
    )(grad_z, x2, x1, x0, w_out, w_mid, u2, u1, vec)


def copy_kernel(*refs):
    pairs = (len(refs) - 6 - 6) // 2
    ins, small, outs, small_outs = refs[:pairs], refs[pairs], refs[pairs + 1 : 2 * pairs + 1], refs[2 * pairs + 1 : -6]
    buf, small_buf, in_sem, out_sem, small_sem, near_sem = refs[-6:]
    blocks = [(i, r) for i in range(pairs - 1) for r in range(0, ins[i].shape[0], COPY_ROWS)]
    near = pltpu.make_async_copy(ins[-1], outs[-1], near_sem.at[0])

    def read(b):
        i, r = blocks[b]
        return pltpu.make_async_copy(ins[i].at[pl.ds(r, COPY_ROWS)], buf.at[b % COPY_BUFS], in_sem.at[b % COPY_BUFS])

    def write(b):
        i, r = blocks[b]
        return pltpu.make_async_copy(buf.at[b % COPY_BUFS], outs[i].at[pl.ds(r, COPY_ROWS)], out_sem.at[b % COPY_BUFS])

    for b in range(len(blocks)):
        read(b).start()
    small_read = pltpu.make_async_copy(small, small_buf, small_sem.at[4])
    small_read.start()

    def small_write(row):
        return pltpu.make_async_copy(small_buf.at[pl.ds(row, 1)], small_outs[row], small_sem.at[row])

    for b in range(len(blocks)):
        read(b).wait()
    near.start()
    for b in range(len(blocks)):
        write(b).start()
    small_read.wait()
    small_outs[4][...] = small_buf[4:5, :1]
    for row in range(4):
        small_write(row).start()
    for row in range(4):
        small_write(row).wait()
    near.wait()
    for b in range(len(blocks)):
        write(b).wait()


def copy_out(arrays, small):
    any_spec = pl.BlockSpec(memory_space=pl.ANY)
    vmem_spec = pl.BlockSpec(memory_space=pltpu.VMEM)
    dma = pltpu.SemaphoreType.DMA
    width = small.shape[1]
    row = jax.ShapeDtypeStruct((1, width), jnp.float32)
    return pl.pallas_call(
        copy_kernel,
        name="copy_out",
        out_shape=[jax.ShapeDtypeStruct(a.shape, a.dtype) for a in arrays] + [row] * 4 + [jax.ShapeDtypeStruct((1, 1), jnp.float32)],
        in_specs=[any_spec] * (len(arrays) - 1) + [vmem_spec, any_spec],
        out_specs=[any_spec] * (len(arrays) + 4) + [vmem_spec],
        scratch_shapes=[
            pltpu.VMEM((COPY_BUFS, COPY_ROWS, width), jnp.float32),
            pltpu.VMEM(small.shape, jnp.float32),
            dma((COPY_BUFS,)),
            dma((COPY_BUFS,)),
            dma((5,)),
            dma((1,)),
        ],
        compiler_params=pltpu.CompilerParams(vmem_limit_bytes=COPY_VMEM),
    )(*arrays[:-1], pltpu.with_memory_space_constraint(arrays[-1], pltpu.VMEM), small)


def solution(mesh):
    row_part = P(DATA_AXIS, None)
    replicated = P()

    def local_step(feat_a, feat_b, w_in, w_mid, w_out, t_in, t_mid, t_out, gain_1, bias_1, gain_2, bias_2, off_weight):
        affine = [v.reshape(1, -1) for v in (gain_1, bias_1, gain_2, bias_2)]
        pre_1, pre_2, xs_2, xs_1, xs_0, grad_z, grad_emb, vec = front(
            feat_a, feat_b, (w_in, t_in, w_mid, t_mid, w_out, t_out), affine, off_weight.reshape(1)
        )
        grad_w_out, grad_w_mid, grad_w_in, sums = backward(grad_z, xs_2, xs_1, xs_0, w_out, w_mid, pre_2, pre_1, vec)
        (grad_emb, grad_w_out, grad_w_mid, grad_w_in, gain_2, bias_2, gain_1, bias_1, loss) = copy_out((grad_emb, grad_w_out, grad_w_mid, grad_w_in), sums)
        gain_1, bias_1, gain_2, bias_2 = (v.reshape(-1) for v in (gain_1, bias_1, gain_2, bias_2))
        return (loss.reshape(()), grad_emb, grad_w_in, grad_w_mid, grad_w_out, gain_1, bias_1, gain_2, bias_2)

    return jax.shard_map(local_step, mesh=mesh, in_specs=(row_part, row_part) + (replicated,) * 11, out_specs=(replicated, row_part) + (replicated,) * 7, check_vma=False)
```

```python
import functools

import jax
import jax.numpy as jnp
from jax import lax
from jax.experimental import pallas as pl
from jax.experimental.pallas import tpu as pltpu
from jax.sharding import PartitionSpec as P

NORM_EPS = 1e-5
DATA_AXIS = "data"
MESH = pl.DeviceIdType.MESH
VMEM_BYTES = 67_043_328
PLANE = 8
DEPTH = 4
TILE = 256
WIDE = 512
BLOCK = 128
SUM_ROWS = 2
SUM_PARTS = ((0, 6), (6, 2))
PARTS = 16
GROUP = 4
MATS = 3
ACC_SLOTS = 16
GATHER_SLOTS = 14
BACK_VMEM = 49_800_000
COPY_VMEM = 42 * 1024 * 1024
JOBS = 6
W_BUFS = 3
LAYER_SLOTS = 15
COPY_ROWS = 256
COPY_BUFS = 18
FRONT_PLAN = ((0, 0, 3, 5, 7, 9, 12, 13, 16, 17, 18), (0, 6, 3, 4, 9, 10, 8, 5, 2, 7, 1))
BACK_PLAN = ((0, 0, 3, 5, 7, 8, 9, 11, 14, 17, 19), (0, 4, 8, 7, 10, 1, 2, 3, 5, 6, 9))


def front_kind(kind, k):
    s, l = (k % 5 == 2) & (k > 2), k == 2
    return {"s": s, "l": l, "x": (k % 5 != 2)}[kind]


def back_kind(kind, k):
    l = ((k % 5 == 2) & (k < 43)) | ((k % 5 == 0) & (k >= 10) & (k < 36))
    return l if kind == "l" else jnp.logical_not(l)


def contract_rows(left_op, right_op):
    return lax.dot_general(left_op, right_op, (((0,), (0,)), ((), ())), preferred_element_type=jnp.float32)


def contract_cols(left_op, right_op):
    return lax.dot_general(left_op, right_op, (((1,), (1,)), ((), ())), preferred_element_type=jnp.float32)


def rows(off, size):
    return pl.ds(pl.multiple_of(off, size), size)


def pick(index, choices, what):
    for i, c in enumerate(choices):
        pl.when(index == i)(functools.partial(what, c))


def loop(lo, hi, body):
    def step(i, carry):
        body(i)
        return carry

    lax.fori_loop(lo, hi, step, 0)


def remote_copy(src, dst, send, recv, mate):
    return pltpu.make_async_remote_copy(src, dst, send, recv, device_id=(mate,), device_id_type=MESH)


class Place:
    def __init__(self):
        me = lax.axis_index(DATA_AXIS)
        self.me = me
        self.pos, self.plane = me % PLANE, me // PLANE
        self.core, self.bx, self.by, self.bz0, self.bz1 = me % 2, (me // 2) % 2, (me // 4) % 2, (me // 8) % 2, (me // 16) % 2
        self.other_core = me + 1 - 2 * self.core
        self.mates = [(self.pos + d) % PLANE for d in range(1, PLANE)]
        self.levels = [(self.plane + d) % DEPTH for d in range(1, DEPTH)]

    def peers(self):
        return [self.plane * PLANE + m for m in self.mates] + [lv * PLANE + self.pos for lv in self.levels]

    def arrive(self):
        sem = pltpu.get_barrier_semaphore()
        for peer in self.peers():
            pl.semaphore_signal(sem, inc=1, device_id=(peer,), device_id_type=MESH)

    def all_here(self):
        pl.semaphore_wait(pltpu.get_barrier_semaphore(), PLANE + DEPTH - 2)


class SmallSum:
    def __init__(self, place, payload, total, depth_buf, line_sum, plane_buf, sems):
        self.p, self.payload, self.total = place, payload, total
        self.depth_buf, self.line_sum, self.plane_buf, self.sems = depth_buf, line_sum, plane_buf, sems

    def along(self, j, part, lv, slot):
        (s, r), at = self.sems[:2], pl.ds(*SUM_PARTS[part])
        n = part * DEPTH
        return remote_copy(self.payload.at[j, at], self.depth_buf.at[j, slot, at], s.at[j, n + lv], r.at[j, n + slot], lv * PLANE + self.p.pos)

    def within(self, j, part, m, slot):
        (s, r), at = self.sems[2:], pl.ds(*SUM_PARTS[part])
        n = part * PLANE
        return remote_copy(self.line_sum.at[j, at], self.plane_buf.at[j, slot, at], s.at[j, n + m], r.at[j, n + slot], self.p.plane * PLANE + m)

    def begin(self, j, part):
        at = pl.ds(*SUM_PARTS[part])
        for lv in self.p.levels:
            self.along(j, part, lv, self.p.plane).start()
        self.depth_buf[j, self.p.plane, at] = self.payload[j, at]

    def middle(self, j, part):
        at = pl.ds(*SUM_PARTS[part])
        for lv in self.p.levels:
            self.along(j, part, lv, lv).wait_recv()
        total = self.depth_buf[j, 0, at]
        for i in range(1, DEPTH):
            total = total + self.depth_buf[j, i, at]
        self.line_sum[j, at] = total
        for m in self.p.mates:
            self.within(j, part, m, self.p.pos).start()
        self.plane_buf[j, self.p.pos, at] = total

    def end(self, j):
        for part in range(len(SUM_PARTS)):
            for m in self.p.mates:
                self.within(j, part, m, m).wait_recv()
        total = self.plane_buf[j, 0]
        for i in range(1, PLANE):
            total = total + self.plane_buf[j, i]
        self.total[j] = total
        for part in range(len(SUM_PARTS)):
            for lv in self.p.levels:
                self.along(j, part, lv, self.p.plane).wait_send()
            for m in self.p.mates:
                self.within(j, part, m, self.p.pos).wait_send()


def small_scratch(count):
    def buf(*lead):
        return pltpu.VMEM((count, *lead, PLANE, SUM_ROWS, TILE), jnp.float32)

    return [buf(), buf(), buf(DEPTH), buf(), buf(PLANE)] + [pltpu.SemaphoreType.DMA((count, n * len(SUM_PARTS))) for n in (DEPTH, DEPTH, PLANE, PLANE)]


SMALL_REFS = 9


def small_sum(place, refs):
    return SmallSum(place, *refs[:5], refs[5:])


class Homed:
    def __init__(self, homes, make):
        self.homes, self.make = homes, make

    def do(self, what):
        for when, home in self.homes:
            run = lambda home=home: getattr(self.make(home), what)()
            run() if when is None else pl.when(when)(run)

    def start(self):
        self.do("start")

    def wait_recv(self):
        self.do("wait_recv")

    def wait_send(self):
        self.do("wait_send")


class ChunkSum:
    def __init__(self, place, kinds, is_kind, acc, homes, landing, send, recv, finish):
        self.p, self.kinds, self.is_kind, self.slots, self.homes = place, kinds, is_kind, acc.shape[0], homes
        self.acc, self.landing, self.send, self.recv, self.finish = acc, landing, send, recv, finish
        self.size = acc.shape[1]
        self.s2, self.s4 = self.size // 2, self.size // 4
        core, bx, by, me = place.core, place.bx, place.by, place.me
        first, second = core * by + (1 - core) * bx, core * bx + (1 - core) * by
        self.xy = ((me + (2 + 2 * core) * (1 - 2 * first), first), (me + (4 - 2 * core) * (1 - 2 * second), second))
        self.zz = ((me + 8 * (1 - 2 * place.bz0), place.bz0), (me + 16 * (1 - 2 * place.bz1), place.bz1))
        self.is_mid = place.bz0 + place.bz1 - 2 * place.bz0 * place.bz1
        self.mid, self.end = self.is_mid == 1, self.is_mid == 0
        self.z_mate = self.zz[0][0]
        self.mid_mate = me + 8 * (1 - 2 * place.bz1)

    def copy(self, src, dst, stage, k, mate):
        return remote_copy(src, dst, self.send.at[stage, k], self.recv.at[stage, k], mate)

    def span(self, off, size):
        return pl.ds(pl.multiple_of(off, self.s4), size)

    def down(self, stage, k, off, size, mate, buf=None):
        j = k % self.slots
        buf = self.landing[stage] if buf is None else buf
        return self.copy(self.acc.at[j, self.span(off, size)], buf.at[j, pl.ds(0, size)], stage, k, mate)

    def up(self, stage, k, off, size, mate):
        return Homed(self.homes(k), lambda home: self.copy(home(off, size), home(off, size), stage, k, mate))

    def add(self, k, off, size, buf):
        step = min(size, 16)
        j = k % self.slots

        def body(i):
            at = pl.ds(pl.multiple_of(off + i * step, step), step)
            self.acc[j, at] = self.acc[j, at] + buf[j, rows(i * step, step)]

        loop(0, size // step, body)

    def stage(self, i, k):
        for kind in self.kinds:
            run = {"x": self.stage_x, "s": self.stage_s, "l": self.stage_l}[kind]
            pl.when(self.is_kind(kind, k))(functools.partial(run, i, k))

    def stage_x(self, i, k):
        (m1, b1), (m2, b2), s2, s4 = *self.xy, self.s2, self.s4
        off1, off2 = b1 * s2, b1 * s2 + b2 * s4
        half = lambda: self.down(0, k, (1 - b1) * s2, s2, m1)
        quarter = lambda: self.down(1, k, off1 + (1 - b2) * s4, s4, m2)
        inward = lambda: self.down(2, k, off2, s4, self.z_mate)
        across = lambda: self.down(3, k, off2, s4, self.mid_mate)
        outward = lambda: self.up(4, k, off2, s4, self.z_mate)
        back4 = lambda: self.up(5, k, off2, s4, m2)
        back2 = lambda: self.up(6, k, off1, s2, m1)
        if i == 1:
            half().start()
        elif i == 2:
            half().wait_recv()
            self.add(k, off1, s2, self.landing[0])
            quarter().start()
        elif i == 3:
            quarter().wait_recv()
            self.add(k, off2, s4, self.landing[1])
            pl.when(self.end)(lambda: inward().start())
        elif i == 4:

            @pl.when(self.mid)
            def _():
                inward().wait_recv()
                self.add(k, off2, s4, self.landing[2])
                across().start()

        elif i == 5:

            @pl.when(self.mid)
            def _():
                across().wait_recv()
                self.finish(k, off2, s4, self.landing[3])
                outward().start()

        elif i == 6:
            pl.when(self.end)(lambda: outward().wait_recv())
            back4().start()
            half().wait_send()
            quarter().wait_send()
            pl.when(self.end)(lambda: inward().wait_send())
            pl.when(self.mid)(lambda: across().wait_send())
        elif i == 7:
            back4().wait_recv()
            back2().start()
        elif i == 8:
            back2().wait_recv()
        elif i == 10:
            pl.when(self.mid)(lambda: outward().wait_send())
            back4().wait_send()
            back2().wait_send()

    def stage_s(self, i, k):
        (m1, b1), (m2, b2), s2, s4 = *self.zz, self.s2, self.s4
        off1, off2 = b1 * s2, b1 * s2 + b2 * s4
        half = lambda: self.down(0, k, (1 - b1) * s2, s2, m1)
        quarter = lambda: self.down(1, k, off1 + (1 - b2) * s4, s4, m2)
        whole_1 = lambda: self.down(2, k, off2, s4, self.xy[0][0])
        whole_2 = lambda: self.down(3, k, off2, s4, self.xy[1][0])
        back4 = lambda: self.up(5, k, off2, s4, m2)
        back2 = lambda: self.up(6, k, off1, s2, m1)
        if i == 1:
            half().start()
        elif i == 2:
            half().wait_recv()
            self.add(k, off1, s2, self.landing[0])
            quarter().start()
        elif i == 3:
            quarter().wait_recv()
            self.add(k, off2, s4, self.landing[1])
            whole_1().start()
        elif i == 4:
            whole_1().wait_recv()
            whole_1().wait_send()
            self.add(k, off2, s4, self.landing[2])
            whole_2().start()
        elif i == 5:
            whole_2().wait_recv()
            self.finish(k, off2, s4, self.landing[3])
        elif i == 6:
            back4().start()
            half().wait_send()
            quarter().wait_send()
            whole_2().wait_send()
        elif i == 7:
            back4().wait_recv()
            back2().start()
        elif i == 8:
            back2().wait_recv()
        elif i == 10:
            back4().wait_send()
            back2().wait_send()

    def stage_l(self, i, k):
        s2, s4 = self.s2, self.s4
        s3 = s2 + s4
        b0, b1 = self.p.bz0, self.p.bz1
        own, side, tip, rest = (2 * b1 + b0) * s4, b1 * s2, 3 * b1 * s4, (1 - b1) * s4
        inward = lambda: self.down(0, k, rest, s3, self.z_mate)
        across = lambda: self.down(1, k, (1 - b1) * s2, s2, self.mid_mate)
        outward = lambda: self.down(2, k, tip, s4, self.z_mate)
        whole_1 = lambda: self.down(3, k, own, s4, self.xy[0][0])
        whole_2 = lambda: self.down(8, k, own, s4, self.xy[1][0], self.landing[4])
        tip_back = lambda: self.up(4, k, tip, s4, self.z_mate)
        side_back = lambda: self.up(5, k, side, s2, self.mid_mate)
        rest_back = lambda: self.up(6, k, rest, s3, self.z_mate)
        if i == 1:
            pl.when(self.end)(lambda: inward().start())
        elif i == 2:

            @pl.when(self.mid)
            def _():
                inward().wait_recv()
                self.add(k, rest, s3, self.landing[0])
                across().start()

        elif i == 3:

            @pl.when(self.mid)
            def _():
                across().wait_recv()
                self.add(k, side, s2, self.landing[1])
                outward().start()

        elif i == 4:

            @pl.when(self.end)
            def _():
                outward().wait_recv()
                self.add(k, own, s4, self.landing[2])

            whole_1().start()
        elif i == 5:
            whole_1().wait_recv()
            whole_1().wait_send()
            pl.when(self.mid)(lambda: outward().wait_send())
            self.add(k, own, s4, self.landing[3])
            whole_2().start()
        elif i == 6:
            whole_2().wait_recv()
            self.finish(k, own, s4, self.landing[4])
            pl.when(self.end)(lambda: tip_back().start())
            whole_2().wait_send()
            pl.when(self.end)(lambda: inward().wait_send())
            pl.when(self.mid)(lambda: across().wait_send())
        elif i == 7:

            @pl.when(self.mid)
            def _():
                tip_back().wait_recv()
                side_back().start()

        elif i == 8:

            @pl.when(self.mid)
            def _():
                side_back().wait_recv()
                rest_back().start()

        elif i == 9:
            pl.when(self.end)(lambda: rest_back().wait_recv())
        elif i == 10:
            pl.when(self.end)(lambda: tip_back().wait_send())

            @pl.when(self.mid)
            def _():
                side_back().wait_send()
                rest_back().wait_send()


def form_next(k, form):
    pl.when(k == 1)(lambda: form(GROUP // 2, GROUP // 2))
    pl.when((k % GROUP == 0) & (k > 0))(lambda: form(k, GROUP))


def run_slots(plan, count, stage, between):
    lags, order = plan

    def slot(t):
        for i in order:
            k = t - lags[i]

            @pl.when((k >= 0) & (k < count))
            def _():
                stage(i, k)

            if i == 1:
                between(t)

    loop(0, count + lags[-1], slot)


def chunk_scratch(slots, gather_slots, part_rows, width, count, dtype):
    def buf(n):
        return pltpu.VMEM((slots, n, width), jnp.float32)

    gathered = pltpu.VMEM((gather_slots, part_rows, width), dtype)

    dma = pltpu.SemaphoreType.DMA
    quarter = part_rows // 4
    return [buf(part_rows), gathered, *(buf(n * quarter) for n in (3, 2, 1, 1, 1)), dma((9, count)), dma((9, count))]


def fold(value):
    return jnp.sum(value.reshape(value.shape[0] // 8, 8, value.shape[1]), axis=0)


def front_kernel(feat_a, feat_b, w_in, t_in, w_mid, t_mid, w_out, t_out, gain1, bias1, gain2, bias2, off_hbm, pre1, pre2, xs2, xs1, xs0, dz, grad_emb, vec_hbm, *scratch):
    (x_buf, u_buf, w_buf, stats, affine, loss, vec, off_weight, ea, eb, g_peer) = scratch[:11]
    (x_sem, w_sem, row_sem, pre_sem, keep_sem, keep_send, keep_recv, ge_sem, e_send, e_recv) = scratch[11:21]
    small_refs = scratch[21 : 21 + SMALL_REFS]
    acc, gathered, *landing, send, recv = scratch[21 + SMALL_REFS :]
    rows_dev, width = feat_a.shape
    wide = w_buf.shape[2]
    tiles = width // wide
    half = width // 2
    part_rows = half // PARTS
    row_count = rows_dev * DEPTH * PLANE
    weights, feats = (w_in, t_in, w_mid, t_mid, w_out, t_out), (feat_a, feat_b)
    place = Place()
    core = place.core
    mine = rows(core * rows_dev, rows_dev)
    place.arrive()
    small = small_sum(place, small_refs)
    payload, total = small.payload, small.total

    def feat(v):
        return pltpu.make_async_copy(feats[v], x_buf.at[v], x_sem.at[v])

    def w_tile(ref, g):
        return pltpu.make_async_copy(ref.at[:, rows((g % tiles) * wide, wide)], w_buf.at[g % W_BUFS], w_sem.at[g % W_BUFS])

    def start_w(g):
        pick(g // tiles, weights, lambda ref: w_tile(ref, g).start())

    feat(0).start()
    w_tile(weights[0], 0).start()
    feat(1).start()
    for g in range(1, W_BUFS - 1):
        start_w(g)
    row_loads = [pltpu.make_async_copy(ref, affine.at[j], row_sem.at[j]) for j, ref in enumerate((gain1, bias1, gain2, bias2))]
    row_loads.append(pltpu.make_async_copy(off_hbm, off_weight, row_sem.at[4]))
    for c in row_loads:
        c.start()
    early_rows = pltpu.make_async_copy(vec.at[pl.ds(0, 8)], vec_hbm.at[pl.ds(0, 8)], row_sem.at[5])
    late_row = pltpu.make_async_copy(vec.at[pl.ds(8, 1)], vec_hbm.at[pl.ds(8, 1)], row_sem.at[6])
    feat(0).wait()
    payload[...] = jnp.zeros_like(payload)

    def keep_pre(ref):
        return pltpu.make_async_copy(u_buf.at[0], ref, pre_sem.at[0])

    kept = (xs0, xs1, xs2)

    def keep_x(w):
        here = pltpu.make_async_copy(x_buf.at[0, :, rows(core * half, half)], kept[w].at[mine], keep_sem.at[w])
        there = remote_copy(x_buf.at[0, :, rows((1 - core) * half, half)], kept[w].at[mine], keep_send.at[w], keep_recv.at[w], place.other_core)
        return here, there

    def start_x(w):
        for c in keep_x(w):
            c.start()

    def free_x(w):
        here, there = keep_x(w)
        here.wait()
        there.wait_send()

    def keep_dz(i):
        at = (slice(None), rows(i * wide, wide))
        here = pltpu.make_async_copy(x_buf.at[(0, *at)], dz.at[mine, at[1]], keep_sem.at[3 + i])
        there = remote_copy(x_buf.at[(0, *at)], dz.at[mine, at[1]], keep_send.at[3 + i], keep_recv.at[3 + i], place.other_core)
        return here, there

    def row_loop(body, carry):
        return lax.fori_loop(0, rows_dev // BLOCK, lambda r, c: body(rows(r * BLOCK, BLOCK), c), carry)

    def put_sums(j, i, row, value):
        value = jnp.sum(value, axis=0, keepdims=True)
        for c in range(value.shape[1] // TILE):
            payload[j, i + c, row : row + 1] = value[:, c * TILE : (c + 1) * TILE]

    def product(g):
        job, i = g // tiles, g % tiles
        view = job % 2
        w_tile(w_in, g).wait()
        pl.when(g + W_BUFS - 1 < JOBS * tiles)(lambda: start_w(g + W_BUFS - 1))
        at_cols = rows(i * wide, wide)
        u_buf[view, :, at_cols] = jnp.dot(x_buf[view], w_buf[g % W_BUFS], preferred_element_type=jnp.float32)

        def block(at, sums):
            u = u_buf[view, at, at_cols]
            return sums[0] + fold(u), sums[1] + fold(u * u)

        zero = jnp.zeros((8, wide), jnp.float32)
        for row, value in enumerate(row_loop(block, (zero, zero))):
            put_sums(job, i * (wide // TILE), row, value)

    def keep(job):
        @pl.when(job % 2 == 0)
        def _():
            pick(job // 2, (pre1, pre2), lambda ref: keep_pre(ref).start())

    def norm(job):
        layer, view = job // 2, job % 2
        small.end(job)
        for c in range(PLANE):
            at = slice(c * TILE, (c + 1) * TILE)
            means = total[job, c] / row_count
            stats[job, 0, :, at] = means[0:1]
            stats[job, 1, :, at] = lax.rsqrt(means[1:2] - means[0:1] * means[0:1] + NORM_EPS)

        pl.when(view == 0)(lambda: pick(layer, (0, 1, 2), free_x))

        def hidden(i):
            at_cols = rows(i * wide, wide)
            mean, inv = stats[job, 0, :, at_cols], stats[job, 1, :, at_cols]
            gain, bias = affine[layer * 2, :, at_cols], affine[layer * 2 + 1, :, at_cols]

            def block(at, c):
                n = (u_buf[view, at, at_cols] - mean) * inv
                x_buf[view, at, at_cols] = jnp.maximum(n * gain + bias, 0.0).astype(jnp.bfloat16)
                return c

            row_loop(block, 0)

        def student(i):
            at_cols = rows(i * wide, wide)
            mean, inv = stats[job, 0, :, at_cols], stats[job, 1, :, at_cols]

            def block(at, c):
                n = (u_buf[0, at, at_cols] - mean) * inv
                u_buf[0, at, at_cols] = n
                x_buf[0, at, at_cols] = n.astype(jnp.bfloat16)
                return c

            row_loop(block, 0)

        def student_own(i):
            def block(r, c):
                ea[rows(core * rows_dev + r * BLOCK, BLOCK), rows(i * wide, wide)] = x_buf[0, rows(r * BLOCK, BLOCK), rows(core * half + i * wide, wide)]
                return c

            lax.fori_loop(0, rows_dev // BLOCK, block, 0)

        def teacher(i):
            at_cols = rows(i * wide, wide)
            mean, inv = stats[job, 0, :, at_cols], stats[job, 1, :, at_cols]

            def block(r, c):
                n = (u_buf[1, rows(r * BLOCK, BLOCK), at_cols] - mean) * inv
                eb[rows(core * rows_dev + r * BLOCK, BLOCK), at_cols] = n.astype(jnp.bfloat16)
                return c

            lax.fori_loop(0, rows_dev // BLOCK, block, 0)
            eb_copy(i).start()

        @pl.when(layer < 2)
        def _():
            loop(0, tiles, hidden)

            @pl.when(view == 0)
            def _():
                pick(layer, (1, 2), start_x)
                keep_pre(pre1).wait()

        @pl.when((layer == 2) & (view == 0))
        def _():
            loop(0, tiles, student)
            ea_copy().start()
            loop(0, tiles // 2, student_own)

        @pl.when((layer == 2) & (view == 1))
        def _():
            loop(0, tiles, teacher)

    ea_copy = lambda: remote_copy(x_buf.at[0, :, rows((1 - core) * half, half)], ea.at[mine], e_send.at[0], e_recv.at[0], place.other_core)

    def eb_copy(i):
        block = eb.at[mine, rows(i * wide, wide)]
        return remote_copy(block, block, e_send.at[1 + i], e_recv.at[1 + i], place.other_core)

    def step(g):
        job, i = g // tiles, g % tiles
        view = job % 2
        pl.when(g == tiles)(lambda: feat(1).wait())
        product(g)

        @pl.when(g == 0)
        def _():
            place.all_here()
            start_x(0)
            for c in row_loads:
                c.wait()

        pl.when(i == tiles - 2)(lambda: small.begin(job, 0))
        pl.when((i == 0) & (job > 0))(lambda: small.middle(job - 1, 0))
        pl.when((i == 1) & (job > 0))(lambda: small.middle(job - 1, 1))

        @pl.when(i == tiles - 1)
        def _():
            small.begin(job, 1)
            keep(job)
            pl.when(job == JOBS - 1)(lambda: small.middle(job, 0))
            pl.when(job > 0)(lambda: norm(job - 1))

    loop(0, JOBS * tiles, step)
    small.middle(JOBS - 1, 1)
    norm(JOBS - 1)
    for j, source in enumerate((affine.at[2], affine.at[3], stats.at[2, 0], stats.at[2, 1], affine.at[0], affine.at[1], stats.at[0, 0], stats.at[0, 1])):
        vec[j] = source[...]
    early_rows.start()

    loss[...] = jnp.zeros_like(loss)

    def finish(k, off, size, buf):
        share = jnp.where(front_kind("x", k), 0.5, 0.25)
        at = rows(off, size)
        corr = (acc[k, at] + buf[k]) / row_count
        row = core * half + k * part_rows + off
        diag = (row + lax.broadcasted_iota(jnp.int32, (size, width), 0)) == lax.broadcasted_iota(jnp.int32, (size, width), 1)
        weight = off_weight[0]
        miss = 1.0 - corr
        loss[...] += share * jnp.sum(jnp.where(diag, miss * miss, weight * (corr * corr)), axis=0, keepdims=True)
        gathered[k, at] = jnp.where(diag, -2.0 * miss, 2.0 * weight * corr).astype(jnp.bfloat16)

    def homes(k):
        return [(None, lambda off, size: gathered.at[k, pl.ds(pl.multiple_of(off, part_rows // 4), size)])]

    chunks = ChunkSum(place, "xsl", front_kind, acc, homes, landing, send, recv, finish)

    def form(k, group):
        at = rows(k * part_rows, group * part_rows)
        size = min(1024, width)

        def col(c):
            @pl.when(k == 0)
            def _():
                for i in range(size // wide):
                    eb_copy(c * (size // wide) + i).wait_recv()

            cs = rows(c * size, size)
            acc[pl.ds(k, group), :, cs] = contract_rows(ea[:, at], eb[:, cs]).reshape(group, part_rows, size)

        loop(0, width // size, col)

    def swap(k):
        return chunks.copy(gathered.at[k], g_peer.at[k], 7, k, place.other_core)

    def ge_cols(k, side):
        return rows(side * half + k * part_rows, GROUP * part_rows)

    def ge_copy(k, side):
        at = ge_cols(k, side)
        return pltpu.make_async_copy(u_buf.at[1, :, at], grad_emb.at[:, at], ge_sem.at[k // GROUP, side])

    def embed(k, side, g_rows):
        at_cols = ge_cols(k, side)
        grad = contract_cols(eb[mine], g_rows.reshape(GROUP * part_rows, width)) / row_count
        u_buf[1, :, at_cols] = grad
        ge_copy(k, side).start()

        def block(at, sums):
            g = u_buf[1, at, at_cols]
            return sums[0] + fold(g * u_buf[0, at, at_cols]), sums[1] + fold(g)

        zero = jnp.zeros((8, GROUP * part_rows), jnp.float32)
        for row, value in enumerate(row_loop(block, (zero, zero))):
            payload[JOBS, 2 * (k // GROUP) + side, row : row + 1] = jnp.sum(value, axis=0, keepdims=True)

    def stage(i, k):
        if i == 0:
            form_next(k, form)
            return
        chunks.stage(i, k)
        if i == 8:
            pl.when(jnp.logical_not(front_kind("l", k)))(lambda: swap(k).start())
        if i == 9:
            pl.when(front_kind("l", k))(lambda: swap(k).start())

            @pl.when(k % GROUP == GROUP - 1)
            def _():
                embed(k - GROUP + 1, core, gathered[pl.ds(k - GROUP + 1, GROUP)])

        if i == 10:
            swap(k).wait_recv()
            swap(k).wait_send()

            @pl.when(k % GROUP == GROUP - 1)
            def _():
                embed(k - GROUP + 1, 1 - core, g_peer[pl.ds(k - GROUP + 1, GROUP)])

            pl.when(k == PARTS - GROUP - 1)(lambda: small.begin(JOBS, 0))
            pl.when(k == PARTS - 2)(lambda: small.middle(JOBS, 0))

    ea_copy().wait_recv()
    form(0, GROUP // 2)
    run_slots(FRONT_PLAN, PARTS, stage, lambda t: None)
    small.begin(JOBS, 1)
    for c in range(PLANE):
        payload[JOBS + 1, c, 0:1] = loss[:, c * TILE : (c + 1) * TILE]
    ea_copy().wait_send()
    for i in range(tiles):
        eb_copy(i).wait_send()
    small.middle(JOBS, 1)
    for part in range(len(SUM_PARTS)):
        small.begin(JOBS + 1, part)
    for k in range(0, PARTS, GROUP):
        for side in range(2):
            ge_copy(k, side).wait()
    small.end(JOBS)

    def dz_tile(i):
        at_cols = rows(i * wide, wide)
        groups, side = tiles // 2, i // (tiles // 2)
        first = (i % groups) * (wide // TILE)
        sums = jnp.concatenate([total[JOBS, 2 * (first + c) + side] for c in range(wide // TILE)], axis=1) / row_count
        mean_gn, mean_g = sums[0:1], sums[1:2]
        inv = stats[JOBS - 2, 1, :, at_cols]

        def block(at, c):
            value = (u_buf[1, at, at_cols] - mean_g - u_buf[0, at, at_cols] * mean_gn) * inv
            x_buf[0, at, at_cols] = value.astype(jnp.bfloat16)
            return c

        row_loop(block, 0)
        for c in keep_dz(i):
            c.start()

    loop(0, tiles, dz_tile)
    for part in range(len(SUM_PARTS)):
        small.middle(JOBS + 1, part)
    small.end(JOBS + 1)
    for c in range(PLANE):
        vec[8, :, c * TILE : (c + 1) * TILE] = total[JOBS + 1, c, 0:1]
    late_row.start()
    for w in range(3):
        keep_x(w)[1].wait_recv()
    for i in range(tiles):
        here, there = keep_dz(i)
        here.wait()
        there.wait()
    early_rows.wait()
    late_row.wait()


def front(feat_a, feat_b, weights, affine, off_weight):
    rows_dev, width = feat_a.shape
    half = width // 2
    part_rows = half // PARTS
    any_spec = pl.BlockSpec(memory_space=pl.ANY)
    wide_f32 = jax.ShapeDtypeStruct((rows_dev, width), jnp.float32)
    kept = jax.ShapeDtypeStruct((2 * rows_dev, half), jnp.bfloat16)
    both_dz = jax.ShapeDtypeStruct((2 * rows_dev, width), jnp.bfloat16)
    keeps = 3 + width // WIDE
    dma = pltpu.SemaphoreType.DMA
    return pl.pallas_call(
        front_kernel,
        name="front",
        out_shape=[wide_f32, wide_f32, kept, kept, kept, both_dz, wide_f32]
        + [jax.ShapeDtypeStruct((9, 1, width), jnp.float32)],
        in_specs=[any_spec] * 13,
        out_specs=[any_spec] * 8,
        scratch_shapes=[
            pltpu.VMEM((2, rows_dev, width), jnp.bfloat16),
            pltpu.VMEM((2, rows_dev, width), jnp.float32),
            pltpu.VMEM((W_BUFS, width, WIDE), jnp.bfloat16),
            pltpu.VMEM((JOBS, 2, 1, width), jnp.float32),
            pltpu.VMEM((4, 1, width), jnp.float32),
            pltpu.VMEM((1, width), jnp.float32),
            pltpu.VMEM((9, 1, width), jnp.float32),
            pltpu.SMEM((1,), jnp.float32),
            pltpu.VMEM((2 * rows_dev, half), jnp.bfloat16),
            pltpu.VMEM((2 * rows_dev, width), jnp.bfloat16),
            pltpu.VMEM((PARTS, part_rows, width), jnp.bfloat16),
            dma((2,)),
            dma((W_BUFS,)),
            dma((7,)),
            dma((1,)),
            dma((keeps,)),
            dma((keeps,)),
            dma((keeps,)),
            dma((PARTS // GROUP, 2)),
            dma((1 + width // WIDE,)),
            dma((1 + width // WIDE,)),
        ]
        + small_scratch(JOBS + 2)
        + chunk_scratch(PARTS, PARTS, part_rows, width, PARTS, jnp.bfloat16),
        compiler_params=pltpu.CompilerParams(collective_id=0, has_side_effects=True, vmem_limit_bytes=VMEM_BYTES),
    )(feat_a, feat_b, *weights, *affine, off_weight)


def back_kernel(dz_hbm, x2, x1, x0, w_out, w_mid, u2, u1, vec_hbm, out2, out1, out0, sums_hbm, *scratch):
    (dy, xs, w_buf, vec, sums_out) = scratch[:5]
    (in_sem, tile_sem, row_sem, peer_send, peer_recv, store_sem) = scratch[5:11]
    small_refs = scratch[11 : 11 + SMALL_REFS]
    acc, gathered, *landing, send, recv = scratch[11 + SMALL_REFS :]
    rows_dev, width = u2.shape
    wide = w_buf.shape[0]
    tiles = width // wide
    row_count = rows_dev * DEPTH * PLANE
    half = width // 2
    part_rows = half // PARTS
    count = MATS * PARTS
    mats_in, outs, weights, pres = (x2, x1, x0), (out2, out1), (w_out, w_mid), (u2, u1)
    dpre = out0.at[pl.ds(0, rows_dev)]

    def u_buf(i):
        return out0.at[pl.ds(rows_dev, rows_dev), rows((i % 2) * wide, wide)]

    place = Place()
    core, other_core = place.core, place.other_core
    mine = rows(core * rows_dev, rows_dev)
    place.arrive()
    small = small_sum(place, small_refs)
    payload, sums = small.payload, small.total

    def load_x(w):
        return pltpu.make_async_copy(mats_in[w], xs.at[w % 2], in_sem.at[w])

    def peer_dy(w):
        block = dy.at[w % 2, mine]
        return remote_copy(block, block, peer_send.at[w], peer_recv.at[w], other_core)

    def w_tile(ref, i):
        return pltpu.make_async_copy(ref.at[rows(i * wide, wide)], w_buf, tile_sem.at[0, 0])

    def u_tile(ref, i):
        return pltpu.make_async_copy(ref.at[:, rows(i * wide, wide)], u_buf(i), tile_sem.at[1, i % 2])

    def start_w(layer, i):
        pick(layer, weights, lambda ref: w_tile(ref, i).start())

    def start_u(layer, i):
        pick(layer, pres, lambda ref: u_tile(ref, i).start())

    size = min(1024, width)

    def load_dz(c):
        return pltpu.make_async_copy(dz_hbm.at[:, rows(c * size, size)], dy.at[0, :, rows(c * size, size)], in_sem.at[MATS + c])

    load_x(0).start()
    for c in range(width // size):
        load_dz(c).start()
    w_tile(weights[0], 0).start()
    u_tile(pres[0], 0).start()
    vec_load = pltpu.make_async_copy(vec_hbm, vec, row_sem.at[0])
    vec_load.start()
    load_x(1).start()
    sums_store = pltpu.make_async_copy(sums_out, sums_hbm, row_sem.at[1])
    payload[...] = jnp.zeros_like(payload)

    def row_loop(body, carry):
        return lax.fori_loop(0, rows_dev // BLOCK, body, carry)

    def chain_tile(layer, i):
        w_tile(w_out, i).wait()
        u_tile(u2, i).wait()

        pl.when(i + 1 < tiles)(lambda: start_u(layer, i + 1))
        at_cols = rows(i * wide, wide)
        dpre[:, at_cols] = contract_cols(dy[layer, mine], w_buf[...])
        pl.when(i + 1 < tiles)(lambda: start_w(layer, i + 1))
        gain, bias, mean, inv = (vec[layer * 4 + j, :, at_cols] for j in range(4))

        def block(r, carry):
            at = rows(r * BLOCK, BLOCK)
            n = (out0[rows(rows_dev + r * BLOCK, BLOCK), rows((i % 2) * wide, wide)] - mean) * inv
            g = jnp.where(n * gain + bias > 0.0, dpre[at, at_cols], 0.0)
            dpre[at, at_cols] = g
            return carry[0] + fold(g * n), carry[1] + fold(g)

        zero = jnp.zeros((8, wide), jnp.float32)
        for row, value in enumerate(row_loop(block, (zero, zero))):
            value = jnp.sum(value, axis=0, keepdims=True)
            for c in range(wide // TILE):
                payload[layer, i * (wide // TILE) + c, row : row + 1] = value[:, c * TILE : (c + 1) * TILE]

    def du_tile(layer, i):
        u_tile(u2, i).wait()
        pl.when(i + 1 < tiles)(lambda: start_u(layer, i + 1))
        at_cols = rows(i * wide, wide)
        gain, mean, inv = (vec[layer * 4 + j, :, at_cols] for j in (0, 2, 3))
        means = jnp.concatenate([sums[layer, i * (wide // TILE) + c] for c in range(wide // TILE)], axis=1) / row_count
        mean_gn, mean_g = means[0:1], means[1:2]
        scale = gain * inv

        def block(r, c):
            at = rows(r * BLOCK, BLOCK)
            n = (out0[rows(rows_dev + r * BLOCK, BLOCK), rows((i % 2) * wide, wide)] - mean) * inv
            value = (dpre[at, at_cols] - mean_g - n * mean_gn) * scale
            dy[1 - layer, rows(core * rows_dev + r * BLOCK, BLOCK), at_cols] = value.astype(jnp.bfloat16)
            return c

        row_loop(block, 0)

    in_last = (MATS - 1) * PARTS
    quarter = part_rows // 4

    def home_row(k):
        return core * half + (k % PARTS) * part_rows

    def homes(k):
        return [
            (k < in_last, lambda off, size: gathered.at[k % GATHER_SLOTS, pl.ds(pl.multiple_of(off, quarter), size)]),
            (k >= in_last, lambda off, size: out0.at[pl.ds(pl.multiple_of(home_row(k) + off, quarter), size)]),
        ]

    def finish(k, off, size, buf):
        j = k % ACC_SLOTS
        value = acc[j, rows(off, size)] + buf[j]

        @pl.when(k < in_last)
        def _():
            gathered[k % GATHER_SLOTS, rows(off, size)] = value

        @pl.when(k >= in_last)
        def _():
            out0[rows(home_row(k) + off, size)] = value

    chunks = ChunkSum(place, "xl", back_kind, acc, homes, landing, send, recv, finish)

    def form(k, group):
        w, j = k // PARTS, k % ACC_SLOTS

        @pl.when(k % PARTS == 0)
        def _():
            pltpu.make_async_copy(xs.at[w % 2], xs.at[w % 2], in_sem.at[w]).wait()
            pl.when(w > 0)(lambda: peer_dy(w).wait_recv())

        at = rows((k % PARTS) * part_rows, group * part_rows)

        def col(c):
            pl.when(k == 0)(lambda: load_dz(c).wait())
            cs = rows(c * size, size)
            acc[pl.ds(j, group), :, cs] = contract_rows(xs[w % 2, :, at], dy[w % 2, :, cs]).reshape(group, part_rows, size)

        loop(0, width // size, col)

    def out_rows(k, side):
        return pl.ds(pl.multiple_of(side * half + (k % PARTS) * part_rows, part_rows), part_rows)

    def last_copy(out, k, side):
        return chunks.copy(gathered.at[k % GATHER_SLOTS], out.at[out_rows(k, side)], 7, k, other_core)

    def store_copy(out, k):
        return pltpu.make_async_copy(gathered.at[k % GATHER_SLOTS], out.at[out_rows(k, core)], store_sem.at[k])

    def stage(i, k):
        if i == 0:
            form_next(k, form)
            return
        chunks.stage(i, k)
        own_rows = out0.at[pl.ds(pl.multiple_of(home_row(k), part_rows), part_rows)]
        in_place = chunks.copy(own_rows, own_rows, 7, k, other_core)
        last = k // PARTS == MATS - 1

        def emit(out):
            last_copy(out, k, core).start()
            store_copy(out, k).start()

        def emit_any():
            pick(k // PARTS, outs, emit)
            pl.when(last)(lambda: in_place.start())

        if i == 8:
            pl.when(back_kind("x", k))(emit_any)
        if i == 9:
            pl.when(back_kind("l", k))(emit_any)
        if i == 10:

            def close(out):
                last_copy(out, k, 1 - core).wait_recv()
                store_copy(out, k).wait()
                last_copy(out, k, core).wait_send()

            pick(k // PARTS, outs, close)

            @pl.when(last)
            def _():
                in_place.wait_recv()
                in_place.wait_send()

    def layer_work(t):
        layer = t // LAYER_SLOTS
        at = t - LAYER_SLOTS * layer
        first_du = 2 * tiles + 3
        pl.when((at < 2 * tiles) & (at % 2 == 1))(lambda: chain_tile(layer, at // 2))
        @pl.when(at == 2 * tiles)
        def _():
            for part in range(len(SUM_PARTS)):
                small.begin(layer, part)

        @pl.when(at == 2 * tiles + 1)
        def _():
            for part in range(len(SUM_PARTS)):
                small.middle(layer, part)


        pl.when(at == 2 * tiles + 2)(lambda: start_u(layer, 0))

        pl.when(at == first_du)(lambda: small.end(layer))
        pl.when(at >= first_du)(lambda: du_tile(layer, at - first_du))

        @pl.when(at == LAYER_SLOTS - 1)
        def _():
            peer_dy(layer + 1).start()

            @pl.when(layer == 0)
            def _():
                w_tile(weights[1], 0).start()
                u_tile(pres[1], 0).start()

            @pl.when(layer == 1)
            def _():
                load_x(2).start()
                for c in range(PLANE):
                    for row in range(4):
                        sums_out[row : row + 1, c * TILE : (c + 1) * TILE] = sums[row // 2, c, row % 2 : row % 2 + 1]
                sums_out[4:5] = jnp.full((1, width), jnp.sum(vec[8]))
                sums_store.start()


    form(0, GROUP // 2)
    place.all_here()
    vec_load.wait()
    run_slots(BACK_PLAN, count, stage, lambda t: pl.when(t < 2 * LAYER_SLOTS)(lambda: layer_work(t)))
    for w in (1, 2):
        peer_dy(w).wait_send()
    sums_store.wait()


def backward(grad_z, x2, x1, x0, w_out, w_mid, u2, u1, vec):
    rows_dev, width = u2.shape
    part_rows = width // 2 // PARTS
    count = MATS * PARTS
    any_spec = pl.BlockSpec(memory_space=pl.ANY)
    vmem_spec = pl.BlockSpec(memory_space=pltpu.VMEM)
    mat = jax.ShapeDtypeStruct((width, width), jnp.float32)
    dma = pltpu.SemaphoreType.DMA
    return pl.pallas_call(
        back_kernel,
        name="backward",
        out_shape=[mat, mat, pltpu.VMEM((width, width), jnp.float32), jax.ShapeDtypeStruct((5, width), jnp.float32)],
        in_specs=[any_spec] * 9,
        out_specs=[any_spec] * 2 + [vmem_spec, any_spec],
        scratch_shapes=[
            pltpu.VMEM((2, 2 * rows_dev, width), jnp.bfloat16),
            pltpu.VMEM((2, 2 * rows_dev, width // 2), jnp.bfloat16),
            pltpu.VMEM((WIDE, width), jnp.bfloat16),
            pltpu.VMEM((9, 1, width), jnp.float32),
            pltpu.VMEM((5, width), jnp.float32),
            dma((MATS + 2,)),
            dma((2, 2)),
            dma((2,)),
            dma((MATS,)),
            dma((MATS,)),
            dma((count,)),
        ]
        + small_scratch(2)
        + chunk_scratch(ACC_SLOTS, GATHER_SLOTS, part_rows, width, count, jnp.float32),
        compiler_params=pltpu.CompilerParams(collective_id=1, has_side_effects=True, vmem_limit_bytes=BACK_VMEM),
    )(grad_z, x2, x1, x0, w_out, w_mid, u2, u1, vec)


def copy_kernel(*refs):
    pairs = (len(refs) - 6 - 6) // 2
    ins, small, outs, small_outs = refs[:pairs], refs[pairs], refs[pairs + 1 : 2 * pairs + 1], refs[2 * pairs + 1 : -6]
    buf, small_buf, in_sem, out_sem, small_sem, near_sem = refs[-6:]
    blocks = [(i, r) for i in range(pairs - 1) for r in range(0, ins[i].shape[0], COPY_ROWS)]
    near = pltpu.make_async_copy(ins[-1], outs[-1], near_sem.at[0])

    def read(b):
        i, r = blocks[b]
        return pltpu.make_async_copy(ins[i].at[pl.ds(r, COPY_ROWS)], buf.at[b % COPY_BUFS], in_sem.at[b % COPY_BUFS])

    def write(b):
        i, r = blocks[b]
        return pltpu.make_async_copy(buf.at[b % COPY_BUFS], outs[i].at[pl.ds(r, COPY_ROWS)], out_sem.at[b % COPY_BUFS])

    for b in range(len(blocks)):
        read(b).start()
    small_read = pltpu.make_async_copy(small, small_buf, small_sem.at[4])
    small_read.start()

    def small_write(row):
        return pltpu.make_async_copy(small_buf.at[pl.ds(row, 1)], small_outs[row], small_sem.at[row])

    for b in range(len(blocks)):
        read(b).wait()
    near.start()
    for b in range(len(blocks)):
        write(b).start()
    small_read.wait()
    small_outs[4][...] = small_buf[4:5, :1]
    for row in range(4):
        small_write(row).start()
    for row in range(4):
        small_write(row).wait()
    near.wait()
    for b in range(len(blocks)):
        write(b).wait()


def copy_out(arrays, small):
    any_spec = pl.BlockSpec(memory_space=pl.ANY)
    vmem_spec = pl.BlockSpec(memory_space=pltpu.VMEM)
    dma = pltpu.SemaphoreType.DMA
    width = small.shape[1]
    row = jax.ShapeDtypeStruct((1, width), jnp.float32)
    return pl.pallas_call(
        copy_kernel,
        name="copy_out",
        out_shape=[jax.ShapeDtypeStruct(a.shape, a.dtype) for a in arrays] + [row] * 4 + [jax.ShapeDtypeStruct((1, 1), jnp.float32)],
        in_specs=[any_spec] * (len(arrays) - 1) + [vmem_spec, any_spec],
        out_specs=[any_spec] * (len(arrays) + 4) + [vmem_spec],
        scratch_shapes=[
            pltpu.VMEM((COPY_BUFS, COPY_ROWS, width), jnp.float32),
            pltpu.VMEM(small.shape, jnp.float32),
            dma((COPY_BUFS,)),
            dma((COPY_BUFS,)),
            dma((5,)),
            dma((1,)),
        ],
        compiler_params=pltpu.CompilerParams(vmem_limit_bytes=COPY_VMEM),
    )(*arrays[:-1], pltpu.with_memory_space_constraint(arrays[-1], pltpu.VMEM), small)


def solution(mesh):
    row_part = P(DATA_AXIS, None)
    replicated = P()

    def local_step(feat_a, feat_b, w_in, w_mid, w_out, t_in, t_mid, t_out, gain_1, bias_1, gain_2, bias_2, off_weight):
        affine = [v.reshape(1, -1) for v in (gain_1, bias_1, gain_2, bias_2)]
        pre_1, pre_2, xs_2, xs_1, xs_0, grad_z, grad_emb, vec = front(
            feat_a, feat_b, (w_in, t_in, w_mid, t_mid, w_out, t_out), affine, off_weight.reshape(1)
        )
        grad_w_out, grad_w_mid, grad_w_in, sums = backward(grad_z, xs_2, xs_1, xs_0, w_out, w_mid, pre_2, pre_1, vec)
        (grad_emb, grad_w_out, grad_w_mid, grad_w_in, gain_2, bias_2, gain_1, bias_1, loss) = copy_out((grad_emb, grad_w_out, grad_w_mid, grad_w_in), sums)
        gain_1, bias_1, gain_2, bias_2 = (v.reshape(-1) for v in (gain_1, bias_1, gain_2, bias_2))
        return (loss.reshape(()), grad_emb, grad_w_in, grad_w_mid, grad_w_out, gain_1, bias_1, gain_2, bias_2)

    return jax.shard_map(local_step, mesh=mesh, in_specs=(row_part, row_part) + (replicated,) * 11, out_specs=(replicated, row_part) + (replicated,) * 7, check_vma=False)
```

```python
import functools

import jax
import jax.numpy as jnp
from jax import lax
from jax.experimental import pallas as pl
from jax.experimental.pallas import tpu as pltpu
from jax.sharding import PartitionSpec as P

NORM_EPS = 1e-5
DATA_AXIS = "data"
MESH = pl.DeviceIdType.MESH
VMEM_BYTES = 67_043_328
PLANE = 8
DEPTH = 4
TILE = 256
WIDE = 512
BLOCK = 256
BACK_BLOCK = 128
SUM_ROWS = 2
SUM_PARTS = ((0, 6), (6, 2))
PARTS = 16
GROUP = 4
MATS = 3
ACC_SLOTS = 16
GATHER_SLOTS = 14
BACK_VMEM = 49_800_000
COPY_VMEM = 42 * 1024 * 1024
JOBS = 6
W_BUFS = 3
LAYER_SLOTS = 15
COPY_ROWS = 256
COPY_BUFS = 18
FRONT_PLAN = ((0, 0, 3, 5, 7, 9, 12, 13, 16, 17, 18), (0, 6, 3, 4, 9, 10, 8, 5, 2, 7, 1))
BACK_PLAN = ((0, 0, 3, 5, 7, 8, 9, 11, 14, 17, 19), (0, 4, 8, 7, 10, 1, 2, 3, 5, 6, 9))


def front_kind(kind, k):
    s, l = (k % 5 == 2) & (k > 2), k == 2
    return {"s": s, "l": l, "x": (k % 5 != 2)}[kind]


def back_kind(kind, k):
    l = ((k % 5 == 2) & (k < 43)) | ((k % 5 == 0) & (k >= 10) & (k < 36))
    return l if kind == "l" else jnp.logical_not(l)


def contract_rows(left_op, right_op):
    return lax.dot_general(left_op, right_op, (((0,), (0,)), ((), ())), preferred_element_type=jnp.float32)


def contract_cols(left_op, right_op):
    return lax.dot_general(left_op, right_op, (((1,), (1,)), ((), ())), preferred_element_type=jnp.float32)


def rows(off, size):
    return pl.ds(pl.multiple_of(off, size), size)


def pick(index, choices, what):
    for i, c in enumerate(choices):
        pl.when(index == i)(functools.partial(what, c))


def loop(lo, hi, body):
    def step(i, carry):
        body(i)
        return carry

    lax.fori_loop(lo, hi, step, 0)


def remote_copy(src, dst, send, recv, mate):
    return pltpu.make_async_remote_copy(src, dst, send, recv, device_id=(mate,), device_id_type=MESH)


class Place:
    def __init__(self):
        me = lax.axis_index(DATA_AXIS)
        self.me = me
        self.pos, self.plane = me % PLANE, me // PLANE
        self.core, self.bx, self.by, self.bz0, self.bz1 = me % 2, (me // 2) % 2, (me // 4) % 2, (me // 8) % 2, (me // 16) % 2
        self.other_core = me + 1 - 2 * self.core
        self.mates = [(self.pos + d) % PLANE for d in range(1, PLANE)]
        self.levels = [(self.plane + d) % DEPTH for d in range(1, DEPTH)]

    def peers(self):
        return [self.plane * PLANE + m for m in self.mates] + [lv * PLANE + self.pos for lv in self.levels]

    def arrive(self):
        sem = pltpu.get_barrier_semaphore()
        for peer in self.peers():
            pl.semaphore_signal(sem, inc=1, device_id=(peer,), device_id_type=MESH)

    def all_here(self):
        pl.semaphore_wait(pltpu.get_barrier_semaphore(), PLANE + DEPTH - 2)


class SmallSum:
    def __init__(self, place, payload, total, depth_buf, line_sum, plane_buf, sems):
        self.p, self.payload, self.total = place, payload, total
        self.depth_buf, self.line_sum, self.plane_buf, self.sems = depth_buf, line_sum, plane_buf, sems

    def along(self, j, part, lv, slot):
        (s, r), at = self.sems[:2], pl.ds(*SUM_PARTS[part])
        n = part * DEPTH
        return remote_copy(self.payload.at[j, at], self.depth_buf.at[j, slot, at], s.at[j, n + lv], r.at[j, n + slot], lv * PLANE + self.p.pos)

    def within(self, j, part, m, slot):
        (s, r), at = self.sems[2:], pl.ds(*SUM_PARTS[part])
        n = part * PLANE
        return remote_copy(self.line_sum.at[j, at], self.plane_buf.at[j, slot, at], s.at[j, n + m], r.at[j, n + slot], self.p.plane * PLANE + m)

    def begin(self, j, part):
        at = pl.ds(*SUM_PARTS[part])
        for lv in self.p.levels:
            self.along(j, part, lv, self.p.plane).start()
        self.depth_buf[j, self.p.plane, at] = self.payload[j, at]

    def middle(self, j, part):
        at = pl.ds(*SUM_PARTS[part])
        for lv in self.p.levels:
            self.along(j, part, lv, lv).wait_recv()
        total = self.depth_buf[j, 0, at]
        for i in range(1, DEPTH):
            total = total + self.depth_buf[j, i, at]
        self.line_sum[j, at] = total
        for m in self.p.mates:
            self.within(j, part, m, self.p.pos).start()
        self.plane_buf[j, self.p.pos, at] = total

    def end(self, j):
        for part in range(len(SUM_PARTS)):
            for m in self.p.mates:
                self.within(j, part, m, m).wait_recv()
        total = self.plane_buf[j, 0]
        for i in range(1, PLANE):
            total = total + self.plane_buf[j, i]
        self.total[j] = total
        for part in range(len(SUM_PARTS)):
            for lv in self.p.levels:
                self.along(j, part, lv, self.p.plane).wait_send()
            for m in self.p.mates:
                self.within(j, part, m, self.p.pos).wait_send()


def small_scratch(count):
    def buf(*lead):
        return pltpu.VMEM((count, *lead, PLANE, SUM_ROWS, TILE), jnp.float32)

    return [buf(), buf(), buf(DEPTH), buf(), buf(PLANE)] + [pltpu.SemaphoreType.DMA((count, n * len(SUM_PARTS))) for n in (DEPTH, DEPTH, PLANE, PLANE)]


SMALL_REFS = 9


def small_sum(place, refs):
    return SmallSum(place, *refs[:5], refs[5:])


class Homed:
    def __init__(self, homes, make):
        self.homes, self.make = homes, make

    def do(self, what):
        for when, home in self.homes:
            run = lambda home=home: getattr(self.make(home), what)()
            run() if when is None else pl.when(when)(run)

    def start(self):
        self.do("start")

    def wait_recv(self):
        self.do("wait_recv")

    def wait_send(self):
        self.do("wait_send")


class ChunkSum:
    def __init__(self, place, kinds, is_kind, acc, homes, landing, send, recv, finish):
        self.p, self.kinds, self.is_kind, self.slots, self.homes = place, kinds, is_kind, acc.shape[0], homes
        self.acc, self.landing, self.send, self.recv, self.finish = acc, landing, send, recv, finish
        self.size = acc.shape[1]
        self.s2, self.s4 = self.size // 2, self.size // 4
        core, bx, by, me = place.core, place.bx, place.by, place.me
        first, second = core * by + (1 - core) * bx, core * bx + (1 - core) * by
        self.xy = ((me + (2 + 2 * core) * (1 - 2 * first), first), (me + (4 - 2 * core) * (1 - 2 * second), second))
        self.zz = ((me + 8 * (1 - 2 * place.bz0), place.bz0), (me + 16 * (1 - 2 * place.bz1), place.bz1))
        self.is_mid = place.bz0 + place.bz1 - 2 * place.bz0 * place.bz1
        self.mid, self.end = self.is_mid == 1, self.is_mid == 0
        self.z_mate = self.zz[0][0]
        self.mid_mate = me + 8 * (1 - 2 * place.bz1)

    def copy(self, src, dst, stage, k, mate):
        return remote_copy(src, dst, self.send.at[stage, k], self.recv.at[stage, k], mate)

    def span(self, off, size):
        return pl.ds(pl.multiple_of(off, self.s4), size)

    def down(self, stage, k, off, size, mate, buf=None):
        j = k % self.slots
        buf = self.landing[stage] if buf is None else buf
        return self.copy(self.acc.at[j, self.span(off, size)], buf.at[j, pl.ds(0, size)], stage, k, mate)

    def up(self, stage, k, off, size, mate):
        return Homed(self.homes(k), lambda home: self.copy(home(off, size), home(off, size), stage, k, mate))

    def add(self, k, off, size, buf):
        step = min(size, 16)
        j = k % self.slots

        def body(i):
            at = pl.ds(pl.multiple_of(off + i * step, step), step)
            self.acc[j, at] = self.acc[j, at] + buf[j, rows(i * step, step)]

        loop(0, size // step, body)

    def stage(self, i, k):
        for kind in self.kinds:
            run = {"x": self.stage_x, "s": self.stage_s, "l": self.stage_l}[kind]
            pl.when(self.is_kind(kind, k))(functools.partial(run, i, k))

    def stage_x(self, i, k):
        (m1, b1), (m2, b2), s2, s4 = *self.xy, self.s2, self.s4
        off1, off2 = b1 * s2, b1 * s2 + b2 * s4
        half = lambda: self.down(0, k, (1 - b1) * s2, s2, m1)
        quarter = lambda: self.down(1, k, off1 + (1 - b2) * s4, s4, m2)
        inward = lambda: self.down(2, k, off2, s4, self.z_mate)
        across = lambda: self.down(3, k, off2, s4, self.mid_mate)
        outward = lambda: self.up(4, k, off2, s4, self.z_mate)
        back4 = lambda: self.up(5, k, off2, s4, m2)
        back2 = lambda: self.up(6, k, off1, s2, m1)
        if i == 1:
            half().start()
        elif i == 2:
            half().wait_recv()
            self.add(k, off1, s2, self.landing[0])
            quarter().start()
        elif i == 3:
            quarter().wait_recv()
            self.add(k, off2, s4, self.landing[1])
            pl.when(self.end)(lambda: inward().start())
        elif i == 4:

            @pl.when(self.mid)
            def _():
                inward().wait_recv()
                self.add(k, off2, s4, self.landing[2])
                across().start()

        elif i == 5:

            @pl.when(self.mid)
            def _():
                across().wait_recv()
                self.finish(k, off2, s4, self.landing[3])
                outward().start()

        elif i == 6:
            pl.when(self.end)(lambda: outward().wait_recv())
            back4().start()
            half().wait_send()
            quarter().wait_send()
            pl.when(self.end)(lambda: inward().wait_send())
            pl.when(self.mid)(lambda: across().wait_send())
        elif i == 7:
            back4().wait_recv()
            back2().start()
        elif i == 8:
            back2().wait_recv()
        elif i == 10:
            pl.when(self.mid)(lambda: outward().wait_send())
            back4().wait_send()
            back2().wait_send()

    def stage_s(self, i, k):
        (m1, b1), (m2, b2), s2, s4 = *self.zz, self.s2, self.s4
        off1, off2 = b1 * s2, b1 * s2 + b2 * s4
        half = lambda: self.down(0, k, (1 - b1) * s2, s2, m1)
        quarter = lambda: self.down(1, k, off1 + (1 - b2) * s4, s4, m2)
        whole_1 = lambda: self.down(2, k, off2, s4, self.xy[0][0])
        whole_2 = lambda: self.down(3, k, off2, s4, self.xy[1][0])
        back4 = lambda: self.up(5, k, off2, s4, m2)
        back2 = lambda: self.up(6, k, off1, s2, m1)
        if i == 1:
            half().start()
        elif i == 2:
            half().wait_recv()
            self.add(k, off1, s2, self.landing[0])
            quarter().start()
        elif i == 3:
            quarter().wait_recv()
            self.add(k, off2, s4, self.landing[1])
            whole_1().start()
        elif i == 4:
            whole_1().wait_recv()
            whole_1().wait_send()
            self.add(k, off2, s4, self.landing[2])
            whole_2().start()
        elif i == 5:
            whole_2().wait_recv()
            self.finish(k, off2, s4, self.landing[3])
        elif i == 6:
            back4().start()
            half().wait_send()
            quarter().wait_send()
            whole_2().wait_send()
        elif i == 7:
            back4().wait_recv()
            back2().start()
        elif i == 8:
            back2().wait_recv()
        elif i == 10:
            back4().wait_send()
            back2().wait_send()

    def stage_l(self, i, k):
        s2, s4 = self.s2, self.s4
        s3 = s2 + s4
        b0, b1 = self.p.bz0, self.p.bz1
        own, side, tip, rest = (2 * b1 + b0) * s4, b1 * s2, 3 * b1 * s4, (1 - b1) * s4
        inward = lambda: self.down(0, k, rest, s3, self.z_mate)
        across = lambda: self.down(1, k, (1 - b1) * s2, s2, self.mid_mate)
        outward = lambda: self.down(2, k, tip, s4, self.z_mate)
        whole_1 = lambda: self.down(3, k, own, s4, self.xy[0][0])
        whole_2 = lambda: self.down(8, k, own, s4, self.xy[1][0], self.landing[4])
        tip_back = lambda: self.up(4, k, tip, s4, self.z_mate)
        side_back = lambda: self.up(5, k, side, s2, self.mid_mate)
        rest_back = lambda: self.up(6, k, rest, s3, self.z_mate)
        if i == 1:
            pl.when(self.end)(lambda: inward().start())
        elif i == 2:

            @pl.when(self.mid)
            def _():
                inward().wait_recv()
                self.add(k, rest, s3, self.landing[0])
                across().start()

        elif i == 3:

            @pl.when(self.mid)
            def _():
                across().wait_recv()
                self.add(k, side, s2, self.landing[1])
                outward().start()

        elif i == 4:

            @pl.when(self.end)
            def _():
                outward().wait_recv()
                self.add(k, own, s4, self.landing[2])

            whole_1().start()
        elif i == 5:
            whole_1().wait_recv()
            whole_1().wait_send()
            pl.when(self.mid)(lambda: outward().wait_send())
            self.add(k, own, s4, self.landing[3])
            whole_2().start()
        elif i == 6:
            whole_2().wait_recv()
            self.finish(k, own, s4, self.landing[4])
            pl.when(self.end)(lambda: tip_back().start())
            whole_2().wait_send()
            pl.when(self.end)(lambda: inward().wait_send())
            pl.when(self.mid)(lambda: across().wait_send())
        elif i == 7:

            @pl.when(self.mid)
            def _():
                tip_back().wait_recv()
                side_back().start()

        elif i == 8:

            @pl.when(self.mid)
            def _():
                side_back().wait_recv()
                rest_back().start()

        elif i == 9:
            pl.when(self.end)(lambda: rest_back().wait_recv())
        elif i == 10:
            pl.when(self.end)(lambda: tip_back().wait_send())

            @pl.when(self.mid)
            def _():
                side_back().wait_send()
                rest_back().wait_send()


def form_next(k, form):
    pl.when(k == 1)(lambda: form(GROUP // 2, GROUP // 2))
    pl.when((k % GROUP == 0) & (k > 0))(lambda: form(k, GROUP))


def run_slots(plan, count, stage, between):
    lags, order = plan

    def slot(t):
        for i in order:
            k = t - lags[i]

            @pl.when((k >= 0) & (k < count))
            def _():
                stage(i, k)

            if i == 1:
                between(t)

    loop(0, count + lags[-1], slot)


def chunk_scratch(slots, gather_slots, part_rows, width, count, dtype):
    def buf(n):
        return pltpu.VMEM((slots, n, width), jnp.float32)

    gathered = pltpu.VMEM((gather_slots, part_rows, width), dtype)

    dma = pltpu.SemaphoreType.DMA
    quarter = part_rows // 4
    return [buf(part_rows), gathered, *(buf(n * quarter) for n in (3, 2, 1, 1, 1)), dma((9, count)), dma((9, count))]


def fold(value):
    return jnp.sum(value.reshape(value.shape[0] // 8, 8, value.shape[1]), axis=0)


def front_kernel(feat_a, feat_b, w_in, t_in, w_mid, t_mid, w_out, t_out, gain1, bias1, gain2, bias2, off_hbm, pre1, pre2, xs2, xs1, xs0, dz, grad_emb, vec_hbm, *scratch):
    (x_buf, u_buf, w_buf, stats, affine, loss, vec, off_weight, ea, eb, g_peer) = scratch[:11]
    (x_sem, w_sem, row_sem, pre_sem, keep_sem, keep_send, keep_recv, ge_sem, e_send, e_recv) = scratch[11:21]
    small_refs = scratch[21 : 21 + SMALL_REFS]
    acc, gathered, *landing, send, recv = scratch[21 + SMALL_REFS :]
    rows_dev, width = feat_a.shape
    wide = w_buf.shape[2]
    tiles = width // wide
    half = width // 2
    part_rows = half // PARTS
    row_count = rows_dev * DEPTH * PLANE
    weights, feats = (w_in, t_in, w_mid, t_mid, w_out, t_out), (feat_a, feat_b)
    place = Place()
    core = place.core
    mine = rows(core * rows_dev, rows_dev)
    place.arrive()
    small = small_sum(place, small_refs)
    payload, total = small.payload, small.total

    def feat(v):
        return pltpu.make_async_copy(feats[v], x_buf.at[v], x_sem.at[v])

    def w_tile(ref, g):
        return pltpu.make_async_copy(ref.at[:, rows((g % tiles) * wide, wide)], w_buf.at[g % W_BUFS], w_sem.at[g % W_BUFS])

    def start_w(g):
        pick(g // tiles, weights, lambda ref: w_tile(ref, g).start())

    feat(0).start()
    w_tile(weights[0], 0).start()
    feat(1).start()
    for g in range(1, W_BUFS - 1):
        start_w(g)
    row_loads = [pltpu.make_async_copy(ref, affine.at[j], row_sem.at[j]) for j, ref in enumerate((gain1, bias1, gain2, bias2))]
    row_loads.append(pltpu.make_async_copy(off_hbm, off_weight, row_sem.at[4]))
    for c in row_loads:
        c.start()
    early_rows = pltpu.make_async_copy(vec.at[pl.ds(0, 8)], vec_hbm.at[pl.ds(0, 8)], row_sem.at[5])
    late_row = pltpu.make_async_copy(vec.at[pl.ds(8, 1)], vec_hbm.at[pl.ds(8, 1)], row_sem.at[6])
    feat(0).wait()
    payload[...] = jnp.zeros_like(payload)

    def keep_pre(ref):
        return pltpu.make_async_copy(u_buf.at[0], ref, pre_sem.at[0])

    kept = (xs0, xs1, xs2)

    def keep_x(w):
        here = pltpu.make_async_copy(x_buf.at[0, :, rows(core * half, half)], kept[w].at[mine], keep_sem.at[w])
        there = remote_copy(x_buf.at[0, :, rows((1 - core) * half, half)], kept[w].at[mine], keep_send.at[w], keep_recv.at[w], place.other_core)
        return here, there

    def start_x(w):
        for c in keep_x(w):
            c.start()

    def free_x(w):
        here, there = keep_x(w)
        here.wait()
        there.wait_send()

    def keep_dz(i):
        at = (slice(None), rows(i * wide, wide))
        here = pltpu.make_async_copy(x_buf.at[(0, *at)], dz.at[mine, at[1]], keep_sem.at[3 + i])
        there = remote_copy(x_buf.at[(0, *at)], dz.at[mine, at[1]], keep_send.at[3 + i], keep_recv.at[3 + i], place.other_core)
        return here, there

    def row_loop(body, carry):
        return lax.fori_loop(0, rows_dev // BLOCK, lambda r, c: body(rows(r * BLOCK, BLOCK), c), carry)

    def put_sums(j, i, row, value):
        value = jnp.sum(value, axis=0, keepdims=True)
        for c in range(value.shape[1] // TILE):
            payload[j, i + c, row : row + 1] = value[:, c * TILE : (c + 1) * TILE]

    def product(g):
        job, i = g // tiles, g % tiles
        view = job % 2
        w_tile(w_in, g).wait()
        pl.when(g + W_BUFS - 1 < JOBS * tiles)(lambda: start_w(g + W_BUFS - 1))
        at_cols = rows(i * wide, wide)
        u_buf[view, :, at_cols] = jnp.dot(x_buf[view], w_buf[g % W_BUFS], preferred_element_type=jnp.float32)

        def block(at, sums):
            u = u_buf[view, at, at_cols]
            return sums[0] + fold(u), sums[1] + fold(u * u)

        zero = jnp.zeros((8, wide), jnp.float32)
        for row, value in enumerate(row_loop(block, (zero, zero))):
            put_sums(job, i * (wide // TILE), row, value)

    def keep(job):
        @pl.when(job % 2 == 0)
        def _():
            pick(job // 2, (pre1, pre2), lambda ref: keep_pre(ref).start())

    def norm(job):
        layer, view = job // 2, job % 2
        small.end(job)
        for c in range(PLANE):
            at = slice(c * TILE, (c + 1) * TILE)
            means = total[job, c] / row_count
            stats[job, 0, :, at] = means[0:1]
            stats[job, 1, :, at] = lax.rsqrt(means[1:2] - means[0:1] * means[0:1] + NORM_EPS)

        pl.when(view == 0)(lambda: pick(layer, (0, 1, 2), free_x))

        def hidden(i):
            at_cols = rows(i * wide, wide)
            mean, inv = stats[job, 0, :, at_cols], stats[job, 1, :, at_cols]
            gain, bias = affine[layer * 2, :, at_cols], affine[layer * 2 + 1, :, at_cols]

            def block(at, c):
                n = (u_buf[view, at, at_cols] - mean) * inv
                x_buf[view, at, at_cols] = jnp.maximum(n * gain + bias, 0.0).astype(jnp.bfloat16)
                return c

            row_loop(block, 0)

        def student(i):
            at_cols = rows(i * wide, wide)
            mean, inv = stats[job, 0, :, at_cols], stats[job, 1, :, at_cols]

            def block(at, c):
                n = (u_buf[0, at, at_cols] - mean) * inv
                u_buf[0, at, at_cols] = n
                x_buf[0, at, at_cols] = n.astype(jnp.bfloat16)
                return c

            row_loop(block, 0)

        def student_own(i):
            def block(r, c):
                ea[rows(core * rows_dev + r * BLOCK, BLOCK), rows(i * wide, wide)] = x_buf[0, rows(r * BLOCK, BLOCK), rows(core * half + i * wide, wide)]
                return c

            lax.fori_loop(0, rows_dev // BLOCK, block, 0)

        def teacher(i):
            at_cols = rows(i * wide, wide)
            mean, inv = stats[job, 0, :, at_cols], stats[job, 1, :, at_cols]

            def block(r, c):
                n = (u_buf[1, rows(r * BLOCK, BLOCK), at_cols] - mean) * inv
                eb[rows(core * rows_dev + r * BLOCK, BLOCK), at_cols] = n.astype(jnp.bfloat16)
                return c

            lax.fori_loop(0, rows_dev // BLOCK, block, 0)
            eb_copy(i).start()

        @pl.when(layer < 2)
        def _():
            loop(0, tiles, hidden)

            @pl.when(view == 0)
            def _():
                pick(layer, (1, 2), start_x)
                keep_pre(pre1).wait()

        @pl.when((layer == 2) & (view == 0))
        def _():
            loop(0, tiles, student)
            ea_copy().start()
            loop(0, tiles // 2, student_own)

        @pl.when((layer == 2) & (view == 1))
        def _():
            loop(0, tiles, teacher)

    ea_copy = lambda: remote_copy(x_buf.at[0, :, rows((1 - core) * half, half)], ea.at[mine], e_send.at[0], e_recv.at[0], place.other_core)

    def eb_copy(i):
        block = eb.at[mine, rows(i * wide, wide)]
        return remote_copy(block, block, e_send.at[1 + i], e_recv.at[1 + i], place.other_core)

    def step(g):
        job, i = g // tiles, g % tiles
        view = job % 2
        pl.when(g == tiles)(lambda: feat(1).wait())
        product(g)

        @pl.when(g == 0)
        def _():
            place.all_here()
            start_x(0)
            for c in row_loads:
                c.wait()

        pl.when(i == tiles - 2)(lambda: small.begin(job, 0))
        pl.when((i == 0) & (job > 0))(lambda: small.middle(job - 1, 0))
        pl.when((i == 1) & (job > 0))(lambda: small.middle(job - 1, 1))

        @pl.when(i == tiles - 1)
        def _():
            small.begin(job, 1)
            keep(job)
            pl.when(job == JOBS - 1)(lambda: small.middle(job, 0))
            pl.when(job > 0)(lambda: norm(job - 1))

    loop(0, JOBS * tiles, step)
    small.middle(JOBS - 1, 1)
    norm(JOBS - 1)
    for j, source in enumerate((affine.at[2], affine.at[3], stats.at[2, 0], stats.at[2, 1], affine.at[0], affine.at[1], stats.at[0, 0], stats.at[0, 1])):
        vec[j] = source[...]
    early_rows.start()

    loss[...] = jnp.zeros_like(loss)

    def finish(k, off, size, buf):
        share = jnp.where(front_kind("x", k), 0.5, 0.25)
        at = rows(off, size)
        corr = (acc[k, at] + buf[k]) / row_count
        row = core * half + k * part_rows + off
        diag = (row + lax.broadcasted_iota(jnp.int32, (size, width), 0)) == lax.broadcasted_iota(jnp.int32, (size, width), 1)
        weight = off_weight[0]
        miss = 1.0 - corr
        loss[...] += share * jnp.sum(jnp.where(diag, miss * miss, weight * (corr * corr)), axis=0, keepdims=True)
        gathered[k, at] = jnp.where(diag, -2.0 * miss, 2.0 * weight * corr).astype(jnp.bfloat16)

    def homes(k):
        return [(None, lambda off, size: gathered.at[k, pl.ds(pl.multiple_of(off, part_rows // 4), size)])]

    chunks = ChunkSum(place, "xsl", front_kind, acc, homes, landing, send, recv, finish)

    def form(k, group):
        at = rows(k * part_rows, group * part_rows)
        size = min(1024, width)

        def col(c):
            @pl.when(k == 0)
            def _():
                for i in range(size // wide):
                    eb_copy(c * (size // wide) + i).wait_recv()

            cs = rows(c * size, size)
            acc[pl.ds(k, group), :, cs] = contract_rows(ea[:, at], eb[:, cs]).reshape(group, part_rows, size)

        loop(0, width // size, col)

    def swap(k):
        return chunks.copy(gathered.at[k], g_peer.at[k], 7, k, place.other_core)

    def ge_cols(k, side):
        return rows(side * half + k * part_rows, GROUP * part_rows)

    def ge_copy(k, side):
        at = ge_cols(k, side)
        return pltpu.make_async_copy(u_buf.at[1, :, at], grad_emb.at[:, at], ge_sem.at[k // GROUP, side])

    def embed(k, side, g_rows):
        at_cols = ge_cols(k, side)
        grad = contract_cols(eb[mine], g_rows.reshape(GROUP * part_rows, width)) / row_count
        u_buf[1, :, at_cols] = grad
        ge_copy(k, side).start()

        def block(at, sums):
            g = u_buf[1, at, at_cols]
            return sums[0] + fold(g * u_buf[0, at, at_cols]), sums[1] + fold(g)

        zero = jnp.zeros((8, GROUP * part_rows), jnp.float32)
        for row, value in enumerate(row_loop(block, (zero, zero))):
            payload[JOBS, 2 * (k // GROUP) + side, row : row + 1] = jnp.sum(value, axis=0, keepdims=True)

    def stage(i, k):
        if i == 0:
            form_next(k, form)
            return
        chunks.stage(i, k)
        if i == 8:
            pl.when(jnp.logical_not(front_kind("l", k)))(lambda: swap(k).start())
        if i == 9:
            pl.when(front_kind("l", k))(lambda: swap(k).start())

            @pl.when(k % GROUP == GROUP - 1)
            def _():
                embed(k - GROUP + 1, core, gathered[pl.ds(k - GROUP + 1, GROUP)])

        if i == 10:
            swap(k).wait_recv()
            swap(k).wait_send()

            @pl.when(k % GROUP == GROUP - 1)
            def _():
                embed(k - GROUP + 1, 1 - core, g_peer[pl.ds(k - GROUP + 1, GROUP)])

            pl.when(k == PARTS - GROUP - 1)(lambda: small.begin(JOBS, 0))
            pl.when(k == PARTS - 2)(lambda: small.middle(JOBS, 0))

    ea_copy().wait_recv()
    form(0, GROUP // 2)
    run_slots(FRONT_PLAN, PARTS, stage, lambda t: None)
    small.begin(JOBS, 1)
    for c in range(PLANE):
        payload[JOBS + 1, c, 0:1] = loss[:, c * TILE : (c + 1) * TILE]
    ea_copy().wait_send()
    for i in range(tiles):
        eb_copy(i).wait_send()
    small.middle(JOBS, 1)
    for part in range(len(SUM_PARTS)):
        small.begin(JOBS + 1, part)
    for k in range(0, PARTS, GROUP):
        for side in range(2):
            ge_copy(k, side).wait()
    small.end(JOBS)

    def dz_tile(i):
        at_cols = rows(i * wide, wide)
        groups, side = tiles // 2, i // (tiles // 2)
        first = (i % groups) * (wide // TILE)
        sums = jnp.concatenate([total[JOBS, 2 * (first + c) + side] for c in range(wide // TILE)], axis=1) / row_count
        mean_gn, mean_g = sums[0:1], sums[1:2]
        inv = stats[JOBS - 2, 1, :, at_cols]

        def block(at, c):
            value = (u_buf[1, at, at_cols] - mean_g - u_buf[0, at, at_cols] * mean_gn) * inv
            x_buf[0, at, at_cols] = value.astype(jnp.bfloat16)
            return c

        row_loop(block, 0)
        for c in keep_dz(i):
            c.start()

    loop(0, tiles, dz_tile)
    for part in range(len(SUM_PARTS)):
        small.middle(JOBS + 1, part)
    small.end(JOBS + 1)
    for c in range(PLANE):
        vec[8, :, c * TILE : (c + 1) * TILE] = total[JOBS + 1, c, 0:1]
    late_row.start()
    for w in range(3):
        keep_x(w)[1].wait_recv()
    for i in range(tiles):
        here, there = keep_dz(i)
        here.wait()
        there.wait()
    early_rows.wait()
    late_row.wait()


def front(feat_a, feat_b, weights, affine, off_weight):
    rows_dev, width = feat_a.shape
    half = width // 2
    part_rows = half // PARTS
    any_spec = pl.BlockSpec(memory_space=pl.ANY)
    wide_f32 = jax.ShapeDtypeStruct((rows_dev, width), jnp.float32)
    kept = jax.ShapeDtypeStruct((2 * rows_dev, half), jnp.bfloat16)
    both_dz = jax.ShapeDtypeStruct((2 * rows_dev, width), jnp.bfloat16)
    keeps = 3 + width // WIDE
    dma = pltpu.SemaphoreType.DMA
    return pl.pallas_call(
        front_kernel,
        name="front",
        out_shape=[wide_f32, wide_f32, kept, kept, kept, both_dz, wide_f32]
        + [jax.ShapeDtypeStruct((9, 1, width), jnp.float32)],
        in_specs=[any_spec] * 13,
        out_specs=[any_spec] * 8,
        scratch_shapes=[
            pltpu.VMEM((2, rows_dev, width), jnp.bfloat16),
            pltpu.VMEM((2, rows_dev, width), jnp.float32),
            pltpu.VMEM((W_BUFS, width, WIDE), jnp.bfloat16),
            pltpu.VMEM((JOBS, 2, 1, width), jnp.float32),
            pltpu.VMEM((4, 1, width), jnp.float32),
            pltpu.VMEM((1, width), jnp.float32),
            pltpu.VMEM((9, 1, width), jnp.float32),
            pltpu.SMEM((1,), jnp.float32),
            pltpu.VMEM((2 * rows_dev, half), jnp.bfloat16),
            pltpu.VMEM((2 * rows_dev, width), jnp.bfloat16),
            pltpu.VMEM((PARTS, part_rows, width), jnp.bfloat16),
            dma((2,)),
            dma((W_BUFS,)),
            dma((7,)),
            dma((1,)),
            dma((keeps,)),
            dma((keeps,)),
            dma((keeps,)),
            dma((PARTS // GROUP, 2)),
            dma((1 + width // WIDE,)),
            dma((1 + width // WIDE,)),
        ]
        + small_scratch(JOBS + 2)
        + chunk_scratch(PARTS, PARTS, part_rows, width, PARTS, jnp.bfloat16),
        compiler_params=pltpu.CompilerParams(collective_id=0, has_side_effects=True, vmem_limit_bytes=VMEM_BYTES),
    )(feat_a, feat_b, *weights, *affine, off_weight)


def back_kernel(dz_hbm, x2, x1, x0, w_out, w_mid, u2, u1, vec_hbm, out2, out1, out0, sums_hbm, *scratch):
    (dy, xs, w_buf, vec, sums_out) = scratch[:5]
    (in_sem, tile_sem, row_sem, peer_send, peer_recv, store_sem) = scratch[5:11]
    small_refs = scratch[11 : 11 + SMALL_REFS]
    acc, gathered, *landing, send, recv = scratch[11 + SMALL_REFS :]
    rows_dev, width = u2.shape
    wide = w_buf.shape[0]
    tiles = width // wide
    row_count = rows_dev * DEPTH * PLANE
    half = width // 2
    part_rows = half // PARTS
    count = MATS * PARTS
    mats_in, outs, weights, pres = (x2, x1, x0), (out2, out1), (w_out, w_mid), (u2, u1)
    dpre = out0.at[pl.ds(0, rows_dev)]

    def u_buf(i):
        return out0.at[pl.ds(rows_dev, rows_dev), rows((i % 2) * wide, wide)]

    place = Place()
    core, other_core = place.core, place.other_core
    mine = rows(core * rows_dev, rows_dev)
    place.arrive()
    small = small_sum(place, small_refs)
    payload, sums = small.payload, small.total

    def load_x(w):
        return pltpu.make_async_copy(mats_in[w], xs.at[w % 2], in_sem.at[w])

    def peer_dy(w):
        block = dy.at[w % 2, mine]
        return remote_copy(block, block, peer_send.at[w], peer_recv.at[w], other_core)

    def w_tile(ref, i):
        return pltpu.make_async_copy(ref.at[rows(i * wide, wide)], w_buf, tile_sem.at[0, 0])

    def u_tile(ref, i):
        return pltpu.make_async_copy(ref.at[:, rows(i * wide, wide)], u_buf(i), tile_sem.at[1, i % 2])

    def start_w(layer, i):
        pick(layer, weights, lambda ref: w_tile(ref, i).start())

    def start_u(layer, i):
        pick(layer, pres, lambda ref: u_tile(ref, i).start())

    size = min(1024, width)

    def load_dz(c):
        return pltpu.make_async_copy(dz_hbm.at[:, rows(c * size, size)], dy.at[0, :, rows(c * size, size)], in_sem.at[MATS + c])

    ahead = GROUP // 2 * part_rows

    def load_first(lo, n, sem):
        return pltpu.make_async_copy(mats_in[0].at[:, pl.ds(lo, n)], xs.at[0, :, pl.ds(lo, n)], sem)

    first_x = load_first(0, ahead, row_sem.at[2])
    rest_x = load_first(ahead, half - ahead, in_sem.at[0])
    first_x.start()
    for c in range(width // size):
        load_dz(c).start()
    rest_x.start()
    w_tile(weights[0], 0).start()
    u_tile(pres[0], 0).start()
    vec_load = pltpu.make_async_copy(vec_hbm, vec, row_sem.at[0])
    vec_load.start()
    load_x(1).start()
    sums_store = pltpu.make_async_copy(sums_out, sums_hbm, row_sem.at[1])
    payload[...] = jnp.zeros_like(payload)

    def row_loop(body, carry):
        return lax.fori_loop(0, rows_dev // BACK_BLOCK, body, carry)

    def chain_tile(layer, i):
        w_tile(w_out, i).wait()
        u_tile(u2, i).wait()

        pl.when(i + 1 < tiles)(lambda: start_u(layer, i + 1))
        at_cols = rows(i * wide, wide)
        dpre[:, at_cols] = contract_cols(dy[layer, mine], w_buf[...])
        pl.when(i + 1 < tiles)(lambda: start_w(layer, i + 1))
        gain, bias, mean, inv = (vec[layer * 4 + j, :, at_cols] for j in range(4))

        def block(r, carry):
            at = rows(r * BACK_BLOCK, BACK_BLOCK)
            n = (out0[rows(rows_dev + r * BACK_BLOCK, BACK_BLOCK), rows((i % 2) * wide, wide)] - mean) * inv
            g = jnp.where(n * gain + bias > 0.0, dpre[at, at_cols], 0.0)
            dpre[at, at_cols] = g
            return carry[0] + fold(g * n), carry[1] + fold(g)

        zero = jnp.zeros((8, wide), jnp.float32)
        for row, value in enumerate(row_loop(block, (zero, zero))):
            value = jnp.sum(value, axis=0, keepdims=True)
            for c in range(wide // TILE):
                payload[layer, i * (wide // TILE) + c, row : row + 1] = value[:, c * TILE : (c + 1) * TILE]

    def du_tile(layer, i):
        u_tile(u2, i).wait()
        pl.when(i + 1 < tiles)(lambda: start_u(layer, i + 1))
        at_cols = rows(i * wide, wide)
        gain, mean, inv = (vec[layer * 4 + j, :, at_cols] for j in (0, 2, 3))
        means = jnp.concatenate([sums[layer, i * (wide // TILE) + c] for c in range(wide // TILE)], axis=1) / row_count
        mean_gn, mean_g = means[0:1], means[1:2]
        scale = gain * inv

        def block(r, c):
            at = rows(r * BACK_BLOCK, BACK_BLOCK)
            n = (out0[rows(rows_dev + r * BACK_BLOCK, BACK_BLOCK), rows((i % 2) * wide, wide)] - mean) * inv
            value = (dpre[at, at_cols] - mean_g - n * mean_gn) * scale
            dy[1 - layer, rows(core * rows_dev + r * BACK_BLOCK, BACK_BLOCK), at_cols] = value.astype(jnp.bfloat16)
            return c

        row_loop(block, 0)

    in_last = (MATS - 1) * PARTS
    quarter = part_rows // 4

    def home_row(k):
        return core * half + (k % PARTS) * part_rows

    def homes(k):
        return [
            (k < in_last, lambda off, size: gathered.at[k % GATHER_SLOTS, pl.ds(pl.multiple_of(off, quarter), size)]),
            (k >= in_last, lambda off, size: out0.at[pl.ds(pl.multiple_of(home_row(k) + off, quarter), size)]),
        ]

    def finish(k, off, size, buf):
        j = k % ACC_SLOTS
        value = acc[j, rows(off, size)] + buf[j]

        @pl.when(k < in_last)
        def _():
            gathered[k % GATHER_SLOTS, rows(off, size)] = value

        @pl.when(k >= in_last)
        def _():
            out0[rows(home_row(k) + off, size)] = value

    chunks = ChunkSum(place, "xl", back_kind, acc, homes, landing, send, recv, finish)

    def form(k, group):
        w, j = k // PARTS, k % ACC_SLOTS

        if isinstance(k, int):
            (rest_x if k else first_x).wait()
        else:

            @pl.when(k % PARTS == 0)
            def _():
                pltpu.make_async_copy(xs.at[w % 2], xs.at[w % 2], in_sem.at[w]).wait()
                peer_dy(w).wait_recv()

        at = rows((k % PARTS) * part_rows, group * part_rows)

        def col(c):
            pl.when(k == 0)(lambda: load_dz(c).wait())
            cs = rows(c * size, size)
            acc[pl.ds(j, group), :, cs] = contract_rows(xs[w % 2, :, at], dy[w % 2, :, cs]).reshape(group, part_rows, size)

        loop(0, width // size, col)

    def out_rows(k, side):
        return pl.ds(pl.multiple_of(side * half + (k % PARTS) * part_rows, part_rows), part_rows)

    def last_copy(out, k, side):
        return chunks.copy(gathered.at[k % GATHER_SLOTS], out.at[out_rows(k, side)], 7, k, other_core)

    def store_copy(out, k):
        return pltpu.make_async_copy(gathered.at[k % GATHER_SLOTS], out.at[out_rows(k, core)], store_sem.at[k])

    def stage(i, k):
        if i == 0:
            form_next(k, form)
            return
        chunks.stage(i, k)
        own_rows = out0.at[pl.ds(pl.multiple_of(home_row(k), part_rows), part_rows)]
        in_place = chunks.copy(own_rows, own_rows, 7, k, other_core)
        last = k // PARTS == MATS - 1

        def emit(out):
            last_copy(out, k, core).start()
            store_copy(out, k).start()

        def emit_any():
            pick(k // PARTS, outs, emit)
            pl.when(last)(lambda: in_place.start())

        if i == 8:
            pl.when(back_kind("x", k))(emit_any)
        if i == 9:
            pl.when(back_kind("l", k))(emit_any)
        if i == 10:

            def close(out):
                last_copy(out, k, 1 - core).wait_recv()
                store_copy(out, k).wait()
                last_copy(out, k, core).wait_send()

            pick(k // PARTS, outs, close)

            @pl.when(last)
            def _():
                in_place.wait_recv()
                in_place.wait_send()

    def layer_work(t):
        layer = t // LAYER_SLOTS
        at = t - LAYER_SLOTS * layer
        first_du = 2 * tiles + 3
        pl.when((at < 2 * tiles) & (at % 2 == 1))(lambda: chain_tile(layer, at // 2))
        @pl.when(at == 2 * tiles)
        def _():
            for part in range(len(SUM_PARTS)):
                small.begin(layer, part)

        @pl.when(at == 2 * tiles + 1)
        def _():
            for part in range(len(SUM_PARTS)):
                small.middle(layer, part)


        pl.when(at == 2 * tiles + 2)(lambda: start_u(layer, 0))

        pl.when(at == first_du)(lambda: small.end(layer))
        pl.when(at >= first_du)(lambda: du_tile(layer, at - first_du))

        @pl.when(at == LAYER_SLOTS - 1)
        def _():
            peer_dy(layer + 1).start()

            @pl.when(layer == 0)
            def _():
                w_tile(weights[1], 0).start()
                u_tile(pres[1], 0).start()

            @pl.when(layer == 1)
            def _():
                load_x(2).start()
                for c in range(PLANE):
                    for row in range(4):
                        sums_out[row : row + 1, c * TILE : (c + 1) * TILE] = sums[row // 2, c, row % 2 : row % 2 + 1]
                sums_out[4:5] = jnp.full((1, width), jnp.sum(vec[8]))
                sums_store.start()


    form(0, GROUP // 2)
    place.all_here()
    vec_load.wait()
    run_slots(BACK_PLAN, count, stage, lambda t: pl.when(t < 2 * LAYER_SLOTS)(lambda: layer_work(t)))
    for w in (1, 2):
        peer_dy(w).wait_send()
    sums_store.wait()


def backward(grad_z, x2, x1, x0, w_out, w_mid, u2, u1, vec):
    rows_dev, width = u2.shape
    part_rows = width // 2 // PARTS
    count = MATS * PARTS
    any_spec = pl.BlockSpec(memory_space=pl.ANY)
    vmem_spec = pl.BlockSpec(memory_space=pltpu.VMEM)
    mat = jax.ShapeDtypeStruct((width, width), jnp.float32)
    dma = pltpu.SemaphoreType.DMA
    return pl.pallas_call(
        back_kernel,
        name="backward",
        out_shape=[mat, mat, pltpu.VMEM((width, width), jnp.float32), jax.ShapeDtypeStruct((5, width), jnp.float32)],
        in_specs=[any_spec] * 9,
        out_specs=[any_spec] * 2 + [vmem_spec, any_spec],
        scratch_shapes=[
            pltpu.VMEM((2, 2 * rows_dev, width), jnp.bfloat16),
            pltpu.VMEM((2, 2 * rows_dev, width // 2), jnp.bfloat16),
            pltpu.VMEM((WIDE, width), jnp.bfloat16),
            pltpu.VMEM((9, 1, width), jnp.float32),
            pltpu.VMEM((5, width), jnp.float32),
            dma((MATS + 2,)),
            dma((2, 2)),
            dma((3,)),
            dma((MATS,)),
            dma((MATS,)),
            dma((count,)),
        ]
        + small_scratch(2)
        + chunk_scratch(ACC_SLOTS, GATHER_SLOTS, part_rows, width, count, jnp.float32),
        compiler_params=pltpu.CompilerParams(collective_id=1, has_side_effects=True, vmem_limit_bytes=BACK_VMEM),
    )(grad_z, x2, x1, x0, w_out, w_mid, u2, u1, vec)


def copy_kernel(*refs):
    pairs = (len(refs) - 6 - 6) // 2
    ins, small, outs, small_outs = refs[:pairs], refs[pairs], refs[pairs + 1 : 2 * pairs + 1], refs[2 * pairs + 1 : -6]
    buf, small_buf, in_sem, out_sem, small_sem, near_sem = refs[-6:]
    blocks = [(i, r) for i in range(pairs - 1) for r in range(0, ins[i].shape[0], COPY_ROWS)]
    near = pltpu.make_async_copy(ins[-1], outs[-1], near_sem.at[0])

    def read(b):
        i, r = blocks[b]
        return pltpu.make_async_copy(ins[i].at[pl.ds(r, COPY_ROWS)], buf.at[b % COPY_BUFS], in_sem.at[b % COPY_BUFS])

    def write(b):
        i, r = blocks[b]
        return pltpu.make_async_copy(buf.at[b % COPY_BUFS], outs[i].at[pl.ds(r, COPY_ROWS)], out_sem.at[b % COPY_BUFS])

    for b in range(len(blocks)):
        read(b).start()
    small_read = pltpu.make_async_copy(small, small_buf, small_sem.at[4])
    small_read.start()

    def small_write(row):
        return pltpu.make_async_copy(small_buf.at[pl.ds(row, 1)], small_outs[row], small_sem.at[row])

    for b in range(len(blocks)):
        read(b).wait()
    near.start()
    for b in range(len(blocks)):
        write(b).start()
    small_read.wait()
    small_outs[4][...] = small_buf[4:5, :1]
    for row in range(4):
        small_write(row).start()
    for row in range(4):
        small_write(row).wait()
    near.wait()
    for b in range(len(blocks)):
        write(b).wait()


def copy_out(arrays, small):
    any_spec = pl.BlockSpec(memory_space=pl.ANY)
    vmem_spec = pl.BlockSpec(memory_space=pltpu.VMEM)
    dma = pltpu.SemaphoreType.DMA
    width = small.shape[1]
    row = jax.ShapeDtypeStruct((1, width), jnp.float32)
    return pl.pallas_call(
        copy_kernel,
        name="copy_out",
        out_shape=[jax.ShapeDtypeStruct(a.shape, a.dtype) for a in arrays] + [row] * 4 + [jax.ShapeDtypeStruct((1, 1), jnp.float32)],
        in_specs=[any_spec] * (len(arrays) - 1) + [vmem_spec, any_spec],
        out_specs=[any_spec] * (len(arrays) + 4) + [vmem_spec],
        scratch_shapes=[
            pltpu.VMEM((COPY_BUFS, COPY_ROWS, width), jnp.float32),
            pltpu.VMEM(small.shape, jnp.float32),
            dma((COPY_BUFS,)),
            dma((COPY_BUFS,)),
            dma((5,)),
            dma((1,)),
        ],
        compiler_params=pltpu.CompilerParams(vmem_limit_bytes=COPY_VMEM),
    )(*arrays[:-1], pltpu.with_memory_space_constraint(arrays[-1], pltpu.VMEM), small)


def solution(mesh):
    row_part = P(DATA_AXIS, None)
    replicated = P()

    def local_step(feat_a, feat_b, w_in, w_mid, w_out, t_in, t_mid, t_out, gain_1, bias_1, gain_2, bias_2, off_weight):
        affine = [v.reshape(1, -1) for v in (gain_1, bias_1, gain_2, bias_2)]
        pre_1, pre_2, xs_2, xs_1, xs_0, grad_z, grad_emb, vec = front(
            feat_a, feat_b, (w_in, t_in, w_mid, t_mid, w_out, t_out), affine, off_weight.reshape(1)
        )
        grad_w_out, grad_w_mid, grad_w_in, sums = backward(grad_z, xs_2, xs_1, xs_0, w_out, w_mid, pre_2, pre_1, vec)
        (grad_emb, grad_w_out, grad_w_mid, grad_w_in, gain_2, bias_2, gain_1, bias_1, loss) = copy_out((grad_emb, grad_w_out, grad_w_mid, grad_w_in), sums)
        gain_1, bias_1, gain_2, bias_2 = (v.reshape(-1) for v in (gain_1, bias_1, gain_2, bias_2))
        return (loss.reshape(()), grad_emb, grad_w_in, grad_w_mid, grad_w_out, gain_1, bias_1, gain_2, bias_2)

    return jax.shard_map(local_step, mesh=mesh, in_specs=(row_part, row_part) + (replicated,) * 11, out_specs=(replicated, row_part) + (replicated,) * 7, check_vma=False)
```
